32 devices in a mesh: wide: 8 (over y, x, core), narrow: 4 (over z).
Axes of the slice: x: 2, y: 2, z: 4, core: 2. Of those that a mesh axis runs over, the one named last changes fastest.
Arguments:
- layer_input: bfloat16 [4, 2048, 2048], P(None, 'wide'), may hold values from -6 to 6
- grad_out: bfloat16 [4, 2048, 2048], P(None, 'wide'), may hold values from -6 to 6
- lengths: int32 [4, 8], replicated, may hold values from 1 to 1024, 2048 in all within a row
- w_query: bfloat16 [2048, 2048], P('wide', 'narrow'), may hold values from -0.125 to 0.125
- w_key: bfloat16 [2048, 1024], P('wide', 'narrow'), may hold values from -0.125 to 0.125
- w_value: bfloat16 [2048, 1024], P('wide', 'narrow'), may hold values from -0.125 to 0.125
- w_out: bfloat16 [2048, 2048], P('narrow', 'wide'), may hold values from -0.75 to 0.75
- w_gate: bfloat16 [2048, 6144], P('wide', 'narrow'), may hold values from -0.125 to 0.125
- w_up: bfloat16 [2048, 6144], P('wide', 'narrow'), may hold values from -0.125 to 0.125
- w_down: bfloat16 [6144, 2048], P('narrow', 'wide'), may hold values from -0.078125 to 0.078125
- gain_attn: float32 [2048], replicated, may hold values from 0.25 to 1.75
- gain_ffn: float32 [2048], replicated, may hold values from 0.25 to 1.75
- gain_query: float32 [128], replicated, may hold values from 0.25 to 1.75
- gain_key: float32 [128], replicated, may hold values from 0.25 to 1.75
Outputs:
- output: bfloat16 [4, 2048, 2048], P(None, 'wide')
- grad_input: float32 [4, 2048, 2048], P(None, 'wide')
- grad_wquery: float32 [2048, 2048], P('wide', 'narrow')
- grad_wkey: float32 [2048, 1024], P('wide', 'narrow')
- grad_wvalue: float32 [2048, 1024], P('wide', 'narrow')
- grad_wout: float32 [2048, 2048], P('narrow', 'wide')
- grad_wgate: float32 [2048, 6144], P('wide', 'narrow')
- grad_wup: float32 [2048, 6144], P('wide', 'narrow')
- grad_wdown: float32 [6144, 2048], P('narrow', 'wide')
- grad_gattn: float32 [2048], replicated
- grad_gffn: float32 [2048], replicated
- grad_gquery: float32 [128], replicated
- grad_gkey: float32 [128], replicated
The draws below stay inside these ranges and needn't reach their ends.
Inputs may be any that keep to these rules, and one draw needn't show every extreme that they name: `lengths`: each row cuts the 2048 tokens of its micro-batch into 8 consecutive pieces in order; pieces 0 to 6 are documents and the last piece is padding. A row's pieces sum to 2048, and its largest piece is exactly 1024.
All inputs are finite; a program needn't handle non-finite values.
Results may differ from the reference program's by a relative error of at most 0.022.
Values may be sent and summed in bfloat16 or wider, within the bound.
A program may use at most 256 MiB of HBM per device.

```python
import math
import jax
import jax.numpy as jnp
import numpy as np
from jax import lax

D = 2048
NH = 16
KV = 8
HD = 128
FF = 6144
MICRO = 4
NDOC = 8
LEN = 2048
MOST = 1024


def block_levels(rng, dims, split, low, largest):
    def one(dim, blocks):
        draws = jax.random.uniform(jax.random.fold_in(jax.random.fold_in(rng, 6), dim), (blocks,), jnp.float32, low / len(split), largest / len(split))
        return jnp.repeat(jnp.exp(draws), dims[dim] // blocks).reshape((-1,) + (1,) * (len(dims) - dim - 1))

    level = one(*split[0])
    for cut in split[1:]:
        level = level * one(*cut)
    return level


def profile(number_of, total, reach, skew):
    portions = [(1 << 20) // math.isqrt(grade ** skew) + 1 for grade in range(2, number_of + 1)]
    spare, counts = total - reach - (number_of - 1), [1] * (number_of - 1)
    while spare > 0:
        free = [i for i in range(number_of - 1) if counts[i] < reach]
        whole, remaining = sum([portions[i] for i in free]), spare
        for i in free:
            extra = min(reach - counts[i], max(1, remaining * portions[i] // whole), spare)
            counts[i] = counts[i] + extra
            spare = spare - extra
    return np.array([reach] + counts)


def uneven_parts(rng, number_of, total, limit, slope):
    if number_of == 2:
        one = jax.random.randint(rng, (), max(1, total - limit), min(limit, total - 1) + 1)
        return jnp.stack([one, total - one])
    tallies = jnp.asarray(profile(number_of, total, limit, slope), jnp.int32)
    couples = (number_of - 1) // 2
    donor, sink = tallies[1:1 + 2 * couples:2], tallies[2:2 + 2 * couples:2]
    room = jnp.minimum(donor - 1, limit - sink)
    moved = jax.random.randint(jax.random.fold_in(rng, 1), (couples,), 0, 1 << 20) % (room + 1)
    tallies = tallies.at[1:1 + 2 * couples:2].set(donor - moved).at[2:2 + 2 * couples:2].set(sink + moved)
    return tallies[jax.random.permutation(jax.random.fold_in(rng, 2), number_of)]


def noise(own_key, extent, spread, bound, cuts=(), held_as=jnp.bfloat16):
    level = block_levels(own_key, extent, cuts, -0.22, 0.18) if cuts else 1.0
    array = jax.random.normal(own_key, extent, jnp.float32) * spread * level
    return jnp.minimum(jnp.maximum(array, -bound), bound).astype(held_as)


def setup_inputs(seed: int = 0) -> dict:
    streams_of = jax.random.split(jax.random.key(seed), 15)
    return {
        "layer_input": noise(streams_of[0], (MICRO, LEN, D), 1.0, 6.0, ((1, 8),)),
        "grad_out": noise(streams_of[1], (MICRO, LEN, D), 1.0, 6.0, ((1, 8),)),
        "lengths": jax.vmap(lambda own: uneven_parts(own, NDOC, LEN, MOST, 2))(jax.random.split(streams_of[2], MICRO)).reshape((MICRO, NDOC)).astype(jnp.int32),
        "w_query": noise(streams_of[3], (D, NH * HD), D ** -0.5, 0.125, ((0, 8), (1, 4))),
        "w_key": noise(streams_of[4], (D, KV * HD), D ** -0.5, 0.125, ((0, 8), (1, 4))),
        "w_value": noise(streams_of[5], (D, KV * HD), D ** -0.5, 0.125, ((0, 8), (1, 4))),
        "w_out": noise(streams_of[6], (NH * HD, D), (NH * HD // 32) ** -0.5, 0.75, ((0, 4), (1, 8))),
        "w_gate": noise(streams_of[7], (D, FF), D ** -0.5, 0.125, ((0, 8), (1, 4))),
        "w_up": noise(streams_of[8], (D, FF), D ** -0.5, 0.125, ((0, 8), (1, 4))),
        "w_down": noise(streams_of[9], (FF, D), FF ** -0.5, 0.078125, ((0, 4), (1, 8))),
        "gain_attn": jnp.clip(1.0 + 0.15 * jax.random.normal(streams_of[10], (D,), jnp.float32), 0.25, 1.75),
        "gain_ffn": jnp.clip(1.0 + 0.15 * jax.random.normal(streams_of[11], (D,), jnp.float32), 0.25, 1.75),
        "gain_query": jnp.clip(1.0 + 0.15 * jax.random.normal(streams_of[12], (HD,), jnp.float32), 0.25, 1.75),
        "gain_key": jnp.clip(1.0 + 0.15 * jax.random.normal(streams_of[13], (HD,), jnp.float32), 0.25, 1.75),
    }


@jax.custom_vjp
def low(v):
    return lax.optimization_barrier(v.astype(jnp.bfloat16)).astype(jnp.float32)

@jax.custom_vjp
def low_back(v):
    return v

def low_keep(v):
    return (low(v), None)

def low_pass(kept, grad):
    return (grad,)

def back_keep(v):
    return (v, None)

def back_low(kept, grad):
    return (low(grad),)
low.defvjp(low_keep, low_pass)
low_back.defvjp(back_keep, back_low)
EPSILON = 1e-06
THETA = 1000000.0
HIGHEST = lax.Precision.HIGHEST

def rms_norm(values, gain):
    return values * lax.rsqrt(lax.optimization_barrier(jnp.mean(values * values, axis=-1, keepdims=True)) + EPSILON) * gain

def rotate(values, cosine, sine):
    midway = values.shape[-1] // 2
    turned = jnp.concatenate([-values[..., midway:], values[..., :midway]], axis=-1)
    return values * cosine + turned * sine

def layout(lengths_row, total):
    finish = jnp.cumsum(lengths_row).astype(jnp.int32)
    starts = (finish - lengths_row).astype(jnp.int32)
    places = jnp.arange(total, dtype=jnp.int32)
    segment = lax.optimization_barrier(jnp.sum((places[:, None] >= finish[None, :]).astype(jnp.int32), axis=1)).astype(jnp.int32)
    member = segment[:, None] == jnp.arange(finish.shape[0], dtype=jnp.int32)[None, :]
    opening = lax.optimization_barrier(jnp.sum(jnp.where(member, starts[None, :], 0), axis=1)).astype(jnp.int32)
    return (segment, (places - opening).astype(jnp.int32))

def angles(place):
    frequency = jnp.exp(-math.log(THETA) * jnp.arange(0, HD, 2).astype(jnp.float32) / HD)
    turning = place.astype(jnp.float32)[:, None] * frequency[None, :]
    turning = jnp.concatenate([turning, turning], axis=-1)
    return (jnp.cos(turning), jnp.sin(turning))

def allowed(query_seg, query_idx, key_seg, key_idx):
    same_doc = query_seg[:, None] == key_seg[None, :]
    causal = key_idx[None, :] <= query_idx[:, None]
    usable = (key_seg[None, :] != NDOC - 1) | (key_idx[None, :] == query_idx[:, None])
    return same_doc & causal & usable

def forward_one(row_input, params, segment, place):
    w_query, w_key, w_value, w_out, w_gate, w_up, w_down, gain_attn, gain_ffn, gain_query, gain_key = params
    total = row_input.shape[0]
    factor = 1.0 / math.sqrt(HD)
    cosine, sine = angles(place)
    hidden_one = low(rms_norm(row_input, gain_attn))
    queries = low_back(jnp.dot(hidden_one, w_query, precision=HIGHEST)).reshape(total, NH, HD)
    keys = low_back(jnp.dot(hidden_one, w_key, precision=HIGHEST)).reshape(total, KV, HD)
    values = low(low_back(jnp.dot(hidden_one, w_value, precision=HIGHEST))).reshape(total, KV, HD)
    query_rot = low(rotate(rms_norm(queries, gain_query), cosine[:, None, :], sine[:, None, :]))
    key_rot = low(rotate(rms_norm(keys, gain_key), cosine[:, None, :], sine[:, None, :]))
    key_rep = jnp.repeat(key_rot, NH // KV, axis=1)
    value_rep = jnp.repeat(values, NH // KV, axis=1)
    block_rows = min(512, total)
    block_count = total // block_rows
    positions = jnp.arange(total, dtype=jnp.int32)

    def attend(pieces):
        query_block, query_seg, query_idx = pieces
        scores = low_back(jnp.einsum('qhd,khd->hqk', query_block, key_rep, precision=HIGHEST) * factor)
        scores = jnp.where(allowed(query_seg, query_idx, segment, positions)[None], scores, -1e+30)
        shifted = scores - lax.optimization_barrier(jnp.max(scores, axis=-1, keepdims=True))
        exponent = jnp.exp(shifted)
        probs = low(exponent / lax.optimization_barrier(jnp.sum(exponent, axis=-1, keepdims=True)))
        return jnp.einsum('hqk,khd->qhd', probs, value_rep, precision=HIGHEST)
    mixed = lax.map(jax.checkpoint(attend), (query_rot.reshape(block_count, block_rows, NH, HD), segment.reshape(block_count, block_rows), positions.reshape(block_count, block_rows)))
    attn_low = low(low_back(mixed.reshape(total, NH * HD)))
    branch = low_back(jnp.dot(attn_low, w_out, precision=HIGHEST))
    middle = row_input + branch
    hidden_two = low(rms_norm(middle, gain_ffn))
    gate = low_back(jnp.dot(hidden_two, w_gate, precision=HIGHEST))
    up_proj = low_back(jnp.dot(hidden_two, w_up, precision=HIGHEST))
    active = low(jax.nn.silu(gate) * up_proj)
    return middle + low_back(jnp.dot(active, w_down, precision=HIGHEST))

def reference(layer_input, grad_out, lengths, w_query, w_key, w_value, w_out, w_gate, w_up, w_down, gain_attn, gain_ffn, gain_query, gain_key):
    params = (w_query.astype(jnp.float32), w_key.astype(jnp.float32), w_value.astype(jnp.float32), w_out.astype(jnp.float32), w_gate.astype(jnp.float32), w_up.astype(jnp.float32), w_down.astype(jnp.float32), gain_attn.astype(jnp.float32), gain_ffn.astype(jnp.float32), gain_query.astype(jnp.float32), gain_key.astype(jnp.float32))
    total = layer_input.shape[1]

    def one_step(carry, inputs):
        row_input, grad_row, lengths_row = inputs
        segment, place = layout(lengths_row, total)

        def forward(rows, *weights):
            return forward_one(rows, weights, segment, place)
        result, pull = jax.vjp(forward, row_input.astype(jnp.float32), *params)
        gradients = pull(grad_row.astype(jnp.float32))
        summed = tuple((running + fresh for running, fresh in zip(carry, gradients[1:])))
        return (summed, (result.astype(jnp.bfloat16), gradients[0]))
    starting = tuple((jnp.zeros(param.shape, jnp.float32) for param in params))
    totals, (outputs, grad_inputs) = lax.scan(one_step, starting, (layer_input, grad_out, lengths))
    return (outputs, grad_inputs, totals[0], totals[1], totals[2], totals[3], totals[4], totals[5], totals[6], totals[7], totals[8], totals[9], totals[10])
```

```python
import functools
import math

import jax
import jax.numpy as jnp
from jax import lax
from jax.experimental import pallas as pl
from jax.experimental.pallas import tpu as pltpu
from jax.sharding import PartitionSpec as P

HD = 128
NDOC = 8


EPSILON = 1e-06
THETA = 1000000.0


def rms_norm(values, gain):
    return values * lax.rsqrt(jnp.mean(values * values, axis=-1, keepdims=True) + EPSILON) * gain


def unit_rows(values):
    return values * lax.rsqrt(jnp.mean(values * values, axis=-1, keepdims=True) + EPSILON)


def rotate(values, cosine, sine):
    midway = values.shape[-1] // 2
    turned = jnp.concatenate([-values[..., midway:], values[..., :midway]], axis=-1)
    return values * cosine + turned * sine


def layout(lengths_row, total):
    finish = jnp.cumsum(lengths_row)
    starts = finish - lengths_row
    places = jnp.arange(total, dtype=jnp.int32)
    segment = jnp.sum((places[:, None] >= finish[None, :]).astype(jnp.int32), axis=1)
    member = segment[:, None] == jnp.arange(finish.shape[0], dtype=jnp.int32)[None, :]
    opening = jnp.sum(jnp.where(member, starts[None, :], 0), axis=1)
    return (segment, places - opening)


def angles(place):
    frequency = jnp.exp(-math.log(THETA) * jnp.arange(0, HD, 2).astype(jnp.float32) / HD)
    turning = place.astype(jnp.float32)[:, None] * frequency[None, :]
    turning = jnp.concatenate([turning, turning], axis=-1)
    return (jnp.cos(turning), jnp.sin(turning))


def allowed(query_seg, query_idx, key_seg, key_idx):
    same_doc = query_seg[:, None] == key_seg[None, :]
    causal = key_idx[None, :] <= query_idx[:, None]
    usable = (key_seg[None, :] != NDOC - 1) | (key_idx[None, :] == query_idx[:, None])
    return same_doc & causal & usable


def attention_scores(query_low, key_all, mask_local, factor):
    scores = (
        jnp.einsum("tgrd,kgd->grtk", query_low, key_all, preferred_element_type=jnp.float32)
        * factor
    )
    return jnp.where(mask_local[None, None], scores, -1e30)


def one_batch(row_input, grad_row, lengths_row, gathered, gains):
    w_query, w_key, w_value, w_out, w_gate, w_up, w_down = gathered
    gain_attn, gain_ffn, gain_query, gain_key = gains
    tok_rows = row_input.shape[0]
    total = tok_rows * lax.axis_size("wide")
    groups = w_key.shape[1] // HD
    repeat = w_query.shape[1] // w_key.shape[1]
    factor = 1.0 / math.sqrt(HD)
    first_row = lax.axis_index("wide") * tok_rows
    segment, place = layout(lengths_row, total)
    positions = jnp.arange(total, dtype=jnp.int32)
    query_seg = lax.dynamic_slice_in_dim(segment, first_row, tok_rows)
    query_idx = lax.dynamic_slice_in_dim(positions, first_row, tok_rows)
    mask_local = allowed(query_seg, query_idx, segment, positions)
    cosine, sine = angles(lax.dynamic_slice_in_dim(place, first_row, tok_rows))

    def head_norm(rows, gain):
        return rotate(rms_norm(rows, gain), cosine[:, None, :], sine[:, None, :])

    input_float = row_input.astype(jnp.float32)
    grad_float = grad_row.astype(jnp.float32)
    normed_one, pull_one = jax.vjp(lambda rows: rms_norm(rows, gain_attn), input_float)
    hidden_one = normed_one.astype(jnp.bfloat16)
    query_raw = jnp.dot(hidden_one, w_query, preferred_element_type=jnp.float32).reshape(
        tok_rows, groups * repeat, HD
    )
    key_raw = jnp.dot(hidden_one, w_key, preferred_element_type=jnp.float32).reshape(
        tok_rows, groups, HD
    )
    value_low = jnp.dot(hidden_one, w_value, preferred_element_type=jnp.float32).astype(
        jnp.bfloat16
    )
    query_turned, pull_query = jax.vjp(head_norm, query_raw, gain_query)
    key_turned, pull_key = jax.vjp(head_norm, key_raw, gain_key)
    query_low = query_turned.astype(jnp.bfloat16).reshape(tok_rows, groups, repeat, HD)
    key_low = key_turned.astype(jnp.bfloat16).reshape(tok_rows, groups * HD)
    key_all, value_all = (
        lax.all_gather(key_low, "wide", axis=0, tiled=True),
        lax.all_gather(value_low, "wide", axis=0, tiled=True),
    )
    key_all = key_all.reshape(total, groups, HD)
    value_all = value_all.reshape(total, groups, HD)
    scores = attention_scores(query_low, key_all, mask_local, factor)
    highest = jnp.max(scores, axis=-1, keepdims=True)
    exponent = jnp.exp(scores - highest)
    denominator = jnp.sum(exponent, axis=-1, keepdims=True)
    log_total = highest + jnp.log(denominator)
    probs_low = (exponent / denominator).astype(jnp.bfloat16)
    mixed = jnp.einsum("grtk,kgd->tgrd", probs_low, value_all, preferred_element_type=jnp.float32)
    mixed_low = mixed.reshape(tok_rows, groups * repeat * HD).astype(jnp.bfloat16)
    attn_part = jnp.dot(mixed_low, w_out, preferred_element_type=jnp.float32)
    middle = input_float + lax.psum(attn_part.astype(jnp.bfloat16), "narrow").astype(jnp.float32)
    normed_two, pull_two = jax.vjp(lambda rows: rms_norm(rows, gain_ffn), middle)
    hidden_two = normed_two.astype(jnp.bfloat16)
    unit_two = unit_rows(middle)
    gate = jnp.dot(hidden_two, w_gate, preferred_element_type=jnp.float32)
    up_proj = jnp.dot(hidden_two, w_up, preferred_element_type=jnp.float32)
    active, pull_active = jax.vjp(
        lambda gate_in, up_in: jax.nn.silu(gate_in) * up_in, gate, up_proj
    )
    active_low = active.astype(jnp.bfloat16)
    ffn_part = jnp.dot(active_low, w_down, preferred_element_type=jnp.float32)
    output_low = (
        middle + lax.psum(ffn_part.astype(jnp.bfloat16), "narrow").astype(jnp.float32)
    ).astype(jnp.bfloat16)
    grad_wdown = jnp.einsum("tf,td->fd", active_low, grad_row, preferred_element_type=jnp.float32)
    grad_active = jnp.einsum("td,fd->tf", grad_row, w_down, preferred_element_type=jnp.float32)
    grad_gate, grad_upper = pull_active(grad_active)
    gate_back = grad_gate.astype(jnp.bfloat16)
    upper_back = grad_upper.astype(jnp.bfloat16)
    grad_wgate = jnp.einsum("td,tf->df", hidden_two, gate_back, preferred_element_type=jnp.float32)
    grad_wup = jnp.einsum("td,tf->df", hidden_two, upper_back, preferred_element_type=jnp.float32)
    partial_two = jnp.einsum(
        "tf,df->td", gate_back, w_gate, preferred_element_type=jnp.float32
    ) + jnp.einsum("tf,df->td", upper_back, w_up, preferred_element_type=jnp.float32)
    gain_two = jnp.sum(partial_two * unit_two, axis=0)
    grad_middle = (
        grad_float
        + pull_two(lax.psum(partial_two.astype(jnp.bfloat16), "narrow").astype(jnp.float32))[0]
    )
    middle_low = grad_middle.astype(jnp.bfloat16)
    grad_wout = jnp.einsum("th,td->hd", mixed_low, middle_low, preferred_element_type=jnp.float32)
    grad_mixed = jnp.einsum("td,hd->th", middle_low, w_out, preferred_element_type=jnp.float32)
    grad_mixed = grad_mixed.astype(jnp.bfloat16).reshape(tok_rows, groups, repeat, HD)
    scores = attention_scores(query_low, key_all, mask_local, factor)
    probs = jnp.exp(scores - log_total)
    grad_probs = jnp.einsum(
        "tgrd,kgd->grtk", grad_mixed, value_all, preferred_element_type=jnp.float32
    )
    weighted = jnp.sum(probs * grad_probs, axis=-1, keepdims=True)
    grad_scores = (probs * (grad_probs - weighted)).astype(jnp.bfloat16)
    grad_turned = (
        jnp.einsum("grtk,kgd->tgrd", grad_scores, key_all, preferred_element_type=jnp.float32)
        * factor
    )
    grad_keyall = (
        jnp.einsum("grtk,tgrd->kgd", grad_scores, query_low, preferred_element_type=jnp.float32)
        * factor
    )
    grad_valueall = jnp.einsum(
        "grtk,tgrd->kgd", probs.astype(jnp.bfloat16), grad_mixed, preferred_element_type=jnp.float32
    )
    grad_keys, grad_values = (
        lax.psum_scatter(
            grad_keyall.reshape(total, groups * HD).astype(jnp.bfloat16),
            "wide",
            scatter_dimension=0,
            tiled=True,
        ).astype(jnp.float32),
        lax.psum_scatter(
            grad_valueall.reshape(total, groups * HD).astype(jnp.bfloat16),
            "wide",
            scatter_dimension=0,
            tiled=True,
        ).astype(jnp.float32),
    )
    grad_qraw, gain_q = pull_query(grad_turned.reshape(tok_rows, groups * repeat, HD))
    grad_kraw, gain_k = pull_key(grad_keys.reshape(tok_rows, groups, HD))
    query_back = grad_qraw.reshape(tok_rows, groups * repeat * HD).astype(jnp.bfloat16)
    key_back = grad_kraw.reshape(tok_rows, groups * HD).astype(jnp.bfloat16)
    value_back = grad_values.astype(jnp.bfloat16)
    grad_wquery = jnp.einsum(
        "td,th->dh", hidden_one, query_back, preferred_element_type=jnp.float32
    )
    grad_wkey = jnp.einsum("td,th->dh", hidden_one, key_back, preferred_element_type=jnp.float32)
    grad_wvalue = jnp.einsum(
        "td,th->dh", hidden_one, value_back, preferred_element_type=jnp.float32
    )
    partial_one = (
        jnp.einsum("th,dh->td", query_back, w_query, preferred_element_type=jnp.float32)
        + jnp.einsum("th,dh->td", key_back, w_key, preferred_element_type=jnp.float32)
        + jnp.einsum("th,dh->td", value_back, w_value, preferred_element_type=jnp.float32)
    )
    gain_one = jnp.sum(partial_one * unit_rows(input_float), axis=0)
    grad_input = (
        grad_middle
        + pull_one(lax.psum(partial_one.astype(jnp.bfloat16), "narrow").astype(jnp.float32))[0]
    )
    weight_grads = (
        grad_wquery,
        grad_wkey,
        grad_wvalue,
        grad_wout,
        grad_wgate,
        grad_wup,
        grad_wdown,
    )
    return (output_low, grad_input, weight_grads, (gain_one, gain_two, gain_q, gain_k))


def local_general(
    layer_input,
    grad_out,
    lengths,
    w_query,
    w_key,
    w_value,
    w_out,
    w_gate,
    w_up,
    w_down,
    gain_attn,
    gain_ffn,
    gain_query,
    gain_key,
):
    width = lax.axis_size("wide")
    shards = (w_query, w_key, w_value, w_out, w_gate, w_up, w_down)
    along_rows = (True, True, True, False, True, True, False)
    gains = (gain_attn, gain_ffn, gain_query, gain_key)
    totals = tuple(
        (
            jnp.zeros(
                (
                    (piece.shape[0] * width, piece.shape[1])
                    if rows_first
                    else (piece.shape[0], piece.shape[1] * width)
                ),
                jnp.float32,
            )
            for piece, rows_first in zip(shards, along_rows)
        )
    )
    gain_terms = tuple((jnp.zeros(gain.shape, jnp.float32) for gain in gains))
    outputs = []
    grad_inputs = []
    for micro in range(layer_input.shape[0]):
        gathered = (
            lax.all_gather(w_query, "wide", axis=0, tiled=True),
            lax.all_gather(w_key, "wide", axis=0, tiled=True),
            lax.all_gather(w_value, "wide", axis=0, tiled=True),
            lax.all_gather(w_out, "wide", axis=1, tiled=True),
            lax.all_gather(w_gate, "wide", axis=0, tiled=True),
            lax.all_gather(w_up, "wide", axis=0, tiled=True),
            lax.all_gather(w_down, "wide", axis=1, tiled=True),
        )
        output, grad_input, weight_grads, gain_grads = one_batch(
            layer_input[micro], grad_out[micro], lengths[micro], gathered, gains
        )
        outputs.append(output)
        grad_inputs.append(grad_input)
        gain_terms = tuple((running + fresh for running, fresh in zip(gain_terms, gain_grads)))
        totals = tuple((running + fresh for running, fresh in zip(totals, weight_grads)))
    results = (
        lax.psum_scatter(
            totals[0].astype(jnp.bfloat16), "wide", scatter_dimension=0, tiled=True
        ).astype(jnp.float32),
        lax.psum_scatter(
            totals[1].astype(jnp.bfloat16), "wide", scatter_dimension=0, tiled=True
        ).astype(jnp.float32),
        lax.psum_scatter(
            totals[2].astype(jnp.bfloat16), "wide", scatter_dimension=0, tiled=True
        ).astype(jnp.float32),
        lax.psum_scatter(
            totals[3].astype(jnp.bfloat16), "wide", scatter_dimension=1, tiled=True
        ).astype(jnp.float32),
        lax.psum_scatter(
            totals[4].astype(jnp.bfloat16), "wide", scatter_dimension=0, tiled=True
        ).astype(jnp.float32),
        lax.psum_scatter(
            totals[5].astype(jnp.bfloat16), "wide", scatter_dimension=0, tiled=True
        ).astype(jnp.float32),
        lax.psum_scatter(
            totals[6].astype(jnp.bfloat16), "wide", scatter_dimension=1, tiled=True
        ).astype(jnp.float32),
    )
    gain_total = lax.psum(gain_terms, ("wide", "narrow"))
    return (
        jnp.stack(outputs),
        jnp.stack(grad_inputs),
        results[0],
        results[1],
        results[2],
        results[3],
        results[4],
        results[5],
        results[6],
        gain_total[0],
        gain_total[1],
        gain_total[2],
        gain_total[3],
    )


BLOCK = 256
NT = (((1,), (1,)), ((), ()))
TN = (((0,), (0,)), ((), ()))


def attend_forward(first_ref, qkv_ref, start_ref, mixed_ref, kept_ref, log_ref):
    step_q = pl.program_id(0)
    rows = pl.ds(step_q * BLOCK, BLOCK)
    factor = 1.0 / math.sqrt(HD)
    query = jnp.concatenate([qkv_ref[rows, 0:HD], qkv_ref[rows, HD : 2 * HD]], axis=0)
    start = start_ref[rows, :]
    start = jnp.concatenate([start, start], axis=0)
    spot = lax.broadcasted_iota(jnp.int32, (BLOCK, 1), 0) + step_q * BLOCK
    spot = jnp.concatenate([spot, spot], axis=0)

    def one(step_k, carry):
        highest, total, mixed = carry
        cols = pl.ds(step_k * BLOCK, BLOCK)
        scores = lax.dot_general(
            query, qkv_ref[cols, 2 * HD : 3 * HD], NT, preferred_element_type=jnp.float32
        )
        key_spot = lax.broadcasted_iota(jnp.int32, (1, BLOCK), 1) + step_k * BLOCK
        fits = (key_spot >= start) & (key_spot <= spot)
        scores = jnp.where(fits, scores * factor, -1e30)
        fresh = jnp.maximum(highest, jnp.max(scores, axis=-1, keepdims=True))
        shrink = jnp.exp(highest - fresh)
        exponent = jnp.exp(scores - fresh)
        total = total * shrink + jnp.sum(exponent, axis=-1, keepdims=True)
        mixed = mixed * shrink + jnp.dot(
            exponent.astype(jnp.bfloat16),
            qkv_ref[cols, 3 * HD : 4 * HD],
            preferred_element_type=jnp.float32,
        )
        return (fresh, total, mixed)

    highest, total, mixed = lax.fori_loop(
        first_ref[step_q],
        step_q + 1,
        one,
        (
            jnp.full((2 * BLOCK, 1), -1e30, jnp.float32),
            jnp.zeros((2 * BLOCK, 1), jnp.float32),
            jnp.zeros((2 * BLOCK, HD), jnp.float32),
        ),
    )
    mixed = mixed / total
    mixed = jnp.concatenate([mixed[:BLOCK], mixed[BLOCK:]], axis=1)
    mixed_ref[...] = mixed.astype(jnp.bfloat16)
    kept_ref[...] = mixed
    log_total = highest + jnp.log(total)
    log_ref[...] = jnp.concatenate([log_total[:BLOCK], log_total[BLOCK:]], axis=1)


def attend_backward(
    first_ref, qkv_ref, start_ref, grad_ref, kept_ref, log_ref, back_ref, key_sum, value_sum
):
    step_q = pl.program_id(0)
    rows = pl.ds(step_q * BLOCK, BLOCK)
    factor = 1.0 / math.sqrt(HD)

    @pl.when(step_q == 0)
    def _():
        key_sum[...] = jnp.zeros_like(key_sum)
        value_sum[...] = jnp.zeros_like(value_sum)

    query = jnp.concatenate([qkv_ref[rows, 0:HD], qkv_ref[rows, HD : 2 * HD]], axis=0)
    grad = jnp.concatenate([grad_ref[:, 0:HD], grad_ref[:, HD : 2 * HD]], axis=0)
    kept = jnp.concatenate([kept_ref[:, 0:HD], kept_ref[:, HD : 2 * HD]], axis=0)
    log_total = jnp.concatenate([log_ref[:, 0:1], log_ref[:, 1:2]], axis=0)
    weighted = jnp.sum(grad.astype(jnp.float32) * kept, axis=-1, keepdims=True)
    start = start_ref[rows, :]
    start = jnp.concatenate([start, start], axis=0)
    spot = lax.broadcasted_iota(jnp.int32, (BLOCK, 1), 0) + step_q * BLOCK
    spot = jnp.concatenate([spot, spot], axis=0)

    def one(step_k, query_sum):
        cols = pl.ds(step_k * BLOCK, BLOCK)
        key = qkv_ref[cols, 2 * HD : 3 * HD]
        scores = lax.dot_general(query, key, NT, preferred_element_type=jnp.float32) * factor
        key_spot = lax.broadcasted_iota(jnp.int32, (1, BLOCK), 1) + step_k * BLOCK
        fits = (key_spot >= start) & (key_spot <= spot)
        probs = jnp.where(fits, jnp.exp(scores - log_total), 0.0)
        grad_probs = lax.dot_general(
            grad, qkv_ref[cols, 3 * HD : 4 * HD], NT, preferred_element_type=jnp.float32
        )
        grad_scores = (probs * (grad_probs - weighted)).astype(jnp.bfloat16)
        value_sum[cols, :] += lax.dot_general(
            probs.astype(jnp.bfloat16), grad, TN, preferred_element_type=jnp.float32
        )
        key_sum[cols, :] += lax.dot_general(
            grad_scores, query, TN, preferred_element_type=jnp.float32
        )
        return query_sum + jnp.dot(grad_scores, key, preferred_element_type=jnp.float32)

    query_sum = lax.fori_loop(
        first_ref[step_q], step_q + 1, one, jnp.zeros((2 * BLOCK, HD), jnp.float32)
    )
    query_sum = (query_sum * factor).astype(jnp.bfloat16)
    back_ref[rows, 0:HD] = query_sum[:BLOCK]
    back_ref[rows, HD : 2 * HD] = query_sum[BLOCK:]

    @pl.when(step_q == pl.num_programs(0) - 1)
    def _():
        back_ref[:, 2 * HD : 3 * HD] = (key_sum[...] * factor).astype(jnp.bfloat16)
        back_ref[:, 3 * HD : 4 * HD] = value_sum[...].astype(jnp.bfloat16)


def row_starts(lengths_row, total):
    segment, place = layout(lengths_row, total)
    positions = jnp.arange(total, dtype=jnp.int32)
    starts = jnp.where(segment == NDOC - 1, positions, positions - place)
    return (starts, place)


def attention_out(qkv, starts, first):
    total = qkv.shape[0]
    whole = lambda i, *_: (0, 0)
    return pl.pallas_call(
        attend_forward,
        out_shape=(
            jax.ShapeDtypeStruct((total, 2 * HD), jnp.bfloat16),
            jax.ShapeDtypeStruct((total, 2 * HD), jnp.float32),
            jax.ShapeDtypeStruct((total, 2), jnp.float32),
        ),
        grid_spec=pltpu.PrefetchScalarGridSpec(
            num_scalar_prefetch=1,
            grid=(total // BLOCK,),
            in_specs=[
                pl.BlockSpec((total, 4 * HD), whole),
                pl.BlockSpec((total, 1), whole),
            ],
            out_specs=[
                pl.BlockSpec((BLOCK, 2 * HD), lambda i, *_: (i, 0)),
                pl.BlockSpec((BLOCK, 2 * HD), lambda i, *_: (i, 0)),
                pl.BlockSpec((BLOCK, 2), lambda i, *_: (i, 0)),
            ],
        ),
        name="attend_forward",
    )(first, qkv, starts[:, None])


def attention_back(qkv, starts, first, grad, kept, log_total):
    total = qkv.shape[0]
    whole = lambda i, *_: (0, 0)
    block = lambda i, *_: (i, 0)
    return pl.pallas_call(
        attend_backward,
        out_shape=jax.ShapeDtypeStruct((total, 4 * HD), jnp.bfloat16),
        grid_spec=pltpu.PrefetchScalarGridSpec(
            num_scalar_prefetch=1,
            grid=(total // BLOCK,),
            in_specs=[
                pl.BlockSpec((total, 4 * HD), whole),
                pl.BlockSpec((total, 1), whole),
                pl.BlockSpec((BLOCK, 2 * HD), block),
                pl.BlockSpec((BLOCK, 2 * HD), block),
                pl.BlockSpec((BLOCK, 2), block),
            ],
            out_specs=pl.BlockSpec((total, 4 * HD), whole),
            scratch_shapes=[
                pltpu.VMEM((total, HD), jnp.float32),
                pltpu.VMEM((total, HD), jnp.float32),
            ],
        ),
        name="attend_backward",
    )(first, qkv, starts[:, None], grad, kept, log_total)


def dot_f32(left, right, dims=(((1,), (0,)), ((), ()))):
    return lax.dot_general(left, right, dims, preferred_element_type=jnp.float32)


SUB = 64
RING = 8
LANES = 512
MESH = pl.DeviceIdType.MESH


class Relay:
    def __init__(self, count, own, landed, cross, sems):
        self.count, self.own, self.landed, self.cross = count, own, landed, cross
        self.out_sem, self.land_sem, self.back_sem, self.cross_sem = sems
        spot = lax.axis_index("narrow")
        self.is_end = (spot == 0) | (spot == 3)
        self.is_mid = (spot == 1) | (spot == 2)
        self.inner = 1 + spot // 3
        self.other = 3 - spot
        self.outer = jnp.where(spot == 2, 3, 0)

    def to_inner(self, k):
        return pltpu.make_async_remote_copy(
            src_ref=self.own.at[k],
            dst_ref=self.landed.at[k],
            send_sem=self.out_sem.at[k],
            recv_sem=self.land_sem.at[k],
            device_id={"narrow": self.inner},
            device_id_type=MESH,
        )

    def to_other(self, k):
        return pltpu.make_async_remote_copy(
            src_ref=self.own.at[k],
            dst_ref=self.cross.at[k % RING],
            send_sem=self.out_sem.at[k],
            recv_sem=self.cross_sem.at[k % RING],
            device_id={"narrow": self.other},
            device_id_type=MESH,
        )

    def to_outer(self, k):
        return pltpu.make_async_remote_copy(
            src_ref=self.landed.at[k],
            dst_ref=self.landed.at[k],
            send_sem=self.back_sem.at[k],
            recv_sem=self.land_sem.at[k],
            device_id={"narrow": self.outer},
            device_id_type=MESH,
        )

    def greet(self):
        barrier = pltpu.get_barrier_semaphore()

        @pl.when(self.is_end)
        def _():
            pl.semaphore_signal(
                barrier, inc=1, device_id={"narrow": self.inner}, device_id_type=MESH
            )
            pl.semaphore_wait(barrier, 1)

        @pl.when(self.is_mid)
        def _():
            pl.semaphore_signal(
                barrier, inc=1, device_id={"narrow": self.outer}, device_id_type=MESH
            )
            pl.semaphore_signal(
                barrier, inc=1, device_id={"narrow": self.other}, device_id_type=MESH
            )
            pl.semaphore_wait(barrier, 2)

    def send(self, first, number):
        @pl.when(self.is_end)
        def _():
            @pl.loop(0, number)
            def _(i):
                self.to_inner(first + i).start()

    def tick(self, k):
        @pl.when(self.is_mid & (k < self.count))
        def _():
            self.to_inner(k).wait_recv()
            self.own[k] = (
                self.own[k].astype(jnp.float32) + self.landed[k].astype(jnp.float32)
            ).astype(jnp.bfloat16)
            self.to_other(k).start()

        @pl.when(self.is_mid & (k >= 2) & (k < self.count + 2))
        def _():
            j = k - 2
            self.to_other(j).wait_recv()
            self.landed[j] = (
                self.own[j].astype(jnp.float32) + self.cross[j % RING].astype(jnp.float32)
            ).astype(jnp.bfloat16)
            self.to_outer(j).start()

        @pl.when(self.is_end & (k >= 4) & (k < self.count + 4))
        def _():
            self.to_outer(k - 4).wait_recv()

    def drain(self):
        @pl.loop(0, self.count)
        def _(k):
            self.to_inner(k).wait_send()

            @pl.when(self.is_mid)
            def _():
                self.to_outer(k).wait_send()


def relay_scratch(count, model):
    return [
        pltpu.VMEM((count, SUB, model), jnp.bfloat16),
        pltpu.VMEM((count, SUB, model), jnp.bfloat16),
        pltpu.VMEM((RING, SUB, model), jnp.bfloat16),
        pltpu.SemaphoreType.DMA((count,)),
        pltpu.SemaphoreType.DMA((count,)),
        pltpu.SemaphoreType.DMA((count,)),
        pltpu.SemaphoreType.DMA((RING,)),
    ]


def feed_kernel(
    mixed_ref,
    input_ref,
    grad_ref,
    gain_ref,
    out_w,
    gate_w,
    up_w,
    down_w,
    hidden_out,
    active_out,
    gate_out,
    upper_out,
    output_out,
    middle_out,
    low_out,
    mixed_out,
    gain_out,
    own,
    landed,
    cross,
    out_sem,
    land_sem,
    back_sem,
    cross_sem,
    out_v,
    gate_v,
    up_v,
    down_v,
    mixed_v,
    rows_v,
    grads_v,
    hidden_v,
    stage_v,
    scale_v,
    middle_v,
    output_v,
    mixback_v,
    weight_sem,
    attn_sem,
    load_sem,
    hidden_sem,
    stage_sem,
    final_sem,
):
    micro, tok, model = input_ref.shape
    width = out_w.shape[0]
    piece = out_w.shape[2]
    groups = width // micro
    per = tok // SUB
    hid = gate_w.shape[1]
    relay = Relay(3 * micro * per, own, landed, cross, (out_sem, land_sem, back_sem, cross_sem))
    n_up = hid // LANES
    n_down = model // LANES
    slots = n_up + n_down

    attn_copies = [
        pltpu.make_async_copy(
            mixed_ref.at[i],
            mixed_v.at[i // groups, :, pl.ds((i % groups) * 2 * HD, 2 * HD)],
            attn_sem.at[i],
        )
        for i in range(width)
    ] + [
        pltpu.make_async_copy(
            out_w.at[i], out_v.at[:, pl.ds(i * piece, piece)], attn_sem.at[width + i]
        )
        for i in range(width)
    ]
    weight_copies = [
        pltpu.make_async_copy(gate_w, gate_v, weight_sem.at[0]),
        pltpu.make_async_copy(up_w, up_v, weight_sem.at[1]),
    ] + [
        pltpu.make_async_copy(
            down_w.at[i], down_v.at[:, pl.ds(i * piece, piece)], weight_sem.at[2 + i]
        )
        for i in range(width)
    ]
    for copy in attn_copies + weight_copies:
        copy.start()

    def loads(n):
        slot = n % 2
        return (
            pltpu.make_async_copy(input_ref.at[n % micro], rows_v.at[slot], load_sem.at[slot, 0]),
            pltpu.make_async_copy(grad_ref.at[n % micro], grads_v.at[slot], load_sem.at[slot, 1]),
        )

    def start_loads(n):
        for copy in loads(n):
            copy.start()

    def wait_loads(n):
        for copy in loads(n):
            copy.wait()

    start_loads(0)
    gain_out[...] = jnp.zeros_like(gain_out)
    relay.greet()
    for copy in attn_copies:
        copy.wait()

    @pl.loop(0, micro)
    def _(m):
        for n in range(n_down):
            cols = pl.ds(n * LANES, LANES)
            part = dot_f32(mixed_v[m], out_v[:, cols]).astype(jnp.bfloat16)
            for r in range(per):
                own[m * per + r, :, cols] = part[r * SUB : (r + 1) * SUB]
        relay.send(m * per, per)

    first_ticks = per + 4

    @pl.loop(0, first_ticks)
    def _(k):
        relay.tick(k)

    for copy in weight_copies:
        copy.wait()

    def hidden_copy(m):
        return pltpu.make_async_copy(hidden_v, hidden_out.at[m], hidden_sem)

    def stage_copies(m):
        return [
            pltpu.make_async_copy(stage_v.at[i], target.at[m], stage_sem.at[i])
            for i, target in enumerate((active_out, gate_out, upper_out))
        ]

    base = micro * per

    @pl.loop(0, micro)
    def _(m):
        slot = m % 2
        wait_loads(m)
        start_loads(m + 1)

        @pl.when(m > 0)
        def _():
            hidden_copy(m - 1).wait()
            for copy in stage_copies(m - 1):
                copy.wait()

        for r in range(per):
            span = pl.ds(r * SUB, SUB)
            middle = rows_v[slot, span, :].astype(jnp.float32) + landed[m * per + r].astype(
                jnp.float32
            )
            scale = lax.rsqrt(jnp.mean(middle * middle, axis=-1, keepdims=True) + EPSILON)
            scale_v[span, :] = scale
            hidden_v[span, :] = (middle * scale * gain_ref[...]).astype(jnp.bfloat16)
        hidden_copy(m).start()
        for j in range(n_up):
            relay.tick(first_ticks + slots * m + j)
            cols = pl.ds(j * LANES, LANES)
            gate = dot_f32(hidden_v[...], gate_v[:, cols])
            up_proj = dot_f32(hidden_v[...], up_v[:, cols])
            grad_active = dot_f32(grads_v[slot], down_v[cols, :], NT)
            squash = 1.0 / (1.0 + jnp.exp(-gate))
            silu = gate * squash
            stage_v[0, :, cols] = (silu * up_proj).astype(jnp.bfloat16)
            stage_v[1, :, cols] = (
                grad_active * up_proj * (squash * (1.0 + gate * (1.0 - squash)))
            ).astype(jnp.bfloat16)
            stage_v[2, :, cols] = (grad_active * silu).astype(jnp.bfloat16)
        for copy in stage_copies(m):
            copy.start()
        for n in range(n_down):
            relay.tick(first_ticks + slots * m + n_up + n)
            cols = pl.ds(n * LANES, LANES)
            back = dot_f32(stage_v[1], gate_v[cols, :], NT) + dot_f32(
                stage_v[2], up_v[cols, :], NT
            )
            ahead = dot_f32(stage_v[0], down_v[:, cols]).astype(jnp.bfloat16)
            gain_sum = jnp.zeros((1, LANES), jnp.float32)
            for r in range(per):
                part = slice(r * SUB, (r + 1) * SUB)
                own[base + 2 * per * m + r, :, cols] = back[part].astype(jnp.bfloat16)
                own[base + 2 * per * m + per + r, :, cols] = ahead[part]
                unit = (
                    rows_v[slot, pl.ds(r * SUB, SUB), cols].astype(jnp.float32)
                    + landed[m * per + r, :, cols].astype(jnp.float32)
                ) * scale_v[pl.ds(r * SUB, SUB), :]
                gain_sum += jnp.sum(back[part] * unit, axis=0, keepdims=True)
            gain_out[:, cols] += gain_sum
        relay.send(base + 2 * per * m, 2 * per)

    hidden_copy(micro - 1).wait()
    for copy in stage_copies(micro - 1):
        copy.wait()

    def final_copies(m):
        return [
            pltpu.make_async_copy(middle_v, middle_out.at[m], final_sem.at[0]),
            pltpu.make_async_copy(hidden_v, low_out.at[m], final_sem.at[1]),
            pltpu.make_async_copy(output_v, output_out.at[m], final_sem.at[2]),
        ] + [
            pltpu.make_async_copy(
                mixback_v.at[:, pl.ds(g * 2 * HD, 2 * HD)],
                mixed_out.at[m * groups + g],
                final_sem.at[3 + g],
            )
            for g in range(groups)
        ]

    last_ticks = first_ticks + slots * micro
    rest = 3 * micro * per + 4 - last_ticks
    turns = rest // micro

    @pl.loop(0, micro)
    def _(m):
        slot = m % 2
        wait_loads(m + micro)

        @pl.when(m < micro - 1)
        def _():
            start_loads(m + micro + 1)

        @pl.when(m > 0)
        def _():
            for copy in final_copies(m - 1):
                copy.wait()

        for t in range(turns // 2):
            relay.tick(last_ticks + turns * m + t)
        for r in range(per):
            span = pl.ds(r * SUB, SUB)
            middle = rows_v[slot, span, :].astype(jnp.float32) + landed[m * per + r].astype(
                jnp.float32
            )
            scale = lax.rsqrt(jnp.mean(middle * middle, axis=-1, keepdims=True) + EPSILON)
            pulled = landed[base + 2 * per * m + r].astype(jnp.float32) * gain_ref[...]
            along = jnp.mean(pulled * middle, axis=-1, keepdims=True)
            grad_middle = grads_v[slot, span, :].astype(jnp.float32) + scale * (
                pulled - middle * (scale * scale * along)
            )
            middle_v[span, :] = grad_middle
            hidden_v[span, :] = grad_middle.astype(jnp.bfloat16)
        mixback_v[...] = dot_f32(hidden_v[...], out_v[...], NT).astype(jnp.bfloat16)
        for t in range(turns // 2, turns):
            relay.tick(last_ticks + turns * m + t)
        for r in range(per):
            span = pl.ds(r * SUB, SUB)
            output_v[span, :] = (
                rows_v[slot, span, :].astype(jnp.float32)
                + landed[m * per + r].astype(jnp.float32)
                + landed[base + 2 * per * m + per + r].astype(jnp.float32)
            ).astype(jnp.bfloat16)
        for copy in final_copies(m):
            copy.start()

    for copy in final_copies(micro - 1):
        copy.wait()
    relay.drain()


def feed_forward(mixed, layer_input, grad_out, gain_ffn, out_w, gate_w, up_w, down_w):
    micro, tok, model = layer_input.shape
    width, heads_in, piece = out_w.shape
    hid = gate_w.shape[1]
    groups = width // micro
    low = jnp.bfloat16
    count = 3 * micro * (tok // SUB)
    anywhere = pl.BlockSpec(memory_space=pl.ANY)
    inside = pl.BlockSpec(memory_space=pltpu.VMEM)
    return pl.pallas_call(
        feed_kernel,
        out_shape=(
            jax.ShapeDtypeStruct((micro, tok, model), low),
            jax.ShapeDtypeStruct((micro, tok, hid), low),
            jax.ShapeDtypeStruct((micro, tok, hid), low),
            jax.ShapeDtypeStruct((micro, tok, hid), low),
            jax.ShapeDtypeStruct((micro, tok, model), low),
            jax.ShapeDtypeStruct((micro, tok, model), jnp.float32),
            jax.ShapeDtypeStruct((micro, tok, model), low),
            jax.ShapeDtypeStruct((width, tok, 2 * HD), low),
            jax.ShapeDtypeStruct((1, model), jnp.float32),
        ),
        in_specs=[anywhere] * 3 + [inside] + [anywhere] * 4,
        out_specs=[anywhere] * 8 + [inside],
        scratch_shapes=relay_scratch(count, model)
        + [
            pltpu.VMEM((heads_in, model), low),
            pltpu.VMEM((model, hid), low),
            pltpu.VMEM((model, hid), low),
            pltpu.VMEM((hid, model), low),
            pltpu.VMEM((micro, tok, heads_in), low),
            pltpu.VMEM((2, tok, model), low),
            pltpu.VMEM((2, tok, model), low),
            pltpu.VMEM((tok, model), low),
            pltpu.VMEM((3, tok, hid), low),
            pltpu.VMEM((tok, 1), jnp.float32),
            pltpu.VMEM((tok, model), jnp.float32),
            pltpu.VMEM((tok, model), low),
            pltpu.VMEM((tok, heads_in), low),
            pltpu.SemaphoreType.DMA((2 + width,)),
            pltpu.SemaphoreType.DMA((2 * width,)),
            pltpu.SemaphoreType.DMA((2, 2)),
            pltpu.SemaphoreType.DMA,
            pltpu.SemaphoreType.DMA((3,)),
            pltpu.SemaphoreType.DMA((3 + groups,)),
        ],
        compiler_params=pltpu.CompilerParams(
            collective_id=0, has_side_effects=True, vmem_limit_bytes=67043328
        ),
        cost_estimate=pl.CostEstimate(
            flops=200_000_000_000, bytes_accessed=900_000_000, transcendentals=0
        ),
        name="feed_forward",
    )(mixed, layer_input, grad_out, gain_ffn[None, :], out_w, gate_w, up_w, down_w)


def local_batched(
    layer_input,
    grad_out,
    lengths,
    w_query,
    w_key,
    w_value,
    w_out,
    w_gate,
    w_up,
    w_down,
    gain_attn,
    gain_ffn,
    gain_query,
    gain_key,
):
    micro, tok_rows, model = layer_input.shape
    width = lax.axis_size("wide")
    groups = w_key.shape[1] // HD
    total = tok_rows * width
    count = micro * tok_rows
    me = lax.axis_index("wide")
    w_qkv = lax.all_gather(
        jnp.concatenate([w_query, w_key, w_value], axis=1), "wide", axis=0, tiled=True
    )
    w_out_all = lax.all_gather(w_out, "wide", axis=0)
    w_gate_full = lax.all_gather(w_gate, "wide", axis=0, tiled=True)
    w_up_full = lax.all_gather(w_up, "wide", axis=0, tiled=True)
    w_down_all = lax.all_gather(w_down, "wide", axis=0)
    starts, places = jax.vmap(lambda row: row_starts(row, total))(lengths)
    my_places = lax.dynamic_slice_in_dim(places, me * tok_rows, tok_rows, axis=1)
    cosine, sine = jax.vmap(angles)(my_places)
    cosine = cosine.reshape(count, 1, HD)
    sine = sine.reshape(count, 1, HD)
    my_starts = lax.dynamic_index_in_dim(starts, me // groups, axis=0, keepdims=False)
    my_first = my_starts[::BLOCK] // BLOCK

    def head_norm(rows, gain):
        return rotate(rms_norm(rows, gain), cosine, sine)

    input_float = layer_input.reshape(count, model).astype(jnp.float32)
    grad_rows = grad_out.reshape(count, model)
    normed_one, pull_one = jax.vjp(lambda rows: rms_norm(rows, gain_attn), input_float)
    hidden_one = normed_one.astype(jnp.bfloat16)
    qkv = dot_f32(hidden_one, w_qkv)
    q_cols = w_query.shape[1]
    k_cols = w_key.shape[1]
    query_turned, pull_query = jax.vjp(
        head_norm, qkv[:, :q_cols].reshape(count, -1, HD), gain_query
    )
    key_turned, pull_key = jax.vjp(
        head_norm, qkv[:, q_cols : q_cols + k_cols].reshape(count, -1, HD), gain_key
    )
    packed = jnp.concatenate(
        [
            query_turned.reshape(micro, tok_rows, groups, 2 * HD),
            key_turned.reshape(micro, tok_rows, groups, HD),
            qkv[:, q_cols + k_cols :].reshape(micro, tok_rows, groups, HD),
        ],
        axis=-1,
    ).astype(jnp.bfloat16)
    packed = jnp.moveaxis(packed, 2, 1).reshape(width, tok_rows, 4 * HD)
    packed = lax.all_to_all(packed, "wide", split_axis=0, concat_axis=0).reshape(total, 4 * HD)
    mixed, kept, log_total = attention_out(packed, my_starts, my_first)
    mixed = lax.all_to_all(
        mixed.reshape(width, tok_rows, 2 * HD), "wide", split_axis=0, concat_axis=0
    )
    (
        hidden_two,
        active_low,
        gate_back,
        upper_back,
        output,
        grad_middle,
        middle_low,
        grad_mixed,
        gain_two,
    ) = feed_forward(
        mixed, layer_input, grad_out, gain_ffn, w_out_all, w_gate_full, w_up_full, w_down_all
    )
    gain_two = gain_two[0]
    hidden_two = hidden_two.reshape(count, model)
    active_low = active_low.reshape(count, -1)
    gate_back = gate_back.reshape(count, -1)
    upper_back = upper_back.reshape(count, -1)
    grad_middle = grad_middle.reshape(count, model)
    middle_low = middle_low.reshape(count, model)
    mixed_low = jnp.moveaxis(
        mixed.reshape(micro, groups, tok_rows, 2 * HD), 1, 2
    ).reshape(count, groups * 2 * HD)
    grad_mixed = lax.all_to_all(grad_mixed, "wide", split_axis=0, concat_axis=0)
    back = attention_back(
        packed, my_starts, my_first, grad_mixed.reshape(total, 2 * HD), kept, log_total
    )
    back = lax.all_to_all(
        back.reshape(width, tok_rows, 4 * HD), "wide", split_axis=0, concat_axis=0
    )
    back = jnp.moveaxis(back.reshape(micro, groups, tok_rows, 4 * HD), 1, 2)
    back = back.reshape(count, groups, 4 * HD)
    grad_qraw, gain_q = pull_query(
        back[..., : 2 * HD].reshape(count, -1, HD).astype(jnp.float32)
    )
    grad_kraw, gain_k = pull_key(back[..., 2 * HD : 3 * HD].astype(jnp.float32))
    qkv_back = jnp.concatenate(
        [
            grad_qraw.reshape(count, -1).astype(jnp.bfloat16),
            grad_kraw.reshape(count, -1).astype(jnp.bfloat16),
            back[..., 3 * HD :].reshape(count, -1),
        ],
        axis=1,
    )
    partial_one = dot_f32(qkv_back, w_qkv, NT)
    gain_one = jnp.sum(partial_one * unit_rows(input_float), axis=0)
    grad_input = (
        grad_middle
        + pull_one(lax.psum(partial_one.astype(jnp.bfloat16), "narrow").astype(jnp.float32))[0]
    )

    def scatter(left, right):
        part = dot_f32(left, right, TN).astype(jnp.bfloat16)
        return lax.psum_scatter(part, "wide", scatter_dimension=0, tiled=True).astype(jnp.float32)

    def scatter_cols(left, right):
        part = dot_f32(left, right, TN).astype(jnp.bfloat16)
        return lax.psum_scatter(part, "wide", scatter_dimension=1, tiled=True).astype(jnp.float32)

    grad_wgate = scatter(hidden_two, gate_back)
    grad_wup = scatter(hidden_two, upper_back)
    grad_wdown = scatter_cols(active_low, grad_rows)
    grad_wout = scatter_cols(mixed_low, middle_low)
    grad_wqkv = scatter(hidden_one, qkv_back)
    gains = lax.psum((gain_one, gain_two, gain_q, gain_k), ("wide", "narrow"))
    return (
        output,
        grad_input.reshape(micro, tok_rows, model),
        grad_wqkv[:, :q_cols],
        grad_wqkv[:, q_cols : q_cols + k_cols],
        grad_wqkv[:, q_cols + k_cols :],
        grad_wout,
        grad_wgate,
        grad_wup,
        grad_wdown,
    ) + tuple(gains)


def local(mesh, layer_input, grad_out, lengths, w_query, w_key, *rest):
    width = mesh.shape["wide"]
    micro, tok_rows = layer_input.shape[:2]
    groups = w_key.shape[1] // HD
    fits = (
        micro * groups == width
        and w_query.shape[1] == 2 * w_key.shape[1]
        and mesh.shape["narrow"] == 4
        and tok_rows == BLOCK
    )
    chosen = local_batched if fits else local_general
    return chosen(layer_input, grad_out, lengths, w_query, w_key, *rest)


def solution(mesh):
    in_specs = (
        P(None, "wide", None),
        P(None, "wide", None),
        P(),
        P("wide", "narrow"),
        P("wide", "narrow"),
        P("wide", "narrow"),
        P("narrow", "wide"),
        P("wide", "narrow"),
        P("wide", "narrow"),
        P("narrow", "wide"),
        P(),
        P(),
        P(),
        P(),
    )
    out_specs = (
        P(None, "wide", None),
        P(None, "wide", None),
        P("wide", "narrow"),
        P("wide", "narrow"),
        P("wide", "narrow"),
        P("narrow", "wide"),
        P("wide", "narrow"),
        P("wide", "narrow"),
        P("narrow", "wide"),
        P(),
        P(),
        P(),
        P(),
    )
    return jax.shard_map(
        functools.partial(local, mesh), mesh=mesh, in_specs=in_specs, out_specs=out_specs, check_vma=False)
```

```python
import functools
import math

import jax
import jax.numpy as jnp
from jax import lax
from jax.experimental import pallas as pl
from jax.experimental.pallas import tpu as pltpu
from jax.sharding import PartitionSpec as P

HD = 128
NDOC = 8


EPSILON = 1e-06
THETA = 1000000.0


def rms_norm(values, gain):
    return values * lax.rsqrt(jnp.mean(values * values, axis=-1, keepdims=True) + EPSILON) * gain


def unit_rows(values):
    return values * lax.rsqrt(jnp.mean(values * values, axis=-1, keepdims=True) + EPSILON)


def rotate(values, cosine, sine):
    midway = values.shape[-1] // 2
    turned = jnp.concatenate([-values[..., midway:], values[..., :midway]], axis=-1)
    return values * cosine + turned * sine


def layout(lengths_row, total):
    finish = jnp.cumsum(lengths_row)
    starts = finish - lengths_row
    places = jnp.arange(total, dtype=jnp.int32)
    segment = jnp.sum((places[:, None] >= finish[None, :]).astype(jnp.int32), axis=1)
    member = segment[:, None] == jnp.arange(finish.shape[0], dtype=jnp.int32)[None, :]
    opening = jnp.sum(jnp.where(member, starts[None, :], 0), axis=1)
    return (segment, places - opening)


def angles(place):
    frequency = jnp.exp(-math.log(THETA) * jnp.arange(0, HD, 2).astype(jnp.float32) / HD)
    turning = place.astype(jnp.float32)[:, None] * frequency[None, :]
    turning = jnp.concatenate([turning, turning], axis=-1)
    return (jnp.cos(turning), jnp.sin(turning))


def allowed(query_seg, query_idx, key_seg, key_idx):
    same_doc = query_seg[:, None] == key_seg[None, :]
    causal = key_idx[None, :] <= query_idx[:, None]
    usable = (key_seg[None, :] != NDOC - 1) | (key_idx[None, :] == query_idx[:, None])
    return same_doc & causal & usable


def attention_scores(query_low, key_all, mask_local, factor):
    scores = (
        jnp.einsum("tgrd,kgd->grtk", query_low, key_all, preferred_element_type=jnp.float32)
        * factor
    )
    return jnp.where(mask_local[None, None], scores, -1e30)


def one_batch(row_input, grad_row, lengths_row, gathered, gains):
    w_query, w_key, w_value, w_out, w_gate, w_up, w_down = gathered
    gain_attn, gain_ffn, gain_query, gain_key = gains
    tok_rows = row_input.shape[0]
    total = tok_rows * lax.axis_size("wide")
    groups = w_key.shape[1] // HD
    repeat = w_query.shape[1] // w_key.shape[1]
    factor = 1.0 / math.sqrt(HD)
    first_row = lax.axis_index("wide") * tok_rows
    segment, place = layout(lengths_row, total)
    positions = jnp.arange(total, dtype=jnp.int32)
    query_seg = lax.dynamic_slice_in_dim(segment, first_row, tok_rows)
    query_idx = lax.dynamic_slice_in_dim(positions, first_row, tok_rows)
    mask_local = allowed(query_seg, query_idx, segment, positions)
    cosine, sine = angles(lax.dynamic_slice_in_dim(place, first_row, tok_rows))

    def head_norm(rows, gain):
        return rotate(rms_norm(rows, gain), cosine[:, None, :], sine[:, None, :])

    input_float = row_input.astype(jnp.float32)
    grad_float = grad_row.astype(jnp.float32)
    normed_one, pull_one = jax.vjp(lambda rows: rms_norm(rows, gain_attn), input_float)
    hidden_one = normed_one.astype(jnp.bfloat16)
    query_raw = jnp.dot(hidden_one, w_query, preferred_element_type=jnp.float32).reshape(
        tok_rows, groups * repeat, HD
    )
    key_raw = jnp.dot(hidden_one, w_key, preferred_element_type=jnp.float32).reshape(
        tok_rows, groups, HD
    )
    value_low = jnp.dot(hidden_one, w_value, preferred_element_type=jnp.float32).astype(
        jnp.bfloat16
    )
    query_turned, pull_query = jax.vjp(head_norm, query_raw, gain_query)
    key_turned, pull_key = jax.vjp(head_norm, key_raw, gain_key)
    query_low = query_turned.astype(jnp.bfloat16).reshape(tok_rows, groups, repeat, HD)
    key_low = key_turned.astype(jnp.bfloat16).reshape(tok_rows, groups * HD)
    key_all, value_all = (
        lax.all_gather(key_low, "wide", axis=0, tiled=True),
        lax.all_gather(value_low, "wide", axis=0, tiled=True),
    )
    key_all = key_all.reshape(total, groups, HD)
    value_all = value_all.reshape(total, groups, HD)
    scores = attention_scores(query_low, key_all, mask_local, factor)
    highest = jnp.max(scores, axis=-1, keepdims=True)
    exponent = jnp.exp(scores - highest)
    denominator = jnp.sum(exponent, axis=-1, keepdims=True)
    log_total = highest + jnp.log(denominator)
    probs_low = (exponent / denominator).astype(jnp.bfloat16)
    mixed = jnp.einsum("grtk,kgd->tgrd", probs_low, value_all, preferred_element_type=jnp.float32)
    mixed_low = mixed.reshape(tok_rows, groups * repeat * HD).astype(jnp.bfloat16)
    attn_part = jnp.dot(mixed_low, w_out, preferred_element_type=jnp.float32)
    middle = input_float + lax.psum(attn_part.astype(jnp.bfloat16), "narrow").astype(jnp.float32)
    normed_two, pull_two = jax.vjp(lambda rows: rms_norm(rows, gain_ffn), middle)
    hidden_two = normed_two.astype(jnp.bfloat16)
    unit_two = unit_rows(middle)
    gate = jnp.dot(hidden_two, w_gate, preferred_element_type=jnp.float32)
    up_proj = jnp.dot(hidden_two, w_up, preferred_element_type=jnp.float32)
    active, pull_active = jax.vjp(
        lambda gate_in, up_in: jax.nn.silu(gate_in) * up_in, gate, up_proj
    )
    active_low = active.astype(jnp.bfloat16)
    ffn_part = jnp.dot(active_low, w_down, preferred_element_type=jnp.float32)
    output_low = (
        middle + lax.psum(ffn_part.astype(jnp.bfloat16), "narrow").astype(jnp.float32)
    ).astype(jnp.bfloat16)
    grad_wdown = jnp.einsum("tf,td->fd", active_low, grad_row, preferred_element_type=jnp.float32)
    grad_active = jnp.einsum("td,fd->tf", grad_row, w_down, preferred_element_type=jnp.float32)
    grad_gate, grad_upper = pull_active(grad_active)
    gate_back = grad_gate.astype(jnp.bfloat16)
    upper_back = grad_upper.astype(jnp.bfloat16)
    grad_wgate = jnp.einsum("td,tf->df", hidden_two, gate_back, preferred_element_type=jnp.float32)
    grad_wup = jnp.einsum("td,tf->df", hidden_two, upper_back, preferred_element_type=jnp.float32)
    partial_two = jnp.einsum(
        "tf,df->td", gate_back, w_gate, preferred_element_type=jnp.float32
    ) + jnp.einsum("tf,df->td", upper_back, w_up, preferred_element_type=jnp.float32)
    gain_two = jnp.sum(partial_two * unit_two, axis=0)
    grad_middle = (
        grad_float
        + pull_two(lax.psum(partial_two.astype(jnp.bfloat16), "narrow").astype(jnp.float32))[0]
    )
    middle_low = grad_middle.astype(jnp.bfloat16)
    grad_wout = jnp.einsum("th,td->hd", mixed_low, middle_low, preferred_element_type=jnp.float32)
    grad_mixed = jnp.einsum("td,hd->th", middle_low, w_out, preferred_element_type=jnp.float32)
    grad_mixed = grad_mixed.astype(jnp.bfloat16).reshape(tok_rows, groups, repeat, HD)
    scores = attention_scores(query_low, key_all, mask_local, factor)
    probs = jnp.exp(scores - log_total)
    grad_probs = jnp.einsum(
        "tgrd,kgd->grtk", grad_mixed, value_all, preferred_element_type=jnp.float32
    )
    weighted = jnp.sum(probs * grad_probs, axis=-1, keepdims=True)
    grad_scores = (probs * (grad_probs - weighted)).astype(jnp.bfloat16)
    grad_turned = (
        jnp.einsum("grtk,kgd->tgrd", grad_scores, key_all, preferred_element_type=jnp.float32)
        * factor
    )
    grad_keyall = (
        jnp.einsum("grtk,tgrd->kgd", grad_scores, query_low, preferred_element_type=jnp.float32)
        * factor
    )
    grad_valueall = jnp.einsum(
        "grtk,tgrd->kgd", probs.astype(jnp.bfloat16), grad_mixed, preferred_element_type=jnp.float32
    )
    grad_keys, grad_values = (
        lax.psum_scatter(
            grad_keyall.reshape(total, groups * HD).astype(jnp.bfloat16),
            "wide",
            scatter_dimension=0,
            tiled=True,
        ).astype(jnp.float32),
        lax.psum_scatter(
            grad_valueall.reshape(total, groups * HD).astype(jnp.bfloat16),
            "wide",
            scatter_dimension=0,
            tiled=True,
        ).astype(jnp.float32),
    )
    grad_qraw, gain_q = pull_query(grad_turned.reshape(tok_rows, groups * repeat, HD))
    grad_kraw, gain_k = pull_key(grad_keys.reshape(tok_rows, groups, HD))
    query_back = grad_qraw.reshape(tok_rows, groups * repeat * HD).astype(jnp.bfloat16)
    key_back = grad_kraw.reshape(tok_rows, groups * HD).astype(jnp.bfloat16)
    value_back = grad_values.astype(jnp.bfloat16)
    grad_wquery = jnp.einsum(
        "td,th->dh", hidden_one, query_back, preferred_element_type=jnp.float32
    )
    grad_wkey = jnp.einsum("td,th->dh", hidden_one, key_back, preferred_element_type=jnp.float32)
    grad_wvalue = jnp.einsum(
        "td,th->dh", hidden_one, value_back, preferred_element_type=jnp.float32
    )
    partial_one = (
        jnp.einsum("th,dh->td", query_back, w_query, preferred_element_type=jnp.float32)
        + jnp.einsum("th,dh->td", key_back, w_key, preferred_element_type=jnp.float32)
        + jnp.einsum("th,dh->td", value_back, w_value, preferred_element_type=jnp.float32)
    )
    gain_one = jnp.sum(partial_one * unit_rows(input_float), axis=0)
    grad_input = (
        grad_middle
        + pull_one(lax.psum(partial_one.astype(jnp.bfloat16), "narrow").astype(jnp.float32))[0]
    )
    weight_grads = (
        grad_wquery,
        grad_wkey,
        grad_wvalue,
        grad_wout,
        grad_wgate,
        grad_wup,
        grad_wdown,
    )
    return (output_low, grad_input, weight_grads, (gain_one, gain_two, gain_q, gain_k))


def local_general(
    layer_input,
    grad_out,
    lengths,
    w_query,
    w_key,
    w_value,
    w_out,
    w_gate,
    w_up,
    w_down,
    gain_attn,
    gain_ffn,
    gain_query,
    gain_key,
):
    width = lax.axis_size("wide")
    shards = (w_query, w_key, w_value, w_out, w_gate, w_up, w_down)
    along_rows = (True, True, True, False, True, True, False)
    gains = (gain_attn, gain_ffn, gain_query, gain_key)
    totals = tuple(
        (
            jnp.zeros(
                (
                    (piece.shape[0] * width, piece.shape[1])
                    if rows_first
                    else (piece.shape[0], piece.shape[1] * width)
                ),
                jnp.float32,
            )
            for piece, rows_first in zip(shards, along_rows)
        )
    )
    gain_terms = tuple((jnp.zeros(gain.shape, jnp.float32) for gain in gains))
    outputs = []
    grad_inputs = []
    for micro in range(layer_input.shape[0]):
        gathered = (
            lax.all_gather(w_query, "wide", axis=0, tiled=True),
            lax.all_gather(w_key, "wide", axis=0, tiled=True),
            lax.all_gather(w_value, "wide", axis=0, tiled=True),
            lax.all_gather(w_out, "wide", axis=1, tiled=True),
            lax.all_gather(w_gate, "wide", axis=0, tiled=True),
            lax.all_gather(w_up, "wide", axis=0, tiled=True),
            lax.all_gather(w_down, "wide", axis=1, tiled=True),
        )
        output, grad_input, weight_grads, gain_grads = one_batch(
            layer_input[micro], grad_out[micro], lengths[micro], gathered, gains
        )
        outputs.append(output)
        grad_inputs.append(grad_input)
        gain_terms = tuple((running + fresh for running, fresh in zip(gain_terms, gain_grads)))
        totals = tuple((running + fresh for running, fresh in zip(totals, weight_grads)))
    results = (
        lax.psum_scatter(
            totals[0].astype(jnp.bfloat16), "wide", scatter_dimension=0, tiled=True
        ).astype(jnp.float32),
        lax.psum_scatter(
            totals[1].astype(jnp.bfloat16), "wide", scatter_dimension=0, tiled=True
        ).astype(jnp.float32),
        lax.psum_scatter(
            totals[2].astype(jnp.bfloat16), "wide", scatter_dimension=0, tiled=True
        ).astype(jnp.float32),
        lax.psum_scatter(
            totals[3].astype(jnp.bfloat16), "wide", scatter_dimension=1, tiled=True
        ).astype(jnp.float32),
        lax.psum_scatter(
            totals[4].astype(jnp.bfloat16), "wide", scatter_dimension=0, tiled=True
        ).astype(jnp.float32),
        lax.psum_scatter(
            totals[5].astype(jnp.bfloat16), "wide", scatter_dimension=0, tiled=True
        ).astype(jnp.float32),
        lax.psum_scatter(
            totals[6].astype(jnp.bfloat16), "wide", scatter_dimension=1, tiled=True
        ).astype(jnp.float32),
    )
    gain_total = lax.psum(gain_terms, ("wide", "narrow"))
    return (
        jnp.stack(outputs),
        jnp.stack(grad_inputs),
        results[0],
        results[1],
        results[2],
        results[3],
        results[4],
        results[5],
        results[6],
        gain_total[0],
        gain_total[1],
        gain_total[2],
        gain_total[3],
    )


BLOCK = 256
NT = (((1,), (1,)), ((), ()))
TN = (((0,), (0,)), ((), ()))


def attend_forward(first_ref, qkv_ref, start_ref, mixed_ref, kept_ref, log_ref):
    step_q = pl.program_id(0)
    rows = pl.ds(step_q * BLOCK, BLOCK)
    factor = 1.0 / math.sqrt(HD)
    query = jnp.concatenate([qkv_ref[rows, 0:HD], qkv_ref[rows, HD : 2 * HD]], axis=0)
    start = start_ref[rows, :]
    start = jnp.concatenate([start, start], axis=0)
    spot = lax.broadcasted_iota(jnp.int32, (BLOCK, 1), 0) + step_q * BLOCK
    spot = jnp.concatenate([spot, spot], axis=0)

    def one(step_k, carry):
        highest, total, mixed = carry
        cols = pl.ds(step_k * BLOCK, BLOCK)
        scores = lax.dot_general(
            query, qkv_ref[cols, 2 * HD : 3 * HD], NT, preferred_element_type=jnp.float32
        )
        key_spot = lax.broadcasted_iota(jnp.int32, (1, BLOCK), 1) + step_k * BLOCK
        fits = (key_spot >= start) & (key_spot <= spot)
        scores = jnp.where(fits, scores * factor, -1e30)
        fresh = jnp.maximum(highest, jnp.max(scores, axis=-1, keepdims=True))
        shrink = jnp.exp(highest - fresh)
        exponent = jnp.exp(scores - fresh)
        total = total * shrink + jnp.sum(exponent, axis=-1, keepdims=True)
        mixed = mixed * shrink + jnp.dot(
            exponent.astype(jnp.bfloat16),
            qkv_ref[cols, 3 * HD : 4 * HD],
            preferred_element_type=jnp.float32,
        )
        return (fresh, total, mixed)

    highest, total, mixed = lax.fori_loop(
        first_ref[step_q],
        step_q + 1,
        one,
        (
            jnp.full((2 * BLOCK, 1), -1e30, jnp.float32),
            jnp.zeros((2 * BLOCK, 1), jnp.float32),
            jnp.zeros((2 * BLOCK, HD), jnp.float32),
        ),
    )
    mixed = mixed / total
    mixed = jnp.concatenate([mixed[:BLOCK], mixed[BLOCK:]], axis=1)
    mixed_ref[...] = mixed.astype(jnp.bfloat16)
    kept_ref[...] = mixed
    log_total = highest + jnp.log(total)
    log_ref[...] = jnp.concatenate([log_total[:BLOCK], log_total[BLOCK:]], axis=1)


def attend_backward(
    first_ref, qkv_ref, start_ref, grad_ref, kept_ref, log_ref, back_ref, key_sum, value_sum
):
    step_q = pl.program_id(0)
    rows = pl.ds(step_q * BLOCK, BLOCK)
    factor = 1.0 / math.sqrt(HD)

    @pl.when(step_q == 0)
    def _():
        key_sum[...] = jnp.zeros_like(key_sum)
        value_sum[...] = jnp.zeros_like(value_sum)

    query = jnp.concatenate([qkv_ref[rows, 0:HD], qkv_ref[rows, HD : 2 * HD]], axis=0)
    grad = jnp.concatenate([grad_ref[:, 0:HD], grad_ref[:, HD : 2 * HD]], axis=0)
    kept = jnp.concatenate([kept_ref[:, 0:HD], kept_ref[:, HD : 2 * HD]], axis=0)
    log_total = jnp.concatenate([log_ref[:, 0:1], log_ref[:, 1:2]], axis=0)
    weighted = jnp.sum(grad.astype(jnp.float32) * kept, axis=-1, keepdims=True)
    start = start_ref[rows, :]
    start = jnp.concatenate([start, start], axis=0)
    spot = lax.broadcasted_iota(jnp.int32, (BLOCK, 1), 0) + step_q * BLOCK
    spot = jnp.concatenate([spot, spot], axis=0)

    def one(step_k, query_sum):
        cols = pl.ds(step_k * BLOCK, BLOCK)
        key = qkv_ref[cols, 2 * HD : 3 * HD]
        scores = lax.dot_general(query, key, NT, preferred_element_type=jnp.float32) * factor
        key_spot = lax.broadcasted_iota(jnp.int32, (1, BLOCK), 1) + step_k * BLOCK
        fits = (key_spot >= start) & (key_spot <= spot)
        probs = jnp.where(fits, jnp.exp(scores - log_total), 0.0)
        grad_probs = lax.dot_general(
            grad, qkv_ref[cols, 3 * HD : 4 * HD], NT, preferred_element_type=jnp.float32
        )
        grad_scores = (probs * (grad_probs - weighted)).astype(jnp.bfloat16)
        value_sum[cols, :] += lax.dot_general(
            probs.astype(jnp.bfloat16), grad, TN, preferred_element_type=jnp.float32
        )
        key_sum[cols, :] += lax.dot_general(
            grad_scores, query, TN, preferred_element_type=jnp.float32
        )
        return query_sum + jnp.dot(grad_scores, key, preferred_element_type=jnp.float32)

    query_sum = lax.fori_loop(
        first_ref[step_q], step_q + 1, one, jnp.zeros((2 * BLOCK, HD), jnp.float32)
    )
    query_sum = (query_sum * factor).astype(jnp.bfloat16)
    back_ref[rows, 0:HD] = query_sum[:BLOCK]
    back_ref[rows, HD : 2 * HD] = query_sum[BLOCK:]

    @pl.when(step_q == pl.num_programs(0) - 1)
    def _():
        back_ref[:, 2 * HD : 3 * HD] = (key_sum[...] * factor).astype(jnp.bfloat16)
        back_ref[:, 3 * HD : 4 * HD] = value_sum[...].astype(jnp.bfloat16)


def row_starts(lengths_row, total):
    segment, place = layout(lengths_row, total)
    positions = jnp.arange(total, dtype=jnp.int32)
    starts = jnp.where(segment == NDOC - 1, positions, positions - place)
    return (starts, place)


def attention_out(qkv, starts, first):
    total = qkv.shape[0]
    whole = lambda i, *_: (0, 0)
    return pl.pallas_call(
        attend_forward,
        out_shape=(
            jax.ShapeDtypeStruct((total, 2 * HD), jnp.bfloat16),
            jax.ShapeDtypeStruct((total, 2 * HD), jnp.float32),
            jax.ShapeDtypeStruct((total, 2), jnp.float32),
        ),
        grid_spec=pltpu.PrefetchScalarGridSpec(
            num_scalar_prefetch=1,
            grid=(total // BLOCK,),
            in_specs=[
                pl.BlockSpec((total, 4 * HD), whole),
                pl.BlockSpec((total, 1), whole),
            ],
            out_specs=[
                pl.BlockSpec((BLOCK, 2 * HD), lambda i, *_: (i, 0)),
                pl.BlockSpec((BLOCK, 2 * HD), lambda i, *_: (i, 0)),
                pl.BlockSpec((BLOCK, 2), lambda i, *_: (i, 0)),
            ],
        ),
        name="attend_forward",
    )(first, qkv, starts[:, None])


def attention_back(qkv, starts, first, grad, kept, log_total):
    total = qkv.shape[0]
    whole = lambda i, *_: (0, 0)
    block = lambda i, *_: (i, 0)
    return pl.pallas_call(
        attend_backward,
        out_shape=jax.ShapeDtypeStruct((total, 4 * HD), jnp.bfloat16),
        grid_spec=pltpu.PrefetchScalarGridSpec(
            num_scalar_prefetch=1,
            grid=(total // BLOCK,),
            in_specs=[
                pl.BlockSpec((total, 4 * HD), whole),
                pl.BlockSpec((total, 1), whole),
                pl.BlockSpec((BLOCK, 2 * HD), block),
                pl.BlockSpec((BLOCK, 2 * HD), block),
                pl.BlockSpec((BLOCK, 2), block),
            ],
            out_specs=pl.BlockSpec((total, 4 * HD), whole),
            scratch_shapes=[
                pltpu.VMEM((total, HD), jnp.float32),
                pltpu.VMEM((total, HD), jnp.float32),
            ],
        ),
        name="attend_backward",
    )(first, qkv, starts[:, None], grad, kept, log_total)


def dot_f32(left, right, dims=(((1,), (0,)), ((), ()))):
    return lax.dot_general(left, right, dims, preferred_element_type=jnp.float32)


SUB = 64
RING = 8
LANES = 512
MESH = pl.DeviceIdType.MESH


class Relay:
    def __init__(self, count, own, landed, cross, sems):
        self.count, self.own, self.landed, self.cross = count, own, landed, cross
        self.out_sem, self.land_sem, self.back_sem, self.cross_sem = sems
        spot = lax.axis_index("narrow")
        self.is_end = (spot == 0) | (spot == 3)
        self.is_mid = (spot == 1) | (spot == 2)
        self.inner = 1 + spot // 3
        self.other = 3 - spot
        self.outer = jnp.where(spot == 2, 3, 0)

    def to_inner(self, k):
        return pltpu.make_async_remote_copy(
            src_ref=self.own.at[k],
            dst_ref=self.landed.at[k],
            send_sem=self.out_sem.at[k],
            recv_sem=self.land_sem.at[k],
            device_id={"narrow": self.inner},
            device_id_type=MESH,
        )

    def to_other(self, k):
        return pltpu.make_async_remote_copy(
            src_ref=self.own.at[k],
            dst_ref=self.cross.at[k % RING],
            send_sem=self.out_sem.at[k],
            recv_sem=self.cross_sem.at[k % RING],
            device_id={"narrow": self.other},
            device_id_type=MESH,
        )

    def to_outer(self, k):
        return pltpu.make_async_remote_copy(
            src_ref=self.landed.at[k],
            dst_ref=self.landed.at[k],
            send_sem=self.back_sem.at[k],
            recv_sem=self.land_sem.at[k],
            device_id={"narrow": self.outer},
            device_id_type=MESH,
        )

    def greet(self, peers):
        barrier = pltpu.get_barrier_semaphore()
        for peer in peers:
            pl.semaphore_signal(barrier, inc=1, device_id={"wide": peer}, device_id_type=MESH)

        @pl.when(self.is_end)
        def _():
            pl.semaphore_signal(
                barrier, inc=1, device_id={"narrow": self.inner}, device_id_type=MESH
            )
            pl.semaphore_wait(barrier, 1 + len(peers))

        @pl.when(self.is_mid)
        def _():
            pl.semaphore_signal(
                barrier, inc=1, device_id={"narrow": self.outer}, device_id_type=MESH
            )
            pl.semaphore_signal(
                barrier, inc=1, device_id={"narrow": self.other}, device_id_type=MESH
            )
            pl.semaphore_wait(barrier, 2 + len(peers))

    def send(self, first, number):
        @pl.when(self.is_end)
        def _():
            @pl.loop(0, number)
            def _(i):
                self.to_inner(first + i).start()

    def tick(self, k):
        @pl.when(self.is_mid & (k < self.count))
        def _():
            self.to_inner(k).wait_recv()
            self.own[k] = (
                self.own[k].astype(jnp.float32) + self.landed[k].astype(jnp.float32)
            ).astype(jnp.bfloat16)
            self.to_other(k).start()

        @pl.when(self.is_mid & (k >= 2) & (k < self.count + 2))
        def _():
            j = k - 2
            self.to_other(j).wait_recv()
            self.landed[j] = (
                self.own[j].astype(jnp.float32) + self.cross[j % RING].astype(jnp.float32)
            ).astype(jnp.bfloat16)
            self.to_outer(j).start()

        @pl.when(self.is_end & (k >= 4) & (k < self.count + 4))
        def _():
            self.to_outer(k - 4).wait_recv()

    def drain(self, first):
        @pl.loop(first, self.count)
        def _(k):
            self.to_inner(k).wait_send()

        @pl.loop(0, self.count)
        def _(k):
            @pl.when(self.is_mid)
            def _():
                self.to_outer(k).wait_send()


def wide_peers(width):
    spot = lax.axis_index("wide")
    return [lax.rem(spot + step, width) for step in range(1, width)]


def greet_wide(width):
    barrier = pltpu.get_barrier_semaphore()
    for peer in wide_peers(width):
        pl.semaphore_signal(barrier, inc=1, device_id={"wide": peer}, device_id_type=MESH)
    pl.semaphore_wait(barrier, width - 1)


class Exchange:
    def __init__(self, block, slot, send_sem, land_sem):
        self.block, self.slot = block, slot
        self.send_sem, self.land_sem = send_sem, land_sem
        self.spot = lax.axis_index("wide")

    def remote(self, target, source):
        return pltpu.make_async_remote_copy(
            src_ref=self.block(target),
            dst_ref=self.slot(source),
            send_sem=self.send_sem.at[target],
            recv_sem=self.land_sem.at[source],
            device_id={"wide": target},
            device_id_type=MESH,
        )

    def here(self):
        return pltpu.make_async_copy(
            self.block(self.spot), self.slot(self.spot), self.land_sem.at[self.spot]
        )

    def send(self, target):
        @pl.when(target == self.spot)
        def _():
            self.here().start()

        @pl.when(target != self.spot)
        def _():
            self.remote(target, self.spot).start()

    def sent(self, target, home=False):
        @pl.when(target != self.spot)
        def _():
            self.remote(target, self.spot).wait_send()

        if home:

            @pl.when(target == self.spot)
            def _():
                self.here().wait()

    def wait(self, source, home=True):
        if home:

            @pl.when(source == self.spot)
            def _():
                self.here().wait()

        @pl.when(source != self.spot)
        def _():
            self.remote(self.spot, source).wait_recv()


def project_kernel(
    input_ref,
    gain_ref,
    weight_ref,
    cosine_ref,
    sine_ref,
    head_gain_ref,
    hidden_out,
    raw_out,
    packed_out,
    rows_v,
    weight_v,
    hidden_v,
    raw_v,
    pack_v,
    load_sem,
    keep_sem,
    send_sem,
    land_sem,
):
    micro, tok, model = input_ref.shape
    width = packed_out.shape[0]
    groups = width // micro
    heads = 2 * groups
    spot = lax.axis_index("wide")
    swap = Exchange(
        lambda target: pack_v.at[target], lambda source: packed_out.at[source], send_sem, land_sem
    )
    loads = [
        pltpu.make_async_copy(input_ref, rows_v, load_sem.at[0]),
        pltpu.make_async_copy(weight_ref, weight_v, load_sem.at[1]),
    ]
    for copy in loads:
        copy.start()
    greet_wide(width)
    for copy in loads:
        copy.wait()

    def keeps(step, m):
        return [
            pltpu.make_async_copy(hidden_v.at[step % 2], hidden_out.at[m], keep_sem.at[step % 2, 0]),
            pltpu.make_async_copy(raw_v.at[step % 2], raw_out.at[m], keep_sem.at[step % 2, 1]),
        ]

    kept = []
    for step in range(micro):
        far = micro - 1 - step
        own = spot // groups
        if micro == 4:
            m = lax.rem(own + far % 2, 2) + 2 * lax.rem(own // 2 + far // 2, 2)
        else:
            m = lax.rem(own + far, micro)
        if step >= 2:
            for copy in kept[step - 2]:
                copy.wait()
        rows = rows_v[m].astype(jnp.float32)
        scale = lax.rsqrt(jnp.mean(rows * rows, axis=-1, keepdims=True) + EPSILON)
        hidden_v[step % 2] = (rows * scale * gain_ref[...]).astype(jnp.bfloat16)
        heads_all = dot_f32(hidden_v[step % 2], weight_v[...])
        span = pl.ds(pl.multiple_of(m * tok, tok), tok)
        cosine, sine = cosine_ref[span, :], sine_ref[span, :]
        raw_v[step % 2] = heads_all[:, : (heads + groups) * HD]
        for h in range(heads + groups):
            raw = heads_all[:, h * HD : (h + 1) * HD]
            gain = head_gain_ref[0:1, :] if h < heads else head_gain_ref[1:2, :]
            unit = raw * lax.rsqrt(jnp.mean(raw * raw, axis=-1, keepdims=True) + EPSILON) * gain
            turned = unit * cosine + pltpu.roll(unit, HD // 2, 1) * sine
            g, place = (h // 2, h % 2) if h < heads else (h - heads, 2)
            pack_v[m * groups + g, :, place * HD : (place + 1) * HD] = turned.astype(jnp.bfloat16)
        for g in range(groups):
            first = (heads + groups + g) * HD
            pack_v[m * groups + g, :, 3 * HD :] = heads_all[:, first : first + HD].astype(
                jnp.bfloat16
            )
            swap.send(m * groups + g)
        kept.append(keeps(step, m))
        for copy in kept[step]:
            copy.start()
    for copy in kept[micro - 2] + kept[micro - 1]:
        copy.wait()

    @pl.loop(0, width)
    def _(d):
        swap.sent(d)
        swap.wait(d)


def project(layer_input, gain_attn, weight, cosine, sine, head_gains, width):
    micro, tok, model = layer_input.shape
    groups = width // micro
    low = jnp.bfloat16
    anywhere = pl.BlockSpec(memory_space=pl.ANY)
    inside = pl.BlockSpec(memory_space=pltpu.VMEM)
    raw = 3 * groups * HD
    return pl.pallas_call(
        project_kernel,
        out_shape=(
            jax.ShapeDtypeStruct((micro, tok, model), low),
            jax.ShapeDtypeStruct((micro, tok, raw), jnp.float32),
            jax.ShapeDtypeStruct((width, tok, 4 * HD), low),
        ),
        in_specs=[anywhere, inside, anywhere, inside, inside, inside],
        out_specs=[anywhere] * 3,
        scratch_shapes=[
            pltpu.VMEM((micro, tok, model), low),
            pltpu.VMEM(weight.shape, low),
            pltpu.VMEM((2, tok, model), low),
            pltpu.VMEM((2, tok, raw), jnp.float32),
            pltpu.VMEM((width, tok, 4 * HD), low),
            pltpu.SemaphoreType.DMA((2,)),
            pltpu.SemaphoreType.DMA((2, 2)),
            pltpu.SemaphoreType.DMA((width,)),
            pltpu.SemaphoreType.DMA((width,)),
        ],
        compiler_params=pltpu.CompilerParams(
            collective_id=2, has_side_effects=True, vmem_limit_bytes=40 << 20
        ),
        cost_estimate=pl.CostEstimate(
            flops=20_000_000_000, bytes_accessed=40_000_000, transcendentals=0
        ),
        name="project",
    )(layer_input, gain_attn[None, :], weight, cosine, sine, head_gains)


def weights_kernel(
    back_ref,
    raw_ref,
    hidden_ref,
    mixed_ref,
    low_ref,
    cosine_ref,
    sine_ref,
    head_gain_ref,
    back_out,
    grad_out,
    gain_out,
    land_v,
    raw_v,
    hidden_v,
    mixed_v,
    low_v,
    back_v,
    grad_v,
    load_sem,
    back_sem,
    tile_sem,
    send_sem,
    land_sem,
):
    micro, tok, heads_in = mixed_ref.shape
    width = back_ref.shape[0]
    groups = width // micro
    heads = 2 * groups
    model = hidden_ref.shape[2]
    piece = model // width
    count = micro * tok
    swap = Exchange(
        lambda target: back_ref.at[target], lambda source: land_v.at[source], send_sem, land_sem
    )
    loads = [
        pltpu.make_async_copy(mixed_ref, mixed_v, load_sem.at[0]),
        pltpu.make_async_copy(low_ref, low_v, load_sem.at[1]),
        pltpu.make_async_copy(raw_ref, raw_v, load_sem.at[2]),
        pltpu.make_async_copy(hidden_ref, hidden_v, load_sem.at[3]),
    ]
    for copy in loads:
        copy.start()
    greet_wide(width)
    spot = lax.axis_index("wide")
    for step in range(width - 1, -1, -1):
        swap.send(lax.rem(spot + step, width))
    loads[0].wait()
    loads[1].wait()
    mixed_all = mixed_v[...].reshape(count, heads_in)
    for n in range(model // LANES):
        low = low_v[:, :, n * LANES : (n + 1) * LANES].reshape(count, LANES)
        part = dot_f32(mixed_all, low, TN).astype(jnp.bfloat16)
        for i in range(LANES // piece):
            for b in range(heads_in // piece):
                grad_v[
                    n * (LANES // piece) + i, :, pl.ds(2 * heads_in + b * piece, piece)
                ] = part[b * piece : (b + 1) * piece, i * piece : (i + 1) * piece]
    loads[2].wait()
    gain_out[...] = jnp.zeros_like(gain_out)

    @pl.loop(0, width)
    def _(d):
        swap.wait(d)

    def back_copy(m):
        return pltpu.make_async_copy(back_v.at[m], back_out.at[m], back_sem.at[m])

    @pl.loop(0, micro)
    def _(m):
        span = pl.ds(pl.multiple_of(m * tok, tok), tok)
        cosine, sine = cosine_ref[span, :], sine_ref[span, :]
        for h in range(heads + groups):
            raw = raw_v[m, :, h * HD : (h + 1) * HD]
            kind = 0 if h < heads else 1
            gain = head_gain_ref[kind : kind + 1, :]
            g, place = (h // 2, h % 2) if h < heads else (h - heads, 2)
            grad = land_v[m * groups + g, :, place * HD : (place + 1) * HD].astype(jnp.float32)
            straight = grad * cosine + pltpu.roll(grad * sine, HD // 2, 1)
            scale = lax.rsqrt(jnp.mean(raw * raw, axis=-1, keepdims=True) + EPSILON)
            gain_out[kind : kind + 1, :] += jnp.sum(straight * (raw * scale), axis=0, keepdims=True)
            pulled = straight * gain
            along = jnp.mean(pulled * raw, axis=-1, keepdims=True)
            back_v[m, :, h * HD : (h + 1) * HD] = (
                scale * (pulled - raw * (scale * scale * along))
            ).astype(jnp.bfloat16)
        for g in range(groups):
            first = (heads + groups + g) * HD
            back_v[m, :, first : first + HD] = land_v[m * groups + g, :, 3 * HD :]
        back_copy(m).start()

    loads[3].wait()

    def tile_copy(i):
        return pltpu.make_async_copy(grad_v.at[i], grad_out.at[i], tile_sem.at[i])

    @pl.loop(0, width)
    def _(i):
        left = hidden_v[:, :, pl.ds(pl.multiple_of(i * piece, piece), piece)].reshape(count, piece)
        right = back_v[...].reshape(count, 2 * heads_in)
        grad_v[i, :, 0 : 2 * heads_in] = dot_f32(left, right, TN).astype(jnp.bfloat16)
        tile_copy(i).start()

    @pl.loop(0, width)
    def _(i):
        tile_copy(i).wait()
        swap.sent(i)

    for m in range(micro):
        back_copy(m).wait()


def weight_gradients(back, raw, hidden, mixed, middle_low, cosine, sine, head_gains):
    micro, tok, heads_in = mixed.shape
    width = back.shape[0]
    model = hidden.shape[2]
    low = jnp.bfloat16
    anywhere = pl.BlockSpec(memory_space=pl.ANY)
    inside = pl.BlockSpec(memory_space=pltpu.VMEM)
    return pl.pallas_call(
        weights_kernel,
        out_shape=(
            jax.ShapeDtypeStruct((micro, tok, 2 * heads_in), low),
            jax.ShapeDtypeStruct((width, model // width, 3 * heads_in), low),
            jax.ShapeDtypeStruct((2, HD), jnp.float32),
        ),
        in_specs=[anywhere] * 5 + [inside] * 3,
        out_specs=[anywhere, anywhere, inside],
        scratch_shapes=[
            pltpu.VMEM(back.shape, low),
            pltpu.VMEM(raw.shape, jnp.float32),
            pltpu.VMEM(hidden.shape, low),
            pltpu.VMEM(mixed.shape, low),
            pltpu.VMEM(middle_low.shape, low),
            pltpu.VMEM((micro, tok, 2 * heads_in), low),
            pltpu.VMEM((width, model // width, 3 * heads_in), low),
            pltpu.SemaphoreType.DMA((4,)),
            pltpu.SemaphoreType.DMA((micro,)),
            pltpu.SemaphoreType.DMA((width,)),
            pltpu.SemaphoreType.DMA((width,)),
            pltpu.SemaphoreType.DMA((width,)),
        ],
        compiler_params=pltpu.CompilerParams(
            collective_id=3, has_side_effects=True, vmem_limit_bytes=48 << 20
        ),
        cost_estimate=pl.CostEstimate(
            flops=1_000_000_000, bytes_accessed=1_000_000, transcendentals=0
        ),
        name="weight_gradients",
    )(back, raw, hidden, mixed, middle_low, cosine, sine, head_gains)


def relay_scratch(count, model):
    return [
        pltpu.VMEM((count, SUB, model), jnp.bfloat16),
        pltpu.VMEM((count, SUB, model), jnp.bfloat16),
        pltpu.VMEM((RING, SUB, model), jnp.bfloat16),
        pltpu.SemaphoreType.DMA((count,)),
        pltpu.SemaphoreType.DMA((count,)),
        pltpu.SemaphoreType.DMA((count,)),
        pltpu.SemaphoreType.DMA((RING,)),
    ]


def feed_kernel(
    mixed_ref,
    input_ref,
    grad_ref,
    gain_ref,
    pack_ref,
    hidden_out,
    active_out,
    gate_out,
    upper_out,
    output_out,
    middle_out,
    low_out,
    mixed_out,
    gain_out,
    weight_out,
    heads_out,
    own,
    landed,
    cross,
    out_sem,
    land_sem,
    back_sem,
    cross_sem,
    out_v,
    gate_v,
    up_v,
    down_v,
    mixed_v,
    rows_v,
    grads_v,
    hidden_v,
    stage_v,
    scale_v,
    middle_v,
    output_v,
    mixback_v,
    weight_sem,
    attn_sem,
    load_sem,
    hidden_sem,
    stage_sem,
    final_sem,
    reload_sem,
    tile_sem,
    ahead_sems,
    behind_sems,
    heads_sem,
):
    micro, tok, model = input_ref.shape
    width, _, piece = pack_ref.shape
    heads_in = out_v.shape[0]
    groups = width // micro
    per = tok // SUB
    hid = gate_v.shape[1]
    count = micro * tok
    blocks = hid // piece
    relay = Relay(3 * micro * per, own, landed, cross, (out_sem, land_sem, back_sem, cross_sem))
    n_up = hid // LANES
    n_down = model // LANES
    slots = n_up + n_down

    ahead = Exchange(
        lambda target: mixed_ref.at[target],
        lambda source: mixed_v.at[
            source // groups, :, pl.ds(pl.multiple_of((source % groups) * 2 * HD, 2 * HD), 2 * HD)
        ],
        ahead_sems.at[0],
        ahead_sems.at[1],
    )
    behind = Exchange(
        lambda target: mixback_v.at[
            target // groups % 2,
            :,
            pl.ds(pl.multiple_of((target % groups) * 2 * HD, 2 * HD), 2 * HD),
        ],
        lambda source: mixed_out.at[source],
        behind_sems.at[0],
        behind_sems.at[1],
    )
    attn_copies = [
        pltpu.make_async_copy(
            pack_ref.at[i, pl.ds(0, heads_in)],
            out_v.at[:, pl.ds(i * piece, piece)],
            attn_sem.at[i],
        )
        for i in range(width)
    ]
    weight_copies = [
        pltpu.make_async_copy(
            pack_ref.at[i, pl.ds(heads_in + (1 + q) * hid + j * piece, piece)],
            target.at[pl.ds(i * piece, piece), pl.ds(j * piece, piece)],
            weight_sem.at[1 + q, i, j],
        )
        for q, target in enumerate((gate_v, up_v))
        for i in range(width)
        for j in range(blocks)
    ] + [
        pltpu.make_async_copy(
            pack_ref.at[i, pl.ds(heads_in, hid)],
            down_v.at[:, pl.ds(i * piece, piece)],
            weight_sem.at[0, i, 0],
        )
        for i in range(width)
    ]
    for copy in attn_copies + weight_copies:
        copy.start()

    def loads(n):
        slot = n % 2
        return (
            pltpu.make_async_copy(input_ref.at[n % micro], rows_v.at[slot], load_sem.at[slot, 0]),
            pltpu.make_async_copy(grad_ref.at[n % micro], grads_v.at[slot], load_sem.at[slot, 1]),
        )

    def start_loads(n):
        for copy in loads(n):
            copy.start()

    def wait_loads(n):
        for copy in loads(n):
            copy.wait()

    start_loads(0)
    gain_out[...] = jnp.zeros_like(gain_out)
    relay.greet(wide_peers(width))
    spot = lax.axis_index("wide")
    for step in range(width):
        ahead.send(lax.rem(spot + step, width))
    for copy in attn_copies:
        copy.wait()

    def heads_copy(m):
        return pltpu.make_async_copy(mixed_v.at[m], heads_out.at[m], heads_sem.at[m])

    @pl.loop(0, micro)
    def _(m):
        for g in range(groups):
            ahead.wait(m * groups + g)
        heads_copy(m).start()
        for n in range(n_down):
            cols = pl.ds(n * LANES, LANES)
            part = dot_f32(mixed_v[m], out_v[:, cols]).astype(jnp.bfloat16)
            for r in range(per):
                own[m * per + r, :, cols] = part[r * SUB : (r + 1) * SUB]
        relay.send(m * per, per)

    first_ticks = per + 4

    @pl.loop(0, first_ticks)
    def _(k):
        relay.tick(k)

    for copy in weight_copies:
        copy.wait()

    def hidden_copy(m):
        return pltpu.make_async_copy(hidden_v, hidden_out.at[m], hidden_sem)

    def stage_copies(m):
        return [
            pltpu.make_async_copy(stage_v.at[i], target.at[m], stage_sem.at[i])
            for i, target in enumerate((active_out, gate_out, upper_out))
        ]

    base = micro * per

    @pl.loop(0, micro)
    def _(m):
        slot = m % 2
        wait_loads(m)
        start_loads(m + 1)

        @pl.when(m > 0)
        def _():
            hidden_copy(m - 1).wait()
            for copy in stage_copies(m - 1):
                copy.wait()

        for r in range(per):
            span = pl.ds(r * SUB, SUB)
            middle = rows_v[slot, span, :].astype(jnp.float32) + landed[m * per + r].astype(
                jnp.float32
            )
            scale = lax.rsqrt(jnp.mean(middle * middle, axis=-1, keepdims=True) + EPSILON)
            scale_v[span, :] = scale
            hidden_v[span, :] = (middle * scale * gain_ref[...]).astype(jnp.bfloat16)
        hidden_copy(m).start()
        for j in range(n_up):
            relay.tick(first_ticks + slots * m + j)
            cols = pl.ds(j * LANES, LANES)
            gate = dot_f32(hidden_v[...], gate_v[:, cols])
            up_proj = dot_f32(hidden_v[...], up_v[:, cols])
            grad_active = dot_f32(grads_v[slot], down_v[cols, :], NT)
            squash = 1.0 / (1.0 + jnp.exp(-gate))
            silu = gate * squash
            stage_v[0, :, cols] = (silu * up_proj).astype(jnp.bfloat16)
            stage_v[1, :, cols] = (
                grad_active * up_proj * (squash * (1.0 + gate * (1.0 - squash)))
            ).astype(jnp.bfloat16)
            stage_v[2, :, cols] = (grad_active * silu).astype(jnp.bfloat16)
        for copy in stage_copies(m):
            copy.start()
        for n in range(n_down):
            relay.tick(first_ticks + slots * m + n_up + n)
            cols = pl.ds(n * LANES, LANES)
            back = dot_f32(stage_v[1], gate_v[cols, :], NT) + dot_f32(
                stage_v[2], up_v[cols, :], NT
            )
            ahead = dot_f32(stage_v[0], down_v[:, cols]).astype(jnp.bfloat16)
            gain_sum = jnp.zeros((1, LANES), jnp.float32)
            for r in range(per):
                part = slice(r * SUB, (r + 1) * SUB)
                own[base + 2 * per * m + r, :, cols] = back[part].astype(jnp.bfloat16)
                own[base + 2 * per * m + per + r, :, cols] = ahead[part]
                unit = (
                    rows_v[slot, pl.ds(r * SUB, SUB), cols].astype(jnp.float32)
                    + landed[m * per + r, :, cols].astype(jnp.float32)
                ) * scale_v[pl.ds(r * SUB, SUB), :]
                gain_sum += jnp.sum(back[part] * unit, axis=0, keepdims=True)
            gain_out[:, cols] += gain_sum
        relay.send(base + 2 * per * m, 2 * per)

    hidden_copy(micro - 1).wait()
    for copy in stage_copies(micro - 1):
        copy.wait()

    @pl.loop(0, base)
    def _(k):
        relay.to_inner(k).wait_send()

    def reloads(m):
        rows = pl.ds(m * tok, tok)
        return [
            pltpu.make_async_copy(hidden_out.at[m], down_v.at[rows], reload_sem.at[m, 0]),
            pltpu.make_async_copy(gate_out.at[m], gate_v.at[rows], reload_sem.at[m, 1]),
            pltpu.make_async_copy(
                upper_out.at[m], gate_v.at[pl.ds(count + m * tok, tok)], reload_sem.at[m, 2]
            ),
            pltpu.make_async_copy(active_out.at[m], up_v.at[rows], reload_sem.at[m, 3]),
        ] + [
            pltpu.make_async_copy(
                grad_ref.at[m, pl.ds(r * SUB, SUB)], own.at[m * per + r], reload_sem.at[m, 4 + r]
            )
            for r in range(per)
        ]

    for m in range(micro):
        for copy in reloads(m):
            copy.start()

    def tile_copy(i, q):
        return pltpu.make_async_copy(stage_v.at[q], weight_out.at[i, q], tile_sem.at[q])

    def tile(i, q):
        cols = pl.ds(pl.multiple_of(i * piece, piece), piece)

        @pl.when(i > 0)
        def _():
            tile_copy(i - 1, q).wait()

        if q == 2:
            right = own[0:base, :, cols].reshape(count, piece)
            for j in range(blocks):
                span = slice(j * piece, (j + 1) * piece)
                stage_v[q, :, span] = dot_f32(up_v[0:count, span], right, TN).astype(jnp.bfloat16)
        else:
            right = (gate_v[0:count], gate_v[count : 2 * count])[q]
            stage_v[q] = dot_f32(down_v[0:count, cols], right, TN).astype(jnp.bfloat16)
        tile_copy(i, q).start()

    def final_copies(m):
        return [
            pltpu.make_async_copy(middle_v, middle_out.at[m], final_sem.at[0]),
            pltpu.make_async_copy(hidden_v, low_out.at[m], final_sem.at[1]),
            pltpu.make_async_copy(output_v, output_out.at[m], final_sem.at[2]),
        ]

    last_ticks = first_ticks + slots * micro
    rest = 3 * micro * per + 4 - last_ticks
    turns = rest // micro

    @pl.loop(0, micro)
    def _(m):
        slot = m % 2
        wait_loads(m + micro)

        @pl.when(m < micro - 1)
        def _():
            start_loads(m + micro + 1)

        @pl.when(m > 0)
        def _():
            for copy in final_copies(m - 1):
                copy.wait()

        @pl.when(m == 0)
        def _():
            for i in range(micro):
                for copy in reloads(i):
                    copy.wait()

        relay.tick(last_ticks + turns * m)
        tile(2 * m, 0)
        tile(2 * m, 1)
        relay.tick(last_ticks + turns * m + 1)
        for r in range(per):
            span = pl.ds(r * SUB, SUB)
            middle = rows_v[slot, span, :].astype(jnp.float32) + landed[m * per + r].astype(
                jnp.float32
            )
            scale = lax.rsqrt(jnp.mean(middle * middle, axis=-1, keepdims=True) + EPSILON)
            pulled = landed[base + 2 * per * m + r].astype(jnp.float32) * gain_ref[...]
            along = jnp.mean(pulled * middle, axis=-1, keepdims=True)
            grad_middle = grads_v[slot, span, :].astype(jnp.float32) + scale * (
                pulled - middle * (scale * scale * along)
            )
            middle_v[span, :] = grad_middle
            hidden_v[span, :] = grad_middle.astype(jnp.bfloat16)
        @pl.when(m >= 2)
        def _():
            for g in range(groups):
                behind.sent((m - 2) * groups + g, home=True)

        mixback_v[m % 2] = dot_f32(hidden_v[...], out_v[...], NT).astype(jnp.bfloat16)
        for g in range(groups):
            behind.send(m * groups + g)
        tile(2 * m, 2)
        relay.tick(last_ticks + turns * m + 2)
        tile(2 * m + 1, 0)
        tile(2 * m + 1, 1)
        relay.tick(last_ticks + turns * m + 3)
        tile(2 * m + 1, 2)
        for r in range(per):
            span = pl.ds(r * SUB, SUB)
            output_v[span, :] = (
                rows_v[slot, span, :].astype(jnp.float32)
                + landed[m * per + r].astype(jnp.float32)
                + landed[base + 2 * per * m + per + r].astype(jnp.float32)
            ).astype(jnp.bfloat16)
        for copy in final_copies(m):
            copy.start()

    for copy in final_copies(micro - 1) + [tile_copy(width - 1, q) for q in range(3)]:
        copy.wait()
    for m in range(micro):
        heads_copy(m).wait()

    @pl.loop(0, width)
    def _(d):
        ahead.sent(d)
        behind.wait(d, home=False)

    @pl.loop((micro - 2) * groups, width)
    def _(d):
        behind.sent(d, home=True)

    relay.drain(base)


def feed_forward(mixed, layer_input, grad_out, gain_ffn, pack, heads_in, hid):
    micro, tok, model = layer_input.shape
    width, _, piece = pack.shape
    groups = width // micro
    low = jnp.bfloat16
    count = 3 * micro * (tok // SUB)
    anywhere = pl.BlockSpec(memory_space=pl.ANY)
    inside = pl.BlockSpec(memory_space=pltpu.VMEM)
    return pl.pallas_call(
        feed_kernel,
        out_shape=(
            jax.ShapeDtypeStruct((micro, tok, model), low),
            jax.ShapeDtypeStruct((micro, tok, hid), low),
            jax.ShapeDtypeStruct((micro, tok, hid), low),
            jax.ShapeDtypeStruct((micro, tok, hid), low),
            jax.ShapeDtypeStruct((micro, tok, model), low),
            jax.ShapeDtypeStruct((micro, tok, model), jnp.float32),
            jax.ShapeDtypeStruct((micro, tok, model), low),
            jax.ShapeDtypeStruct((width, tok, 2 * HD), low),
            jax.ShapeDtypeStruct((1, model), jnp.float32),
            jax.ShapeDtypeStruct((width, 3, piece, hid), low),
            jax.ShapeDtypeStruct((micro, tok, heads_in), low),
        ),
        in_specs=[anywhere] * 3 + [inside, anywhere],
        out_specs=[anywhere] * 8 + [inside, anywhere, anywhere],
        scratch_shapes=relay_scratch(count, model)
        + [
            pltpu.VMEM((heads_in, model), low),
            pltpu.VMEM((model, hid), low),
            pltpu.VMEM((model, hid), low),
            pltpu.VMEM((hid, model), low),
            pltpu.VMEM((micro, tok, heads_in), low),
            pltpu.VMEM((2, tok, model), low),
            pltpu.VMEM((2, tok, model), low),
            pltpu.VMEM((tok, model), low),
            pltpu.VMEM((3, tok, hid), low),
            pltpu.VMEM((tok, 1), jnp.float32),
            pltpu.VMEM((tok, model), jnp.float32),
            pltpu.VMEM((tok, model), low),
            pltpu.VMEM((2, tok, heads_in), low),
            pltpu.SemaphoreType.DMA((3, width, hid // piece)),
            pltpu.SemaphoreType.DMA((width,)),
            pltpu.SemaphoreType.DMA((2, 2)),
            pltpu.SemaphoreType.DMA,
            pltpu.SemaphoreType.DMA((3,)),
            pltpu.SemaphoreType.DMA((3,)),
            pltpu.SemaphoreType.DMA((micro, 4 + tok // SUB)),
            pltpu.SemaphoreType.DMA((3,)),
            pltpu.SemaphoreType.DMA((2, width)),
            pltpu.SemaphoreType.DMA((2, width)),
            pltpu.SemaphoreType.DMA((micro,)),
        ],
        compiler_params=pltpu.CompilerParams(
            collective_id=0, has_side_effects=True, vmem_limit_bytes=67043328
        ),
        cost_estimate=pl.CostEstimate(
            flops=240_000_000_000, bytes_accessed=900_000_000, transcendentals=0
        ),
        name="feed_forward",
    )(mixed, layer_input, grad_out, gain_ffn[None, :], pack)


def input_kernel(
    back_ref,
    input_ref,
    middle_ref,
    gain_ref,
    weight_ref,
    gain_two_ref,
    gain_heads_ref,
    output_out,
    gains_out,
    own,
    landed,
    cross,
    out_sem,
    land_sem,
    back_sem,
    cross_sem,
    weight_v,
    back_v,
    rows_v,
    middle_v,
    output_v,
    term_v,
    other_v,
    first_sem,
    load_sem,
    final_sem,
    term_sem,
    other_sem,
):
    micro, tok, model = input_ref.shape
    per = tok // SUB
    spot = lax.axis_index("wide")
    flips = [spot + bit - 2 * bit * (spot // bit % 2) for bit in (1, 2, 4)]
    relay = Relay(micro * per, own, landed, cross, (out_sem, land_sem, back_sem, cross_sem))
    weight_copy = pltpu.make_async_copy(weight_ref, weight_v, first_sem.at[0])
    back_copy = pltpu.make_async_copy(back_ref, back_v, first_sem.at[1])
    weight_copy.start()
    back_copy.start()

    rows_copy = pltpu.make_async_copy(input_ref, rows_v, first_sem.at[2])
    rows_copy.start()

    def load(m):
        return pltpu.make_async_copy(middle_ref.at[m], middle_v.at[m % 2], load_sem.at[m % 2])

    def final_copy(m):
        return pltpu.make_async_copy(output_v.at[m % 2], output_out.at[m], final_sem.at[m % 2])

    def pass_on(step, where):
        return pltpu.make_async_remote_copy(
            src_ref=term_v.at[step],
            dst_ref=other_v.at[step],
            send_sem=term_sem.at[step],
            recv_sem=other_sem.at[step],
            device_id=where,
            device_id_type=MESH,
        )

    targets = [{"wide": flip} for flip in flips] + [
        {"narrow": spot} for spot in (relay.inner, relay.other, relay.outer)
    ]

    def gain_step(step):
        if step == 0:
            pass_on(0, targets[0]).start()
        if 1 <= step <= 3:
            pass_on(step - 1, targets[step - 1]).wait_recv()
            term_v[step] = term_v[step - 1] + other_v[step - 1]
        if step in (1, 2):
            pass_on(step, targets[step]).start()
        if step == 3:

            @pl.when(relay.is_end)
            def _():
                pass_on(3, targets[3]).start()

        if step in (4, 5):

            @pl.when(relay.is_mid)
            def _():
                pass_on(step - 1, targets[step - 1]).wait_recv()
                term_v[step] = term_v[step - 1] + other_v[step - 1]
                pass_on(step, targets[step]).start()

        if step == 6:

            @pl.when(relay.is_mid)
            def _():
                gains_out[...] = term_v[5]
                pass_on(4, targets[4]).wait_send()
                pass_on(5, targets[5]).wait_send()

            @pl.when(relay.is_end)
            def _():
                pass_on(5, targets[5]).wait_recv()
                gains_out[...] = other_v[5]
                pass_on(3, targets[3]).wait_send()

            for early in range(3):
                pass_on(early, targets[early]).wait_send()

    load(0).start()
    relay.greet(flips)
    term_v[0] = jnp.zeros(term_v.shape[1:], jnp.float32)
    weight_copy.wait()
    back_copy.wait()
    rows_copy.wait()

    @pl.loop(0, micro)
    def _(m):
        rows = rows_v[m].astype(jnp.float32)
        scale = lax.rsqrt(jnp.mean(rows * rows, axis=-1, keepdims=True) + EPSILON)
        for n in range(model // LANES):
            cols = pl.ds(n * LANES, LANES)
            part = dot_f32(back_v[m], weight_v[cols, :], NT)
            term_v[0, 0:1, cols] += jnp.sum(
                part * (rows_v[m, :, cols].astype(jnp.float32) * scale), axis=0, keepdims=True
            )
            part = part.astype(jnp.bfloat16)
            for r in range(per):
                own[m * per + r, :, cols] = part[r * SUB : (r + 1) * SUB]
        relay.send(m * per, per)

    term_v[0, 1:2, :] = gain_two_ref[...]
    term_v[0, 2:3, 0:HD] = gain_heads_ref[0:1, :]
    term_v[0, 2:3, HD : 2 * HD] = gain_heads_ref[1:2, :]
    for k in range(4):
        if k % 3 == 0:
            gain_step(k // 3)
        relay.tick(k)

    @pl.loop(0, micro)
    def _(m):
        slot = m % 2

        @pl.when(m < micro - 1)
        def _():
            load(m + 1).start()

        load(m).wait()

        @pl.when(m >= 2)
        def _():
            final_copy(m - 2).wait()

        for r in range(per):
            for turn in range(micro):
                if (4 + turn * per + r) % 3 == 0:

                    @pl.when(m == turn)
                    def _(step=(4 + turn * per + r) // 3):
                        gain_step(step)

            relay.tick(4 + m * per + r)
            span = pl.ds(r * SUB, SUB)
            rows = rows_v[m, span, :].astype(jnp.float32)
            scale = lax.rsqrt(jnp.mean(rows * rows, axis=-1, keepdims=True) + EPSILON)
            pulled = landed[m * per + r].astype(jnp.float32) * gain_ref[...]
            along = jnp.mean(pulled * rows, axis=-1, keepdims=True)
            output_v[slot, span, :] = middle_v[slot, span, :] + scale * (
                pulled - rows * (scale * scale * along)
            )
        final_copy(m).start()

    final_copy(micro - 2).wait()
    final_copy(micro - 1).wait()
    relay.drain(0)


def input_gradient(back, layer_input, grad_middle, gain_attn, weight, gain_two, gain_heads):
    micro, tok, model = layer_input.shape
    low = jnp.bfloat16
    count = micro * (tok // SUB)
    anywhere = pl.BlockSpec(memory_space=pl.ANY)
    inside = pl.BlockSpec(memory_space=pltpu.VMEM)
    return pl.pallas_call(
        input_kernel,
        out_shape=(
            jax.ShapeDtypeStruct((micro, tok, model), jnp.float32),
            jax.ShapeDtypeStruct((8, model), jnp.float32),
        ),
        in_specs=[anywhere] * 3 + [inside, anywhere, inside, inside],
        out_specs=[anywhere, inside],
        scratch_shapes=relay_scratch(count, model)
        + [
            pltpu.VMEM(weight.shape, low),
            pltpu.VMEM((micro, tok, weight.shape[1]), low),
            pltpu.VMEM((micro, tok, model), low),
            pltpu.VMEM((2, tok, model), jnp.float32),
            pltpu.VMEM((2, tok, model), jnp.float32),
            pltpu.VMEM((6, 8, model), jnp.float32),
            pltpu.VMEM((6, 8, model), jnp.float32),
            pltpu.SemaphoreType.DMA((3,)),
            pltpu.SemaphoreType.DMA((2,)),
            pltpu.SemaphoreType.DMA((2,)),
            pltpu.SemaphoreType.DMA((6,)),
            pltpu.SemaphoreType.DMA((6,)),
        ],
        compiler_params=pltpu.CompilerParams(
            collective_id=1, has_side_effects=True, vmem_limit_bytes=48 << 20
        ),
        cost_estimate=pl.CostEstimate(
            flops=1_000_000_000, bytes_accessed=1_000_000, transcendentals=0
        ),
        name="input_gradient",
    )(back, layer_input, grad_middle, gain_attn[None, :], weight, gain_two, gain_heads)


def widen_feed(rows_ref, gate_ref, up_ref, down_ref):
    piece = gate_ref.shape[0]
    gate_ref[...] = rows_ref[0:piece, :].astype(jnp.float32)
    up_ref[...] = rows_ref[piece : 2 * piece, :].astype(jnp.float32)
    for j in range(down_ref.shape[0] // piece):
        span = slice(j * piece, (j + 1) * piece)
        down_ref[span, :] = rows_ref[2 * piece :, span].astype(jnp.float32)


def widen_attn(rows_ref, query_ref, key_ref, value_ref, out_ref):
    piece = query_ref.shape[0]
    first = 0
    for target in (query_ref, key_ref, value_ref):
        target[...] = rows_ref[:, first : first + target.shape[1]].astype(jnp.float32)
        first += target.shape[1]
    for j in range(out_ref.shape[0] // piece):
        part = rows_ref[:, first + j * piece : first + (j + 1) * piece]
        out_ref[j * piece : (j + 1) * piece, :] = part.astype(jnp.float32)


def widen(kernel, rows, shapes):
    return pl.pallas_call(
        kernel,
        out_shape=tuple(jax.ShapeDtypeStruct(shape, jnp.float32) for shape in shapes),
        name=kernel.__name__,
    )(rows)


def local_batched(
    layer_input,
    grad_out,
    lengths,
    w_query,
    w_key,
    w_value,
    w_out,
    w_gate,
    w_up,
    w_down,
    gain_attn,
    gain_ffn,
    gain_query,
    gain_key,
):
    micro, tok_rows, model = layer_input.shape
    width = lax.axis_size("wide")
    groups = w_key.shape[1] // HD
    total = tok_rows * width
    count = micro * tok_rows
    me = lax.axis_index("wide")
    w_qkv = lax.all_gather(
        jnp.concatenate([w_query, w_key, w_value], axis=1), "wide", axis=0, tiled=True
    )
    hid = w_gate.shape[1]
    piece = w_out.shape[1]

    def stacked(weight):
        return jnp.moveaxis(weight.reshape(piece, -1, piece), 1, 0).reshape(-1, piece)

    pack = lax.all_gather(
        jnp.concatenate([w_out, w_down, stacked(w_gate), stacked(w_up)], axis=0), "wide", axis=0
    )

    starts, places = jax.vmap(lambda row: row_starts(row, total))(lengths)
    my_places = lax.dynamic_slice_in_dim(places, me * tok_rows, tok_rows, axis=1)
    cosine, sine = angles(my_places.reshape(count))
    sine = jnp.where(jnp.arange(HD) < HD // 2, -sine, sine)
    head_gains = jnp.stack([gain_query, gain_key])
    my_starts = lax.dynamic_index_in_dim(starts, me // groups, axis=0, keepdims=False)
    my_first = my_starts[::BLOCK] // BLOCK

    hidden_one, raw, packed = project(
        layer_input, gain_attn, w_qkv, cosine, sine, head_gains, width
    )
    packed = packed.reshape(total, 4 * HD)
    mixed, kept, log_total = attention_out(packed, my_starts, my_first)
    (
        _,
        _,
        _,
        _,
        output,
        grad_middle,
        middle_low,
        grad_mixed,
        gain_two,
        feed_grads,
        mixed_low,
    ) = feed_forward(
        mixed.reshape(width, tok_rows, 2 * HD),
        layer_input,
        grad_out,
        gain_ffn,
        pack,
        w_out.shape[0],
        hid,
    )
    feed_grads = lax.psum_scatter(
        feed_grads.reshape(width * 3 * piece, hid), "wide", scatter_dimension=0, tiled=True
    )
    back = attention_back(
        packed, my_starts, my_first, grad_mixed.reshape(total, 2 * HD), kept, log_total
    )
    qkv_back, attn_grads, gain_heads = weight_gradients(
        back.reshape(width, tok_rows, 4 * HD),
        raw,
        hidden_one,
        mixed_low,
        middle_low,
        cosine,
        sine,
        head_gains,
    )
    attn_grads = lax.psum_scatter(
        attn_grads.reshape(model, -1), "wide", scatter_dimension=0, tiled=True
    )
    grad_input, gains = input_gradient(
        qkv_back, layer_input, grad_middle, gain_attn, w_qkv, gain_two, gain_heads
    )

    grad_gate, grad_up, grad_down = widen(
        widen_feed, feed_grads, (w_gate.shape, w_up.shape, w_down.shape)
    )
    grad_gate, attn_grads = lax.optimization_barrier((grad_gate, attn_grads))
    grad_query, grad_key, grad_value, grad_wout = widen(
        widen_attn, attn_grads, (w_query.shape, w_key.shape, w_value.shape, w_out.shape)
    )
    return (
        output,
        grad_input,
        grad_query,
        grad_key,
        grad_value,
        grad_wout,
        grad_gate,
        grad_up,
        grad_down,
        gains[0],
        gains[1],
        gains[2, :HD],
        gains[2, HD : 2 * HD],
    )


def local(mesh, layer_input, grad_out, lengths, w_query, w_key, *rest):
    width = mesh.shape["wide"]
    micro, tok_rows = layer_input.shape[:2]
    groups = w_key.shape[1] // HD
    fits = (
        micro * groups == width
        and w_query.shape[1] == 2 * w_key.shape[1]
        and mesh.shape["narrow"] == 4
        and tok_rows == BLOCK
    )
    chosen = local_batched if fits else local_general
    return chosen(layer_input, grad_out, lengths, w_query, w_key, *rest)


def solution(mesh):
    in_specs = (
        P(None, "wide", None),
        P(None, "wide", None),
        P(),
        P("wide", "narrow"),
        P("wide", "narrow"),
        P("wide", "narrow"),
        P("narrow", "wide"),
        P("wide", "narrow"),
        P("wide", "narrow"),
        P("narrow", "wide"),
        P(),
        P(),
        P(),
        P(),
    )
    out_specs = (
        P(None, "wide", None),
        P(None, "wide", None),
        P("wide", "narrow"),
        P("wide", "narrow"),
        P("wide", "narrow"),
        P("narrow", "wide"),
        P("wide", "narrow"),
        P("wide", "narrow"),
        P("narrow", "wide"),
        P(),
        P(),
        P(),
        P(),
    )
    return jax.shard_map(
        functools.partial(local, mesh), mesh=mesh, in_specs=in_specs, out_specs=out_specs, check_vma=False)
```

```python
import functools
import math

import jax
import jax.numpy as jnp
from jax import lax
from jax.experimental import pallas as pl
from jax.experimental.pallas import tpu as pltpu
from jax.sharding import PartitionSpec as P

HD = 128
NDOC = 8


EPSILON = 1e-06
THETA = 1000000.0


def rms_norm(values, gain):
    return values * lax.rsqrt(jnp.mean(values * values, axis=-1, keepdims=True) + EPSILON) * gain


def unit_rows(values):
    return values * lax.rsqrt(jnp.mean(values * values, axis=-1, keepdims=True) + EPSILON)


def rotate(values, cosine, sine):
    midway = values.shape[-1] // 2
    turned = jnp.concatenate([-values[..., midway:], values[..., :midway]], axis=-1)
    return values * cosine + turned * sine


def layout(lengths_row, total):
    finish = jnp.cumsum(lengths_row)
    starts = finish - lengths_row
    places = jnp.arange(total, dtype=jnp.int32)
    segment = jnp.sum((places[:, None] >= finish[None, :]).astype(jnp.int32), axis=1)
    member = segment[:, None] == jnp.arange(finish.shape[0], dtype=jnp.int32)[None, :]
    opening = jnp.sum(jnp.where(member, starts[None, :], 0), axis=1)
    return (segment, places - opening)


def angles(place):
    frequency = jnp.exp(-math.log(THETA) * jnp.arange(0, HD, 2).astype(jnp.float32) / HD)
    turning = place.astype(jnp.float32)[:, None] * frequency[None, :]
    turning = jnp.concatenate([turning, turning], axis=-1)
    return (jnp.cos(turning), jnp.sin(turning))


def allowed(query_seg, query_idx, key_seg, key_idx):
    same_doc = query_seg[:, None] == key_seg[None, :]
    causal = key_idx[None, :] <= query_idx[:, None]
    usable = (key_seg[None, :] != NDOC - 1) | (key_idx[None, :] == query_idx[:, None])
    return same_doc & causal & usable


def attention_scores(query_low, key_all, mask_local, factor):
    scores = (
        jnp.einsum("tgrd,kgd->grtk", query_low, key_all, preferred_element_type=jnp.float32)
        * factor
    )
    return jnp.where(mask_local[None, None], scores, -1e30)


def one_batch(row_input, grad_row, lengths_row, gathered, gains):
    w_query, w_key, w_value, w_out, w_gate, w_up, w_down = gathered
    gain_attn, gain_ffn, gain_query, gain_key = gains
    tok_rows = row_input.shape[0]
    total = tok_rows * lax.axis_size("wide")
    groups = w_key.shape[1] // HD
    repeat = w_query.shape[1] // w_key.shape[1]
    factor = 1.0 / math.sqrt(HD)
    first_row = lax.axis_index("wide") * tok_rows
    segment, place = layout(lengths_row, total)
    positions = jnp.arange(total, dtype=jnp.int32)
    query_seg = lax.dynamic_slice_in_dim(segment, first_row, tok_rows)
    query_idx = lax.dynamic_slice_in_dim(positions, first_row, tok_rows)
    mask_local = allowed(query_seg, query_idx, segment, positions)
    cosine, sine = angles(lax.dynamic_slice_in_dim(place, first_row, tok_rows))

    def head_norm(rows, gain):
        return rotate(rms_norm(rows, gain), cosine[:, None, :], sine[:, None, :])

    input_float = row_input.astype(jnp.float32)
    grad_float = grad_row.astype(jnp.float32)
    normed_one, pull_one = jax.vjp(lambda rows: rms_norm(rows, gain_attn), input_float)
    hidden_one = normed_one.astype(jnp.bfloat16)
    query_raw = jnp.dot(hidden_one, w_query, preferred_element_type=jnp.float32).reshape(
        tok_rows, groups * repeat, HD
    )
    key_raw = jnp.dot(hidden_one, w_key, preferred_element_type=jnp.float32).reshape(
        tok_rows, groups, HD
    )
    value_low = jnp.dot(hidden_one, w_value, preferred_element_type=jnp.float32).astype(
        jnp.bfloat16
    )
    query_turned, pull_query = jax.vjp(head_norm, query_raw, gain_query)
    key_turned, pull_key = jax.vjp(head_norm, key_raw, gain_key)
    query_low = query_turned.astype(jnp.bfloat16).reshape(tok_rows, groups, repeat, HD)
    key_low = key_turned.astype(jnp.bfloat16).reshape(tok_rows, groups * HD)
    key_all, value_all = (
        lax.all_gather(key_low, "wide", axis=0, tiled=True),
        lax.all_gather(value_low, "wide", axis=0, tiled=True),
    )
    key_all = key_all.reshape(total, groups, HD)
    value_all = value_all.reshape(total, groups, HD)
    scores = attention_scores(query_low, key_all, mask_local, factor)
    highest = jnp.max(scores, axis=-1, keepdims=True)
    exponent = jnp.exp(scores - highest)
    denominator = jnp.sum(exponent, axis=-1, keepdims=True)
    log_total = highest + jnp.log(denominator)
    probs_low = (exponent / denominator).astype(jnp.bfloat16)
    mixed = jnp.einsum("grtk,kgd->tgrd", probs_low, value_all, preferred_element_type=jnp.float32)
    mixed_low = mixed.reshape(tok_rows, groups * repeat * HD).astype(jnp.bfloat16)
    attn_part = jnp.dot(mixed_low, w_out, preferred_element_type=jnp.float32)
    middle = input_float + lax.psum(attn_part.astype(jnp.bfloat16), "narrow").astype(jnp.float32)
    normed_two, pull_two = jax.vjp(lambda rows: rms_norm(rows, gain_ffn), middle)
    hidden_two = normed_two.astype(jnp.bfloat16)
    unit_two = unit_rows(middle)
    gate = jnp.dot(hidden_two, w_gate, preferred_element_type=jnp.float32)
    up_proj = jnp.dot(hidden_two, w_up, preferred_element_type=jnp.float32)
    active, pull_active = jax.vjp(
        lambda gate_in, up_in: jax.nn.silu(gate_in) * up_in, gate, up_proj
    )
    active_low = active.astype(jnp.bfloat16)
    ffn_part = jnp.dot(active_low, w_down, preferred_element_type=jnp.float32)
    output_low = (
        middle + lax.psum(ffn_part.astype(jnp.bfloat16), "narrow").astype(jnp.float32)
    ).astype(jnp.bfloat16)
    grad_wdown = jnp.einsum("tf,td->fd", active_low, grad_row, preferred_element_type=jnp.float32)
    grad_active = jnp.einsum("td,fd->tf", grad_row, w_down, preferred_element_type=jnp.float32)
    grad_gate, grad_upper = pull_active(grad_active)
    gate_back = grad_gate.astype(jnp.bfloat16)
    upper_back = grad_upper.astype(jnp.bfloat16)
    grad_wgate = jnp.einsum("td,tf->df", hidden_two, gate_back, preferred_element_type=jnp.float32)
    grad_wup = jnp.einsum("td,tf->df", hidden_two, upper_back, preferred_element_type=jnp.float32)
    partial_two = jnp.einsum(
        "tf,df->td", gate_back, w_gate, preferred_element_type=jnp.float32
    ) + jnp.einsum("tf,df->td", upper_back, w_up, preferred_element_type=jnp.float32)
    gain_two = jnp.sum(partial_two * unit_two, axis=0)
    grad_middle = (
        grad_float
        + pull_two(lax.psum(partial_two.astype(jnp.bfloat16), "narrow").astype(jnp.float32))[0]
    )
    middle_low = grad_middle.astype(jnp.bfloat16)
    grad_wout = jnp.einsum("th,td->hd", mixed_low, middle_low, preferred_element_type=jnp.float32)
    grad_mixed = jnp.einsum("td,hd->th", middle_low, w_out, preferred_element_type=jnp.float32)
    grad_mixed = grad_mixed.astype(jnp.bfloat16).reshape(tok_rows, groups, repeat, HD)
    scores = attention_scores(query_low, key_all, mask_local, factor)
    probs = jnp.exp(scores - log_total)
    grad_probs = jnp.einsum(
        "tgrd,kgd->grtk", grad_mixed, value_all, preferred_element_type=jnp.float32
    )
    weighted = jnp.sum(probs * grad_probs, axis=-1, keepdims=True)
    grad_scores = (probs * (grad_probs - weighted)).astype(jnp.bfloat16)
    grad_turned = (
        jnp.einsum("grtk,kgd->tgrd", grad_scores, key_all, preferred_element_type=jnp.float32)
        * factor
    )
    grad_keyall = (
        jnp.einsum("grtk,tgrd->kgd", grad_scores, query_low, preferred_element_type=jnp.float32)
        * factor
    )
    grad_valueall = jnp.einsum(
        "grtk,tgrd->kgd", probs.astype(jnp.bfloat16), grad_mixed, preferred_element_type=jnp.float32
    )
    grad_keys, grad_values = (
        lax.psum_scatter(
            grad_keyall.reshape(total, groups * HD).astype(jnp.bfloat16),
            "wide",
            scatter_dimension=0,
            tiled=True,
        ).astype(jnp.float32),
        lax.psum_scatter(
            grad_valueall.reshape(total, groups * HD).astype(jnp.bfloat16),
            "wide",
            scatter_dimension=0,
            tiled=True,
        ).astype(jnp.float32),
    )
    grad_qraw, gain_q = pull_query(grad_turned.reshape(tok_rows, groups * repeat, HD))
    grad_kraw, gain_k = pull_key(grad_keys.reshape(tok_rows, groups, HD))
    query_back = grad_qraw.reshape(tok_rows, groups * repeat * HD).astype(jnp.bfloat16)
    key_back = grad_kraw.reshape(tok_rows, groups * HD).astype(jnp.bfloat16)
    value_back = grad_values.astype(jnp.bfloat16)
    grad_wquery = jnp.einsum(
        "td,th->dh", hidden_one, query_back, preferred_element_type=jnp.float32
    )
    grad_wkey = jnp.einsum("td,th->dh", hidden_one, key_back, preferred_element_type=jnp.float32)
    grad_wvalue = jnp.einsum(
        "td,th->dh", hidden_one, value_back, preferred_element_type=jnp.float32
    )
    partial_one = (
        jnp.einsum("th,dh->td", query_back, w_query, preferred_element_type=jnp.float32)
        + jnp.einsum("th,dh->td", key_back, w_key, preferred_element_type=jnp.float32)
        + jnp.einsum("th,dh->td", value_back, w_value, preferred_element_type=jnp.float32)
    )
    gain_one = jnp.sum(partial_one * unit_rows(input_float), axis=0)
    grad_input = (
        grad_middle
        + pull_one(lax.psum(partial_one.astype(jnp.bfloat16), "narrow").astype(jnp.float32))[0]
    )
    weight_grads = (
        grad_wquery,
        grad_wkey,
        grad_wvalue,
        grad_wout,
        grad_wgate,
        grad_wup,
        grad_wdown,
    )
    return (output_low, grad_input, weight_grads, (gain_one, gain_two, gain_q, gain_k))


def local_general(
    layer_input,
    grad_out,
    lengths,
    w_query,
    w_key,
    w_value,
    w_out,
    w_gate,
    w_up,
    w_down,
    gain_attn,
    gain_ffn,
    gain_query,
    gain_key,
):
    width = lax.axis_size("wide")
    shards = (w_query, w_key, w_value, w_out, w_gate, w_up, w_down)
    along_rows = (True, True, True, False, True, True, False)
    gains = (gain_attn, gain_ffn, gain_query, gain_key)
    totals = tuple(
        (
            jnp.zeros(
                (
                    (piece.shape[0] * width, piece.shape[1])
                    if rows_first
                    else (piece.shape[0], piece.shape[1] * width)
                ),
                jnp.float32,
            )
            for piece, rows_first in zip(shards, along_rows)
        )
    )
    gain_terms = tuple((jnp.zeros(gain.shape, jnp.float32) for gain in gains))
    outputs = []
    grad_inputs = []
    for micro in range(layer_input.shape[0]):
        gathered = (
            lax.all_gather(w_query, "wide", axis=0, tiled=True),
            lax.all_gather(w_key, "wide", axis=0, tiled=True),
            lax.all_gather(w_value, "wide", axis=0, tiled=True),
            lax.all_gather(w_out, "wide", axis=1, tiled=True),
            lax.all_gather(w_gate, "wide", axis=0, tiled=True),
            lax.all_gather(w_up, "wide", axis=0, tiled=True),
            lax.all_gather(w_down, "wide", axis=1, tiled=True),
        )
        output, grad_input, weight_grads, gain_grads = one_batch(
            layer_input[micro], grad_out[micro], lengths[micro], gathered, gains
        )
        outputs.append(output)
        grad_inputs.append(grad_input)
        gain_terms = tuple((running + fresh for running, fresh in zip(gain_terms, gain_grads)))
        totals = tuple((running + fresh for running, fresh in zip(totals, weight_grads)))
    results = (
        lax.psum_scatter(
            totals[0].astype(jnp.bfloat16), "wide", scatter_dimension=0, tiled=True
        ).astype(jnp.float32),
        lax.psum_scatter(
            totals[1].astype(jnp.bfloat16), "wide", scatter_dimension=0, tiled=True
        ).astype(jnp.float32),
        lax.psum_scatter(
            totals[2].astype(jnp.bfloat16), "wide", scatter_dimension=0, tiled=True
        ).astype(jnp.float32),
        lax.psum_scatter(
            totals[3].astype(jnp.bfloat16), "wide", scatter_dimension=1, tiled=True
        ).astype(jnp.float32),
        lax.psum_scatter(
            totals[4].astype(jnp.bfloat16), "wide", scatter_dimension=0, tiled=True
        ).astype(jnp.float32),
        lax.psum_scatter(
            totals[5].astype(jnp.bfloat16), "wide", scatter_dimension=0, tiled=True
        ).astype(jnp.float32),
        lax.psum_scatter(
            totals[6].astype(jnp.bfloat16), "wide", scatter_dimension=1, tiled=True
        ).astype(jnp.float32),
    )
    gain_total = lax.psum(gain_terms, ("wide", "narrow"))
    return (
        jnp.stack(outputs),
        jnp.stack(grad_inputs),
        results[0],
        results[1],
        results[2],
        results[3],
        results[4],
        results[5],
        results[6],
        gain_total[0],
        gain_total[1],
        gain_total[2],
        gain_total[3],
    )


BLOCK = 256
NT = (((1,), (1,)), ((), ()))
TN = (((0,), (0,)), ((), ()))


def attend_forward(first_ref, qkv_ref, start_ref, mixed_ref, kept_ref, log_ref):
    step_q = pl.program_id(0)
    rows = pl.ds(step_q * BLOCK, BLOCK)
    factor = 1.0 / math.sqrt(HD)
    query = jnp.concatenate([qkv_ref[rows, 0:HD], qkv_ref[rows, HD : 2 * HD]], axis=0)
    start = start_ref[rows, :]
    start = jnp.concatenate([start, start], axis=0)
    spot = lax.broadcasted_iota(jnp.int32, (BLOCK, 1), 0) + step_q * BLOCK
    spot = jnp.concatenate([spot, spot], axis=0)

    def one(step_k, carry):
        highest, total, mixed = carry
        cols = pl.ds(step_k * BLOCK, BLOCK)
        scores = lax.dot_general(
            query, qkv_ref[cols, 2 * HD : 3 * HD], NT, preferred_element_type=jnp.float32
        )
        key_spot = lax.broadcasted_iota(jnp.int32, (1, BLOCK), 1) + step_k * BLOCK
        fits = (key_spot >= start) & (key_spot <= spot)
        scores = jnp.where(fits, scores * factor, -1e30)
        fresh = jnp.maximum(highest, jnp.max(scores, axis=-1, keepdims=True))
        shrink = jnp.exp(highest - fresh)
        exponent = jnp.exp(scores - fresh)
        total = total * shrink + jnp.sum(exponent, axis=-1, keepdims=True)
        mixed = mixed * shrink + jnp.dot(
            exponent.astype(jnp.bfloat16),
            qkv_ref[cols, 3 * HD : 4 * HD],
            preferred_element_type=jnp.float32,
        )
        return (fresh, total, mixed)

    highest, total, mixed = lax.fori_loop(
        first_ref[step_q],
        step_q + 1,
        one,
        (
            jnp.full((2 * BLOCK, 1), -1e30, jnp.float32),
            jnp.zeros((2 * BLOCK, 1), jnp.float32),
            jnp.zeros((2 * BLOCK, HD), jnp.float32),
        ),
    )
    mixed = mixed / total
    mixed = jnp.concatenate([mixed[:BLOCK], mixed[BLOCK:]], axis=1)
    mixed_ref[...] = mixed.astype(jnp.bfloat16)
    kept_ref[...] = mixed
    log_total = highest + jnp.log(total)
    log_ref[...] = jnp.concatenate([log_total[:BLOCK], log_total[BLOCK:]], axis=1)


def attend_backward(
    first_ref, qkv_ref, start_ref, grad_ref, kept_ref, log_ref, back_ref, key_sum, value_sum
):
    step_q = pl.program_id(0)
    rows = pl.ds(step_q * BLOCK, BLOCK)
    factor = 1.0 / math.sqrt(HD)

    @pl.when(step_q == 0)
    def _():
        key_sum[...] = jnp.zeros_like(key_sum)
        value_sum[...] = jnp.zeros_like(value_sum)

    query = jnp.concatenate([qkv_ref[rows, 0:HD], qkv_ref[rows, HD : 2 * HD]], axis=0)
    grad = jnp.concatenate([grad_ref[:, 0:HD], grad_ref[:, HD : 2 * HD]], axis=0)
    kept = jnp.concatenate([kept_ref[:, 0:HD], kept_ref[:, HD : 2 * HD]], axis=0)
    log_total = jnp.concatenate([log_ref[:, 0:1], log_ref[:, 1:2]], axis=0)
    weighted = jnp.sum(grad.astype(jnp.float32) * kept, axis=-1, keepdims=True)
    start = start_ref[rows, :]
    start = jnp.concatenate([start, start], axis=0)
    spot = lax.broadcasted_iota(jnp.int32, (BLOCK, 1), 0) + step_q * BLOCK
    spot = jnp.concatenate([spot, spot], axis=0)

    def one(step_k, query_sum):
        cols = pl.ds(step_k * BLOCK, BLOCK)
        key = qkv_ref[cols, 2 * HD : 3 * HD]
        scores = lax.dot_general(query, key, NT, preferred_element_type=jnp.float32) * factor
        key_spot = lax.broadcasted_iota(jnp.int32, (1, BLOCK), 1) + step_k * BLOCK
        fits = (key_spot >= start) & (key_spot <= spot)
        probs = jnp.where(fits, jnp.exp(scores - log_total), 0.0)
        grad_probs = lax.dot_general(
            grad, qkv_ref[cols, 3 * HD : 4 * HD], NT, preferred_element_type=jnp.float32
        )
        grad_scores = (probs * (grad_probs - weighted)).astype(jnp.bfloat16)
        value_sum[cols, :] += lax.dot_general(
            probs.astype(jnp.bfloat16), grad, TN, preferred_element_type=jnp.float32
        )
        key_sum[cols, :] += lax.dot_general(
            grad_scores, query, TN, preferred_element_type=jnp.float32
        )
        return query_sum + jnp.dot(grad_scores, key, preferred_element_type=jnp.float32)

    query_sum = lax.fori_loop(
        first_ref[step_q], step_q + 1, one, jnp.zeros((2 * BLOCK, HD), jnp.float32)
    )
    query_sum = (query_sum * factor).astype(jnp.bfloat16)
    back_ref[rows, 0:HD] = query_sum[:BLOCK]
    back_ref[rows, HD : 2 * HD] = query_sum[BLOCK:]

    @pl.when(step_q == pl.num_programs(0) - 1)
    def _():
        back_ref[:, 2 * HD : 3 * HD] = (key_sum[...] * factor).astype(jnp.bfloat16)
        back_ref[:, 3 * HD : 4 * HD] = value_sum[...].astype(jnp.bfloat16)


def row_starts(lengths_row, total):
    segment, place = layout(lengths_row, total)
    positions = jnp.arange(total, dtype=jnp.int32)
    starts = jnp.where(segment == NDOC - 1, positions, positions - place)
    return (starts, place)


def attention_out(qkv, starts, first):
    total = qkv.shape[0]
    whole = lambda i, *_: (0, 0)
    return pl.pallas_call(
        attend_forward,
        out_shape=(
            jax.ShapeDtypeStruct((total, 2 * HD), jnp.bfloat16),
            jax.ShapeDtypeStruct((total, 2 * HD), jnp.float32),
            jax.ShapeDtypeStruct((total, 2), jnp.float32),
        ),
        grid_spec=pltpu.PrefetchScalarGridSpec(
            num_scalar_prefetch=1,
            grid=(total // BLOCK,),
            in_specs=[
                pl.BlockSpec((total, 4 * HD), whole),
                pl.BlockSpec((total, 1), whole),
            ],
            out_specs=[
                pl.BlockSpec((BLOCK, 2 * HD), lambda i, *_: (i, 0)),
                pl.BlockSpec((BLOCK, 2 * HD), lambda i, *_: (i, 0)),
                pl.BlockSpec((BLOCK, 2), lambda i, *_: (i, 0)),
            ],
        ),
        name="attend_forward",
    )(first, qkv, starts[:, None])


def attention_back(qkv, starts, first, grad, kept, log_total):
    total = qkv.shape[0]
    whole = lambda i, *_: (0, 0)
    block = lambda i, *_: (i, 0)
    return pl.pallas_call(
        attend_backward,
        out_shape=jax.ShapeDtypeStruct((total, 4 * HD), jnp.bfloat16),
        grid_spec=pltpu.PrefetchScalarGridSpec(
            num_scalar_prefetch=1,
            grid=(total // BLOCK,),
            in_specs=[
                pl.BlockSpec((total, 4 * HD), whole),
                pl.BlockSpec((total, 1), whole),
                pl.BlockSpec((BLOCK, 2 * HD), block),
                pl.BlockSpec((BLOCK, 2 * HD), block),
                pl.BlockSpec((BLOCK, 2), block),
            ],
            out_specs=pl.BlockSpec((total, 4 * HD), whole),
            scratch_shapes=[
                pltpu.VMEM((total, HD), jnp.float32),
                pltpu.VMEM((total, HD), jnp.float32),
            ],
        ),
        name="attend_backward",
    )(first, qkv, starts[:, None], grad, kept, log_total)


def dot_f32(left, right, dims=(((1,), (0,)), ((), ()))):
    return lax.dot_general(left, right, dims, preferred_element_type=jnp.float32)


SUB = 64
RING = 8
AHEAD = 3
GAIN_TICKS = (0, 2, 4, 6, 11, 14, 17)
LANES = 512
MESH = pl.DeviceIdType.MESH


class Relay:
    def __init__(self, count, own, landed, cross, sems):
        self.count, self.own, self.landed, self.cross = count, own, landed, cross
        self.out_sem, self.land_sem, self.back_sem, self.cross_sem = sems
        spot = lax.axis_index("narrow")
        self.is_end = (spot == 0) | (spot == 3)
        self.is_mid = (spot == 1) | (spot == 2)
        self.inner = 1 + spot // 3
        self.other = 3 - spot
        self.outer = jnp.where(spot == 2, 3, 0)

    def to_inner(self, k):
        return pltpu.make_async_remote_copy(
            src_ref=self.own.at[k],
            dst_ref=self.landed.at[k],
            send_sem=self.out_sem.at[k],
            recv_sem=self.land_sem.at[k],
            device_id={"narrow": self.inner},
            device_id_type=MESH,
        )

    def to_other(self, k):
        return pltpu.make_async_remote_copy(
            src_ref=self.own.at[k],
            dst_ref=self.cross.at[k % RING],
            send_sem=self.out_sem.at[k],
            recv_sem=self.cross_sem.at[k % RING],
            device_id={"narrow": self.other},
            device_id_type=MESH,
        )

    def to_outer(self, k):
        return pltpu.make_async_remote_copy(
            src_ref=self.landed.at[k],
            dst_ref=self.landed.at[k],
            send_sem=self.back_sem.at[k],
            recv_sem=self.land_sem.at[k],
            device_id={"narrow": self.outer},
            device_id_type=MESH,
        )

    def greet(self, peers):
        barrier = pltpu.get_barrier_semaphore()
        for peer in peers:
            pl.semaphore_signal(barrier, inc=1, device_id={"wide": peer}, device_id_type=MESH)

        @pl.when(self.is_end)
        def _():
            pl.semaphore_signal(
                barrier, inc=1, device_id={"narrow": self.inner}, device_id_type=MESH
            )
            pl.semaphore_wait(barrier, 1 + len(peers))

        @pl.when(self.is_mid)
        def _():
            pl.semaphore_signal(
                barrier, inc=1, device_id={"narrow": self.outer}, device_id_type=MESH
            )
            pl.semaphore_signal(
                barrier, inc=1, device_id={"narrow": self.other}, device_id_type=MESH
            )
            pl.semaphore_wait(barrier, 2 + len(peers))

    def send(self, first, number):
        @pl.when(self.is_end)
        def _():
            @pl.loop(0, number)
            def _(i):
                self.to_inner(first + i).start()

    def tick(self, k):
        @pl.when(self.is_mid & (k < self.count))
        def _():
            self.to_inner(k).wait_recv()
            self.own[k] = (
                self.own[k].astype(jnp.float32) + self.landed[k].astype(jnp.float32)
            ).astype(jnp.bfloat16)
            self.to_other(k).start()

        @pl.when(self.is_mid & (k >= 2) & (k < self.count + 2))
        def _():
            j = k - 2
            self.to_other(j).wait_recv()
            self.landed[j] = (
                self.own[j].astype(jnp.float32) + self.cross[j % RING].astype(jnp.float32)
            ).astype(jnp.bfloat16)
            self.to_outer(j).start()

        @pl.when(self.is_end & (k >= 4) & (k < self.count + 4))
        def _():
            self.to_outer(k - 4).wait_recv()

    def drain(self, first):
        @pl.loop(first, self.count)
        def _(k):
            self.to_inner(k).wait_send()

        @pl.loop(0, self.count)
        def _(k):
            @pl.when(self.is_mid)
            def _():
                self.to_outer(k).wait_send()


def wide_peers(width):
    spot = lax.axis_index("wide")
    return [lax.rem(spot + step, width) for step in range(1, width)]


def greet_wide(width):
    barrier = pltpu.get_barrier_semaphore()
    for peer in wide_peers(width):
        pl.semaphore_signal(barrier, inc=1, device_id={"wide": peer}, device_id_type=MESH)
    pl.semaphore_wait(barrier, width - 1)


class Exchange:
    def __init__(self, block, slot, send_sem, land_sem):
        self.block, self.slot = block, slot
        self.send_sem, self.land_sem = send_sem, land_sem
        self.spot = lax.axis_index("wide")

    def remote(self, target, source):
        return pltpu.make_async_remote_copy(
            src_ref=self.block(target),
            dst_ref=self.slot(source),
            send_sem=self.send_sem.at[target],
            recv_sem=self.land_sem.at[source],
            device_id={"wide": target},
            device_id_type=MESH,
        )

    def here(self):
        return pltpu.make_async_copy(
            self.block(self.spot), self.slot(self.spot), self.land_sem.at[self.spot]
        )

    def send(self, target):
        @pl.when(target == self.spot)
        def _():
            self.here().start()

        @pl.when(target != self.spot)
        def _():
            self.remote(target, self.spot).start()

    def sent(self, target, home=False):
        @pl.when(target != self.spot)
        def _():
            self.remote(target, self.spot).wait_send()

        if home:

            @pl.when(target == self.spot)
            def _():
                self.here().wait()

    def wait(self, source, home=True):
        if home:

            @pl.when(source == self.spot)
            def _():
                self.here().wait()

        @pl.when(source != self.spot)
        def _():
            self.remote(self.spot, source).wait_recv()


class Gather:
    def __init__(self, parts, send_sem, land_sem):
        self.parts, self.send_sem, self.land_sem = parts, send_sem, land_sem
        me = lax.axis_index("wide")
        flip = lambda spot, bit: spot + bit - 2 * bit * (spot // bit % 2)
        self.me, self.near = me, flip(me, 1)
        self.across, self.along = flip(me, 2), flip(me, 4)
        self.far = flip(self.across, 4)
        self.flip = flip

    def move(self, part, kind, source, target, device):
        return pltpu.make_async_remote_copy(
            src_ref=source,
            dst_ref=target,
            send_sem=self.send_sem.at[part, kind],
            recv_sem=self.land_sem.at[part, kind],
            device_id={"wide": device},
            device_id_type=MESH,
        )

    def going(self, part, kind):
        own, slot, half = self.parts[part]
        across, along, near = self.across, self.along, self.near
        source, target, device = (
            lambda: (own, slot(self.me), across),
            lambda: (own, slot(self.me), along),
            lambda: (own, slot(self.me), near),
            lambda: (half(along, 0), half(along, 0), across),
            lambda: (half(across, 1), half(across, 1), along),
            lambda: (slot(across), slot(across), near),
            lambda: (slot(along), slot(along), near),
            lambda: (half(self.far, 0), half(self.far, 0), near),
            lambda: (half(self.far, 1), half(self.far, 1), near),
        )[kind]()
        return self.move(part, kind, source, target, device)

    def coming(self, part, kind):
        _, slot, half = self.parts[part]
        flip = self.flip
        place = (
            lambda: slot(self.across),
            lambda: slot(self.along),
            lambda: slot(self.near),
            lambda: half(self.far, 0),
            lambda: half(self.far, 1),
            lambda: slot(flip(self.across, 1)),
            lambda: slot(flip(self.along, 1)),
            lambda: half(flip(self.far, 1), 0),
            lambda: half(flip(self.far, 1), 1),
        )[kind]()
        return self.move(part, kind, place, place, self.near)

    def here(self, part):
        own, slot, _ = self.parts[part]
        return pltpu.make_async_copy(own, slot(self.me), self.land_sem.at[part, 9])

    def first(self, part):
        for kind in (0, 1, 2):
            self.going(part, kind).start()
        self.here(part).start()

    def second(self, part):
        self.coming(part, 1).wait_recv()
        self.going(part, 3).start()
        self.coming(part, 0).wait_recv()
        self.going(part, 4).start()
        self.going(part, 6).start()
        self.going(part, 5).start()

    def third(self, part):
        self.coming(part, 3).wait_recv()
        self.going(part, 7).start()
        self.coming(part, 4).wait_recv()
        self.going(part, 8).start()

    def fourth(self, part):
        self.here(part).wait()
        for kind in (2, 5, 6, 7, 8):
            self.coming(part, kind).wait_recv()

    def drain(self):
        for part in range(len(self.parts)):
            for kind in range(9):
                self.going(part, kind).wait_send()


def project_kernel(
    input_ref,
    gain_ref,
    query_w,
    key_w,
    value_w,
    cosine_ref,
    sine_ref,
    head_gain_ref,
    hidden_out,
    raw_out,
    packed_out,
    weight_out,
    rows_v,
    weight_v,
    hidden_v,
    raw_v,
    pack_v,
    load_sem,
    keep_sem,
    hidden_sem,
    send_sem,
    land_sem,
    part_send,
    part_land,
):
    micro, tok, model = input_ref.shape
    width = packed_out.shape[0]
    groups = width // micro
    heads = 2 * groups
    spot = lax.axis_index("wide")
    swap = Exchange(
        lambda target: pack_v.at[target], lambda source: packed_out.at[source], send_sem, land_sem
    )
    load = pltpu.make_async_copy(input_ref, rows_v, load_sem.at[0])
    load.start()
    piece = query_w.shape[0]

    def part(own, first):
        cols = pl.ds(first, own.shape[1])
        return (
            own,
            lambda s: weight_v.at[pl.ds(pl.multiple_of(s * piece, piece), piece), cols],
            lambda s, h: weight_v.at[
                pl.ds(pl.multiple_of(s * piece + h * piece // 2, piece // 2), piece // 2), cols
            ],
        )

    q_cols, k_cols = query_w.shape[1], key_w.shape[1]
    gather = Gather(
        [part(query_w, 0), part(key_w, q_cols), part(value_w, q_cols + k_cols)],
        part_send,
        part_land,
    )
    greet_wide(width)
    for p in range(3):
        gather.first(p)
    load.wait()
    hidden_copy = pltpu.make_async_copy(hidden_v, hidden_out, hidden_sem)

    @pl.loop(0, micro)
    def _(m):
        rows = rows_v[m].astype(jnp.float32)
        scale = lax.rsqrt(jnp.mean(rows * rows, axis=-1, keepdims=True) + EPSILON)
        hidden_v[m] = (rows * scale * gain_ref[...]).astype(jnp.bfloat16)

    hidden_copy.start()
    for p in range(3):
        gather.second(p)
    for p in range(3):
        gather.third(p)
    for p in range(3):
        gather.fourth(p)
    weight_copy = pltpu.make_async_copy(weight_v, weight_out, load_sem.at[1])
    weight_copy.start()

    def keeps(step, m):
        return [pltpu.make_async_copy(raw_v.at[step % 2], raw_out.at[m], keep_sem.at[step % 2])]

    kept = []
    for step in range(micro):
        far = micro - 1 - step
        own = spot // groups
        if micro == 4:
            m = lax.rem(own + far % 2, 2) + 2 * lax.rem(own // 2 + far // 2, 2)
        else:
            m = lax.rem(own + far, micro)
        if step >= 2:
            for copy in kept[step - 2]:
                copy.wait()
        heads_all = dot_f32(hidden_v[m], weight_v[...])
        span = pl.ds(pl.multiple_of(m * tok, tok), tok)
        cosine, sine = cosine_ref[span, :], sine_ref[span, :]
        raw_v[step % 2] = heads_all[:, : (heads + groups) * HD]
        for h in range(heads + groups):
            raw = heads_all[:, h * HD : (h + 1) * HD]
            gain = head_gain_ref[0:1, :] if h < heads else head_gain_ref[1:2, :]
            unit = raw * lax.rsqrt(jnp.mean(raw * raw, axis=-1, keepdims=True) + EPSILON) * gain
            turned = unit * cosine + pltpu.roll(unit, HD // 2, 1) * sine
            g, place = (h // 2, h % 2) if h < heads else (h - heads, 2)
            pack_v[m * groups + g, :, place * HD : (place + 1) * HD] = turned.astype(jnp.bfloat16)
        for g in range(groups):
            first = (heads + groups + g) * HD
            pack_v[m * groups + g, :, 3 * HD :] = heads_all[:, first : first + HD].astype(
                jnp.bfloat16
            )
            swap.send(m * groups + g)
        kept.append(keeps(step, m))
        for copy in kept[step]:
            copy.start()
    for copy in kept[micro - 2] + kept[micro - 1]:
        copy.wait()

    @pl.loop(0, width)
    def _(d):
        swap.sent(d)
        swap.wait(d)

    gather.drain()
    hidden_copy.wait()
    weight_copy.wait()


def project(layer_input, gain_attn, weights, cosine, sine, head_gains, width):
    micro, tok, model = layer_input.shape
    groups = width // micro
    low = jnp.bfloat16
    anywhere = pl.BlockSpec(memory_space=pl.ANY)
    inside = pl.BlockSpec(memory_space=pltpu.VMEM)
    raw = 3 * groups * HD
    columns = sum(weight.shape[1] for weight in weights)
    return pl.pallas_call(
        project_kernel,
        out_shape=(
            jax.ShapeDtypeStruct((micro, tok, model), low),
            jax.ShapeDtypeStruct((micro, tok, raw), jnp.float32),
            jax.ShapeDtypeStruct((width, tok, 4 * HD), low),
            jax.ShapeDtypeStruct((model, columns), low),
        ),
        in_specs=[anywhere, inside, anywhere, anywhere, anywhere, inside, inside, inside],
        out_specs=[anywhere] * 4,
        scratch_shapes=[
            pltpu.VMEM((micro, tok, model), low),
            pltpu.VMEM((model, columns), low),
            pltpu.VMEM((micro, tok, model), low),
            pltpu.VMEM((2, tok, raw), jnp.float32),
            pltpu.VMEM((width, tok, 4 * HD), low),
            pltpu.SemaphoreType.DMA((2,)),
            pltpu.SemaphoreType.DMA((2,)),
            pltpu.SemaphoreType.DMA,
            pltpu.SemaphoreType.DMA((width,)),
            pltpu.SemaphoreType.DMA((width,)),
            pltpu.SemaphoreType.DMA((3, 9)),
            pltpu.SemaphoreType.DMA((3, 10)),
        ],
        compiler_params=pltpu.CompilerParams(
            collective_id=2, has_side_effects=True, vmem_limit_bytes=40 << 20
        ),
        cost_estimate=pl.CostEstimate(
            flops=20_000_000_000, bytes_accessed=40_000_000, transcendentals=0
        ),
        name="project",
    )(layer_input, gain_attn[None, :], *weights, cosine, sine, head_gains)


def weights_kernel(
    back_ref,
    raw_ref,
    hidden_ref,
    mixed_ref,
    low_ref,
    cosine_ref,
    sine_ref,
    head_gain_ref,
    back_out,
    grad_out,
    gain_out,
    land_v,
    raw_v,
    hidden_v,
    mixed_v,
    low_v,
    back_v,
    grad_v,
    pair_v,
    load_sem,
    back_sem,
    tile_sem,
    send_sem,
    land_sem,
    pair_sems,
):
    micro, tok, heads_in = mixed_ref.shape
    width = back_ref.shape[0]
    groups = width // micro
    heads = 2 * groups
    model = hidden_ref.shape[2]
    piece = model // width
    count = micro * tok
    swap = Exchange(
        lambda target: back_ref.at[target], lambda source: land_v.at[source], send_sem, land_sem
    )
    loads = [
        pltpu.make_async_copy(mixed_ref, mixed_v, load_sem.at[0]),
        pltpu.make_async_copy(low_ref, low_v, load_sem.at[1]),
        pltpu.make_async_copy(raw_ref, raw_v, load_sem.at[2]),
        pltpu.make_async_copy(hidden_ref, hidden_v, load_sem.at[3]),
    ]
    for copy in loads:
        copy.start()
    greet_wide(width)
    spot = lax.axis_index("wide")
    for step in range(width - 1, -1, -1):
        swap.send(lax.rem(spot + step, width))
    loads[0].wait()
    loads[1].wait()
    mixed_all = mixed_v[...].reshape(count, heads_in)
    for n in range(model // LANES):
        low = low_v[:, :, n * LANES : (n + 1) * LANES].reshape(count, LANES)
        part = dot_f32(mixed_all, low, TN).astype(jnp.bfloat16)
        for i in range(LANES // piece):
            for b in range(heads_in // piece):
                grad_v[
                    n * (LANES // piece) + i, :, pl.ds(2 * heads_in + b * piece, piece)
                ] = part[b * piece : (b + 1) * piece, i * piece : (i + 1) * piece]
    loads[2].wait()
    gain_out[...] = jnp.zeros_like(gain_out)

    @pl.loop(0, width)
    def _(d):
        swap.wait(d)

    def back_copy(m):
        return pltpu.make_async_copy(back_v.at[m], back_out.at[m], back_sem.at[m])

    @pl.loop(0, micro)
    def _(m):
        span = pl.ds(pl.multiple_of(m * tok, tok), tok)
        cosine, sine = cosine_ref[span, :], sine_ref[span, :]
        for h in range(heads + groups):
            raw = raw_v[m, :, h * HD : (h + 1) * HD]
            kind = 0 if h < heads else 1
            gain = head_gain_ref[kind : kind + 1, :]
            g, place = (h // 2, h % 2) if h < heads else (h - heads, 2)
            grad = land_v[m * groups + g, :, place * HD : (place + 1) * HD].astype(jnp.float32)
            straight = grad * cosine + pltpu.roll(grad * sine, HD // 2, 1)
            scale = lax.rsqrt(jnp.mean(raw * raw, axis=-1, keepdims=True) + EPSILON)
            gain_out[kind : kind + 1, :] += jnp.sum(straight * (raw * scale), axis=0, keepdims=True)
            pulled = straight * gain
            along = jnp.mean(pulled * raw, axis=-1, keepdims=True)
            back_v[m, :, h * HD : (h + 1) * HD] = (
                scale * (pulled - raw * (scale * scale * along))
            ).astype(jnp.bfloat16)
        for g in range(groups):
            first = (heads + groups + g) * HD
            back_v[m, :, first : first + HD] = land_v[m * groups + g, :, 3 * HD :]
        back_copy(m).start()

    loads[3].wait()

    core = lax.rem(spot, 2)
    near = spot + 1 - 2 * core

    def tile_copy(c):
        return pltpu.make_async_copy(grad_v.at[2 * c + core], grad_out.at[c], tile_sem.at[c])

    def pair_copy(c):
        return pltpu.make_async_remote_copy(
            src_ref=grad_v.at[2 * c + 1 - core],
            dst_ref=pair_v.at[c],
            send_sem=pair_sems.at[0, c],
            recv_sem=pair_sems.at[1, c],
            device_id={"wide": near},
            device_id_type=MESH,
        )

    def tile(i):
        left = hidden_v[:, :, pl.ds(pl.multiple_of(i * piece, piece), piece)].reshape(count, piece)
        return dot_f32(left, back_v[...].reshape(count, 2 * heads_in), TN)

    @pl.loop(0, width // 2)
    def _(c):
        i = 2 * c + 1 - core
        grad_v[i, :, 0 : 2 * heads_in] = tile(i).astype(jnp.bfloat16)
        pair_copy(c).start()

    @pl.loop(0, width // 2)
    def _(c):
        i = 2 * c + core
        part = tile(i)
        pair_copy(c).wait_recv()
        grad_v[i, :, 0 : 2 * heads_in] = (
            part + pair_v[c, :, 0 : 2 * heads_in].astype(jnp.float32)
        ).astype(jnp.bfloat16)
        grad_v[i, :, 2 * heads_in :] = (
            grad_v[i, :, 2 * heads_in :].astype(jnp.float32)
            + pair_v[c, :, 2 * heads_in :].astype(jnp.float32)
        ).astype(jnp.bfloat16)
        tile_copy(c).start()

    @pl.loop(0, width // 2)
    def _(c):
        tile_copy(c).wait()
        pair_copy(c).wait_send()

    @pl.loop(0, width)
    def _(i):
        swap.sent(i)

    for m in range(micro):
        back_copy(m).wait()


def weight_gradients(back, raw, hidden, mixed, middle_low, cosine, sine, head_gains):
    micro, tok, heads_in = mixed.shape
    width = back.shape[0]
    model = hidden.shape[2]
    low = jnp.bfloat16
    anywhere = pl.BlockSpec(memory_space=pl.ANY)
    inside = pl.BlockSpec(memory_space=pltpu.VMEM)
    return pl.pallas_call(
        weights_kernel,
        out_shape=(
            jax.ShapeDtypeStruct((micro, tok, 2 * heads_in), low),
            jax.ShapeDtypeStruct((width // 2, model // width, 3 * heads_in), low),
            jax.ShapeDtypeStruct((2, HD), jnp.float32),
        ),
        in_specs=[anywhere] * 5 + [inside] * 3,
        out_specs=[anywhere, anywhere, inside],
        scratch_shapes=[
            pltpu.VMEM(back.shape, low),
            pltpu.VMEM(raw.shape, jnp.float32),
            pltpu.VMEM(hidden.shape, low),
            pltpu.VMEM(mixed.shape, low),
            pltpu.VMEM(middle_low.shape, low),
            pltpu.VMEM((micro, tok, 2 * heads_in), low),
            pltpu.VMEM((width, model // width, 3 * heads_in), low),
            pltpu.VMEM((width // 2, model // width, 3 * heads_in), low),
            pltpu.SemaphoreType.DMA((4,)),
            pltpu.SemaphoreType.DMA((micro,)),
            pltpu.SemaphoreType.DMA((width // 2,)),
            pltpu.SemaphoreType.DMA((width,)),
            pltpu.SemaphoreType.DMA((width,)),
            pltpu.SemaphoreType.DMA((2, width // 2)),
        ],
        compiler_params=pltpu.CompilerParams(
            collective_id=3, has_side_effects=True, vmem_limit_bytes=48 << 20
        ),
        cost_estimate=pl.CostEstimate(
            flops=1_000_000_000, bytes_accessed=1_000_000, transcendentals=0
        ),
        name="weight_gradients",
    )(back, raw, hidden, mixed, middle_low, cosine, sine, head_gains)


def relay_scratch(count, model):
    return [
        pltpu.VMEM((count, SUB, model), jnp.bfloat16),
        pltpu.VMEM((count, SUB, model), jnp.bfloat16),
        pltpu.VMEM((RING, SUB, model), jnp.bfloat16),
        pltpu.SemaphoreType.DMA((count,)),
        pltpu.SemaphoreType.DMA((count,)),
        pltpu.SemaphoreType.DMA((count,)),
        pltpu.SemaphoreType.DMA((RING,)),
    ]


def feed_kernel(
    mixed_ref,
    input_ref,
    grad_ref,
    gain_ref,
    pack_ref,
    up_w,
    down_w,
    hidden_out,
    active_out,
    gate_out,
    upper_out,
    output_out,
    middle_out,
    low_out,
    mixed_out,
    gain_out,
    weight_out,
    heads_out,
    early_out,
    own,
    landed,
    cross,
    out_sem,
    land_sem,
    back_sem,
    cross_sem,
    out_v,
    gate_v,
    up_v,
    down_v,
    mixed_v,
    rows_v,
    grads_v,
    hidden_v,
    stage_v,
    scale_v,
    middle_v,
    output_v,
    mixback_v,
    weight_sem,
    attn_sem,
    load_sem,
    hidden_sem,
    stage_sem,
    final_sem,
    reload_sem,
    tile_sem,
    ahead_sems,
    behind_sems,
    heads_sem,
    part_send,
    part_land,
    pair_sems,
    credit,
):
    micro, tok, model = input_ref.shape
    width, _, piece = pack_ref.shape
    heads_in = out_v.shape[0]
    groups = width // micro
    per = tok // SUB
    hid = gate_v.shape[1]
    count = micro * tok
    blocks = hid // piece
    relay = Relay(3 * micro * per, own, landed, cross, (out_sem, land_sem, back_sem, cross_sem))
    n_up = hid // LANES
    n_down = model // LANES
    slots = n_up + n_down

    ahead = Exchange(
        lambda target: mixed_ref.at[target],
        lambda source: mixed_v.at[
            source // groups, :, pl.ds(pl.multiple_of((source % groups) * 2 * HD, 2 * HD), 2 * HD)
        ],
        ahead_sems.at[0],
        ahead_sems.at[1],
    )
    behind = Exchange(
        lambda target: mixback_v.at[
            target // groups % 2,
            :,
            pl.ds(pl.multiple_of((target % groups) * 2 * HD, 2 * HD), 2 * HD),
        ],
        lambda source: mixed_out.at[source],
        behind_sems.at[0],
        behind_sems.at[1],
    )
    attn_copies = [
        pltpu.make_async_copy(
            pack_ref.at[i, pl.ds(0, heads_in)],
            out_v.at[:, pl.ds(i * piece, piece)],
            attn_sem.at[i],
        )
        for i in range(width)
    ]
    weight_copies = [
        pltpu.make_async_copy(
            pack_ref.at[i, pl.ds(heads_in + j * piece, piece)],
            gate_v.at[pl.ds(i * piece, piece), pl.ds(j * piece, piece)],
            weight_sem.at[i, j],
        )
        for i in range(width)
        for j in range(blocks)
    ]

    def up_part(j):
        cols = pl.ds(j * LANES, LANES)
        return (
            up_w.at[:, cols],
            lambda s: up_v.at[pl.ds(pl.multiple_of(s * piece, piece), piece), cols],
            lambda s, h: up_v.at[
                pl.ds(pl.multiple_of(s * piece + h * piece // 2, piece // 2), piece // 2), cols
            ],
        )

    def down_part(j):
        return (
            down_w.at[pl.ds(j * LANES, LANES)],
            lambda s: down_v.at[
                pl.ds(j * LANES, LANES), pl.ds(pl.multiple_of(s * piece, piece), piece)
            ],
            lambda s, h: down_v.at[
                pl.ds(j * LANES + h * LANES // 2, LANES // 2),
                pl.ds(pl.multiple_of(s * piece, piece), piece),
            ],
        )

    gather = Gather(
        [make(j) for j in range(n_up) for make in (up_part, down_part)], part_send, part_land
    )

    def both(action, j):
        action(2 * j)
        action(2 * j + 1)

    for copy in attn_copies + weight_copies:
        copy.start()

    def loads(n):
        slot = n % 2
        return (
            pltpu.make_async_copy(input_ref.at[n % micro], rows_v.at[slot], load_sem.at[slot, 0]),
            pltpu.make_async_copy(grad_ref.at[n % micro], grads_v.at[slot], load_sem.at[slot, 1]),
        )

    def start_loads(n):
        for copy in loads(n):
            copy.start()

    def wait_loads(n):
        for copy in loads(n):
            copy.wait()

    start_loads(0)
    gain_out[...] = jnp.zeros_like(gain_out)
    relay.greet(wide_peers(width))
    spot = lax.axis_index("wide")
    for step in range(width):
        ahead.send(lax.rem(spot + step, width))
    both(gather.first, 0)
    both(gather.first, 1)
    for copy in attn_copies:
        copy.wait()

    def heads_copy(m):
        return pltpu.make_async_copy(mixed_v.at[m], heads_out.at[m], heads_sem.at[m])

    @pl.loop(0, micro)
    def _(m):
        for g in range(groups):
            ahead.wait(m * groups + g)
        heads_copy(m).start()
        for n in range(n_down):
            cols = pl.ds(n * LANES, LANES)
            part = dot_f32(mixed_v[m], out_v[:, cols]).astype(jnp.bfloat16)
            for r in range(per):
                own[m * per + r, :, cols] = part[r * SUB : (r + 1) * SUB]
        relay.send(m * per, per)

    first_ticks = per + 4

    for k in range(first_ticks):
        if k == 4:
            both(gather.second, 0)
        if k == 5:
            both(gather.first, 2)
        if k == 6:
            both(gather.second, 1)
        if k == 7:
            both(gather.third, 0)
        relay.tick(k)

    for copy in weight_copies:
        copy.wait()

    def hidden_copy(m):
        return pltpu.make_async_copy(hidden_v, hidden_out.at[m], hidden_sem)

    def stage_copies(m):
        return [
            pltpu.make_async_copy(stage_v.at[i], target.at[m], stage_sem.at[i])
            for i, target in enumerate((active_out, gate_out, upper_out))
        ]

    base = micro * per

    @pl.loop(0, micro)
    def _(m):
        slot = m % 2
        wait_loads(m)
        start_loads(m + 1)

        @pl.when(m > 0)
        def _():
            hidden_copy(m - 1).wait()
            for copy in stage_copies(m - 1):
                copy.wait()

        for r in range(per):
            span = pl.ds(r * SUB, SUB)
            middle = rows_v[slot, span, :].astype(jnp.float32) + landed[m * per + r].astype(
                jnp.float32
            )
            scale = lax.rsqrt(jnp.mean(middle * middle, axis=-1, keepdims=True) + EPSILON)
            scale_v[span, :] = scale
            hidden_v[span, :] = (middle * scale * gain_ref[...]).astype(jnp.bfloat16)
        hidden_copy(m).start()
        for j in range(n_up):
            relay.tick(first_ticks + slots * m + j)

            @pl.when(m == 0)
            def _():
                if j == 0:
                    both(gather.second, 2)
                if j + 1 < n_up:
                    both(gather.third, j + 1)
                both(gather.fourth, j)

            cols = pl.ds(j * LANES, LANES)
            gate = dot_f32(hidden_v[...], gate_v[:, cols])
            up_proj = dot_f32(hidden_v[...], up_v[:, cols])
            grad_active = dot_f32(grads_v[slot], down_v[cols, :], NT)
            squash = 1.0 / (1.0 + jnp.exp(-gate))
            silu = gate * squash
            stage_v[0, :, cols] = (silu * up_proj).astype(jnp.bfloat16)
            stage_v[1, :, cols] = (
                grad_active * up_proj * (squash * (1.0 + gate * (1.0 - squash)))
            ).astype(jnp.bfloat16)
            stage_v[2, :, cols] = (grad_active * silu).astype(jnp.bfloat16)
        for copy in stage_copies(m):
            copy.start()
        for n in range(n_down):
            relay.tick(first_ticks + slots * m + n_up + n)
            cols = pl.ds(n * LANES, LANES)
            back = dot_f32(stage_v[1], gate_v[cols, :], NT) + dot_f32(
                stage_v[2], up_v[cols, :], NT
            )
            ahead = dot_f32(stage_v[0], down_v[:, cols]).astype(jnp.bfloat16)
            gain_sum = jnp.zeros((1, LANES), jnp.float32)
            for r in range(per):
                part = slice(r * SUB, (r + 1) * SUB)
                own[base + 2 * per * m + r, :, cols] = back[part].astype(jnp.bfloat16)
                own[base + 2 * per * m + per + r, :, cols] = ahead[part]
                unit = (
                    rows_v[slot, pl.ds(r * SUB, SUB), cols].astype(jnp.float32)
                    + landed[m * per + r, :, cols].astype(jnp.float32)
                ) * scale_v[pl.ds(r * SUB, SUB), :]
                gain_sum += jnp.sum(back[part] * unit, axis=0, keepdims=True)
            gain_out[:, cols] += gain_sum
        relay.send(base + 2 * per * m, 2 * per)

    hidden_copy(micro - 1).wait()
    for copy in stage_copies(micro - 1):
        copy.wait()

    gather.drain()
    core = lax.rem(spot, 2)
    near = gather.near

    def offer():
        pl.semaphore_signal(credit, inc=1, device_id={"wide": near}, device_id_type=MESH)

    offer()

    @pl.loop(0, base)
    def _(k):
        relay.to_inner(k).wait_send()

    def reloads(m):
        rows = pl.ds(m * tok, tok)
        return [
            pltpu.make_async_copy(hidden_out.at[m], down_v.at[rows], reload_sem.at[m, 0]),
            pltpu.make_async_copy(gate_out.at[m], gate_v.at[rows], reload_sem.at[m, 1]),
            pltpu.make_async_copy(
                upper_out.at[m], gate_v.at[pl.ds(count + m * tok, tok)], reload_sem.at[m, 2]
            ),
            pltpu.make_async_copy(active_out.at[m], up_v.at[rows], reload_sem.at[m, 3]),
        ] + [
            pltpu.make_async_copy(
                grad_ref.at[m, pl.ds(r * SUB, SUB)], own.at[m * per + r], reload_sem.at[m, 4 + r]
            )
            for r in range(per)
        ]

    for m in range(micro):
        for copy in reloads(m):
            copy.start()

    def pair_slot(q):
        return up_v.at[pl.ds(count + q * piece, piece)]

    def tile_copy(m, q):
        target = early_out.at[m] if q == 0 else weight_out.at[m, q - 1]
        return pltpu.make_async_copy(pair_slot(q), target, tile_sem.at[q])

    def pair_copy(q):
        return pltpu.make_async_remote_copy(
            src_ref=stage_v.at[q],
            dst_ref=pair_slot(q),
            send_sem=pair_sems.at[0, q],
            recv_sem=pair_sems.at[1, q],
            device_id={"wide": near},
            device_id_type=MESH,
        )

    def tile(i, q, store):
        cols = pl.ds(pl.multiple_of(i * piece, piece), piece)
        if q == 2:
            right = own[0:base, :, cols].reshape(count, piece)
            for j in range(blocks):
                span = slice(j * piece, (j + 1) * piece)
                store(span, dot_f32(up_v[0:count, span], right, TN))
        else:
            right = (gate_v[0:count], gate_v[count : 2 * count])[q]
            store(slice(0, hid), dot_f32(down_v[0:count, cols], right, TN))

    def give(m, q):
        @pl.when(m > 0)
        def _():
            pair_copy(q).wait_send()

        def store(span, part):
            stage_v[q, :, span] = part.astype(jnp.bfloat16)

        tile(2 * m + 1 - core, q, store)

    def keep(m, q):
        rows = pl.ds(count + q * piece, piece)
        pair_copy(q).wait_recv()

        def store(span, part):
            up_v[rows, span] = (part + up_v[rows, span].astype(jnp.float32)).astype(jnp.bfloat16)

        tile(2 * m + core, q, store)
        tile_copy(m, q).start()

    def final_copies(m):
        return [
            pltpu.make_async_copy(middle_v, middle_out.at[m], final_sem.at[0]),
            pltpu.make_async_copy(hidden_v, low_out.at[m], final_sem.at[1]),
            pltpu.make_async_copy(output_v, output_out.at[m], final_sem.at[2]),
        ]

    last_ticks = first_ticks + slots * micro
    rest = 3 * micro * per + 4 - last_ticks
    turns = rest // micro

    @pl.loop(0, micro)
    def _(m):
        slot = m % 2
        wait_loads(m + micro)

        @pl.when(m < micro - 1)
        def _():
            start_loads(m + micro + 1)

        @pl.when(m > 0)
        def _():
            for copy in final_copies(m - 1):
                copy.wait()

        @pl.when(m == 0)
        def _():
            for i in range(micro):
                for copy in reloads(i):
                    copy.wait()

        relay.tick(last_ticks + turns * m)
        give(m, 0)
        give(m, 1)
        relay.tick(last_ticks + turns * m + 1)
        give(m, 2)
        pl.semaphore_wait(credit, 1)
        for q in range(3):
            pair_copy(q).start()
        for r in range(per):
            span = pl.ds(r * SUB, SUB)
            middle = rows_v[slot, span, :].astype(jnp.float32) + landed[m * per + r].astype(
                jnp.float32
            )
            scale = lax.rsqrt(jnp.mean(middle * middle, axis=-1, keepdims=True) + EPSILON)
            pulled = landed[base + 2 * per * m + r].astype(jnp.float32) * gain_ref[...]
            along = jnp.mean(pulled * middle, axis=-1, keepdims=True)
            grad_middle = grads_v[slot, span, :].astype(jnp.float32) + scale * (
                pulled - middle * (scale * scale * along)
            )
            middle_v[span, :] = grad_middle
            hidden_v[span, :] = grad_middle.astype(jnp.bfloat16)
        @pl.when(m >= 2)
        def _():
            for g in range(groups):
                behind.sent((m - 2) * groups + g, home=True)

        mixback_v[m % 2] = dot_f32(hidden_v[...], out_v[...], NT).astype(jnp.bfloat16)
        for g in range(groups):
            behind.send(m * groups + g)
        relay.tick(last_ticks + turns * m + 2)
        keep(m, 0)
        keep(m, 1)
        relay.tick(last_ticks + turns * m + 3)
        keep(m, 2)
        for r in range(per):
            span = pl.ds(r * SUB, SUB)
            output_v[span, :] = (
                rows_v[slot, span, :].astype(jnp.float32)
                + landed[m * per + r].astype(jnp.float32)
                + landed[base + 2 * per * m + per + r].astype(jnp.float32)
            ).astype(jnp.bfloat16)
        for copy in final_copies(m):
            copy.start()
        for q in range(3):
            tile_copy(m, q).wait()

        @pl.when(m < micro - 1)
        def _():
            offer()

    for copy in final_copies(micro - 1):
        copy.wait()
    for q in range(3):
        pair_copy(q).wait_send()
    for m in range(micro):
        heads_copy(m).wait()

    @pl.loop(0, width)
    def _(d):
        ahead.sent(d)
        behind.wait(d, home=False)

    @pl.loop((micro - 2) * groups, width)
    def _(d):
        behind.sent(d, home=True)

    relay.drain(base)


def feed_forward(mixed, layer_input, grad_out, gain_ffn, pack, up_w, down_w, heads_in):
    micro, tok, model = layer_input.shape
    hid = up_w.shape[1]
    parts = 2 * (hid // LANES)
    width, _, piece = pack.shape
    groups = width // micro
    low = jnp.bfloat16
    count = 3 * micro * (tok // SUB)
    anywhere = pl.BlockSpec(memory_space=pl.ANY)
    inside = pl.BlockSpec(memory_space=pltpu.VMEM)
    return pl.pallas_call(
        feed_kernel,
        out_shape=(
            jax.ShapeDtypeStruct((micro, tok, model), low),
            jax.ShapeDtypeStruct((micro, tok, hid), low),
            jax.ShapeDtypeStruct((micro, tok, hid), low),
            jax.ShapeDtypeStruct((micro, tok, hid), low),
            jax.ShapeDtypeStruct((micro, tok, model), low),
            jax.ShapeDtypeStruct((micro, tok, model), jnp.float32),
            jax.ShapeDtypeStruct((micro, tok, model), low),
            jax.ShapeDtypeStruct((width, tok, 2 * HD), low),
            jax.ShapeDtypeStruct((1, model), jnp.float32),
            jax.ShapeDtypeStruct((width // 2, 2, piece, hid), low),
            jax.ShapeDtypeStruct((micro, tok, heads_in), low),
            jax.ShapeDtypeStruct((width // 2, piece, hid), low),
        ),
        in_specs=[anywhere] * 3 + [inside, anywhere, anywhere, anywhere],
        out_specs=[anywhere] * 8 + [inside] + [anywhere] * 3,
        scratch_shapes=relay_scratch(count, model)
        + [
            pltpu.VMEM((heads_in, model), low),
            pltpu.VMEM((model, hid), low),
            pltpu.VMEM((model, hid), low),
            pltpu.VMEM((hid, model), low),
            pltpu.VMEM((micro, tok, heads_in), low),
            pltpu.VMEM((2, tok, model), low),
            pltpu.VMEM((2, tok, model), low),
            pltpu.VMEM((tok, model), low),
            pltpu.VMEM((3, tok, hid), low),
            pltpu.VMEM((tok, 1), jnp.float32),
            pltpu.VMEM((tok, model), jnp.float32),
            pltpu.VMEM((tok, model), low),
            pltpu.VMEM((2, tok, heads_in), low),
            pltpu.SemaphoreType.DMA((width, hid // piece)),
            pltpu.SemaphoreType.DMA((width,)),
            pltpu.SemaphoreType.DMA((2, 2)),
            pltpu.SemaphoreType.DMA,
            pltpu.SemaphoreType.DMA((3,)),
            pltpu.SemaphoreType.DMA((3,)),
            pltpu.SemaphoreType.DMA((micro, 4 + tok // SUB)),
            pltpu.SemaphoreType.DMA((3,)),
            pltpu.SemaphoreType.DMA((2, width)),
            pltpu.SemaphoreType.DMA((2, width)),
            pltpu.SemaphoreType.DMA((micro,)),
            pltpu.SemaphoreType.DMA((parts, 9)),
            pltpu.SemaphoreType.DMA((parts, 10)),
            pltpu.SemaphoreType.DMA((2, 3)),
            pltpu.SemaphoreType.REGULAR,
        ],
        compiler_params=pltpu.CompilerParams(
            collective_id=0, has_side_effects=True, vmem_limit_bytes=67043328
        ),
        cost_estimate=pl.CostEstimate(
            flops=240_000_000_000, bytes_accessed=900_000_000, transcendentals=0
        ),
        name="feed_forward",
    )(mixed, layer_input, grad_out, gain_ffn[None, :], pack, up_w, down_w)


def input_kernel(
    back_ref,
    input_ref,
    middle_ref,
    gain_ref,
    weight_ref,
    gain_two_ref,
    gain_heads_ref,
    output_out,
    gains_out,
    own,
    landed,
    cross,
    out_sem,
    land_sem,
    back_sem,
    cross_sem,
    weight_v,
    back_v,
    rows_v,
    middle_v,
    output_v,
    term_v,
    other_v,
    first_sem,
    load_sem,
    final_sem,
    term_sem,
    other_sem,
):
    micro, tok, model = input_ref.shape
    per = tok // SUB
    spot = lax.axis_index("wide")
    flips = [spot + bit - 2 * bit * (spot // bit % 2) for bit in (1, 2, 4)]
    relay = Relay(micro * per, own, landed, cross, (out_sem, land_sem, back_sem, cross_sem))
    weight_copy = pltpu.make_async_copy(weight_ref, weight_v, first_sem.at[0])
    back_copy = pltpu.make_async_copy(back_ref, back_v, first_sem.at[1])
    weight_copy.start()
    back_copy.start()

    rows_copy = pltpu.make_async_copy(input_ref, rows_v, first_sem.at[2])
    rows_copy.start()

    def load(m):
        return pltpu.make_async_copy(middle_ref.at[m], middle_v.at[m % 2], load_sem.at[m % 2])

    def final_copy(m):
        return pltpu.make_async_copy(output_v.at[m % 2], output_out.at[m], final_sem.at[m % 2])

    def pass_on(step, where):
        return pltpu.make_async_remote_copy(
            src_ref=term_v.at[step],
            dst_ref=other_v.at[step],
            send_sem=term_sem.at[step],
            recv_sem=other_sem.at[step],
            device_id=where,
            device_id_type=MESH,
        )

    targets = [{"wide": flip} for flip in flips] + [
        {"narrow": spot} for spot in (relay.inner, relay.other, relay.outer)
    ]

    def gain_step(step):
        if step == 0:
            pass_on(0, targets[0]).start()
        if 1 <= step <= 3:
            pass_on(step - 1, targets[step - 1]).wait_recv()
            term_v[step] = term_v[step - 1] + other_v[step - 1]
        if step in (1, 2):
            pass_on(step, targets[step]).start()
        if step == 3:

            @pl.when(relay.is_end)
            def _():
                pass_on(3, targets[3]).start()

        if step in (4, 5):

            @pl.when(relay.is_mid)
            def _():
                pass_on(step - 1, targets[step - 1]).wait_recv()
                term_v[step] = term_v[step - 1] + other_v[step - 1]
                pass_on(step, targets[step]).start()

        if step == 6:

            @pl.when(relay.is_mid)
            def _():
                gains_out[...] = term_v[5]
                pass_on(4, targets[4]).wait_send()
                pass_on(5, targets[5]).wait_send()

            @pl.when(relay.is_end)
            def _():
                pass_on(5, targets[5]).wait_recv()
                gains_out[...] = other_v[5]
                pass_on(3, targets[3]).wait_send()

            for early in range(3):
                pass_on(early, targets[early]).wait_send()

    load(0).start()
    relay.greet(flips)
    term_v[0] = jnp.zeros(term_v.shape[1:], jnp.float32)
    weight_copy.wait()
    back_copy.wait()
    rows_copy.wait()

    @pl.loop(0, micro)
    def _(m):
        rows = rows_v[m].astype(jnp.float32)
        scale = lax.rsqrt(jnp.mean(rows * rows, axis=-1, keepdims=True) + EPSILON)
        for n in range(model // LANES):
            cols = pl.ds(n * LANES, LANES)
            part = dot_f32(back_v[m], weight_v[cols, :], NT)
            term_v[0, 0:1, cols] += jnp.sum(
                part * (rows_v[m, :, cols].astype(jnp.float32) * scale), axis=0, keepdims=True
            )
            part = part.astype(jnp.bfloat16)
            for r in range(per):
                own[m * per + r, :, cols] = part[r * SUB : (r + 1) * SUB]

        @pl.when(m == 0)
        def _():
            relay.send(0, AHEAD)

    term_v[0, 1:2, :] = gain_two_ref[...]
    term_v[0, 2:3, 0:HD] = gain_heads_ref[0:1, :]
    term_v[0, 2:3, HD : 2 * HD] = gain_heads_ref[1:2, :]
    for k in range(4):
        if k in GAIN_TICKS:
            gain_step(GAIN_TICKS.index(k))
        relay.send(AHEAD + k, 1)
        relay.tick(k)

    @pl.loop(0, micro)
    def _(m):
        slot = m % 2

        @pl.when(m < micro - 1)
        def _():
            load(m + 1).start()

        load(m).wait()

        @pl.when(m >= 2)
        def _():
            final_copy(m - 2).wait()

        for r in range(per):
            for turn in range(micro):
                if 4 + turn * per + r in GAIN_TICKS:

                    @pl.when(m == turn)
                    def _(step=GAIN_TICKS.index(4 + turn * per + r)):
                        gain_step(step)

            @pl.when(AHEAD + 4 + m * per + r < relay.count)
            def _():
                relay.send(AHEAD + 4 + m * per + r, 1)

            relay.tick(4 + m * per + r)
            span = pl.ds(r * SUB, SUB)
            rows = rows_v[m, span, :].astype(jnp.float32)
            scale = lax.rsqrt(jnp.mean(rows * rows, axis=-1, keepdims=True) + EPSILON)
            pulled = landed[m * per + r].astype(jnp.float32) * gain_ref[...]
            along = jnp.mean(pulled * rows, axis=-1, keepdims=True)
            output_v[slot, span, :] = middle_v[slot, span, :] + scale * (
                pulled - rows * (scale * scale * along)
            )
        final_copy(m).start()

    final_copy(micro - 2).wait()
    final_copy(micro - 1).wait()
    relay.drain(0)


def input_gradient(back, layer_input, grad_middle, gain_attn, weight, gain_two, gain_heads):
    micro, tok, model = layer_input.shape
    low = jnp.bfloat16
    count = micro * (tok // SUB)
    anywhere = pl.BlockSpec(memory_space=pl.ANY)
    inside = pl.BlockSpec(memory_space=pltpu.VMEM)
    return pl.pallas_call(
        input_kernel,
        out_shape=(
            jax.ShapeDtypeStruct((micro, tok, model), jnp.float32),
            jax.ShapeDtypeStruct((8, model), jnp.float32),
        ),
        in_specs=[anywhere] * 3 + [inside, anywhere, inside, inside],
        out_specs=[anywhere, inside],
        scratch_shapes=relay_scratch(count, model)
        + [
            pltpu.VMEM(weight.shape, low),
            pltpu.VMEM((micro, tok, weight.shape[1]), low),
            pltpu.VMEM((micro, tok, model), low),
            pltpu.VMEM((2, tok, model), jnp.float32),
            pltpu.VMEM((2, tok, model), jnp.float32),
            pltpu.VMEM((6, 8, model), jnp.float32),
            pltpu.VMEM((6, 8, model), jnp.float32),
            pltpu.SemaphoreType.DMA((3,)),
            pltpu.SemaphoreType.DMA((2,)),
            pltpu.SemaphoreType.DMA((2,)),
            pltpu.SemaphoreType.DMA((6,)),
            pltpu.SemaphoreType.DMA((6,)),
        ],
        compiler_params=pltpu.CompilerParams(
            collective_id=1, has_side_effects=True, vmem_limit_bytes=48 << 20
        ),
        cost_estimate=pl.CostEstimate(
            flops=1_000_000_000, bytes_accessed=1_000_000, transcendentals=0
        ),
        name="input_gradient",
    )(back, layer_input, grad_middle, gain_attn[None, :], weight, gain_two, gain_heads)


def widen_gate(rows_ref, gate_ref):
    gate_ref[...] = rows_ref[...].astype(jnp.float32)


def widen_feed(rows_ref, up_ref, down_ref):
    piece = up_ref.shape[0]
    up_ref[...] = rows_ref[0:piece, :].astype(jnp.float32)
    for j in range(down_ref.shape[0] // piece):
        span = slice(j * piece, (j + 1) * piece)
        down_ref[span, :] = rows_ref[piece:, span].astype(jnp.float32)


def widen_attn(rows_ref, query_ref, key_ref, value_ref, out_ref):
    piece = query_ref.shape[0]
    first = 0
    for target in (query_ref, key_ref, value_ref):
        target[...] = rows_ref[:, first : first + target.shape[1]].astype(jnp.float32)
        first += target.shape[1]
    for j in range(out_ref.shape[0] // piece):
        part = rows_ref[:, first + j * piece : first + (j + 1) * piece]
        out_ref[j * piece : (j + 1) * piece, :] = part.astype(jnp.float32)


def widen(kernel, rows, shapes):
    return pl.pallas_call(
        kernel,
        out_shape=tuple(jax.ShapeDtypeStruct(shape, jnp.float32) for shape in shapes),
        name=kernel.__name__,
    )(rows)


def local_batched(
    layer_input,
    grad_out,
    lengths,
    w_query,
    w_key,
    w_value,
    w_out,
    w_gate,
    w_up,
    w_down,
    gain_attn,
    gain_ffn,
    gain_query,
    gain_key,
):
    micro, tok_rows, model = layer_input.shape
    width = lax.axis_size("wide")
    groups = w_key.shape[1] // HD
    total = tok_rows * width
    count = micro * tok_rows
    me = lax.axis_index("wide")
    piece = w_out.shape[1]

    def stacked(weight):
        return jnp.moveaxis(weight.reshape(piece, -1, piece), 1, 0).reshape(-1, piece)

    pack = lax.all_gather(
        jnp.concatenate([w_out, stacked(w_gate)], axis=0), "wide", axis=0
    )

    starts, places = jax.vmap(lambda row: row_starts(row, total))(lengths)
    my_places = lax.dynamic_slice_in_dim(places, me * tok_rows, tok_rows, axis=1)
    cosine, sine = angles(my_places.reshape(count))
    sine = jnp.where(jnp.arange(HD) < HD // 2, -sine, sine)
    head_gains = jnp.stack([gain_query, gain_key])
    my_starts = lax.dynamic_index_in_dim(starts, me // groups, axis=0, keepdims=False)
    my_first = my_starts[::BLOCK] // BLOCK

    hidden_one, raw, packed, w_qkv = project(
        layer_input, gain_attn, (w_query, w_key, w_value), cosine, sine, head_gains, width
    )
    packed = packed.reshape(total, 4 * HD)
    mixed, kept, log_total = attention_out(packed, my_starts, my_first)
    (
        _,
        _,
        _,
        _,
        output,
        grad_middle,
        middle_low,
        grad_mixed,
        gain_two,
        feed_grads,
        mixed_low,
        gate_grads,
    ) = feed_forward(
        mixed.reshape(width, tok_rows, 2 * HD),
        layer_input,
        grad_out,
        gain_ffn,
        pack,
        w_up,
        w_down,
        w_out.shape[0],
    )
    cores = [list(range(core, width, 2)) for core in range(2)]

    def scatter(rows):
        return lax.psum_scatter(
            rows, "wide", scatter_dimension=0, axis_index_groups=cores, tiled=True
        )

    back = attention_back(
        packed, my_starts, my_first, grad_mixed.reshape(total, 2 * HD), kept, log_total
    )
    qkv_back, attn_grads, gain_heads = weight_gradients(
        back.reshape(width, tok_rows, 4 * HD),
        raw,
        hidden_one,
        mixed_low,
        middle_low,
        cosine,
        sine,
        head_gains,
    )
    gate_grads = scatter(gate_grads.reshape(-1, w_gate.shape[1]))
    attn_grads, feed_grads = lax.optimization_barrier((attn_grads, feed_grads))
    attn_grads = scatter(attn_grads.reshape(model // 2, -1))
    feed_grads = scatter(feed_grads.reshape(-1, w_up.shape[1]))
    grad_input, gains = input_gradient(
        qkv_back, layer_input, grad_middle, gain_attn, w_qkv, gain_two, gain_heads
    )

    (grad_gate,) = widen(widen_gate, gate_grads, (w_gate.shape,))
    grad_up, grad_down = widen(widen_feed, feed_grads, (w_up.shape, w_down.shape))
    grad_query, grad_key, grad_value, grad_wout = widen(
        widen_attn, attn_grads, (w_query.shape, w_key.shape, w_value.shape, w_out.shape)
    )
    return (
        output,
        grad_input,
        grad_query,
        grad_key,
        grad_value,
        grad_wout,
        grad_gate,
        grad_up,
        grad_down,
        gains[0],
        gains[1],
        gains[2, :HD],
        gains[2, HD : 2 * HD],
    )


def local(mesh, layer_input, grad_out, lengths, w_query, w_key, *rest):
    width = mesh.shape["wide"]
    micro, tok_rows = layer_input.shape[:2]
    groups = w_key.shape[1] // HD
    fits = (
        micro * groups == width == 8
        and w_query.shape[1] == 2 * w_key.shape[1]
        and mesh.shape["narrow"] == 4
        and tok_rows == BLOCK
    )
    chosen = local_batched if fits else local_general
    return chosen(layer_input, grad_out, lengths, w_query, w_key, *rest)


def solution(mesh):
    in_specs = (
        P(None, "wide", None),
        P(None, "wide", None),
        P(),
        P("wide", "narrow"),
        P("wide", "narrow"),
        P("wide", "narrow"),
        P("narrow", "wide"),
        P("wide", "narrow"),
        P("wide", "narrow"),
        P("narrow", "wide"),
        P(),
        P(),
        P(),
        P(),
    )
    out_specs = (
        P(None, "wide", None),
        P(None, "wide", None),
        P("wide", "narrow"),
        P("wide", "narrow"),
        P("wide", "narrow"),
        P("narrow", "wide"),
        P("wide", "narrow"),
        P("wide", "narrow"),
        P("narrow", "wide"),
        P(),
        P(),
        P(),
        P(),
    )
    return jax.shard_map(
        functools.partial(local, mesh), mesh=mesh, in_specs=in_specs, out_specs=out_specs, check_vma=False)
```

```python
import functools
import math

import jax
import jax.numpy as jnp
from jax import lax
from jax.experimental import pallas as pl
from jax.experimental.pallas import tpu as pltpu
from jax.sharding import PartitionSpec as P

HD = 128
NDOC = 8


EPSILON = 1e-06
THETA = 1000000.0


def rms_norm(values, gain):
    return values * lax.rsqrt(jnp.mean(values * values, axis=-1, keepdims=True) + EPSILON) * gain


def unit_rows(values):
    return values * lax.rsqrt(jnp.mean(values * values, axis=-1, keepdims=True) + EPSILON)


def rotate(values, cosine, sine):
    midway = values.shape[-1] // 2
    turned = jnp.concatenate([-values[..., midway:], values[..., :midway]], axis=-1)
    return values * cosine + turned * sine


def layout(lengths_row, total):
    finish = jnp.cumsum(lengths_row)
    starts = finish - lengths_row
    places = jnp.arange(total, dtype=jnp.int32)
    segment = jnp.sum((places[:, None] >= finish[None, :]).astype(jnp.int32), axis=1)
    member = segment[:, None] == jnp.arange(finish.shape[0], dtype=jnp.int32)[None, :]
    opening = jnp.sum(jnp.where(member, starts[None, :], 0), axis=1)
    return (segment, places - opening)


def angles(place):
    frequency = jnp.exp(-math.log(THETA) * jnp.arange(0, HD, 2).astype(jnp.float32) / HD)
    turning = place.astype(jnp.float32)[:, None] * frequency[None, :]
    turning = jnp.concatenate([turning, turning], axis=-1)
    return (jnp.cos(turning), jnp.sin(turning))


def allowed(query_seg, query_idx, key_seg, key_idx):
    same_doc = query_seg[:, None] == key_seg[None, :]
    causal = key_idx[None, :] <= query_idx[:, None]
    usable = (key_seg[None, :] != NDOC - 1) | (key_idx[None, :] == query_idx[:, None])
    return same_doc & causal & usable


def attention_scores(query_low, key_all, mask_local, factor):
    scores = (
        jnp.einsum("tgrd,kgd->grtk", query_low, key_all, preferred_element_type=jnp.float32)
        * factor
    )
    return jnp.where(mask_local[None, None], scores, -1e30)


def one_batch(row_input, grad_row, lengths_row, gathered, gains):
    w_query, w_key, w_value, w_out, w_gate, w_up, w_down = gathered
    gain_attn, gain_ffn, gain_query, gain_key = gains
    tok_rows = row_input.shape[0]
    total = tok_rows * lax.axis_size("wide")
    groups = w_key.shape[1] // HD
    repeat = w_query.shape[1] // w_key.shape[1]
    factor = 1.0 / math.sqrt(HD)
    first_row = lax.axis_index("wide") * tok_rows
    segment, place = layout(lengths_row, total)
    positions = jnp.arange(total, dtype=jnp.int32)
    query_seg = lax.dynamic_slice_in_dim(segment, first_row, tok_rows)
    query_idx = lax.dynamic_slice_in_dim(positions, first_row, tok_rows)
    mask_local = allowed(query_seg, query_idx, segment, positions)
    cosine, sine = angles(lax.dynamic_slice_in_dim(place, first_row, tok_rows))

    def head_norm(rows, gain):
        return rotate(rms_norm(rows, gain), cosine[:, None, :], sine[:, None, :])

    input_float = row_input.astype(jnp.float32)
    grad_float = grad_row.astype(jnp.float32)
    normed_one, pull_one = jax.vjp(lambda rows: rms_norm(rows, gain_attn), input_float)
    hidden_one = normed_one.astype(jnp.bfloat16)
    query_raw = jnp.dot(hidden_one, w_query, preferred_element_type=jnp.float32).reshape(
        tok_rows, groups * repeat, HD
    )
    key_raw = jnp.dot(hidden_one, w_key, preferred_element_type=jnp.float32).reshape(
        tok_rows, groups, HD
    )
    value_low = jnp.dot(hidden_one, w_value, preferred_element_type=jnp.float32).astype(
        jnp.bfloat16
    )
    query_turned, pull_query = jax.vjp(head_norm, query_raw, gain_query)
    key_turned, pull_key = jax.vjp(head_norm, key_raw, gain_key)
    query_low = query_turned.astype(jnp.bfloat16).reshape(tok_rows, groups, repeat, HD)
    key_low = key_turned.astype(jnp.bfloat16).reshape(tok_rows, groups * HD)
    key_all, value_all = (
        lax.all_gather(key_low, "wide", axis=0, tiled=True),
        lax.all_gather(value_low, "wide", axis=0, tiled=True),
    )
    key_all = key_all.reshape(total, groups, HD)
    value_all = value_all.reshape(total, groups, HD)
    scores = attention_scores(query_low, key_all, mask_local, factor)
    highest = jnp.max(scores, axis=-1, keepdims=True)
    exponent = jnp.exp(scores - highest)
    denominator = jnp.sum(exponent, axis=-1, keepdims=True)
    log_total = highest + jnp.log(denominator)
    probs_low = (exponent / denominator).astype(jnp.bfloat16)
    mixed = jnp.einsum("grtk,kgd->tgrd", probs_low, value_all, preferred_element_type=jnp.float32)
    mixed_low = mixed.reshape(tok_rows, groups * repeat * HD).astype(jnp.bfloat16)
    attn_part = jnp.dot(mixed_low, w_out, preferred_element_type=jnp.float32)
    middle = input_float + lax.psum(attn_part.astype(jnp.bfloat16), "narrow").astype(jnp.float32)
    normed_two, pull_two = jax.vjp(lambda rows: rms_norm(rows, gain_ffn), middle)
    hidden_two = normed_two.astype(jnp.bfloat16)
    unit_two = unit_rows(middle)
    gate = jnp.dot(hidden_two, w_gate, preferred_element_type=jnp.float32)
    up_proj = jnp.dot(hidden_two, w_up, preferred_element_type=jnp.float32)
    active, pull_active = jax.vjp(
        lambda gate_in, up_in: jax.nn.silu(gate_in) * up_in, gate, up_proj
    )
    active_low = active.astype(jnp.bfloat16)
    ffn_part = jnp.dot(active_low, w_down, preferred_element_type=jnp.float32)
    output_low = (
        middle + lax.psum(ffn_part.astype(jnp.bfloat16), "narrow").astype(jnp.float32)
    ).astype(jnp.bfloat16)
    grad_wdown = jnp.einsum("tf,td->fd", active_low, grad_row, preferred_element_type=jnp.float32)
    grad_active = jnp.einsum("td,fd->tf", grad_row, w_down, preferred_element_type=jnp.float32)
    grad_gate, grad_upper = pull_active(grad_active)
    gate_back = grad_gate.astype(jnp.bfloat16)
    upper_back = grad_upper.astype(jnp.bfloat16)
    grad_wgate = jnp.einsum("td,tf->df", hidden_two, gate_back, preferred_element_type=jnp.float32)
    grad_wup = jnp.einsum("td,tf->df", hidden_two, upper_back, preferred_element_type=jnp.float32)
    partial_two = jnp.einsum(
        "tf,df->td", gate_back, w_gate, preferred_element_type=jnp.float32
    ) + jnp.einsum("tf,df->td", upper_back, w_up, preferred_element_type=jnp.float32)
    gain_two = jnp.sum(partial_two * unit_two, axis=0)
    grad_middle = (
        grad_float
        + pull_two(lax.psum(partial_two.astype(jnp.bfloat16), "narrow").astype(jnp.float32))[0]
    )
    middle_low = grad_middle.astype(jnp.bfloat16)
    grad_wout = jnp.einsum("th,td->hd", mixed_low, middle_low, preferred_element_type=jnp.float32)
    grad_mixed = jnp.einsum("td,hd->th", middle_low, w_out, preferred_element_type=jnp.float32)
    grad_mixed = grad_mixed.astype(jnp.bfloat16).reshape(tok_rows, groups, repeat, HD)
    scores = attention_scores(query_low, key_all, mask_local, factor)
    probs = jnp.exp(scores - log_total)
    grad_probs = jnp.einsum(
        "tgrd,kgd->grtk", grad_mixed, value_all, preferred_element_type=jnp.float32
    )
    weighted = jnp.sum(probs * grad_probs, axis=-1, keepdims=True)
    grad_scores = (probs * (grad_probs - weighted)).astype(jnp.bfloat16)
    grad_turned = (
        jnp.einsum("grtk,kgd->tgrd", grad_scores, key_all, preferred_element_type=jnp.float32)
        * factor
    )
    grad_keyall = (
        jnp.einsum("grtk,tgrd->kgd", grad_scores, query_low, preferred_element_type=jnp.float32)
        * factor
    )
    grad_valueall = jnp.einsum(
        "grtk,tgrd->kgd", probs.astype(jnp.bfloat16), grad_mixed, preferred_element_type=jnp.float32
    )
    grad_keys, grad_values = (
        lax.psum_scatter(
            grad_keyall.reshape(total, groups * HD).astype(jnp.bfloat16),
            "wide",
            scatter_dimension=0,
            tiled=True,
        ).astype(jnp.float32),
        lax.psum_scatter(
            grad_valueall.reshape(total, groups * HD).astype(jnp.bfloat16),
            "wide",
            scatter_dimension=0,
            tiled=True,
        ).astype(jnp.float32),
    )
    grad_qraw, gain_q = pull_query(grad_turned.reshape(tok_rows, groups * repeat, HD))
    grad_kraw, gain_k = pull_key(grad_keys.reshape(tok_rows, groups, HD))
    query_back = grad_qraw.reshape(tok_rows, groups * repeat * HD).astype(jnp.bfloat16)
    key_back = grad_kraw.reshape(tok_rows, groups * HD).astype(jnp.bfloat16)
    value_back = grad_values.astype(jnp.bfloat16)
    grad_wquery = jnp.einsum(
        "td,th->dh", hidden_one, query_back, preferred_element_type=jnp.float32
    )
    grad_wkey = jnp.einsum("td,th->dh", hidden_one, key_back, preferred_element_type=jnp.float32)
    grad_wvalue = jnp.einsum(
        "td,th->dh", hidden_one, value_back, preferred_element_type=jnp.float32
    )
    partial_one = (
        jnp.einsum("th,dh->td", query_back, w_query, preferred_element_type=jnp.float32)
        + jnp.einsum("th,dh->td", key_back, w_key, preferred_element_type=jnp.float32)
        + jnp.einsum("th,dh->td", value_back, w_value, preferred_element_type=jnp.float32)
    )
    gain_one = jnp.sum(partial_one * unit_rows(input_float), axis=0)
    grad_input = (
        grad_middle
        + pull_one(lax.psum(partial_one.astype(jnp.bfloat16), "narrow").astype(jnp.float32))[0]
    )
    weight_grads = (
        grad_wquery,
        grad_wkey,
        grad_wvalue,
        grad_wout,
        grad_wgate,
        grad_wup,
        grad_wdown,
    )
    return (output_low, grad_input, weight_grads, (gain_one, gain_two, gain_q, gain_k))


def local_general(
    layer_input,
    grad_out,
    lengths,
    w_query,
    w_key,
    w_value,
    w_out,
    w_gate,
    w_up,
    w_down,
    gain_attn,
    gain_ffn,
    gain_query,
    gain_key,
):
    width = lax.axis_size("wide")
    shards = (w_query, w_key, w_value, w_out, w_gate, w_up, w_down)
    along_rows = (True, True, True, False, True, True, False)
    gains = (gain_attn, gain_ffn, gain_query, gain_key)
    totals = tuple(
        (
            jnp.zeros(
                (
                    (piece.shape[0] * width, piece.shape[1])
                    if rows_first
                    else (piece.shape[0], piece.shape[1] * width)
                ),
                jnp.float32,
            )
            for piece, rows_first in zip(shards, along_rows)
        )
    )
    gain_terms = tuple((jnp.zeros(gain.shape, jnp.float32) for gain in gains))
    outputs = []
    grad_inputs = []
    for micro in range(layer_input.shape[0]):
        gathered = (
            lax.all_gather(w_query, "wide", axis=0, tiled=True),
            lax.all_gather(w_key, "wide", axis=0, tiled=True),
            lax.all_gather(w_value, "wide", axis=0, tiled=True),
            lax.all_gather(w_out, "wide", axis=1, tiled=True),
            lax.all_gather(w_gate, "wide", axis=0, tiled=True),
            lax.all_gather(w_up, "wide", axis=0, tiled=True),
            lax.all_gather(w_down, "wide", axis=1, tiled=True),
        )
        output, grad_input, weight_grads, gain_grads = one_batch(
            layer_input[micro], grad_out[micro], lengths[micro], gathered, gains
        )
        outputs.append(output)
        grad_inputs.append(grad_input)
        gain_terms = tuple((running + fresh for running, fresh in zip(gain_terms, gain_grads)))
        totals = tuple((running + fresh for running, fresh in zip(totals, weight_grads)))
    results = (
        lax.psum_scatter(
            totals[0].astype(jnp.bfloat16), "wide", scatter_dimension=0, tiled=True
        ).astype(jnp.float32),
        lax.psum_scatter(
            totals[1].astype(jnp.bfloat16), "wide", scatter_dimension=0, tiled=True
        ).astype(jnp.float32),
        lax.psum_scatter(
            totals[2].astype(jnp.bfloat16), "wide", scatter_dimension=0, tiled=True
        ).astype(jnp.float32),
        lax.psum_scatter(
            totals[3].astype(jnp.bfloat16), "wide", scatter_dimension=1, tiled=True
        ).astype(jnp.float32),
        lax.psum_scatter(
            totals[4].astype(jnp.bfloat16), "wide", scatter_dimension=0, tiled=True
        ).astype(jnp.float32),
        lax.psum_scatter(
            totals[5].astype(jnp.bfloat16), "wide", scatter_dimension=0, tiled=True
        ).astype(jnp.float32),
        lax.psum_scatter(
            totals[6].astype(jnp.bfloat16), "wide", scatter_dimension=1, tiled=True
        ).astype(jnp.float32),
    )
    gain_total = lax.psum(gain_terms, ("wide", "narrow"))
    return (
        jnp.stack(outputs),
        jnp.stack(grad_inputs),
        results[0],
        results[1],
        results[2],
        results[3],
        results[4],
        results[5],
        results[6],
        gain_total[0],
        gain_total[1],
        gain_total[2],
        gain_total[3],
    )


BLOCK = 256
NT = (((1,), (1,)), ((), ()))
TN = (((0,), (0,)), ((), ()))


def piece_starts(lengths_ref, micro, spot):
    start = jnp.zeros_like(spot)
    finish = jnp.int32(0)
    for piece in range(NDOC - 1):
        finish += lengths_ref[micro, piece]
        start = jnp.where(spot >= finish, finish if piece < NDOC - 2 else spot, start)
    return start


def query_rows(lengths_ref, groups, step_q):
    micro = lax.axis_index("wide") // groups
    spot = lax.broadcasted_iota(jnp.int32, (BLOCK, 1), 0) + step_q * BLOCK
    start = piece_starts(lengths_ref, micro, spot)
    first = piece_starts(lengths_ref, micro, step_q * BLOCK) // BLOCK
    spot = jnp.concatenate([spot, spot], axis=0)
    start = jnp.concatenate([start, start], axis=0)
    return spot, start, first


def attend_forward(groups, lengths_ref, qkv_ref, mixed_ref, kept_ref, log_ref):
    step_q = pl.program_id(0)
    rows = pl.ds(step_q * BLOCK, BLOCK)
    factor = 1.0 / math.sqrt(HD)
    query = jnp.concatenate([qkv_ref[rows, 0:HD], qkv_ref[rows, HD : 2 * HD]], axis=0)
    spot, start, first = query_rows(lengths_ref, groups, step_q)

    def one(step_k, carry):
        total, mixed = carry
        cols = pl.ds(step_k * BLOCK, BLOCK)
        scores = lax.dot_general(
            query, qkv_ref[cols, 2 * HD : 3 * HD], NT, preferred_element_type=jnp.float32
        )
        key_spot = lax.broadcasted_iota(jnp.int32, (1, BLOCK), 1) + step_k * BLOCK
        fits = (key_spot >= start) & (key_spot <= spot)
        exponent = jnp.where(fits, jnp.exp(scores * factor), 0.0)
        for half in range(BLOCK // HD):
            total += exponent[:, half * HD : (half + 1) * HD]
        mixed += jnp.dot(
            exponent.astype(jnp.bfloat16),
            qkv_ref[cols, 3 * HD : 4 * HD],
            preferred_element_type=jnp.float32,
        )
        return (total, mixed)

    total, mixed = lax.fori_loop(
        first,
        step_q + 1,
        one,
        (
            jnp.zeros((2 * BLOCK, HD), jnp.float32),
            jnp.zeros((2 * BLOCK, HD), jnp.float32),
        ),
    )
    total = jnp.sum(total, axis=-1, keepdims=True)
    mixed = mixed / total
    mixed = jnp.concatenate([mixed[:BLOCK], mixed[BLOCK:]], axis=1)
    mixed_ref[...] = mixed.astype(jnp.bfloat16)
    kept_ref[...] = mixed
    log_total = jnp.log(total)
    log_ref[...] = jnp.concatenate([log_total[:BLOCK], log_total[BLOCK:]], axis=1)


def attend_backward(
    groups, lengths_ref, qkv_ref, grad_ref, kept_ref, log_ref, back_ref, key_sum, value_sum
):
    step_q = pl.program_id(0)
    rows = pl.ds(step_q * BLOCK, BLOCK)
    factor = 1.0 / math.sqrt(HD)

    @pl.when(step_q == 0)
    def _():
        key_sum[...] = jnp.zeros_like(key_sum)
        value_sum[...] = jnp.zeros_like(value_sum)

    query = jnp.concatenate([qkv_ref[rows, 0:HD], qkv_ref[rows, HD : 2 * HD]], axis=0)
    grad = jnp.concatenate([grad_ref[:, 0:HD], grad_ref[:, HD : 2 * HD]], axis=0)
    kept = jnp.concatenate([kept_ref[:, 0:HD], kept_ref[:, HD : 2 * HD]], axis=0)
    log_total = jnp.concatenate([log_ref[:, 0:1], log_ref[:, 1:2]], axis=0)
    weighted = jnp.sum(grad.astype(jnp.float32) * kept, axis=-1, keepdims=True)
    spot, start, first = query_rows(lengths_ref, groups, step_q)

    def one(step_k, query_sum):
        cols = pl.ds(step_k * BLOCK, BLOCK)
        key = qkv_ref[cols, 2 * HD : 3 * HD]
        scores = lax.dot_general(query, key, NT, preferred_element_type=jnp.float32) * factor
        key_spot = lax.broadcasted_iota(jnp.int32, (1, BLOCK), 1) + step_k * BLOCK
        fits = (key_spot >= start) & (key_spot <= spot)
        probs = jnp.where(fits, jnp.exp(scores - log_total), 0.0)
        grad_probs = lax.dot_general(
            grad, qkv_ref[cols, 3 * HD : 4 * HD], NT, preferred_element_type=jnp.float32
        )
        grad_scores = (probs * (grad_probs - weighted)).astype(jnp.bfloat16)
        value_sum[cols, :] += lax.dot_general(
            probs.astype(jnp.bfloat16), grad, TN, preferred_element_type=jnp.float32
        )
        key_sum[cols, :] += lax.dot_general(
            grad_scores, query, TN, preferred_element_type=jnp.float32
        )
        return query_sum + jnp.dot(grad_scores, key, preferred_element_type=jnp.float32)

    query_sum = lax.fori_loop(first, step_q + 1, one, jnp.zeros((2 * BLOCK, HD), jnp.float32))
    query_sum = (query_sum * factor).astype(jnp.bfloat16)
    back_ref[rows, 0:HD] = query_sum[:BLOCK]
    back_ref[rows, HD : 2 * HD] = query_sum[BLOCK:]

    @pl.when(step_q == pl.num_programs(0) - 1)
    def _():
        back_ref[:, 2 * HD : 3 * HD] = (key_sum[...] * factor).astype(jnp.bfloat16)
        back_ref[:, 3 * HD : 4 * HD] = value_sum[...].astype(jnp.bfloat16)


def attention_out(qkv, lengths, groups):
    total = qkv.shape[0]
    block = lambda i, *_: (i, 0)
    return pl.pallas_call(
        functools.partial(attend_forward, groups),
        out_shape=(
            jax.ShapeDtypeStruct((total, 2 * HD), jnp.bfloat16),
            jax.ShapeDtypeStruct((total, 2 * HD), jnp.float32),
            jax.ShapeDtypeStruct((total, 2), jnp.float32),
        ),
        grid_spec=pltpu.PrefetchScalarGridSpec(
            num_scalar_prefetch=1,
            grid=(total // BLOCK,),
            in_specs=[pl.BlockSpec((total, 4 * HD), lambda i, *_: (0, 0))],
            out_specs=[
                pl.BlockSpec((BLOCK, 2 * HD), block),
                pl.BlockSpec((BLOCK, 2 * HD), block),
                pl.BlockSpec((BLOCK, 2), block),
            ],
        ),
        name="attend_forward",
    )(lengths, qkv)


def attention_back(qkv, lengths, groups, grad, kept, log_total):
    total = qkv.shape[0]
    whole = lambda i, *_: (0, 0)
    block = lambda i, *_: (i, 0)
    return pl.pallas_call(
        functools.partial(attend_backward, groups),
        out_shape=jax.ShapeDtypeStruct((total, 4 * HD), jnp.bfloat16),
        grid_spec=pltpu.PrefetchScalarGridSpec(
            num_scalar_prefetch=1,
            grid=(total // BLOCK,),
            in_specs=[
                pl.BlockSpec((total, 4 * HD), whole),
                pl.BlockSpec((BLOCK, 2 * HD), block),
                pl.BlockSpec((BLOCK, 2 * HD), block),
                pl.BlockSpec((BLOCK, 2), block),
            ],
            out_specs=pl.BlockSpec((total, 4 * HD), whole),
            scratch_shapes=[
                pltpu.VMEM((total, HD), jnp.float32),
                pltpu.VMEM((total, HD), jnp.float32),
            ],
        ),
        name="attend_backward",
    )(lengths, qkv, grad, kept, log_total)


def dot_f32(left, right, dims=(((1,), (0,)), ((), ()))):
    return lax.dot_general(left, right, dims, preferred_element_type=jnp.float32)


SUB = 64
RING = 8
STRIP = 16
AHEAD = 3
GAIN_TICKS = (0, 2, 4, 6, 11, 14, 17)
LANES = 512
MESH = pl.DeviceIdType.MESH


class Relay:
    def __init__(self, count, own, landed, cross, sems):
        self.count, self.own, self.landed, self.cross = count, own, landed, cross
        self.out_sem, self.land_sem, self.back_sem, self.cross_sem = sems
        spot = lax.axis_index("narrow")
        self.is_end = (spot == 0) | (spot == 3)
        self.is_mid = (spot == 1) | (spot == 2)
        self.inner = 1 + spot // 3
        self.other = 3 - spot
        self.outer = jnp.where(spot == 2, 3, 0)

    def to_inner(self, k):
        return pltpu.make_async_remote_copy(
            src_ref=self.own.at[k],
            dst_ref=self.landed.at[k],
            send_sem=self.out_sem.at[k],
            recv_sem=self.land_sem.at[k],
            device_id={"narrow": self.inner},
            device_id_type=MESH,
        )

    def to_other(self, k):
        return pltpu.make_async_remote_copy(
            src_ref=self.own.at[k],
            dst_ref=self.cross.at[k % RING],
            send_sem=self.out_sem.at[k],
            recv_sem=self.cross_sem.at[k % RING],
            device_id={"narrow": self.other},
            device_id_type=MESH,
        )

    def to_outer(self, k):
        return pltpu.make_async_remote_copy(
            src_ref=self.landed.at[k],
            dst_ref=self.landed.at[k],
            send_sem=self.back_sem.at[k],
            recv_sem=self.land_sem.at[k],
            device_id={"narrow": self.outer},
            device_id_type=MESH,
        )

    def greet(self, peers):
        barrier = pltpu.get_barrier_semaphore()
        for peer in peers:
            pl.semaphore_signal(barrier, inc=1, device_id={"wide": peer}, device_id_type=MESH)

        @pl.when(self.is_end)
        def _():
            pl.semaphore_signal(
                barrier, inc=1, device_id={"narrow": self.inner}, device_id_type=MESH
            )
            pl.semaphore_wait(barrier, 1 + len(peers))

        @pl.when(self.is_mid)
        def _():
            pl.semaphore_signal(
                barrier, inc=1, device_id={"narrow": self.outer}, device_id_type=MESH
            )
            pl.semaphore_signal(
                barrier, inc=1, device_id={"narrow": self.other}, device_id_type=MESH
            )
            pl.semaphore_wait(barrier, 2 + len(peers))

    def send(self, first, number):
        @pl.when(self.is_end)
        def _():
            @pl.loop(0, number)
            def _(i):
                self.to_inner(first + i).start()

    def tick(self, k):
        @pl.when(self.is_mid & (k < self.count))
        def _():
            self.to_inner(k).wait_recv()

            @pl.loop(0, SUB // STRIP)
            def _(i):
                rows = pl.ds(pl.multiple_of(i * STRIP, STRIP), STRIP)
                self.own[k, rows] = (
                    self.own[k, rows].astype(jnp.float32) + self.landed[k, rows].astype(jnp.float32)
                ).astype(jnp.bfloat16)

            self.to_other(k).start()

        @pl.when(self.is_mid & (k >= 2) & (k < self.count + 2))
        def _():
            j = k - 2
            self.to_other(j).wait_recv()

            @pl.loop(0, SUB // STRIP)
            def _(i):
                rows = pl.ds(pl.multiple_of(i * STRIP, STRIP), STRIP)
                self.landed[j, rows] = (
                    self.own[j, rows].astype(jnp.float32)
                    + self.cross[j % RING, rows].astype(jnp.float32)
                ).astype(jnp.bfloat16)

            self.to_outer(j).start()

        @pl.when(self.is_end & (k >= 4) & (k < self.count + 4))
        def _():
            self.to_outer(k - 4).wait_recv()

    def drain(self, first):
        @pl.loop(first, self.count)
        def _(k):
            self.to_inner(k).wait_send()

        @pl.loop(0, self.count)
        def _(k):
            @pl.when(self.is_mid)
            def _():
                self.to_outer(k).wait_send()


def wide_peers(width):
    spot = lax.axis_index("wide")
    return [lax.rem(spot + step, width) for step in range(1, width)]


def greet_wide(width):
    barrier = pltpu.get_barrier_semaphore()
    for peer in wide_peers(width):
        pl.semaphore_signal(barrier, inc=1, device_id={"wide": peer}, device_id_type=MESH)
    pl.semaphore_wait(barrier, width - 1)


class Exchange:
    def __init__(self, block, slot, send_sem, land_sem):
        self.block, self.slot = block, slot
        self.send_sem, self.land_sem = send_sem, land_sem
        self.spot = lax.axis_index("wide")

    def remote(self, target, source):
        return pltpu.make_async_remote_copy(
            src_ref=self.block(target),
            dst_ref=self.slot(source),
            send_sem=self.send_sem.at[target],
            recv_sem=self.land_sem.at[source],
            device_id={"wide": target},
            device_id_type=MESH,
        )

    def here(self):
        return pltpu.make_async_copy(
            self.block(self.spot), self.slot(self.spot), self.land_sem.at[self.spot]
        )

    def send(self, target):
        @pl.when(target == self.spot)
        def _():
            self.here().start()

        @pl.when(target != self.spot)
        def _():
            self.remote(target, self.spot).start()

    def sent(self, target, home=False):
        @pl.when(target != self.spot)
        def _():
            self.remote(target, self.spot).wait_send()

        if home:

            @pl.when(target == self.spot)
            def _():
                self.here().wait()

    def wait(self, source, home=True):
        if home:

            @pl.when(source == self.spot)
            def _():
                self.here().wait()

        @pl.when(source != self.spot)
        def _():
            self.remote(self.spot, source).wait_recv()


class Gather:
    def __init__(self, parts, send_sem, land_sem):
        self.parts, self.send_sem, self.land_sem = parts, send_sem, land_sem
        me = lax.axis_index("wide")
        flip = lambda spot, bit: spot + bit - 2 * bit * (spot // bit % 2)
        self.me, self.near = me, flip(me, 1)
        self.across, self.along = flip(me, 2), flip(me, 4)
        self.far = flip(self.across, 4)
        self.flip = flip

    def move(self, part, kind, source, target, device):
        return pltpu.make_async_remote_copy(
            src_ref=source,
            dst_ref=target,
            send_sem=self.send_sem.at[part, kind],
            recv_sem=self.land_sem.at[part, kind],
            device_id={"wide": device},
            device_id_type=MESH,
        )

    def going(self, part, kind):
        own, slot, half = self.parts[part]
        across, along, near = self.across, self.along, self.near
        source, target, device = (
            lambda: (own, slot(self.me), across),
            lambda: (own, slot(self.me), along),
            lambda: (own, slot(self.me), near),
            lambda: (half(along, 0), half(along, 0), across),
            lambda: (half(across, 1), half(across, 1), along),
            lambda: (slot(across), slot(across), near),
            lambda: (slot(along), slot(along), near),
            lambda: (half(self.far, 0), half(self.far, 0), near),
            lambda: (half(self.far, 1), half(self.far, 1), near),
        )[kind]()
        return self.move(part, kind, source, target, device)

    def coming(self, part, kind):
        _, slot, half = self.parts[part]
        flip = self.flip
        place = (
            lambda: slot(self.across),
            lambda: slot(self.along),
            lambda: slot(self.near),
            lambda: half(self.far, 0),
            lambda: half(self.far, 1),
            lambda: slot(flip(self.across, 1)),
            lambda: slot(flip(self.along, 1)),
            lambda: half(flip(self.far, 1), 0),
            lambda: half(flip(self.far, 1), 1),
        )[kind]()
        return self.move(part, kind, place, place, self.near)

    def here(self, part):
        own, slot, _ = self.parts[part]
        return pltpu.make_async_copy(own, slot(self.me), self.land_sem.at[part, 9])

    def first(self, part):
        for kind in (0, 1, 2):
            self.going(part, kind).start()
        self.here(part).start()

    def second(self, part):
        self.coming(part, 1).wait_recv()
        self.going(part, 3).start()
        self.coming(part, 0).wait_recv()
        self.going(part, 4).start()
        self.going(part, 6).start()
        self.going(part, 5).start()

    def third(self, part):
        self.coming(part, 3).wait_recv()
        self.going(part, 7).start()
        self.coming(part, 4).wait_recv()
        self.going(part, 8).start()

    def fourth(self, part):
        self.here(part).wait()
        for kind in (2, 5, 6, 7, 8):
            self.coming(part, kind).wait_recv()

    def drain(self):
        for part in range(len(self.parts)):
            for kind in range(9):
                self.going(part, kind).wait_send()


def project_kernel(
    input_ref,
    gain_ref,
    query_w,
    key_w,
    value_w,
    lengths_ref,
    head_gain_ref,
    hidden_out,
    raw_out,
    packed_out,
    weight_out,
    cosine_ref,
    sine_ref,
    rows_v,
    weight_v,
    hidden_v,
    raw_v,
    pack_v,
    load_sem,
    keep_sem,
    hidden_sem,
    send_sem,
    land_sem,
    part_send,
    part_land,
):
    micro, tok, model = input_ref.shape
    width = packed_out.shape[0]
    groups = width // micro
    heads = 2 * groups
    spot = lax.axis_index("wide")
    swap = Exchange(
        lambda target: pack_v.at[target], lambda source: packed_out.at[source], send_sem, land_sem
    )
    load = pltpu.make_async_copy(input_ref, rows_v, load_sem.at[0])
    load.start()
    piece = query_w.shape[0]

    def part(own, first):
        cols = pl.ds(first, own.shape[1])
        return (
            own,
            lambda s: weight_v.at[pl.ds(pl.multiple_of(s * piece, piece), piece), cols],
            lambda s, h: weight_v.at[
                pl.ds(pl.multiple_of(s * piece + h * piece // 2, piece // 2), piece // 2), cols
            ],
        )

    q_cols, k_cols = query_w.shape[1], key_w.shape[1]
    gather = Gather(
        [part(query_w, 0), part(key_w, q_cols), part(value_w, q_cols + k_cols)],
        part_send,
        part_land,
    )
    greet_wide(width)
    for p in range(3):
        gather.first(p)
    load.wait()
    hidden_copy = pltpu.make_async_copy(hidden_v, hidden_out, hidden_sem)

    @pl.loop(0, micro)
    def _(m):
        rows = rows_v[m].astype(jnp.float32)
        scale = lax.rsqrt(jnp.mean(rows * rows, axis=-1, keepdims=True) + EPSILON)
        hidden_v[m] = (rows * scale * gain_ref[...]).astype(jnp.bfloat16)

    hidden_copy.start()
    lane = lax.broadcasted_iota(jnp.int32, (1, HD), 1)
    frequency = jnp.exp(
        -math.log(THETA) * (2 * (lane % (HD // 2))).astype(jnp.float32) / HD
    )
    sign = jnp.where(lane < HD // 2, -1.0, 1.0)
    token = lax.broadcasted_iota(jnp.int32, (tok, 1), 0) + spot * tok

    @pl.loop(0, micro)
    def _(m):
        start = jnp.zeros_like(token)
        finish = jnp.int32(0)
        for piece_index in range(NDOC - 1):
            finish += lengths_ref[m, piece_index]
            start = jnp.where(token >= finish, finish, start)
        turning = (token - start).astype(jnp.float32) * frequency
        span = pl.ds(pl.multiple_of(m * tok, tok), tok)
        cosine_ref[span, :] = jnp.cos(turning)
        sine_ref[span, :] = jnp.sin(turning) * sign

    for p in range(3):
        gather.second(p)
    for p in range(3):
        gather.third(p)
    for p in range(3):
        gather.fourth(p)
    weight_copy = pltpu.make_async_copy(weight_v, weight_out, load_sem.at[1])
    weight_copy.start()

    def turn(step):
        far = micro - 1 - step
        own = spot // groups
        return (own + far) % 2 + 2 * ((own // 2 + far // 2) % 2)

    def keep(step):
        return pltpu.make_async_copy(
            raw_v.at[step % 2], raw_out.at[turn(step)], keep_sem.at[step % 2]
        )

    @pl.loop(0, micro)
    def _(step):
        m = turn(step)

        @pl.when(step >= 2)
        def _():
            keep(step - 2).wait()

        heads_all = dot_f32(hidden_v[m], weight_v[...])
        span = pl.ds(pl.multiple_of(m * tok, tok), tok)
        cosine, sine = cosine_ref[span, :], sine_ref[span, :]
        raw_v[step % 2] = heads_all[:, : (heads + groups) * HD]
        for h in range(heads + groups):
            raw = heads_all[:, h * HD : (h + 1) * HD]
            gain = head_gain_ref[0:1, :] if h < heads else head_gain_ref[1:2, :]
            unit = raw * lax.rsqrt(jnp.mean(raw * raw, axis=-1, keepdims=True) + EPSILON) * gain
            turned = unit * cosine + pltpu.roll(unit, HD // 2, 1) * sine
            g, place = (h // 2, h % 2) if h < heads else (h - heads, 2)
            pack_v[m * groups + g, :, place * HD : (place + 1) * HD] = turned.astype(jnp.bfloat16)
        for g in range(groups):
            first = (heads + groups + g) * HD
            pack_v[m * groups + g, :, 3 * HD :] = heads_all[:, first : first + HD].astype(
                jnp.bfloat16
            )
            swap.send(m * groups + g)
        keep(step).start()

    keep(micro - 2).wait()
    keep(micro - 1).wait()

    @pl.loop(0, width)
    def _(d):
        swap.sent(d)
        swap.wait(d)

    gather.drain()
    hidden_copy.wait()
    weight_copy.wait()


def project(layer_input, gain_attn, weights, lengths, head_gains, width):
    micro, tok, model = layer_input.shape
    groups = width // micro
    low = jnp.bfloat16
    anywhere = pl.BlockSpec(memory_space=pl.ANY)
    inside = pl.BlockSpec(memory_space=pltpu.VMEM)
    raw = 3 * groups * HD
    columns = sum(weight.shape[1] for weight in weights)
    return pl.pallas_call(
        project_kernel,
        out_shape=(
            jax.ShapeDtypeStruct((micro, tok, model), low),
            jax.ShapeDtypeStruct((micro, tok, raw), jnp.float32),
            jax.ShapeDtypeStruct((width, tok, 4 * HD), low),
            jax.ShapeDtypeStruct((model, columns), low),
            jax.ShapeDtypeStruct((micro * tok, HD), jnp.float32),
            jax.ShapeDtypeStruct((micro * tok, HD), jnp.float32),
        ),
        in_specs=[anywhere, inside, anywhere, anywhere, anywhere]
        + [pl.BlockSpec(memory_space=pltpu.SMEM), inside],
        out_specs=[anywhere] * 4 + [inside] * 2,
        scratch_shapes=[
            pltpu.VMEM((micro, tok, model), low),
            pltpu.VMEM((model, columns), low),
            pltpu.VMEM((micro, tok, model), low),
            pltpu.VMEM((2, tok, raw), jnp.float32),
            pltpu.VMEM((width, tok, 4 * HD), low),
            pltpu.SemaphoreType.DMA((2,)),
            pltpu.SemaphoreType.DMA((2,)),
            pltpu.SemaphoreType.DMA,
            pltpu.SemaphoreType.DMA((width,)),
            pltpu.SemaphoreType.DMA((width,)),
            pltpu.SemaphoreType.DMA((3, 9)),
            pltpu.SemaphoreType.DMA((3, 10)),
        ],
        compiler_params=pltpu.CompilerParams(
            collective_id=2, has_side_effects=True, vmem_limit_bytes=40 << 20
        ),
        cost_estimate=pl.CostEstimate(
            flops=20_000_000_000, bytes_accessed=40_000_000, transcendentals=0
        ),
        name="project",
    )(layer_input, gain_attn[None, :], *weights, lengths, head_gains)


def weights_kernel(
    back_ref,
    raw_ref,
    hidden_ref,
    mixed_ref,
    low_ref,
    late_ref,
    input_ref,
    cosine_ref,
    sine_ref,
    head_gain_ref,
    back_out,
    grad_out,
    gain_out,
    output_out,
    own,
    landed,
    cross,
    out_sem,
    relay_sem,
    return_sem,
    cross_sem,
    land_v,
    raw_v,
    hidden_v,
    mixed_v,
    low_v,
    back_v,
    grad_v,
    pair_v,
    middle_v,
    rows_v,
    load_sem,
    back_sem,
    tile_sem,
    send_sem,
    land_sem,
    pair_sems,
    late_sem,
):
    micro, tok, heads_in = mixed_ref.shape
    width = back_ref.shape[0]
    groups = width // micro
    heads = 2 * groups
    model = hidden_ref.shape[2]
    piece = model // width
    count = micro * tok
    swap = Exchange(
        lambda target: back_ref.at[target], lambda source: land_v.at[source], send_sem, land_sem
    )
    loads = [
        pltpu.make_async_copy(mixed_ref, mixed_v, load_sem.at[0]),
        pltpu.make_async_copy(low_ref, low_v, load_sem.at[1]),
        pltpu.make_async_copy(raw_ref, raw_v, load_sem.at[2]),
        pltpu.make_async_copy(hidden_ref, hidden_v, load_sem.at[3]),
    ]
    per = tok // SUB
    relay = Relay(per, own, landed, cross, (out_sem, relay_sem, return_sem, cross_sem))
    late_loads = [
        pltpu.make_async_copy(late_ref.at[0], own, late_sem.at[0]),
        pltpu.make_async_copy(late_ref.at[1], middle_v, late_sem.at[1]),
        pltpu.make_async_copy(input_ref.at[micro - 1], rows_v, late_sem.at[2]),
    ]
    for copy in late_loads + loads:
        copy.start()
    relay.greet(wide_peers(width))
    spot = lax.axis_index("wide")
    for step in range(width - 1, -1, -1):
        swap.send(lax.rem(spot + step, width))
    for copy in late_loads:
        copy.wait()
    relay.send(0, per)
    loads[0].wait()
    loads[1].wait()
    mixed_all = mixed_v[...].reshape(count, heads_in)
    for n in range(model // LANES):
        low = low_v[:, :, n * LANES : (n + 1) * LANES].reshape(count, LANES)
        part = dot_f32(mixed_all, low, TN).astype(jnp.bfloat16)
        for i in range(LANES // piece):
            for b in range(heads_in // piece):
                grad_v[
                    n * (LANES // piece) + i, :, pl.ds(2 * heads_in + b * piece, piece)
                ] = part[b * piece : (b + 1) * piece, i * piece : (i + 1) * piece]
    loads[2].wait()
    gain_out[...] = jnp.zeros_like(gain_out)

    for k in range(4):
        relay.tick(k)

    @pl.loop(0, width)
    def _(d):
        swap.wait(d)

    def back_copy(m):
        return pltpu.make_async_copy(back_v.at[m], back_out.at[m], back_sem.at[m])

    @pl.loop(0, micro)
    def _(m):
        span = pl.ds(pl.multiple_of(m * tok, tok), tok)
        cosine, sine = cosine_ref[span, :], sine_ref[span, :]
        for h in range(heads + groups):
            raw = raw_v[m, :, h * HD : (h + 1) * HD]
            kind = 0 if h < heads else 1
            gain = head_gain_ref[kind : kind + 1, :]
            g, place = (h // 2, h % 2) if h < heads else (h - heads, 2)
            grad = land_v[m * groups + g, :, place * HD : (place + 1) * HD].astype(jnp.float32)
            straight = grad * cosine + pltpu.roll(grad * sine, HD // 2, 1)
            scale = lax.rsqrt(jnp.mean(raw * raw, axis=-1, keepdims=True) + EPSILON)
            gain_out[kind : kind + 1, :] += jnp.sum(straight * (raw * scale), axis=0, keepdims=True)
            pulled = straight * gain
            along = jnp.mean(pulled * raw, axis=-1, keepdims=True)
            back_v[m, :, h * HD : (h + 1) * HD] = (
                scale * (pulled - raw * (scale * scale * along))
            ).astype(jnp.bfloat16)
        for g in range(groups):
            first = (heads + groups + g) * HD
            back_v[m, :, first : first + HD] = land_v[m * groups + g, :, 3 * HD :]
        back_copy(m).start()

        @pl.when(m % 2 == 1)
        def _():
            relay.tick(4 + m // 2)

    loads[3].wait()

    core = lax.rem(spot, 2)
    near = spot + 1 - 2 * core

    def tile_copy(c):
        return pltpu.make_async_copy(grad_v.at[2 * c + core], grad_out.at[c], tile_sem.at[c])

    def pair_copy(c):
        return pltpu.make_async_remote_copy(
            src_ref=grad_v.at[2 * c + 1 - core],
            dst_ref=pair_v.at[c],
            send_sem=pair_sems.at[0, c],
            recv_sem=pair_sems.at[1, c],
            device_id={"wide": near},
            device_id_type=MESH,
        )

    def tile(i):
        left = hidden_v[:, :, pl.ds(pl.multiple_of(i * piece, piece), piece)].reshape(count, piece)
        return dot_f32(left, back_v[...].reshape(count, 2 * heads_in), TN)

    @pl.loop(0, width // 2)
    def _(c):
        i = 2 * c + 1 - core
        grad_v[i, :, 0 : 2 * heads_in] = tile(i).astype(jnp.bfloat16)
        pair_copy(c).start()

        @pl.when(c % 2 == 1)
        def _():
            relay.tick(6 + c // 2)

    output_copy = pltpu.make_async_copy(rows_v, output_out, late_sem.at[3])
    for r in range(per):
        span = slice(r * SUB, (r + 1) * SUB)
        rows_v[span, :] = (
            rows_v[span, :].astype(jnp.float32)
            + middle_v[r].astype(jnp.float32)
            + landed[r].astype(jnp.float32)
        ).astype(jnp.bfloat16)
    output_copy.start()

    @pl.loop(0, width // 2)
    def _(c):
        i = 2 * c + core
        part = tile(i)
        pair_copy(c).wait_recv()
        grad_v[i, :, 0 : 2 * heads_in] = (
            part + pair_v[c, :, 0 : 2 * heads_in].astype(jnp.float32)
        ).astype(jnp.bfloat16)
        grad_v[i, :, 2 * heads_in :] = (
            grad_v[i, :, 2 * heads_in :].astype(jnp.float32)
            + pair_v[c, :, 2 * heads_in :].astype(jnp.float32)
        ).astype(jnp.bfloat16)
        tile_copy(c).start()

    @pl.loop(0, width // 2)
    def _(c):
        tile_copy(c).wait()
        pair_copy(c).wait_send()

    @pl.loop(0, width)
    def _(i):
        swap.sent(i)

    for m in range(micro):
        back_copy(m).wait()
    output_copy.wait()
    relay.drain(0)


def weight_gradients(
    back, raw, hidden, mixed, middle_low, late, layer_input, cosine, sine, head_gains
):
    micro, tok, heads_in = mixed.shape
    width = back.shape[0]
    model = hidden.shape[2]
    low = jnp.bfloat16
    anywhere = pl.BlockSpec(memory_space=pl.ANY)
    inside = pl.BlockSpec(memory_space=pltpu.VMEM)
    return pl.pallas_call(
        weights_kernel,
        out_shape=(
            jax.ShapeDtypeStruct((micro, tok, 2 * heads_in), low),
            jax.ShapeDtypeStruct((width // 2, model // width, 3 * heads_in), low),
            jax.ShapeDtypeStruct((2, HD), jnp.float32),
            jax.ShapeDtypeStruct((tok, model), low),
        ),
        in_specs=[anywhere] * 7 + [inside] * 3,
        out_specs=[anywhere, anywhere, inside, anywhere],
        scratch_shapes=relay_scratch(tok // SUB, model)
        + [
            pltpu.VMEM(back.shape, low),
            pltpu.VMEM(raw.shape, jnp.float32),
            pltpu.VMEM(hidden.shape, low),
            pltpu.VMEM(mixed.shape, low),
            pltpu.VMEM(middle_low.shape, low),
            pltpu.VMEM((micro, tok, 2 * heads_in), low),
            pltpu.VMEM((width, model // width, 3 * heads_in), low),
            pltpu.VMEM((width // 2, model // width, 3 * heads_in), low),
            pltpu.VMEM((tok // SUB, SUB, model), low),
            pltpu.VMEM((tok, model), low),
            pltpu.SemaphoreType.DMA((4,)),
            pltpu.SemaphoreType.DMA((micro,)),
            pltpu.SemaphoreType.DMA((width // 2,)),
            pltpu.SemaphoreType.DMA((width,)),
            pltpu.SemaphoreType.DMA((width,)),
            pltpu.SemaphoreType.DMA((2, width // 2)),
            pltpu.SemaphoreType.DMA((4,)),
        ],
        compiler_params=pltpu.CompilerParams(
            collective_id=3, has_side_effects=True, vmem_limit_bytes=48 << 20
        ),
        cost_estimate=pl.CostEstimate(
            flops=1_000_000_000, bytes_accessed=1_000_000, transcendentals=0
        ),
        name="weight_gradients",
    )(back, raw, hidden, mixed, middle_low, late, layer_input, cosine, sine, head_gains)


def relay_scratch(count, model, extra=0):
    return [
        pltpu.VMEM((count + extra, SUB, model), jnp.bfloat16),
        pltpu.VMEM((count, SUB, model), jnp.bfloat16),
        pltpu.VMEM((RING, SUB, model), jnp.bfloat16),
        pltpu.SemaphoreType.DMA((count,)),
        pltpu.SemaphoreType.DMA((count,)),
        pltpu.SemaphoreType.DMA((count,)),
        pltpu.SemaphoreType.DMA((RING,)),
    ]


def feed_kernel(
    mixed_ref,
    input_ref,
    grad_ref,
    gain_ref,
    pack_ref,
    up_w,
    down_w,
    hidden_out,
    active_out,
    gate_out,
    upper_out,
    output_out,
    middle_out,
    low_out,
    mixed_out,
    gain_out,
    weight_out,
    heads_out,
    early_out,
    late_out,
    own,
    landed,
    cross,
    out_sem,
    land_sem,
    back_sem,
    cross_sem,
    out_v,
    gate_v,
    up_v,
    down_v,
    mixed_v,
    rows_v,
    grads_v,
    hidden_v,
    stage_v,
    scale_v,
    middle_v,
    output_v,
    mixback_v,
    weight_sem,
    attn_sem,
    load_sem,
    hidden_sem,
    stage_sem,
    final_sem,
    reload_sem,
    tile_sem,
    ahead_sems,
    behind_sems,
    heads_sem,
    part_send,
    part_land,
    pair_sems,
    credit,
    late_sem,
):
    micro, tok, model = input_ref.shape
    width, _, piece = pack_ref.shape
    heads_in = out_v.shape[0]
    groups = width // micro
    per = tok // SUB
    hid = gate_v.shape[1]
    count = micro * tok
    blocks = hid // piece
    late = 3 * micro * per - per
    relay = Relay(late, own, landed, cross, (out_sem, land_sem, back_sem, cross_sem))
    n_up = hid // LANES
    n_down = model // LANES
    slots = n_up + n_down

    ahead = Exchange(
        lambda target: mixed_ref.at[target],
        lambda source: mixed_v.at[
            source // groups, :, pl.ds(pl.multiple_of((source % groups) * 2 * HD, 2 * HD), 2 * HD)
        ],
        ahead_sems.at[0],
        ahead_sems.at[1],
    )
    behind = Exchange(
        lambda target: mixback_v.at[
            target // groups % 2,
            :,
            pl.ds(pl.multiple_of((target % groups) * 2 * HD, 2 * HD), 2 * HD),
        ],
        lambda source: mixed_out.at[source],
        behind_sems.at[0],
        behind_sems.at[1],
    )
    attn_copies = [
        pltpu.make_async_copy(
            pack_ref.at[i, pl.ds(0, heads_in)],
            out_v.at[:, pl.ds(i * piece, piece)],
            attn_sem.at[i],
        )
        for i in range(width)
    ]
    weight_copies = [
        pltpu.make_async_copy(
            pack_ref.at[i, pl.ds(heads_in + j * piece, piece)],
            gate_v.at[pl.ds(i * piece, piece), pl.ds(j * piece, piece)],
            weight_sem.at[i, j],
        )
        for i in range(width)
        for j in range(blocks)
    ]

    def up_part(j):
        cols = pl.ds(j * LANES, LANES)
        return (
            up_w.at[:, cols],
            lambda s: up_v.at[pl.ds(pl.multiple_of(s * piece, piece), piece), cols],
            lambda s, h: up_v.at[
                pl.ds(pl.multiple_of(s * piece + h * piece // 2, piece // 2), piece // 2), cols
            ],
        )

    def down_part(j):
        return (
            down_w.at[pl.ds(j * LANES, LANES)],
            lambda s: down_v.at[
                pl.ds(j * LANES, LANES), pl.ds(pl.multiple_of(s * piece, piece), piece)
            ],
            lambda s, h: down_v.at[
                pl.ds(j * LANES + h * LANES // 2, LANES // 2),
                pl.ds(pl.multiple_of(s * piece, piece), piece),
            ],
        )

    gather = Gather(
        [make(j) for j in range(n_up) for make in (up_part, down_part)], part_send, part_land
    )

    def both(action, j):
        action(2 * j)
        action(2 * j + 1)

    for copy in attn_copies + weight_copies:
        copy.start()

    def loads(n):
        slot = n % 2
        return (
            pltpu.make_async_copy(input_ref.at[n % micro], rows_v.at[slot], load_sem.at[slot, 0]),
            pltpu.make_async_copy(grad_ref.at[n % micro], grads_v.at[slot], load_sem.at[slot, 1]),
        )

    def start_loads(n):
        for copy in loads(n):
            copy.start()

    def wait_loads(n):
        for copy in loads(n):
            copy.wait()

    start_loads(0)
    gain_out[...] = jnp.zeros_like(gain_out)
    relay.greet(wide_peers(width))
    spot = lax.axis_index("wide")
    for step in range(width):
        ahead.send(lax.rem(spot + step, width))
    both(gather.first, 0)
    both(gather.first, 1)
    for copy in attn_copies:
        copy.wait()

    def heads_copy(m):
        return pltpu.make_async_copy(mixed_v.at[m], heads_out.at[m], heads_sem.at[m])

    @pl.loop(0, micro)
    def _(m):
        for g in range(groups):
            ahead.wait(m * groups + g)
        heads_copy(m).start()
        for n in range(n_down):
            cols = pl.ds(n * LANES, LANES)
            part = dot_f32(mixed_v[m], out_v[:, cols]).astype(jnp.bfloat16)
            for r in range(per):
                own[m * per + r, :, cols] = part[r * SUB : (r + 1) * SUB]
        relay.send(m * per, per)

    first_ticks = per + 4

    for k in range(first_ticks):
        if k == 4:
            both(gather.second, 0)
        if k == 5:
            both(gather.first, 2)
        if k == 6:
            both(gather.second, 1)
        if k == 7:
            both(gather.third, 0)
        relay.tick(k)

    for copy in weight_copies:
        copy.wait()

    def hidden_copy(m):
        return pltpu.make_async_copy(hidden_v, hidden_out.at[m], hidden_sem)

    def stage_copies(m):
        return [
            pltpu.make_async_copy(stage_v.at[i], target.at[m], stage_sem.at[i])
            for i, target in enumerate((active_out, gate_out, upper_out))
        ]

    base = micro * per

    @pl.loop(0, micro)
    def _(m):
        slot = m % 2
        wait_loads(m)
        start_loads(m + 1)

        @pl.when(m > 0)
        def _():
            hidden_copy(m - 1).wait()
            for copy in stage_copies(m - 1):
                copy.wait()

        @pl.loop(0, per)
        def _(r):
            span = pl.ds(pl.multiple_of(r * SUB, SUB), SUB)
            middle = rows_v[slot, span, :].astype(jnp.float32) + landed[m * per + r].astype(
                jnp.float32
            )
            scale = lax.rsqrt(jnp.mean(middle * middle, axis=-1, keepdims=True) + EPSILON)
            scale_v[span, :] = scale
            hidden_v[span, :] = (middle * scale * gain_ref[...]).astype(jnp.bfloat16)

        hidden_copy(m).start()

        @pl.loop(0, n_up)
        def _(j):
            relay.tick(first_ticks + slots * m + j)
            for turn in range(n_up):

                @pl.when((m == 0) & (j == turn))
                def _():
                    if turn == 0:
                        both(gather.second, 2)
                    if turn + 1 < n_up:
                        both(gather.third, turn + 1)
                    both(gather.fourth, turn)

            cols = pl.ds(pl.multiple_of(j * LANES, LANES), LANES)
            gate = dot_f32(hidden_v[...], gate_v[:, cols])
            up_proj = dot_f32(hidden_v[...], up_v[:, cols])
            grad_active = dot_f32(grads_v[slot], down_v[cols, :], NT)
            squash = 1.0 / (1.0 + jnp.exp(-gate))
            silu = gate * squash
            stage_v[0, :, cols] = (silu * up_proj).astype(jnp.bfloat16)
            stage_v[1, :, cols] = (
                grad_active * up_proj * (squash * (1.0 + gate * (1.0 - squash)))
            ).astype(jnp.bfloat16)
            stage_v[2, :, cols] = (grad_active * silu).astype(jnp.bfloat16)
        for copy in stage_copies(m):
            copy.start()

        @pl.loop(0, n_down)
        def _(n):
            relay.tick(first_ticks + slots * m + n_up + n)
            cols = pl.ds(pl.multiple_of(n * LANES, LANES), LANES)
            back = dot_f32(stage_v[1], gate_v[cols, :], NT) + dot_f32(
                stage_v[2], up_v[cols, :], NT
            )
            ahead = dot_f32(stage_v[0], down_v[:, cols]).astype(jnp.bfloat16)
            gain_sum = jnp.zeros((1, LANES), jnp.float32)
            for r in range(per):
                part = slice(r * SUB, (r + 1) * SUB)
                own[base + 2 * per * m + r, :, cols] = back[part].astype(jnp.bfloat16)
                own[base + 2 * per * m + per + r, :, cols] = ahead[part]
                unit = (
                    rows_v[slot, pl.ds(r * SUB, SUB), cols].astype(jnp.float32)
                    + landed[m * per + r, :, cols].astype(jnp.float32)
                ) * scale_v[pl.ds(r * SUB, SUB), :]
                gain_sum += jnp.sum(back[part] * unit, axis=0, keepdims=True)
            gain_out[:, cols] += gain_sum

        relay.send(base + 2 * per * m, per)

        @pl.when(m < micro - 1)
        def _():
            relay.send(base + 2 * per * m + per, per)

    hidden_copy(micro - 1).wait()
    for copy in stage_copies(micro - 1):
        copy.wait()
    late_copies = [
        pltpu.make_async_copy(own.at[pl.ds(late, per)], late_out.at[0], late_sem.at[0]),
        pltpu.make_async_copy(
            landed.at[pl.ds((micro - 1) * per, per)], late_out.at[1], late_sem.at[1]
        ),
    ]
    for copy in late_copies:
        copy.start()

    gather.drain()
    core = lax.rem(spot, 2)
    near = gather.near

    def offer():
        pl.semaphore_signal(credit, inc=1, device_id={"wide": near}, device_id_type=MESH)

    offer()

    @pl.loop(0, base)
    def _(k):
        relay.to_inner(k).wait_send()

    def reloads(m):
        rows = pl.ds(m * tok, tok)
        return [
            pltpu.make_async_copy(hidden_out.at[m], down_v.at[rows], reload_sem.at[m, 0]),
            pltpu.make_async_copy(gate_out.at[m], gate_v.at[rows], reload_sem.at[m, 1]),
            pltpu.make_async_copy(
                upper_out.at[m], gate_v.at[pl.ds(count + m * tok, tok)], reload_sem.at[m, 2]
            ),
            pltpu.make_async_copy(active_out.at[m], up_v.at[rows], reload_sem.at[m, 3]),
        ] + [
            pltpu.make_async_copy(
                grad_ref.at[m, pl.ds(r * SUB, SUB)], own.at[m * per + r], reload_sem.at[m, 4 + r]
            )
            for r in range(per)
        ]

    for m in range(micro):
        for copy in reloads(m):
            copy.start()

    def pair_slot(q):
        return up_v.at[pl.ds(count + q * piece, piece)]

    def tile_copy(m, q):
        target = early_out.at[m] if q == 0 else weight_out.at[m, q - 1]
        return pltpu.make_async_copy(pair_slot(q), target, tile_sem.at[q])

    def pair_copy(q):
        return pltpu.make_async_remote_copy(
            src_ref=stage_v.at[q],
            dst_ref=pair_slot(q),
            send_sem=pair_sems.at[0, q],
            recv_sem=pair_sems.at[1, q],
            device_id={"wide": near},
            device_id_type=MESH,
        )

    def tile(i, q, store):
        cols = pl.ds(pl.multiple_of(i * piece, piece), piece)
        if q == 2:
            right = own[0:base, :, cols].reshape(count, piece)
            for j in range(blocks):
                span = slice(j * piece, (j + 1) * piece)
                store(span, dot_f32(up_v[0:count, span], right, TN))
        else:
            right = (gate_v[0:count], gate_v[count : 2 * count])[q]
            store(slice(0, hid), dot_f32(down_v[0:count, cols], right, TN))

    def give(m, q):
        @pl.when(m > 0)
        def _():
            pair_copy(q).wait_send()

        def store(span, part):
            stage_v[q, :, span] = part.astype(jnp.bfloat16)

        tile(2 * m + 1 - core, q, store)

    def keep(m, q):
        rows = pl.ds(count + q * piece, piece)
        pair_copy(q).wait_recv()

        def store(span, part):
            up_v[rows, span] = (part + up_v[rows, span].astype(jnp.float32)).astype(jnp.bfloat16)

        tile(2 * m + core, q, store)
        tile_copy(m, q).start()

    def final_copies(m):
        return [
            pltpu.make_async_copy(middle_v, middle_out.at[m], final_sem.at[0]),
            pltpu.make_async_copy(hidden_v, low_out.at[m], final_sem.at[1]),
        ]

    def output_copy(m):
        return pltpu.make_async_copy(output_v, output_out.at[m], final_sem.at[2])

    last_ticks = first_ticks + slots * micro
    rest = late + 4 - last_ticks
    turns = rest // micro

    @pl.loop(0, micro)
    def _(m):
        slot = m % 2
        wait_loads(m + micro)

        @pl.when(m < micro - 1)
        def _():
            start_loads(m + micro + 1)

        @pl.when(m > 0)
        def _():
            for copy in final_copies(m - 1):
                copy.wait()
            output_copy(m - 1).wait()

        @pl.when(m == 0)
        def _():
            for i in range(micro):
                for copy in reloads(i):
                    copy.wait()

        relay.tick(last_ticks + turns * m)
        give(m, 0)
        give(m, 1)
        give(m, 2)
        pl.semaphore_wait(credit, 1)
        for q in range(3):
            pair_copy(q).start()
        relay.tick(last_ticks + turns * m + 1)
        keep(m, 0)
        keep(m, 1)
        relay.tick(last_ticks + turns * m + 2)

        @pl.loop(0, per)
        def _(r):
            span = pl.ds(pl.multiple_of(r * SUB, SUB), SUB)
            middle = rows_v[slot, span, :].astype(jnp.float32) + landed[m * per + r].astype(
                jnp.float32
            )
            scale = lax.rsqrt(jnp.mean(middle * middle, axis=-1, keepdims=True) + EPSILON)
            pulled = landed[base + 2 * per * m + r].astype(jnp.float32) * gain_ref[...]
            along = jnp.mean(pulled * middle, axis=-1, keepdims=True)
            grad_middle = grads_v[slot, span, :].astype(jnp.float32) + scale * (
                pulled - middle * (scale * scale * along)
            )
            middle_v[span, :] = grad_middle
            hidden_v[span, :] = grad_middle.astype(jnp.bfloat16)

        @pl.when(m >= 2)
        def _():
            for g in range(groups):
                behind.sent((m - 2) * groups + g, home=True)

        mixback_v[m % 2] = dot_f32(hidden_v[...], out_v[...], NT).astype(jnp.bfloat16)
        for g in range(groups):
            behind.send(m * groups + g)

        @pl.when(m < micro - 1)
        def _():
            @pl.loop(0, per)
            def _(r):
                span = pl.ds(pl.multiple_of(r * SUB, SUB), SUB)
                output_v[span, :] = (
                    rows_v[slot, span, :].astype(jnp.float32)
                    + landed[m * per + r].astype(jnp.float32)
                    + landed[base + 2 * per * m + per + r].astype(jnp.float32)
                ).astype(jnp.bfloat16)

            output_copy(m).start()

        for copy in final_copies(m):
            copy.start()
        keep(m, 2)
        for q in range(3):
            tile_copy(m, q).wait()

        @pl.when(m < micro - 1)
        def _():
            offer()

    for copy in late_copies:
        copy.wait()
    for copy in final_copies(micro - 1):
        copy.wait()
    for q in range(3):
        pair_copy(q).wait_send()
    for m in range(micro):
        heads_copy(m).wait()

    @pl.loop(0, width)
    def _(d):
        ahead.sent(d)
        behind.wait(d, home=False)

    @pl.loop((micro - 2) * groups, width)
    def _(d):
        behind.sent(d, home=True)

    relay.drain(base)


def feed_forward(mixed, layer_input, grad_out, gain_ffn, pack, up_w, down_w, heads_in):
    micro, tok, model = layer_input.shape
    hid = up_w.shape[1]
    parts = 2 * (hid // LANES)
    width, _, piece = pack.shape
    groups = width // micro
    low = jnp.bfloat16
    count = 3 * micro * (tok // SUB)
    late = tok // SUB
    anywhere = pl.BlockSpec(memory_space=pl.ANY)
    inside = pl.BlockSpec(memory_space=pltpu.VMEM)
    return pl.pallas_call(
        feed_kernel,
        out_shape=(
            jax.ShapeDtypeStruct((micro, tok, model), low),
            jax.ShapeDtypeStruct((micro, tok, hid), low),
            jax.ShapeDtypeStruct((micro, tok, hid), low),
            jax.ShapeDtypeStruct((micro, tok, hid), low),
            jax.ShapeDtypeStruct((micro - 1, tok, model), low),
            jax.ShapeDtypeStruct((micro, tok, model), jnp.float32),
            jax.ShapeDtypeStruct((micro, tok, model), low),
            jax.ShapeDtypeStruct((width, tok, 2 * HD), low),
            jax.ShapeDtypeStruct((1, model), jnp.float32),
            jax.ShapeDtypeStruct((width // 2, 2, piece, hid), low),
            jax.ShapeDtypeStruct((micro, tok, heads_in), low),
            jax.ShapeDtypeStruct((width // 2, piece, hid), low),
            jax.ShapeDtypeStruct((2, late, SUB, model), low),
        ),
        in_specs=[anywhere] * 3 + [inside, anywhere, anywhere, anywhere],
        out_specs=[anywhere] * 8 + [inside] + [anywhere] * 4,
        scratch_shapes=relay_scratch(count - late, model, late)
        + [
            pltpu.VMEM((heads_in, model), low),
            pltpu.VMEM((model, hid), low),
            pltpu.VMEM((model, hid), low),
            pltpu.VMEM((hid, model), low),
            pltpu.VMEM((micro, tok, heads_in), low),
            pltpu.VMEM((2, tok, model), low),
            pltpu.VMEM((2, tok, model), low),
            pltpu.VMEM((tok, model), low),
            pltpu.VMEM((3, tok, hid), low),
            pltpu.VMEM((tok, 1), jnp.float32),
            pltpu.VMEM((tok, model), jnp.float32),
            pltpu.VMEM((tok, model), low),
            pltpu.VMEM((2, tok, heads_in), low),
            pltpu.SemaphoreType.DMA((width, hid // piece)),
            pltpu.SemaphoreType.DMA((width,)),
            pltpu.SemaphoreType.DMA((2, 2)),
            pltpu.SemaphoreType.DMA,
            pltpu.SemaphoreType.DMA((3,)),
            pltpu.SemaphoreType.DMA((3,)),
            pltpu.SemaphoreType.DMA((micro, 4 + tok // SUB)),
            pltpu.SemaphoreType.DMA((3,)),
            pltpu.SemaphoreType.DMA((2, width)),
            pltpu.SemaphoreType.DMA((2, width)),
            pltpu.SemaphoreType.DMA((micro,)),
            pltpu.SemaphoreType.DMA((parts, 9)),
            pltpu.SemaphoreType.DMA((parts, 10)),
            pltpu.SemaphoreType.DMA((2, 3)),
            pltpu.SemaphoreType.REGULAR,
            pltpu.SemaphoreType.DMA((2,)),
        ],
        compiler_params=pltpu.CompilerParams(
            collective_id=0, has_side_effects=True, vmem_limit_bytes=67043328
        ),
        cost_estimate=pl.CostEstimate(
            flops=240_000_000_000, bytes_accessed=900_000_000, transcendentals=0
        ),
        name="feed_forward",
    )(mixed, layer_input, grad_out, gain_ffn[None, :], pack, up_w, down_w)


def input_kernel(
    back_ref,
    input_ref,
    middle_ref,
    gain_ref,
    weight_ref,
    gain_two_ref,
    gain_heads_ref,
    output_out,
    gains_out,
    own,
    landed,
    cross,
    out_sem,
    land_sem,
    back_sem,
    cross_sem,
    weight_v,
    back_v,
    rows_v,
    middle_v,
    output_v,
    term_v,
    other_v,
    first_sem,
    load_sem,
    final_sem,
    term_sem,
    other_sem,
):
    micro, tok, model = input_ref.shape
    per = tok // SUB
    spot = lax.axis_index("wide")
    flips = [spot + bit - 2 * bit * (spot // bit % 2) for bit in (1, 2, 4)]
    relay = Relay(micro * per, own, landed, cross, (out_sem, land_sem, back_sem, cross_sem))
    weight_copy = pltpu.make_async_copy(weight_ref, weight_v, first_sem.at[0])
    back_copy = pltpu.make_async_copy(back_ref, back_v, first_sem.at[1])
    weight_copy.start()
    back_copy.start()

    rows_copy = pltpu.make_async_copy(input_ref, rows_v, first_sem.at[2])
    rows_copy.start()

    def load(m):
        return pltpu.make_async_copy(middle_ref.at[m], middle_v.at[m % 2], load_sem.at[m % 2])

    def final_copy(m):
        return pltpu.make_async_copy(output_v.at[m % 2], output_out.at[m], final_sem.at[m % 2])

    def pass_on(step, where):
        return pltpu.make_async_remote_copy(
            src_ref=term_v.at[step],
            dst_ref=other_v.at[step],
            send_sem=term_sem.at[step],
            recv_sem=other_sem.at[step],
            device_id=where,
            device_id_type=MESH,
        )

    targets = [{"wide": flip} for flip in flips] + [
        {"narrow": spot} for spot in (relay.inner, relay.other, relay.outer)
    ]

    def gain_step(step):
        if step == 0:
            pass_on(0, targets[0]).start()
        if 1 <= step <= 3:
            pass_on(step - 1, targets[step - 1]).wait_recv()
            term_v[step] = term_v[step - 1] + other_v[step - 1]
        if step in (1, 2):
            pass_on(step, targets[step]).start()
        if step == 3:

            @pl.when(relay.is_end)
            def _():
                pass_on(3, targets[3]).start()

        if step in (4, 5):

            @pl.when(relay.is_mid)
            def _():
                pass_on(step - 1, targets[step - 1]).wait_recv()
                term_v[step] = term_v[step - 1] + other_v[step - 1]
                pass_on(step, targets[step]).start()

        if step == 6:

            @pl.when(relay.is_mid)
            def _():
                gains_out[...] = term_v[5]
                pass_on(4, targets[4]).wait_send()
                pass_on(5, targets[5]).wait_send()

            @pl.when(relay.is_end)
            def _():
                pass_on(5, targets[5]).wait_recv()
                gains_out[...] = other_v[5]
                pass_on(3, targets[3]).wait_send()

            for early in range(3):
                pass_on(early, targets[early]).wait_send()

    load(0).start()
    relay.greet(flips)
    term_v[0] = jnp.zeros(term_v.shape[1:], jnp.float32)
    weight_copy.wait()
    back_copy.wait()
    rows_copy.wait()

    @pl.loop(0, micro)
    def _(m):
        rows = rows_v[m].astype(jnp.float32)
        scale = lax.rsqrt(jnp.mean(rows * rows, axis=-1, keepdims=True) + EPSILON)
        for n in range(model // LANES):
            cols = pl.ds(n * LANES, LANES)
            part = dot_f32(back_v[m], weight_v[cols, :], NT)
            term_v[0, 0:1, cols] += jnp.sum(
                part * (rows_v[m, :, cols].astype(jnp.float32) * scale), axis=0, keepdims=True
            )
            part = part.astype(jnp.bfloat16)
            for r in range(per):
                own[m * per + r, :, cols] = part[r * SUB : (r + 1) * SUB]

        @pl.when(m == 0)
        def _():
            relay.send(0, AHEAD)

    term_v[0, 1:2, :] = gain_two_ref[...]
    term_v[0, 2:3, 0:HD] = gain_heads_ref[0:1, :]
    term_v[0, 2:3, HD : 2 * HD] = gain_heads_ref[1:2, :]
    for k in range(4):
        if k in GAIN_TICKS:
            gain_step(GAIN_TICKS.index(k))
        relay.send(AHEAD + k, 1)
        relay.tick(k)

    @pl.loop(0, micro)
    def _(m):
        slot = m % 2

        @pl.when(m < micro - 1)
        def _():
            load(m + 1).start()

        load(m).wait()

        @pl.when(m >= 2)
        def _():
            final_copy(m - 2).wait()

        for r in range(per):
            for turn in range(micro):
                if 4 + turn * per + r in GAIN_TICKS:

                    @pl.when(m == turn)
                    def _(step=GAIN_TICKS.index(4 + turn * per + r)):
                        gain_step(step)

            @pl.when(AHEAD + 4 + m * per + r < relay.count)
            def _():
                relay.send(AHEAD + 4 + m * per + r, 1)

            relay.tick(4 + m * per + r)
            span = pl.ds(r * SUB, SUB)
            rows = rows_v[m, span, :].astype(jnp.float32)
            scale = lax.rsqrt(jnp.mean(rows * rows, axis=-1, keepdims=True) + EPSILON)
            pulled = landed[m * per + r].astype(jnp.float32) * gain_ref[...]
            along = jnp.mean(pulled * rows, axis=-1, keepdims=True)
            output_v[slot, span, :] = middle_v[slot, span, :] + scale * (
                pulled - rows * (scale * scale * along)
            )
        final_copy(m).start()

    final_copy(micro - 2).wait()
    final_copy(micro - 1).wait()
    relay.drain(0)


def input_gradient(back, layer_input, grad_middle, gain_attn, weight, gain_two, gain_heads):
    micro, tok, model = layer_input.shape
    low = jnp.bfloat16
    count = micro * (tok // SUB)
    anywhere = pl.BlockSpec(memory_space=pl.ANY)
    inside = pl.BlockSpec(memory_space=pltpu.VMEM)
    return pl.pallas_call(
        input_kernel,
        out_shape=(
            jax.ShapeDtypeStruct((micro, tok, model), jnp.float32),
            jax.ShapeDtypeStruct((8, model), jnp.float32),
        ),
        in_specs=[anywhere] * 3 + [inside, anywhere, inside, inside],
        out_specs=[anywhere, inside],
        scratch_shapes=relay_scratch(count, model)
        + [
            pltpu.VMEM(weight.shape, low),
            pltpu.VMEM((micro, tok, weight.shape[1]), low),
            pltpu.VMEM((micro, tok, model), low),
            pltpu.VMEM((2, tok, model), jnp.float32),
            pltpu.VMEM((2, tok, model), jnp.float32),
            pltpu.VMEM((6, 8, model), jnp.float32),
            pltpu.VMEM((6, 8, model), jnp.float32),
            pltpu.SemaphoreType.DMA((3,)),
            pltpu.SemaphoreType.DMA((2,)),
            pltpu.SemaphoreType.DMA((2,)),
            pltpu.SemaphoreType.DMA((6,)),
            pltpu.SemaphoreType.DMA((6,)),
        ],
        compiler_params=pltpu.CompilerParams(
            collective_id=1, has_side_effects=True, vmem_limit_bytes=48 << 20
        ),
        cost_estimate=pl.CostEstimate(
            flops=1_000_000_000, bytes_accessed=1_000_000, transcendentals=0
        ),
        name="input_gradient",
    )(back, layer_input, grad_middle, gain_attn[None, :], weight, gain_two, gain_heads)


def widen_gate(rows_ref, gate_ref):
    gate_ref[...] = rows_ref[...].astype(jnp.float32)


def finish_kernel(
    input_rows,
    first_rows,
    last_rows,
    up_rows,
    down_rows,
    attn_rows,
    out_rows,
    grad_ref,
    output_ref,
    up_ref,
    down_ref,
    query_ref,
    key_ref,
    value_ref,
    out_ref,
):
    grad_ref[...] = input_rows[...]
    inside = pl.program_id(0) < pl.num_programs(0) * 3 // 4
    output_ref[...] = jnp.where(inside, first_rows[...], last_rows[...])
    up_ref[...] = up_rows[...].astype(jnp.float32)
    down_ref[...] = down_rows[...].astype(jnp.float32)
    first = 0
    for target in (query_ref, key_ref, value_ref):
        target[...] = attn_rows[:, first : first + target.shape[1]].astype(jnp.float32)
        first += target.shape[1]
    out_ref[...] = out_rows[...].astype(jnp.float32)


def finish(grad_input, first, last, feed, attn, columns):
    steps = 8
    rows, model = grad_input.shape
    piece, hid = feed.shape[0] // 2, feed.shape[1]
    part = rows // steps
    early = first.shape[0] // part - 1
    strip = piece // steps
    blocks = hid // piece
    heads = sum(columns) // piece
    rest = (attn.shape[1] - sum(columns)) // piece
    f32 = jnp.float32
    row = lambda i: (i, 0)
    return pl.pallas_call(
        finish_kernel,
        grid=(steps,),
        out_shape=(
            jax.ShapeDtypeStruct((rows, model), f32),
            jax.ShapeDtypeStruct((rows, model), jnp.bfloat16),
            jax.ShapeDtypeStruct((piece, hid), f32),
            jax.ShapeDtypeStruct((hid, piece), f32),
        )
        + tuple(jax.ShapeDtypeStruct((piece, column), f32) for column in columns)
        + (jax.ShapeDtypeStruct((rest * piece, piece), f32),),
        in_specs=[
            pl.BlockSpec((part, model), row),
            pl.BlockSpec((part, model), lambda i: (jnp.minimum(i, early), 0)),
            pl.BlockSpec((part, model), lambda i: (jnp.maximum(i - early - 1, 0), 0)),
            pl.BlockSpec((strip, hid), row),
            pl.BlockSpec((piece, piece), lambda i: (1, jnp.minimum(i, blocks - 1))),
            pl.BlockSpec((strip, attn.shape[1]), row),
            pl.BlockSpec((piece, piece), lambda i: (0, heads + jnp.minimum(i, rest - 1))),
        ],
        out_specs=[
            pl.BlockSpec((part, model), row),
            pl.BlockSpec((part, model), row),
            pl.BlockSpec((strip, hid), row),
            pl.BlockSpec((piece, piece), lambda i: (jnp.minimum(i, blocks - 1), 0)),
        ]
        + [pl.BlockSpec((strip, column), row) for column in columns]
        + [pl.BlockSpec((piece, piece), lambda i: (jnp.minimum(i, rest - 1), 0))],
        name="finish",
    )(grad_input, first, last, feed, feed, attn, attn)


def local_batched(
    layer_input,
    grad_out,
    lengths,
    w_query,
    w_key,
    w_value,
    w_out,
    w_gate,
    w_up,
    w_down,
    gain_attn,
    gain_ffn,
    gain_query,
    gain_key,
):
    micro, tok_rows, model = layer_input.shape
    width = lax.axis_size("wide")
    groups = w_key.shape[1] // HD
    total = tok_rows * width
    piece = w_out.shape[1]

    def stacked(weight):
        return jnp.moveaxis(weight.reshape(piece, -1, piece), 1, 0).reshape(-1, piece)

    pack = lax.all_gather(
        jnp.concatenate([w_out, stacked(w_gate)], axis=0), "wide", axis=0
    )

    head_gains = jnp.stack([gain_query, gain_key])
    hidden_one, raw, packed, w_qkv, cosine, sine = project(
        layer_input, gain_attn, (w_query, w_key, w_value), lengths, head_gains, width
    )
    packed = packed.reshape(total, 4 * HD)
    mixed, kept, log_total = attention_out(packed, lengths, groups)
    (
        _,
        _,
        _,
        _,
        output,
        grad_middle,
        middle_low,
        grad_mixed,
        gain_two,
        feed_grads,
        mixed_low,
        gate_grads,
        late,
    ) = feed_forward(
        mixed.reshape(width, tok_rows, 2 * HD),
        layer_input,
        grad_out,
        gain_ffn,
        pack,
        w_up,
        w_down,
        w_out.shape[0],
    )
    cores = [list(range(core, width, 2)) for core in range(2)]

    def scatter(rows):
        return lax.psum_scatter(
            rows, "wide", scatter_dimension=0, axis_index_groups=cores, tiled=True
        )

    back = attention_back(
        packed, lengths, groups, grad_mixed.reshape(total, 2 * HD), kept, log_total
    )
    qkv_back, attn_grads, gain_heads, last_output = weight_gradients(
        back.reshape(width, tok_rows, 4 * HD),
        raw,
        hidden_one,
        mixed_low,
        middle_low,
        late,
        layer_input,
        cosine,
        sine,
        head_gains,
    )
    gate_grads = scatter(gate_grads.reshape(-1, w_gate.shape[1]))
    attn_grads, feed_grads = lax.optimization_barrier((attn_grads, feed_grads))
    attn_grads = scatter(attn_grads.reshape(model // 2, -1))
    feed_grads = scatter(feed_grads.reshape(-1, w_up.shape[1]))
    grad_input, gains = input_gradient(
        qkv_back, layer_input, grad_middle, gain_attn, w_qkv, gain_two, gain_heads
    )

    grad_gate = pl.pallas_call(
        widen_gate,
        out_shape=jax.ShapeDtypeStruct(w_gate.shape, jnp.float32),
        name="widen_gate",
    )(gate_grads)
    (
        grad_input,
        output,
        grad_up,
        grad_down,
        grad_query,
        grad_key,
        grad_value,
        grad_wout,
    ) = finish(
        grad_input.reshape(-1, model),
        output.reshape(-1, model),
        last_output,
        feed_grads,
        attn_grads,
        (w_query.shape[1], w_key.shape[1], w_value.shape[1]),
    )
    return (
        output.reshape(layer_input.shape),
        grad_input.reshape(layer_input.shape),
        grad_query,
        grad_key,
        grad_value,
        grad_wout,
        grad_gate,
        grad_up,
        grad_down,
        gains[0],
        gains[1],
        gains[2, :HD],
        gains[2, HD : 2 * HD],
    )


def local(mesh, layer_input, grad_out, lengths, w_query, w_key, *rest):
    width = mesh.shape["wide"]
    micro, tok_rows = layer_input.shape[:2]
    groups = w_key.shape[1] // HD
    fits = (
        micro * groups == width == 8
        and w_query.shape[1] == 2 * w_key.shape[1]
        and mesh.shape["narrow"] == 4
        and tok_rows == BLOCK
    )
    chosen = local_batched if fits else local_general
    return chosen(layer_input, grad_out, lengths, w_query, w_key, *rest)


def solution(mesh):
    in_specs = (
        P(None, "wide", None),
        P(None, "wide", None),
        P(),
        P("wide", "narrow"),
        P("wide", "narrow"),
        P("wide", "narrow"),
        P("narrow", "wide"),
        P("wide", "narrow"),
        P("wide", "narrow"),
        P("narrow", "wide"),
        P(),
        P(),
        P(),
        P(),
    )
    out_specs = (
        P(None, "wide", None),
        P(None, "wide", None),
        P("wide", "narrow"),
        P("wide", "narrow"),
        P("wide", "narrow"),
        P("narrow", "wide"),
        P("wide", "narrow"),
        P("wide", "narrow"),
        P("narrow", "wide"),
        P(),
        P(),
        P(),
        P(),
    )
    return jax.shard_map(
        functools.partial(local, mesh), mesh=mesh, in_specs=in_specs, out_specs=out_specs, check_vma=False)
```

```python
import functools
import math

import jax
import jax.numpy as jnp
from jax import lax
from jax.experimental import pallas as pl
from jax.experimental.pallas import tpu as pltpu
from jax.sharding import PartitionSpec as P

HD = 128
NDOC = 8


EPSILON = 1e-06
THETA = 1000000.0


def rms_norm(values, gain):
    return values * lax.rsqrt(jnp.mean(values * values, axis=-1, keepdims=True) + EPSILON) * gain


def unit_rows(values):
    return values * lax.rsqrt(jnp.mean(values * values, axis=-1, keepdims=True) + EPSILON)


def rotate(values, cosine, sine):
    midway = values.shape[-1] // 2
    turned = jnp.concatenate([-values[..., midway:], values[..., :midway]], axis=-1)
    return values * cosine + turned * sine


def layout(lengths_row, total):
    finish = jnp.cumsum(lengths_row)
    starts = finish - lengths_row
    places = jnp.arange(total, dtype=jnp.int32)
    segment = jnp.sum((places[:, None] >= finish[None, :]).astype(jnp.int32), axis=1)
    member = segment[:, None] == jnp.arange(finish.shape[0], dtype=jnp.int32)[None, :]
    opening = jnp.sum(jnp.where(member, starts[None, :], 0), axis=1)
    return (segment, places - opening)


def angles(place):
    frequency = jnp.exp(-math.log(THETA) * jnp.arange(0, HD, 2).astype(jnp.float32) / HD)
    turning = place.astype(jnp.float32)[:, None] * frequency[None, :]
    turning = jnp.concatenate([turning, turning], axis=-1)
    return (jnp.cos(turning), jnp.sin(turning))


def allowed(query_seg, query_idx, key_seg, key_idx):
    same_doc = query_seg[:, None] == key_seg[None, :]
    causal = key_idx[None, :] <= query_idx[:, None]
    usable = (key_seg[None, :] != NDOC - 1) | (key_idx[None, :] == query_idx[:, None])
    return same_doc & causal & usable


def attention_scores(query_low, key_all, mask_local, factor):
    scores = (
        jnp.einsum("tgrd,kgd->grtk", query_low, key_all, preferred_element_type=jnp.float32)
        * factor
    )
    return jnp.where(mask_local[None, None], scores, -1e30)


def one_batch(row_input, grad_row, lengths_row, gathered, gains):
    w_query, w_key, w_value, w_out, w_gate, w_up, w_down = gathered
    gain_attn, gain_ffn, gain_query, gain_key = gains
    tok_rows = row_input.shape[0]
    total = tok_rows * lax.axis_size("wide")
    groups = w_key.shape[1] // HD
    repeat = w_query.shape[1] // w_key.shape[1]
    factor = 1.0 / math.sqrt(HD)
    first_row = lax.axis_index("wide") * tok_rows
    segment, place = layout(lengths_row, total)
    positions = jnp.arange(total, dtype=jnp.int32)
    query_seg = lax.dynamic_slice_in_dim(segment, first_row, tok_rows)
    query_idx = lax.dynamic_slice_in_dim(positions, first_row, tok_rows)
    mask_local = allowed(query_seg, query_idx, segment, positions)
    cosine, sine = angles(lax.dynamic_slice_in_dim(place, first_row, tok_rows))

    def head_norm(rows, gain):
        return rotate(rms_norm(rows, gain), cosine[:, None, :], sine[:, None, :])

    input_float = row_input.astype(jnp.float32)
    grad_float = grad_row.astype(jnp.float32)
    normed_one, pull_one = jax.vjp(lambda rows: rms_norm(rows, gain_attn), input_float)
    hidden_one = normed_one.astype(jnp.bfloat16)
    query_raw = jnp.dot(hidden_one, w_query, preferred_element_type=jnp.float32).reshape(
        tok_rows, groups * repeat, HD
    )
    key_raw = jnp.dot(hidden_one, w_key, preferred_element_type=jnp.float32).reshape(
        tok_rows, groups, HD
    )
    value_low = jnp.dot(hidden_one, w_value, preferred_element_type=jnp.float32).astype(
        jnp.bfloat16
    )
    query_turned, pull_query = jax.vjp(head_norm, query_raw, gain_query)
    key_turned, pull_key = jax.vjp(head_norm, key_raw, gain_key)
    query_low = query_turned.astype(jnp.bfloat16).reshape(tok_rows, groups, repeat, HD)
    key_low = key_turned.astype(jnp.bfloat16).reshape(tok_rows, groups * HD)
    key_all, value_all = (
        lax.all_gather(key_low, "wide", axis=0, tiled=True),
        lax.all_gather(value_low, "wide", axis=0, tiled=True),
    )
    key_all = key_all.reshape(total, groups, HD)
    value_all = value_all.reshape(total, groups, HD)
    scores = attention_scores(query_low, key_all, mask_local, factor)
    highest = jnp.max(scores, axis=-1, keepdims=True)
    exponent = jnp.exp(scores - highest)
    denominator = jnp.sum(exponent, axis=-1, keepdims=True)
    log_total = highest + jnp.log(denominator)
    probs_low = (exponent / denominator).astype(jnp.bfloat16)
    mixed = jnp.einsum("grtk,kgd->tgrd", probs_low, value_all, preferred_element_type=jnp.float32)
    mixed_low = mixed.reshape(tok_rows, groups * repeat * HD).astype(jnp.bfloat16)
    attn_part = jnp.dot(mixed_low, w_out, preferred_element_type=jnp.float32)
    middle = input_float + lax.psum(attn_part.astype(jnp.bfloat16), "narrow").astype(jnp.float32)
    normed_two, pull_two = jax.vjp(lambda rows: rms_norm(rows, gain_ffn), middle)
    hidden_two = normed_two.astype(jnp.bfloat16)
    unit_two = unit_rows(middle)
    gate = jnp.dot(hidden_two, w_gate, preferred_element_type=jnp.float32)
    up_proj = jnp.dot(hidden_two, w_up, preferred_element_type=jnp.float32)
    active, pull_active = jax.vjp(
        lambda gate_in, up_in: jax.nn.silu(gate_in) * up_in, gate, up_proj
    )
    active_low = active.astype(jnp.bfloat16)
    ffn_part = jnp.dot(active_low, w_down, preferred_element_type=jnp.float32)
    output_low = (
        middle + lax.psum(ffn_part.astype(jnp.bfloat16), "narrow").astype(jnp.float32)
    ).astype(jnp.bfloat16)
    grad_wdown = jnp.einsum("tf,td->fd", active_low, grad_row, preferred_element_type=jnp.float32)
    grad_active = jnp.einsum("td,fd->tf", grad_row, w_down, preferred_element_type=jnp.float32)
    grad_gate, grad_upper = pull_active(grad_active)
    gate_back = grad_gate.astype(jnp.bfloat16)
    upper_back = grad_upper.astype(jnp.bfloat16)
    grad_wgate = jnp.einsum("td,tf->df", hidden_two, gate_back, preferred_element_type=jnp.float32)
    grad_wup = jnp.einsum("td,tf->df", hidden_two, upper_back, preferred_element_type=jnp.float32)
    partial_two = jnp.einsum(
        "tf,df->td", gate_back, w_gate, preferred_element_type=jnp.float32
    ) + jnp.einsum("tf,df->td", upper_back, w_up, preferred_element_type=jnp.float32)
    gain_two = jnp.sum(partial_two * unit_two, axis=0)
    grad_middle = (
        grad_float
        + pull_two(lax.psum(partial_two.astype(jnp.bfloat16), "narrow").astype(jnp.float32))[0]
    )
    middle_low = grad_middle.astype(jnp.bfloat16)
    grad_wout = jnp.einsum("th,td->hd", mixed_low, middle_low, preferred_element_type=jnp.float32)
    grad_mixed = jnp.einsum("td,hd->th", middle_low, w_out, preferred_element_type=jnp.float32)
    grad_mixed = grad_mixed.astype(jnp.bfloat16).reshape(tok_rows, groups, repeat, HD)
    scores = attention_scores(query_low, key_all, mask_local, factor)
    probs = jnp.exp(scores - log_total)
    grad_probs = jnp.einsum(
        "tgrd,kgd->grtk", grad_mixed, value_all, preferred_element_type=jnp.float32
    )
    weighted = jnp.sum(probs * grad_probs, axis=-1, keepdims=True)
    grad_scores = (probs * (grad_probs - weighted)).astype(jnp.bfloat16)
    grad_turned = (
        jnp.einsum("grtk,kgd->tgrd", grad_scores, key_all, preferred_element_type=jnp.float32)
        * factor
    )
    grad_keyall = (
        jnp.einsum("grtk,tgrd->kgd", grad_scores, query_low, preferred_element_type=jnp.float32)
        * factor
    )
    grad_valueall = jnp.einsum(
        "grtk,tgrd->kgd", probs.astype(jnp.bfloat16), grad_mixed, preferred_element_type=jnp.float32
    )
    grad_keys, grad_values = (
        lax.psum_scatter(
            grad_keyall.reshape(total, groups * HD).astype(jnp.bfloat16),
            "wide",
            scatter_dimension=0,
            tiled=True,
        ).astype(jnp.float32),
        lax.psum_scatter(
            grad_valueall.reshape(total, groups * HD).astype(jnp.bfloat16),
            "wide",
            scatter_dimension=0,
            tiled=True,
        ).astype(jnp.float32),
    )
    grad_qraw, gain_q = pull_query(grad_turned.reshape(tok_rows, groups * repeat, HD))
    grad_kraw, gain_k = pull_key(grad_keys.reshape(tok_rows, groups, HD))
    query_back = grad_qraw.reshape(tok_rows, groups * repeat * HD).astype(jnp.bfloat16)
    key_back = grad_kraw.reshape(tok_rows, groups * HD).astype(jnp.bfloat16)
    value_back = grad_values.astype(jnp.bfloat16)
    grad_wquery = jnp.einsum(
        "td,th->dh", hidden_one, query_back, preferred_element_type=jnp.float32
    )
    grad_wkey = jnp.einsum("td,th->dh", hidden_one, key_back, preferred_element_type=jnp.float32)
    grad_wvalue = jnp.einsum(
        "td,th->dh", hidden_one, value_back, preferred_element_type=jnp.float32
    )
    partial_one = (
        jnp.einsum("th,dh->td", query_back, w_query, preferred_element_type=jnp.float32)
        + jnp.einsum("th,dh->td", key_back, w_key, preferred_element_type=jnp.float32)
        + jnp.einsum("th,dh->td", value_back, w_value, preferred_element_type=jnp.float32)
    )
    gain_one = jnp.sum(partial_one * unit_rows(input_float), axis=0)
    grad_input = (
        grad_middle
        + pull_one(lax.psum(partial_one.astype(jnp.bfloat16), "narrow").astype(jnp.float32))[0]
    )
    weight_grads = (
        grad_wquery,
        grad_wkey,
        grad_wvalue,
        grad_wout,
        grad_wgate,
        grad_wup,
        grad_wdown,
    )
    return (output_low, grad_input, weight_grads, (gain_one, gain_two, gain_q, gain_k))


def local_general(
    layer_input,
    grad_out,
    lengths,
    w_query,
    w_key,
    w_value,
    w_out,
    w_gate,
    w_up,
    w_down,
    gain_attn,
    gain_ffn,
    gain_query,
    gain_key,
):
    width = lax.axis_size("wide")
    shards = (w_query, w_key, w_value, w_out, w_gate, w_up, w_down)
    along_rows = (True, True, True, False, True, True, False)
    gains = (gain_attn, gain_ffn, gain_query, gain_key)
    totals = tuple(
        (
            jnp.zeros(
                (
                    (piece.shape[0] * width, piece.shape[1])
                    if rows_first
                    else (piece.shape[0], piece.shape[1] * width)
                ),
                jnp.float32,
            )
            for piece, rows_first in zip(shards, along_rows)
        )
    )
    gain_terms = tuple((jnp.zeros(gain.shape, jnp.float32) for gain in gains))
    outputs = []
    grad_inputs = []
    for micro in range(layer_input.shape[0]):
        gathered = (
            lax.all_gather(w_query, "wide", axis=0, tiled=True),
            lax.all_gather(w_key, "wide", axis=0, tiled=True),
            lax.all_gather(w_value, "wide", axis=0, tiled=True),
            lax.all_gather(w_out, "wide", axis=1, tiled=True),
            lax.all_gather(w_gate, "wide", axis=0, tiled=True),
            lax.all_gather(w_up, "wide", axis=0, tiled=True),
            lax.all_gather(w_down, "wide", axis=1, tiled=True),
        )
        output, grad_input, weight_grads, gain_grads = one_batch(
            layer_input[micro], grad_out[micro], lengths[micro], gathered, gains
        )
        outputs.append(output)
        grad_inputs.append(grad_input)
        gain_terms = tuple((running + fresh for running, fresh in zip(gain_terms, gain_grads)))
        totals = tuple((running + fresh for running, fresh in zip(totals, weight_grads)))
    results = (
        lax.psum_scatter(
            totals[0].astype(jnp.bfloat16), "wide", scatter_dimension=0, tiled=True
        ).astype(jnp.float32),
        lax.psum_scatter(
            totals[1].astype(jnp.bfloat16), "wide", scatter_dimension=0, tiled=True
        ).astype(jnp.float32),
        lax.psum_scatter(
            totals[2].astype(jnp.bfloat16), "wide", scatter_dimension=0, tiled=True
        ).astype(jnp.float32),
        lax.psum_scatter(
            totals[3].astype(jnp.bfloat16), "wide", scatter_dimension=1, tiled=True
        ).astype(jnp.float32),
        lax.psum_scatter(
            totals[4].astype(jnp.bfloat16), "wide", scatter_dimension=0, tiled=True
        ).astype(jnp.float32),
        lax.psum_scatter(
            totals[5].astype(jnp.bfloat16), "wide", scatter_dimension=0, tiled=True
        ).astype(jnp.float32),
        lax.psum_scatter(
            totals[6].astype(jnp.bfloat16), "wide", scatter_dimension=1, tiled=True
        ).astype(jnp.float32),
    )
    gain_total = lax.psum(gain_terms, ("wide", "narrow"))
    return (
        jnp.stack(outputs),
        jnp.stack(grad_inputs),
        results[0],
        results[1],
        results[2],
        results[3],
        results[4],
        results[5],
        results[6],
        gain_total[0],
        gain_total[1],
        gain_total[2],
        gain_total[3],
    )


BLOCK = 256
HEAD_GROUPS = 2
NT = (((1,), (1,)), ((), ()))
TN = (((0,), (0,)), ((), ()))


def piece_starts(lengths_ref, micro, spot):
    start = jnp.zeros_like(spot)
    finish = jnp.int32(0)
    for piece in range(NDOC - 1):
        finish += lengths_ref[micro, piece]
        start = jnp.where(spot >= finish, finish if piece < NDOC - 2 else spot, start)
    return start


def query_lanes(lengths_ref, step_q):
    micro = lax.axis_index("wide") // HEAD_GROUPS
    lane = lax.broadcasted_iota(jnp.int32, (1, 2 * BLOCK), 1)
    spot = lane % BLOCK + step_q * BLOCK
    return spot, piece_starts(lengths_ref, micro, spot)


def key_fits(step_k, spot, start):
    key_spot = lax.broadcasted_iota(jnp.int32, (BLOCK, 1), 0) + step_k * BLOCK
    return (key_spot >= start) & (key_spot <= spot)


def attend_forward(lengths_ref, qkv_ref, mixed_ref, kept_ref, log_ref):
    step_q = pl.program_id(0)
    rows = pl.ds(step_q * BLOCK, BLOCK)
    factor = 1.0 / math.sqrt(HD)
    query = jnp.concatenate([qkv_ref[rows, 0:HD], qkv_ref[rows, HD : 2 * HD]], axis=0)
    spot, start = query_lanes(lengths_ref, step_q)
    micro = lax.axis_index("wide") // HEAD_GROUPS
    first = piece_starts(lengths_ref, micro, step_q * BLOCK) // BLOCK

    def one(step_k, carry):
        total, total_low, mixed = carry
        cols = pl.ds(step_k * BLOCK, BLOCK)
        scores = dot_f32(qkv_ref[cols, 2 * HD : 3 * HD], query, NT)
        exponent = jnp.where(key_fits(step_k, spot, start), jnp.exp(scores * factor), 0.0)
        low = exponent.astype(jnp.bfloat16)
        total += jnp.sum(exponent.reshape(-1, 8, 2 * BLOCK), axis=0)
        total_low += jnp.sum(low.astype(jnp.float32).reshape(-1, 8, 2 * BLOCK), axis=0)
        mixed += dot_f32(qkv_ref[cols, 3 * HD : 4 * HD], low, TN)
        return (total, total_low, mixed)

    zeros = jnp.zeros((8, 2 * BLOCK), jnp.float32)
    total, total_low, mixed = lax.fori_loop(
        first, step_q + 1, one, (zeros, zeros, jnp.zeros((HD, 2 * BLOCK), jnp.float32))
    )
    mixed = (mixed / jnp.sum(total_low, axis=0, keepdims=True)).T
    mixed = jnp.concatenate([mixed[:BLOCK], mixed[BLOCK:]], axis=1)
    mixed_ref[...] = mixed.astype(jnp.bfloat16)
    kept_ref[...] = mixed
    log_total = jnp.log(jnp.sum(total, axis=0, keepdims=True))
    log_ref[...] = jnp.broadcast_to(log_total, zeros.shape)[None]


def attention_out(qkv, lengths):
    total = qkv.shape[0]
    block = lambda i, *_: (i, 0)
    return pl.pallas_call(
        attend_forward,
        out_shape=(
            jax.ShapeDtypeStruct((total, 2 * HD), jnp.bfloat16),
            jax.ShapeDtypeStruct((total, 2 * HD), jnp.float32),
            jax.ShapeDtypeStruct((total // BLOCK, 8, 2 * BLOCK), jnp.float32),
        ),
        grid_spec=pltpu.PrefetchScalarGridSpec(
            num_scalar_prefetch=1,
            grid=(total // BLOCK,),
            in_specs=[pl.BlockSpec((total, 4 * HD), lambda i, *_: (0, 0))],
            out_specs=[
                pl.BlockSpec((BLOCK, 2 * HD), block),
                pl.BlockSpec((BLOCK, 2 * HD), block),
                pl.BlockSpec((1, 8, 2 * BLOCK), lambda i, *_: (i, 0, 0)),
            ],
        ),
        name="attend_forward",
    )(lengths, qkv)


def dot_f32(left, right, dims=(((1,), (0,)), ((), ()))):
    return lax.dot_general(left, right, dims, preferred_element_type=jnp.float32)


SUB = 64
RING = 8
STRIP = 16
AHEAD = 3
GAIN_TICKS = (0, 2, 4, 6, 11, 14, 17)
LANES = 512
MESH = pl.DeviceIdType.MESH


class Relay:
    def __init__(self, count, own, landed, cross, sems):
        self.count, self.own, self.landed, self.cross = count, own, landed, cross
        self.out_sem, self.land_sem, self.back_sem, self.cross_sem = sems
        spot = lax.axis_index("narrow")
        self.is_end = (spot == 0) | (spot == 3)
        self.is_mid = (spot == 1) | (spot == 2)
        self.inner = 1 + spot // 3
        self.other = 3 - spot
        self.outer = jnp.where(spot == 2, 3, 0)

    def to_inner(self, k):
        return pltpu.make_async_remote_copy(
            src_ref=self.own.at[k],
            dst_ref=self.landed.at[k],
            send_sem=self.out_sem.at[k],
            recv_sem=self.land_sem.at[k],
            device_id={"narrow": self.inner},
            device_id_type=MESH,
        )

    def to_other(self, k):
        return pltpu.make_async_remote_copy(
            src_ref=self.own.at[k],
            dst_ref=self.cross.at[k % RING],
            send_sem=self.out_sem.at[k],
            recv_sem=self.cross_sem.at[k % RING],
            device_id={"narrow": self.other},
            device_id_type=MESH,
        )

    def to_outer(self, k):
        return pltpu.make_async_remote_copy(
            src_ref=self.landed.at[k],
            dst_ref=self.landed.at[k],
            send_sem=self.back_sem.at[k],
            recv_sem=self.land_sem.at[k],
            device_id={"narrow": self.outer},
            device_id_type=MESH,
        )

    def greet(self, peers):
        barrier = pltpu.get_barrier_semaphore()
        for peer in peers:
            pl.semaphore_signal(barrier, inc=1, device_id={"wide": peer}, device_id_type=MESH)

        @pl.when(self.is_end)
        def _():
            pl.semaphore_signal(
                barrier, inc=1, device_id={"narrow": self.inner}, device_id_type=MESH
            )
            pl.semaphore_wait(barrier, 1 + len(peers))

        @pl.when(self.is_mid)
        def _():
            pl.semaphore_signal(
                barrier, inc=1, device_id={"narrow": self.outer}, device_id_type=MESH
            )
            pl.semaphore_signal(
                barrier, inc=1, device_id={"narrow": self.other}, device_id_type=MESH
            )
            pl.semaphore_wait(barrier, 2 + len(peers))

    def send(self, first, number):
        @pl.when(self.is_end)
        def _():
            @pl.loop(0, number)
            def _(i):
                self.to_inner(first + i).start()

    def tick(self, k):
        @pl.when(self.is_mid & (k < self.count))
        def _():
            self.to_inner(k).wait_recv()

            @pl.loop(0, SUB // STRIP)
            def _(i):
                rows = pl.ds(pl.multiple_of(i * STRIP, STRIP), STRIP)
                self.own[k, rows] = (
                    self.own[k, rows].astype(jnp.float32) + self.landed[k, rows].astype(jnp.float32)
                ).astype(jnp.bfloat16)

            self.to_other(k).start()

        @pl.when(self.is_mid & (k >= 2) & (k < self.count + 2))
        def _():
            j = k - 2
            self.to_other(j).wait_recv()

            @pl.loop(0, SUB // STRIP)
            def _(i):
                rows = pl.ds(pl.multiple_of(i * STRIP, STRIP), STRIP)
                self.landed[j, rows] = (
                    self.own[j, rows].astype(jnp.float32)
                    + self.cross[j % RING, rows].astype(jnp.float32)
                ).astype(jnp.bfloat16)

            self.to_outer(j).start()

        @pl.when(self.is_end & (k >= 4) & (k < self.count + 4))
        def _():
            self.to_outer(k - 4).wait_recv()

    def drain(self, first):
        @pl.loop(first, self.count)
        def _(k):
            self.to_inner(k).wait_send()

        @pl.loop(0, self.count)
        def _(k):
            @pl.when(self.is_mid)
            def _():
                self.to_outer(k).wait_send()


def wide_peers(width):
    spot = lax.axis_index("wide")
    return [lax.rem(spot + step, width) for step in range(1, width)]


def greet_wide(width):
    barrier = pltpu.get_barrier_semaphore()
    for peer in wide_peers(width):
        pl.semaphore_signal(barrier, inc=1, device_id={"wide": peer}, device_id_type=MESH)
    pl.semaphore_wait(barrier, width - 1)


class Exchange:
    def __init__(self, block, slot, send_sem, land_sem):
        self.block, self.slot = block, slot
        self.send_sem, self.land_sem = send_sem, land_sem
        self.spot = lax.axis_index("wide")

    def remote(self, target, source):
        return pltpu.make_async_remote_copy(
            src_ref=self.block(target),
            dst_ref=self.slot(source),
            send_sem=self.send_sem.at[target],
            recv_sem=self.land_sem.at[source],
            device_id={"wide": target},
            device_id_type=MESH,
        )

    def here(self):
        return pltpu.make_async_copy(
            self.block(self.spot), self.slot(self.spot), self.land_sem.at[self.spot]
        )

    def send(self, target):
        @pl.when(target == self.spot)
        def _():
            self.here().start()

        @pl.when(target != self.spot)
        def _():
            self.remote(target, self.spot).start()

    def sent(self, target, home=False):
        @pl.when(target != self.spot)
        def _():
            self.remote(target, self.spot).wait_send()

        if home:

            @pl.when(target == self.spot)
            def _():
                self.here().wait()

    def wait(self, source, home=True):
        if home:

            @pl.when(source == self.spot)
            def _():
                self.here().wait()

        @pl.when(source != self.spot)
        def _():
            self.remote(self.spot, source).wait_recv()


class Gather:
    def __init__(self, parts, send_sem, land_sem):
        self.parts, self.send_sem, self.land_sem = parts, send_sem, land_sem
        me = lax.axis_index("wide")
        flip = lambda spot, bit: spot + bit - 2 * bit * (spot // bit % 2)
        self.me, self.near = me, flip(me, 1)
        self.across, self.along = flip(me, 2), flip(me, 4)
        self.far = flip(self.across, 4)
        self.flip = flip

    def move(self, part, kind, source, target, device):
        return pltpu.make_async_remote_copy(
            src_ref=source,
            dst_ref=target,
            send_sem=self.send_sem.at[part, kind],
            recv_sem=self.land_sem.at[part, kind],
            device_id={"wide": device},
            device_id_type=MESH,
        )

    def going(self, part, kind):
        own, slot, half = self.parts[part]
        across, along, near = self.across, self.along, self.near
        source, target, device = (
            lambda: (own, slot(self.me), across),
            lambda: (own, slot(self.me), along),
            lambda: (own, slot(self.me), near),
            lambda: (half(along, 0), half(along, 0), across),
            lambda: (half(across, 1), half(across, 1), along),
            lambda: (slot(across), slot(across), near),
            lambda: (slot(along), slot(along), near),
            lambda: (half(self.far, 0), half(self.far, 0), near),
            lambda: (half(self.far, 1), half(self.far, 1), near),
        )[kind]()
        return self.move(part, kind, source, target, device)

    def coming(self, part, kind):
        _, slot, half = self.parts[part]
        flip = self.flip
        place = (
            lambda: slot(self.across),
            lambda: slot(self.along),
            lambda: slot(self.near),
            lambda: half(self.far, 0),
            lambda: half(self.far, 1),
            lambda: slot(flip(self.across, 1)),
            lambda: slot(flip(self.along, 1)),
            lambda: half(flip(self.far, 1), 0),
            lambda: half(flip(self.far, 1), 1),
        )[kind]()
        return self.move(part, kind, place, place, self.near)

    def here(self, part):
        own, slot, _ = self.parts[part]
        return pltpu.make_async_copy(own, slot(self.me), self.land_sem.at[part, 9])

    def first(self, part):
        for kind in (0, 1, 2):
            self.going(part, kind).start()
        self.here(part).start()

    def second(self, part):
        self.coming(part, 1).wait_recv()
        self.going(part, 3).start()
        self.coming(part, 0).wait_recv()
        self.going(part, 4).start()
        self.going(part, 6).start()
        self.going(part, 5).start()

    def third(self, part):
        self.coming(part, 3).wait_recv()
        self.going(part, 7).start()
        self.coming(part, 4).wait_recv()
        self.going(part, 8).start()

    def fourth(self, part):
        self.here(part).wait()
        for kind in (2, 5, 6, 7, 8):
            self.coming(part, kind).wait_recv()

    def drain(self):
        for part in range(len(self.parts)):
            for kind in range(9):
                self.going(part, kind).wait_send()


def project_kernel(
    input_ref,
    gain_ref,
    query_w,
    key_w,
    value_w,
    lengths_ref,
    head_gain_ref,
    hidden_out,
    raw_out,
    packed_out,
    weight_out,
    cosine_ref,
    sine_ref,
    rows_v,
    weight_v,
    hidden_v,
    raw_v,
    pack_v,
    load_sem,
    keep_sem,
    hidden_sem,
    send_sem,
    land_sem,
    part_send,
    part_land,
):
    micro, tok, model = input_ref.shape
    width = packed_out.shape[0]
    groups = width // micro
    heads = 2 * groups
    spot = lax.axis_index("wide")
    swap = Exchange(
        lambda target: pack_v.at[target], lambda source: packed_out.at[source], send_sem, land_sem
    )
    load = pltpu.make_async_copy(input_ref, rows_v, load_sem.at[0])
    load.start()
    piece = query_w.shape[0]

    def part(own, first):
        cols = pl.ds(first, own.shape[1])
        return (
            own,
            lambda s: weight_v.at[pl.ds(pl.multiple_of(s * piece, piece), piece), cols],
            lambda s, h: weight_v.at[
                pl.ds(pl.multiple_of(s * piece + h * piece // 2, piece // 2), piece // 2), cols
            ],
        )

    q_cols, k_cols = query_w.shape[1], key_w.shape[1]
    gather = Gather(
        [part(query_w, 0), part(key_w, q_cols), part(value_w, q_cols + k_cols)],
        part_send,
        part_land,
    )
    greet_wide(width)
    for p in range(3):
        gather.first(p)
    load.wait()
    hidden_copy = pltpu.make_async_copy(hidden_v, hidden_out, hidden_sem)

    @pl.loop(0, micro)
    def _(m):
        rows = rows_v[m].astype(jnp.float32)
        scale = lax.rsqrt(jnp.mean(rows * rows, axis=-1, keepdims=True) + EPSILON)
        hidden_v[m] = (rows * scale * gain_ref[...]).astype(jnp.bfloat16)

    hidden_copy.start()
    lane = lax.broadcasted_iota(jnp.int32, (1, HD), 1)
    frequency = jnp.exp(
        -math.log(THETA) * (2 * (lane % (HD // 2))).astype(jnp.float32) / HD
    )
    sign = jnp.where(lane < HD // 2, -1.0, 1.0)
    token = lax.broadcasted_iota(jnp.int32, (tok, 1), 0) + spot * tok

    @pl.loop(0, micro)
    def _(m):
        start = jnp.zeros_like(token)
        finish = jnp.int32(0)
        for piece_index in range(NDOC - 1):
            finish += lengths_ref[m, piece_index]
            start = jnp.where(token >= finish, finish, start)
        turning = (token - start).astype(jnp.float32) * frequency
        span = pl.ds(pl.multiple_of(m * tok, tok), tok)
        cosine_ref[span, :] = jnp.cos(turning)
        sine_ref[span, :] = jnp.sin(turning) * sign

    for p in range(3):
        gather.second(p)
    for p in range(3):
        gather.third(p)
    for p in range(3):
        gather.fourth(p)
    weight_copy = pltpu.make_async_copy(weight_v, weight_out, load_sem.at[1])
    weight_copy.start()

    def turn(step):
        far = micro - 1 - step
        own = spot // groups
        return (own + far) % 2 + 2 * ((own // 2 + far // 2) % 2)

    def keep(step):
        return pltpu.make_async_copy(
            raw_v.at[step % 2], raw_out.at[turn(step)], keep_sem.at[step % 2]
        )

    @pl.loop(0, micro)
    def _(step):
        m = turn(step)

        @pl.when(step >= 2)
        def _():
            keep(step - 2).wait()

        heads_all = dot_f32(hidden_v[m], weight_v[...])
        span = pl.ds(pl.multiple_of(m * tok, tok), tok)
        cosine, sine = cosine_ref[span, :], sine_ref[span, :]
        raw_v[step % 2] = heads_all[:, : (heads + groups) * HD]
        for h in range(heads + groups):
            raw = heads_all[:, h * HD : (h + 1) * HD]
            gain = head_gain_ref[0:1, :] if h < heads else head_gain_ref[1:2, :]
            unit = raw * lax.rsqrt(jnp.mean(raw * raw, axis=-1, keepdims=True) + EPSILON) * gain
            turned = unit * cosine + pltpu.roll(unit, HD // 2, 1) * sine
            g, place = (h // 2, h % 2) if h < heads else (h - heads, 2)
            pack_v[m * groups + g, :, place * HD : (place + 1) * HD] = turned.astype(jnp.bfloat16)
        for g in range(groups):
            first = (heads + groups + g) * HD
            pack_v[m * groups + g, :, 3 * HD :] = heads_all[:, first : first + HD].astype(
                jnp.bfloat16
            )
            swap.send(m * groups + g)
        keep(step).start()

    keep(micro - 2).wait()
    keep(micro - 1).wait()

    @pl.loop(0, width)
    def _(d):
        swap.sent(d)
        swap.wait(d)

    gather.drain()
    hidden_copy.wait()
    weight_copy.wait()


def project(layer_input, gain_attn, weights, lengths, head_gains, width):
    micro, tok, model = layer_input.shape
    groups = width // micro
    low = jnp.bfloat16
    anywhere = pl.BlockSpec(memory_space=pl.ANY)
    inside = pl.BlockSpec(memory_space=pltpu.VMEM)
    raw = 3 * groups * HD
    columns = sum(weight.shape[1] for weight in weights)
    return pl.pallas_call(
        project_kernel,
        out_shape=(
            jax.ShapeDtypeStruct((micro, tok, model), low),
            jax.ShapeDtypeStruct((micro, tok, raw), jnp.float32),
            jax.ShapeDtypeStruct((width, tok, 4 * HD), low),
            jax.ShapeDtypeStruct((model, columns), low),
            jax.ShapeDtypeStruct((micro * tok, HD), jnp.float32),
            jax.ShapeDtypeStruct((micro * tok, HD), jnp.float32),
        ),
        in_specs=[anywhere, inside, anywhere, anywhere, anywhere]
        + [pl.BlockSpec(memory_space=pltpu.SMEM), inside],
        out_specs=[anywhere] * 4 + [inside] * 2,
        scratch_shapes=[
            pltpu.VMEM((micro, tok, model), low),
            pltpu.VMEM((model, columns), low),
            pltpu.VMEM((micro, tok, model), low),
            pltpu.VMEM((2, tok, raw), jnp.float32),
            pltpu.VMEM((width, tok, 4 * HD), low),
            pltpu.SemaphoreType.DMA((2,)),
            pltpu.SemaphoreType.DMA((2,)),
            pltpu.SemaphoreType.DMA,
            pltpu.SemaphoreType.DMA((width,)),
            pltpu.SemaphoreType.DMA((width,)),
            pltpu.SemaphoreType.DMA((3, 9)),
            pltpu.SemaphoreType.DMA((3, 10)),
        ],
        compiler_params=pltpu.CompilerParams(
            collective_id=2, has_side_effects=True, vmem_limit_bytes=40 << 20
        ),
        cost_estimate=pl.CostEstimate(
            flops=20_000_000_000, bytes_accessed=40_000_000, transcendentals=0
        ),
        name="project",
    )(layer_input, gain_attn[None, :], *weights, lengths, head_gains)


def weights_kernel(
    lengths_ref,
    qkv_ref,
    upper_ref,
    kept_ref,
    log_ref,
    raw_ref,
    hidden_ref,
    mixed_ref,
    low_ref,
    late_ref,
    input_ref,
    cosine_ref,
    sine_ref,
    head_gain_ref,
    back_out,
    grad_out,
    gain_out,
    output_out,
    own,
    landed,
    cross,
    out_sem,
    relay_sem,
    return_sem,
    cross_sem,
    land_v,
    raw_v,
    hidden_v,
    mixed_v,
    low_v,
    back_v,
    grad_v,
    pair_v,
    middle_v,
    rows_v,
    qkv_v,
    upper_v,
    kept_v,
    log_v,
    sent_v,
    query_sum,
    key_sum,
    value_sum,
    load_sem,
    back_sem,
    tile_sem,
    send_sems,
    land_sems,
    pair_sems,
    late_sem,
    attn_sem,
):
    micro, tok, heads_in = mixed_ref.shape
    width = upper_ref.shape[0]
    groups = width // micro
    heads = 2 * groups
    model = hidden_ref.shape[2]
    piece = model // width
    count = micro * tok
    factor = 1.0 / math.sqrt(HD)
    halves = (pl.ds(0, 2 * HD), pl.ds(2 * HD, 2 * HD))
    swaps = [
        Exchange(
            lambda target, cols=cols: sent_v.at[target, :, cols],
            lambda source, cols=cols: land_v.at[source, :, cols],
            send_sems.at[i],
            land_sems.at[i],
        )
        for i, cols in enumerate(halves)
    ]
    attn_loads = [
        pltpu.make_async_copy(source, target, attn_sem.at[i])
        for i, (source, target) in enumerate(
            ((qkv_ref, qkv_v), (upper_ref, upper_v), (kept_ref, kept_v), (log_ref, log_v))
        )
    ]
    loads = [
        pltpu.make_async_copy(mixed_ref, mixed_v, load_sem.at[0]),
        pltpu.make_async_copy(low_ref, low_v, load_sem.at[1]),
        pltpu.make_async_copy(raw_ref, raw_v, load_sem.at[2]),
        pltpu.make_async_copy(hidden_ref, hidden_v, load_sem.at[3]),
    ]
    per = tok // SUB
    relay = Relay(per, own, landed, cross, (out_sem, relay_sem, return_sem, cross_sem))
    late_loads = [
        pltpu.make_async_copy(late_ref.at[0], own, late_sem.at[0]),
        pltpu.make_async_copy(late_ref.at[1], middle_v, late_sem.at[1]),
        pltpu.make_async_copy(input_ref.at[micro - 1], rows_v, late_sem.at[2]),
    ]
    for copy in attn_loads + late_loads + loads:
        copy.start()
    key_sum[...] = jnp.zeros_like(key_sum)
    value_sum[...] = jnp.zeros_like(value_sum)
    relay.greet(wide_peers(width))
    spot = lax.axis_index("wide")
    for copy in late_loads:
        copy.wait()
    relay.send(0, per)
    for copy in attn_loads:
        copy.wait()
    band = width * tok // 2 // BLOCK

    @pl.loop(0, width)
    def _(step):
        far = micro - 1 - step // 2
        chip = spot // 2
        turn = (chip + far) % 2 + 2 * ((chip // 2 + far // 2) % 2)
        step_q = 2 * turn + step % 2
        rows = pl.ds(pl.multiple_of(step_q * BLOCK, BLOCK), BLOCK)
        query = jnp.concatenate([qkv_v[rows, 0:HD], qkv_v[rows, HD : 2 * HD]], axis=0)
        grad = jnp.concatenate([upper_v[step_q, :, 0:HD], upper_v[step_q, :, HD : 2 * HD]], axis=0)
        kept = jnp.concatenate([kept_v[rows, 0:HD], kept_v[rows, HD : 2 * HD]], axis=0)
        weighted = lax.dot_general(
            jnp.ones((8, HD), jnp.float32),
            grad.astype(jnp.float32) * kept,
            NT,
            precision=lax.Precision.HIGHEST,
            preferred_element_type=jnp.float32,
        )[0:1]
        log_total = log_v[step_q, 0:1, :]
        spots, start = query_lanes(lengths_ref, step_q)
        query_sum[...] = jnp.zeros_like(query_sum)

        @pl.loop(0, band + 1)
        def _(t):
            step_k = step_q - band + t

            @pl.when(step_k >= 0)
            def _():
                cols = pl.ds(pl.multiple_of(step_k * BLOCK, BLOCK), BLOCK)
                key = qkv_v[cols, 2 * HD : 3 * HD]
                scores = dot_f32(key, query, NT) * factor
                probs = jnp.where(
                    key_fits(step_k, spots, start), jnp.exp(scores - log_total), 0.0
                )
                grad_probs = dot_f32(qkv_v[cols, 3 * HD : 4 * HD], grad, NT)
                grad_scores = (probs * (grad_probs - weighted)).astype(jnp.bfloat16)
                value_sum[cols, :] += dot_f32(probs.astype(jnp.bfloat16), grad)
                key_sum[cols, :] += dot_f32(grad_scores, query)
                query_sum[...] += dot_f32(grad_scores, key, TN)

        part = (query_sum[...] * factor).astype(jnp.bfloat16)
        sent_v[step_q, :, 0:HD] = part[:BLOCK]
        sent_v[step_q, :, HD : 2 * HD] = part[BLOCK:]
        swaps[0].send(step_q)

        @pl.when(step % 2 == 1)
        def _():
            relay.tick(step // 2)

    @pl.loop(0, width)
    def _(i):
        rows = pl.ds(pl.multiple_of(i * BLOCK, BLOCK), BLOCK)
        sent_v[i, :, 2 * HD : 3 * HD] = (key_sum[rows, :] * factor).astype(jnp.bfloat16)
        sent_v[i, :, 3 * HD : 4 * HD] = value_sum[rows, :].astype(jnp.bfloat16)

    for step in range(width - 1, -1, -1):
        swaps[1].send(lax.rem(spot + step, width))
    loads[0].wait()
    loads[1].wait()
    mixed_all = mixed_v[...].reshape(count, heads_in)
    for n in range(model // LANES):
        low = low_v[:, :, n * LANES : (n + 1) * LANES].reshape(count, LANES)
        part = dot_f32(mixed_all, low, TN).astype(jnp.bfloat16)
        for i in range(LANES // piece):
            for b in range(heads_in // piece):
                grad_v[
                    n * (LANES // piece) + i, :, pl.ds(2 * heads_in + b * piece, piece)
                ] = part[b * piece : (b + 1) * piece, i * piece : (i + 1) * piece]
    loads[2].wait()
    gain_out[...] = jnp.zeros_like(gain_out)

    def back_copy(m):
        return pltpu.make_async_copy(back_v.at[m], back_out.at[m], back_sem.at[m])

    def turn_back(m, h):
        span = pl.ds(pl.multiple_of(m * tok, tok), tok)
        raw = raw_v[m, :, h * HD : (h + 1) * HD]
        kind = 0 if h < heads else 1
        gain = head_gain_ref[kind : kind + 1, :]
        g, place = (h // 2, h % 2) if h < heads else (h - heads, 2)
        grad = land_v[m * groups + g, :, place * HD : (place + 1) * HD].astype(jnp.float32)
        straight = grad * cosine_ref[span, :] + pltpu.roll(grad * sine_ref[span, :], HD // 2, 1)
        scale = lax.rsqrt(jnp.mean(raw * raw, axis=-1, keepdims=True) + EPSILON)
        gain_out[kind : kind + 1, :] += jnp.sum(straight * (raw * scale), axis=0, keepdims=True)
        pulled = straight * gain
        along = jnp.mean(pulled * raw, axis=-1, keepdims=True)
        back_v[m, :, h * HD : (h + 1) * HD] = (
            scale * (pulled - raw * (scale * scale * along))
        ).astype(jnp.bfloat16)

    @pl.loop(0, width)
    def _(d):
        swaps[0].wait(d)

    @pl.loop(0, micro)
    def _(m):
        for h in range(heads):
            turn_back(m, h)

        @pl.when(m == 1)
        def _():
            relay.tick(4)

    relay.tick(5)

    @pl.loop(0, width)
    def _(d):
        swaps[1].wait(d)

    @pl.loop(0, micro)
    def _(m):
        for h in range(heads, heads + groups):
            turn_back(m, h)
        for g in range(groups):
            first = (heads + groups + g) * HD
            back_v[m, :, first : first + HD] = land_v[m * groups + g, :, 3 * HD :]
        back_copy(m).start()

    loads[3].wait()

    core = lax.rem(spot, 2)
    near = spot + 1 - 2 * core

    def tile_copy(c):
        return pltpu.make_async_copy(grad_v.at[2 * c + core], grad_out.at[c], tile_sem.at[c])

    def pair_copy(c):
        return pltpu.make_async_remote_copy(
            src_ref=grad_v.at[2 * c + 1 - core],
            dst_ref=pair_v.at[c],
            send_sem=pair_sems.at[0, c],
            recv_sem=pair_sems.at[1, c],
            device_id={"wide": near},
            device_id_type=MESH,
        )

    def tile(i):
        left = hidden_v[:, :, pl.ds(pl.multiple_of(i * piece, piece), piece)].reshape(count, piece)
        return dot_f32(left, back_v[...].reshape(count, 2 * heads_in), TN)

    @pl.loop(0, width // 2)
    def _(c):
        i = 2 * c + 1 - core
        grad_v[i, :, 0 : 2 * heads_in] = tile(i).astype(jnp.bfloat16)
        pair_copy(c).start()

        @pl.when(c % 2 == 1)
        def _():
            relay.tick(6 + c // 2)

    output_copy = pltpu.make_async_copy(rows_v, output_out, late_sem.at[3])
    for r in range(per):
        span = slice(r * SUB, (r + 1) * SUB)
        rows_v[span, :] = (
            rows_v[span, :].astype(jnp.float32)
            + middle_v[r].astype(jnp.float32)
            + landed[r].astype(jnp.float32)
        ).astype(jnp.bfloat16)
    output_copy.start()

    @pl.loop(0, width // 2)
    def _(c):
        i = 2 * c + core
        part = tile(i)
        pair_copy(c).wait_recv()
        grad_v[i, :, 0 : 2 * heads_in] = (
            part + pair_v[c, :, 0 : 2 * heads_in].astype(jnp.float32)
        ).astype(jnp.bfloat16)
        grad_v[i, :, 2 * heads_in :] = (
            grad_v[i, :, 2 * heads_in :].astype(jnp.float32)
            + pair_v[c, :, 2 * heads_in :].astype(jnp.float32)
        ).astype(jnp.bfloat16)
        tile_copy(c).start()

    @pl.loop(0, width // 2)
    def _(c):
        tile_copy(c).wait()
        pair_copy(c).wait_send()

    @pl.loop(0, width)
    def _(i):
        for swap in swaps:
            swap.sent(i)

    for m in range(micro):
        back_copy(m).wait()
    output_copy.wait()
    relay.drain(0)


def attention_gradients(
    lengths, qkv, upper, kept, log_total, raw, hidden, mixed, middle_low, late, layer_input, *rest
):
    micro, tok, heads_in = mixed.shape
    width = upper.shape[0]
    total = qkv.shape[0]
    model = hidden.shape[2]
    low = jnp.bfloat16
    anywhere = pl.BlockSpec(memory_space=pl.ANY)
    inside = pl.BlockSpec(memory_space=pltpu.VMEM)
    return pl.pallas_call(
        weights_kernel,
        out_shape=(
            jax.ShapeDtypeStruct((micro, tok, 2 * heads_in), low),
            jax.ShapeDtypeStruct((width // 2, model // width, 3 * heads_in), low),
            jax.ShapeDtypeStruct((2, HD), jnp.float32),
            jax.ShapeDtypeStruct((tok, model), low),
        ),
        in_specs=[pl.BlockSpec(memory_space=pltpu.SMEM)] + [anywhere] * 10 + [inside] * 3,
        out_specs=[anywhere, anywhere, inside, anywhere],
        scratch_shapes=relay_scratch(tok // SUB, model)
        + [
            pltpu.VMEM((width, tok, 4 * HD), low),
            pltpu.VMEM(raw.shape, jnp.float32),
            pltpu.VMEM(hidden.shape, low),
            pltpu.VMEM(mixed.shape, low),
            pltpu.VMEM(middle_low.shape, low),
            pltpu.VMEM((micro, tok, 2 * heads_in), low),
            pltpu.VMEM((width, model // width, 3 * heads_in), low),
            pltpu.VMEM((width // 2, model // width, 3 * heads_in), low),
            pltpu.VMEM((tok // SUB, SUB, model), low),
            pltpu.VMEM((tok, model), low),
            pltpu.VMEM(qkv.shape, low),
            pltpu.VMEM(upper.shape, low),
            pltpu.VMEM(kept.shape, jnp.float32),
            pltpu.VMEM(log_total.shape, jnp.float32),
            pltpu.VMEM((width, tok, 4 * HD), low),
            pltpu.VMEM((2 * BLOCK, HD), jnp.float32),
            pltpu.VMEM((total, HD), jnp.float32),
            pltpu.VMEM((total, HD), jnp.float32),
            pltpu.SemaphoreType.DMA((4,)),
            pltpu.SemaphoreType.DMA((micro,)),
            pltpu.SemaphoreType.DMA((width // 2,)),
            pltpu.SemaphoreType.DMA((2, width)),
            pltpu.SemaphoreType.DMA((2, width)),
            pltpu.SemaphoreType.DMA((2, width // 2)),
            pltpu.SemaphoreType.DMA((4,)),
            pltpu.SemaphoreType.DMA((4,)),
        ],
        compiler_params=pltpu.CompilerParams(
            collective_id=3, has_side_effects=True, vmem_limit_bytes=56 << 20
        ),
        cost_estimate=pl.CostEstimate(
            flops=1_000_000_000, bytes_accessed=1_000_000, transcendentals=0
        ),
        name="attention_gradients",
    )(lengths, qkv, upper, kept, log_total, raw, hidden, mixed, middle_low, late, layer_input, *rest)


def relay_scratch(count, model, extra=0):
    return [
        pltpu.VMEM((count + extra, SUB, model), jnp.bfloat16),
        pltpu.VMEM((count, SUB, model), jnp.bfloat16),
        pltpu.VMEM((RING, SUB, model), jnp.bfloat16),
        pltpu.SemaphoreType.DMA((count,)),
        pltpu.SemaphoreType.DMA((count,)),
        pltpu.SemaphoreType.DMA((count,)),
        pltpu.SemaphoreType.DMA((RING,)),
    ]


def feed_kernel(
    mixed_ref,
    input_ref,
    grad_ref,
    gain_ref,
    pack_ref,
    up_w,
    down_w,
    hidden_out,
    active_out,
    gate_out,
    upper_out,
    output_out,
    middle_out,
    low_out,
    mixed_out,
    gain_out,
    weight_out,
    heads_out,
    early_out,
    late_out,
    own,
    landed,
    cross,
    out_sem,
    land_sem,
    back_sem,
    cross_sem,
    out_v,
    gate_v,
    up_v,
    down_v,
    mixed_v,
    rows_v,
    grads_v,
    hidden_v,
    stage_v,
    scale_v,
    middle_v,
    output_v,
    mixback_v,
    weight_sem,
    attn_sem,
    load_sem,
    hidden_sem,
    stage_sem,
    final_sem,
    reload_sem,
    tile_sem,
    ahead_sems,
    behind_sems,
    heads_sem,
    part_send,
    part_land,
    pair_sems,
    credit,
    late_sem,
):
    micro, tok, model = input_ref.shape
    width, _, piece = pack_ref.shape
    heads_in = out_v.shape[0]
    groups = width // micro
    per = tok // SUB
    hid = gate_v.shape[1]
    count = micro * tok
    blocks = hid // piece
    late = 3 * micro * per - per
    relay = Relay(late, own, landed, cross, (out_sem, land_sem, back_sem, cross_sem))
    n_up = hid // LANES
    n_down = model // LANES
    slots = n_up + n_down

    ahead = Exchange(
        lambda target: mixed_ref.at[target],
        lambda source: mixed_v.at[
            source // groups, :, pl.ds(pl.multiple_of((source % groups) * 2 * HD, 2 * HD), 2 * HD)
        ],
        ahead_sems.at[0],
        ahead_sems.at[1],
    )
    behind = Exchange(
        lambda target: mixback_v.at[
            target // groups % 2,
            :,
            pl.ds(pl.multiple_of((target % groups) * 2 * HD, 2 * HD), 2 * HD),
        ],
        lambda source: mixed_out.at[source],
        behind_sems.at[0],
        behind_sems.at[1],
    )
    attn_copies = [
        pltpu.make_async_copy(
            pack_ref.at[i, pl.ds(0, heads_in)],
            out_v.at[:, pl.ds(i * piece, piece)],
            attn_sem.at[i],
        )
        for i in range(width)
    ]
    weight_copies = [
        pltpu.make_async_copy(
            pack_ref.at[i, pl.ds(heads_in + j * piece, piece)],
            gate_v.at[pl.ds(i * piece, piece), pl.ds(j * piece, piece)],
            weight_sem.at[i, j],
        )
        for i in range(width)
        for j in range(blocks)
    ]

    def up_part(j):
        cols = pl.ds(j * LANES, LANES)
        return (
            up_w.at[:, cols],
            lambda s: up_v.at[pl.ds(pl.multiple_of(s * piece, piece), piece), cols],
            lambda s, h: up_v.at[
                pl.ds(pl.multiple_of(s * piece + h * piece // 2, piece // 2), piece // 2), cols
            ],
        )

    def down_part(j):
        return (
            down_w.at[pl.ds(j * LANES, LANES)],
            lambda s: down_v.at[
                pl.ds(j * LANES, LANES), pl.ds(pl.multiple_of(s * piece, piece), piece)
            ],
            lambda s, h: down_v.at[
                pl.ds(j * LANES + h * LANES // 2, LANES // 2),
                pl.ds(pl.multiple_of(s * piece, piece), piece),
            ],
        )

    gather = Gather(
        [make(j) for j in range(n_up) for make in (up_part, down_part)], part_send, part_land
    )

    def both(action, j):
        action(2 * j)
        action(2 * j + 1)

    for copy in attn_copies + weight_copies:
        copy.start()

    def loads(n):
        slot = n % 2
        return (
            pltpu.make_async_copy(input_ref.at[n % micro], rows_v.at[slot], load_sem.at[slot, 0]),
            pltpu.make_async_copy(grad_ref.at[n % micro], grads_v.at[slot], load_sem.at[slot, 1]),
        )

    def start_loads(n):
        for copy in loads(n):
            copy.start()

    def wait_loads(n):
        for copy in loads(n):
            copy.wait()

    start_loads(0)
    gain_out[...] = jnp.zeros_like(gain_out)
    relay.greet(wide_peers(width))
    spot = lax.axis_index("wide")
    for step in range(width):
        ahead.send(lax.rem(spot + step, width))
    both(gather.first, 0)
    both(gather.first, 1)
    for copy in attn_copies:
        copy.wait()

    def heads_copy(m):
        return pltpu.make_async_copy(mixed_v.at[m], heads_out.at[m], heads_sem.at[m])

    @pl.loop(0, micro)
    def _(m):
        for g in range(groups):
            ahead.wait(m * groups + g)
        heads_copy(m).start()
        for n in range(n_down):
            cols = pl.ds(n * LANES, LANES)
            part = dot_f32(mixed_v[m], out_v[:, cols]).astype(jnp.bfloat16)
            for r in range(per):
                own[m * per + r, :, cols] = part[r * SUB : (r + 1) * SUB]
        relay.send(m * per, per)

    first_ticks = per + 4

    for k in range(first_ticks):
        if k == 4:
            both(gather.second, 0)
        if k == 5:
            both(gather.first, 2)
        if k == 6:
            both(gather.second, 1)
        if k == 7:
            both(gather.third, 0)
        relay.tick(k)

    for copy in weight_copies:
        copy.wait()

    def hidden_copy(m):
        return pltpu.make_async_copy(hidden_v, hidden_out.at[m], hidden_sem)

    def stage_copies(m):
        return [
            pltpu.make_async_copy(stage_v.at[i], target.at[m], stage_sem.at[i])
            for i, target in enumerate((active_out, gate_out, upper_out))
        ]

    base = micro * per

    @pl.loop(0, micro)
    def _(m):
        slot = m % 2
        wait_loads(m)
        start_loads(m + 1)

        @pl.when(m > 0)
        def _():
            hidden_copy(m - 1).wait()
            for copy in stage_copies(m - 1):
                copy.wait()

        @pl.loop(0, per)
        def _(r):
            span = pl.ds(pl.multiple_of(r * SUB, SUB), SUB)
            middle = rows_v[slot, span, :].astype(jnp.float32) + landed[m * per + r].astype(
                jnp.float32
            )
            scale = lax.rsqrt(jnp.mean(middle * middle, axis=-1, keepdims=True) + EPSILON)
            scale_v[span, :] = scale
            hidden_v[span, :] = (middle * scale * gain_ref[...]).astype(jnp.bfloat16)

        hidden_copy(m).start()

        @pl.loop(0, n_up)
        def _(j):
            relay.tick(first_ticks + slots * m + j)
            for turn in range(n_up):

                @pl.when((m == 0) & (j == turn))
                def _():
                    if turn == 0:
                        both(gather.second, 2)
                    if turn + 1 < n_up:
                        both(gather.third, turn + 1)
                    both(gather.fourth, turn)

            cols = pl.ds(pl.multiple_of(j * LANES, LANES), LANES)
            gate = dot_f32(hidden_v[...], gate_v[:, cols])
            up_proj = dot_f32(hidden_v[...], up_v[:, cols])
            grad_active = dot_f32(grads_v[slot], down_v[cols, :], NT)
            squash = 1.0 / (1.0 + jnp.exp(-gate))
            silu = gate * squash
            stage_v[0, :, cols] = (silu * up_proj).astype(jnp.bfloat16)
            stage_v[1, :, cols] = (
                grad_active * up_proj * (squash * (1.0 + gate * (1.0 - squash)))
            ).astype(jnp.bfloat16)
            stage_v[2, :, cols] = (grad_active * silu).astype(jnp.bfloat16)
        for copy in stage_copies(m):
            copy.start()

        @pl.loop(0, n_down)
        def _(n):
            relay.tick(first_ticks + slots * m + n_up + n)
            cols = pl.ds(pl.multiple_of(n * LANES, LANES), LANES)
            back = dot_f32(stage_v[1], gate_v[cols, :], NT) + dot_f32(
                stage_v[2], up_v[cols, :], NT
            )
            ahead = dot_f32(stage_v[0], down_v[:, cols]).astype(jnp.bfloat16)
            gain_sum = jnp.zeros((1, LANES), jnp.float32)
            for r in range(per):
                part = slice(r * SUB, (r + 1) * SUB)
                own[base + 2 * per * m + r, :, cols] = back[part].astype(jnp.bfloat16)
                own[base + 2 * per * m + per + r, :, cols] = ahead[part]
                unit = (
                    rows_v[slot, pl.ds(r * SUB, SUB), cols].astype(jnp.float32)
                    + landed[m * per + r, :, cols].astype(jnp.float32)
                ) * scale_v[pl.ds(r * SUB, SUB), :]
                gain_sum += jnp.sum(back[part] * unit, axis=0, keepdims=True)
            gain_out[:, cols] += gain_sum

        relay.send(base + 2 * per * m, per)

        @pl.when(m < micro - 1)
        def _():
            relay.send(base + 2 * per * m + per, per)

    hidden_copy(micro - 1).wait()
    for copy in stage_copies(micro - 1):
        copy.wait()
    late_copies = [
        pltpu.make_async_copy(own.at[pl.ds(late, per)], late_out.at[0], late_sem.at[0]),
        pltpu.make_async_copy(
            landed.at[pl.ds((micro - 1) * per, per)], late_out.at[1], late_sem.at[1]
        ),
    ]
    for copy in late_copies:
        copy.start()

    gather.drain()
    core = lax.rem(spot, 2)
    near = gather.near

    def offer():
        pl.semaphore_signal(credit, inc=1, device_id={"wide": near}, device_id_type=MESH)

    offer()

    @pl.loop(0, base)
    def _(k):
        relay.to_inner(k).wait_send()

    def reloads(m):
        rows = pl.ds(m * tok, tok)
        return [
            pltpu.make_async_copy(hidden_out.at[m], down_v.at[rows], reload_sem.at[m, 0]),
            pltpu.make_async_copy(gate_out.at[m], gate_v.at[rows], reload_sem.at[m, 1]),
            pltpu.make_async_copy(
                upper_out.at[m], gate_v.at[pl.ds(count + m * tok, tok)], reload_sem.at[m, 2]
            ),
            pltpu.make_async_copy(active_out.at[m], up_v.at[rows], reload_sem.at[m, 3]),
        ] + [
            pltpu.make_async_copy(
                grad_ref.at[m, pl.ds(r * SUB, SUB)], own.at[m * per + r], reload_sem.at[m, 4 + r]
            )
            for r in range(per)
        ]

    for m in range(micro):
        for copy in reloads(m):
            copy.start()

    def pair_slot(q):
        return up_v.at[pl.ds(count + q * piece, piece)]

    def tile_copy(m, q):
        target = early_out.at[m] if q == 0 else weight_out.at[m, q - 1]
        return pltpu.make_async_copy(pair_slot(q), target, tile_sem.at[q])

    def pair_copy(q):
        return pltpu.make_async_remote_copy(
            src_ref=stage_v.at[q],
            dst_ref=pair_slot(q),
            send_sem=pair_sems.at[0, q],
            recv_sem=pair_sems.at[1, q],
            device_id={"wide": near},
            device_id_type=MESH,
        )

    def tile(i, q, store):
        cols = pl.ds(pl.multiple_of(i * piece, piece), piece)
        if q == 2:
            right = own[0:base, :, cols].reshape(count, piece)
            for j in range(blocks):
                span = slice(j * piece, (j + 1) * piece)
                store(span, dot_f32(up_v[0:count, span], right, TN))
        else:
            right = (gate_v[0:count], gate_v[count : 2 * count])[q]
            store(slice(0, hid), dot_f32(down_v[0:count, cols], right, TN))

    def give(m, q):
        @pl.when(m > 0)
        def _():
            pair_copy(q).wait_send()

        def store(span, part):
            stage_v[q, :, span] = part.astype(jnp.bfloat16)

        tile(2 * m + 1 - core, q, store)

    def keep(m, q):
        rows = pl.ds(count + q * piece, piece)
        pair_copy(q).wait_recv()

        def store(span, part):
            up_v[rows, span] = (part + up_v[rows, span].astype(jnp.float32)).astype(jnp.bfloat16)

        tile(2 * m + core, q, store)
        tile_copy(m, q).start()

    def final_copies(m):
        return [
            pltpu.make_async_copy(middle_v, middle_out.at[m], final_sem.at[0]),
            pltpu.make_async_copy(hidden_v, low_out.at[m], final_sem.at[1]),
        ]

    def output_copy(m):
        return pltpu.make_async_copy(output_v, output_out.at[m], final_sem.at[2])

    last_ticks = first_ticks + slots * micro
    rest = late + 4 - last_ticks
    turns = rest // micro

    @pl.loop(0, micro)
    def _(m):
        slot = m % 2
        wait_loads(m + micro)

        @pl.when(m < micro - 1)
        def _():
            start_loads(m + micro + 1)

        @pl.when(m > 0)
        def _():
            for copy in final_copies(m - 1):
                copy.wait()
            output_copy(m - 1).wait()

        @pl.when(m == 0)
        def _():
            for i in range(micro):
                for copy in reloads(i):
                    copy.wait()

        relay.tick(last_ticks + turns * m)
        give(m, 0)
        give(m, 1)
        give(m, 2)
        pl.semaphore_wait(credit, 1)
        for q in range(3):
            pair_copy(q).start()
        relay.tick(last_ticks + turns * m + 1)
        keep(m, 0)
        keep(m, 1)
        relay.tick(last_ticks + turns * m + 2)

        @pl.loop(0, per)
        def _(r):
            span = pl.ds(pl.multiple_of(r * SUB, SUB), SUB)
            middle = rows_v[slot, span, :].astype(jnp.float32) + landed[m * per + r].astype(
                jnp.float32
            )
            scale = lax.rsqrt(jnp.mean(middle * middle, axis=-1, keepdims=True) + EPSILON)
            pulled = landed[base + 2 * per * m + r].astype(jnp.float32) * gain_ref[...]
            along = jnp.mean(pulled * middle, axis=-1, keepdims=True)
            grad_middle = grads_v[slot, span, :].astype(jnp.float32) + scale * (
                pulled - middle * (scale * scale * along)
            )
            middle_v[span, :] = grad_middle
            hidden_v[span, :] = grad_middle.astype(jnp.bfloat16)

        @pl.when(m >= 2)
        def _():
            for g in range(groups):
                behind.sent((m - 2) * groups + g, home=True)

        mixback_v[m % 2] = dot_f32(hidden_v[...], out_v[...], NT).astype(jnp.bfloat16)
        for g in range(groups):
            behind.send(m * groups + g)

        @pl.when(m < micro - 1)
        def _():
            @pl.loop(0, per)
            def _(r):
                span = pl.ds(pl.multiple_of(r * SUB, SUB), SUB)
                output_v[span, :] = (
                    rows_v[slot, span, :].astype(jnp.float32)
                    + landed[m * per + r].astype(jnp.float32)
                    + landed[base + 2 * per * m + per + r].astype(jnp.float32)
                ).astype(jnp.bfloat16)

            output_copy(m).start()

        for copy in final_copies(m):
            copy.start()
        keep(m, 2)
        for q in range(3):
            tile_copy(m, q).wait()

        @pl.when(m < micro - 1)
        def _():
            offer()

    for copy in late_copies:
        copy.wait()
    for copy in final_copies(micro - 1):
        copy.wait()
    for q in range(3):
        pair_copy(q).wait_send()
    for m in range(micro):
        heads_copy(m).wait()

    @pl.loop(0, width)
    def _(d):
        ahead.sent(d)
        behind.wait(d, home=False)

    @pl.loop((micro - 2) * groups, width)
    def _(d):
        behind.sent(d, home=True)

    relay.drain(base)


def feed_forward(mixed, layer_input, grad_out, gain_ffn, pack, up_w, down_w, heads_in):
    micro, tok, model = layer_input.shape
    hid = up_w.shape[1]
    parts = 2 * (hid // LANES)
    width, _, piece = pack.shape
    groups = width // micro
    low = jnp.bfloat16
    count = 3 * micro * (tok // SUB)
    late = tok // SUB
    anywhere = pl.BlockSpec(memory_space=pl.ANY)
    inside = pl.BlockSpec(memory_space=pltpu.VMEM)
    return pl.pallas_call(
        feed_kernel,
        out_shape=(
            jax.ShapeDtypeStruct((micro, tok, model), low),
            jax.ShapeDtypeStruct((micro, tok, hid), low),
            jax.ShapeDtypeStruct((micro, tok, hid), low),
            jax.ShapeDtypeStruct((micro, tok, hid), low),
            jax.ShapeDtypeStruct((micro - 1, tok, model), low),
            jax.ShapeDtypeStruct((micro, tok, model), jnp.float32),
            jax.ShapeDtypeStruct((micro, tok, model), low),
            jax.ShapeDtypeStruct((width, tok, 2 * HD), low),
            jax.ShapeDtypeStruct((1, model), jnp.float32),
            jax.ShapeDtypeStruct((width // 2, 2, piece, hid), low),
            jax.ShapeDtypeStruct((micro, tok, heads_in), low),
            jax.ShapeDtypeStruct((width // 2, piece, hid), low),
            jax.ShapeDtypeStruct((2, late, SUB, model), low),
        ),
        in_specs=[anywhere] * 3 + [inside, anywhere, anywhere, anywhere],
        out_specs=[anywhere] * 8 + [inside] + [anywhere] * 4,
        scratch_shapes=relay_scratch(count - late, model, late)
        + [
            pltpu.VMEM((heads_in, model), low),
            pltpu.VMEM((model, hid), low),
            pltpu.VMEM((model, hid), low),
            pltpu.VMEM((hid, model), low),
            pltpu.VMEM((micro, tok, heads_in), low),
            pltpu.VMEM((2, tok, model), low),
            pltpu.VMEM((2, tok, model), low),
            pltpu.VMEM((tok, model), low),
            pltpu.VMEM((3, tok, hid), low),
            pltpu.VMEM((tok, 1), jnp.float32),
            pltpu.VMEM((tok, model), jnp.float32),
            pltpu.VMEM((tok, model), low),
            pltpu.VMEM((2, tok, heads_in), low),
            pltpu.SemaphoreType.DMA((width, hid // piece)),
            pltpu.SemaphoreType.DMA((width,)),
            pltpu.SemaphoreType.DMA((2, 2)),
            pltpu.SemaphoreType.DMA,
            pltpu.SemaphoreType.DMA((3,)),
            pltpu.SemaphoreType.DMA((3,)),
            pltpu.SemaphoreType.DMA((micro, 4 + tok // SUB)),
            pltpu.SemaphoreType.DMA((3,)),
            pltpu.SemaphoreType.DMA((2, width)),
            pltpu.SemaphoreType.DMA((2, width)),
            pltpu.SemaphoreType.DMA((micro,)),
            pltpu.SemaphoreType.DMA((parts, 9)),
            pltpu.SemaphoreType.DMA((parts, 10)),
            pltpu.SemaphoreType.DMA((2, 3)),
            pltpu.SemaphoreType.REGULAR,
            pltpu.SemaphoreType.DMA((2,)),
        ],
        compiler_params=pltpu.CompilerParams(
            collective_id=0, has_side_effects=True, vmem_limit_bytes=67043328
        ),
        cost_estimate=pl.CostEstimate(
            flops=240_000_000_000, bytes_accessed=900_000_000, transcendentals=0
        ),
        name="feed_forward",
    )(mixed, layer_input, grad_out, gain_ffn[None, :], pack, up_w, down_w)


def input_kernel(
    back_ref,
    input_ref,
    middle_ref,
    gain_ref,
    weight_ref,
    gain_two_ref,
    gain_heads_ref,
    output_out,
    gains_out,
    own,
    landed,
    cross,
    out_sem,
    land_sem,
    back_sem,
    cross_sem,
    weight_v,
    back_v,
    rows_v,
    middle_v,
    output_v,
    term_v,
    other_v,
    first_sem,
    load_sem,
    final_sem,
    term_sem,
    other_sem,
):
    micro, tok, model = input_ref.shape
    per = tok // SUB
    spot = lax.axis_index("wide")
    flips = [spot + bit - 2 * bit * (spot // bit % 2) for bit in (1, 2, 4)]
    relay = Relay(micro * per, own, landed, cross, (out_sem, land_sem, back_sem, cross_sem))
    weight_copy = pltpu.make_async_copy(weight_ref, weight_v, first_sem.at[0])
    back_copy = pltpu.make_async_copy(back_ref, back_v, first_sem.at[1])
    weight_copy.start()
    back_copy.start()

    rows_copy = pltpu.make_async_copy(input_ref, rows_v, first_sem.at[2])
    rows_copy.start()

    def load(m):
        return pltpu.make_async_copy(middle_ref.at[m], middle_v.at[m % 2], load_sem.at[m % 2])

    def final_copy(m):
        return pltpu.make_async_copy(output_v.at[m % 2], output_out.at[m], final_sem.at[m % 2])

    def pass_on(step, where):
        return pltpu.make_async_remote_copy(
            src_ref=term_v.at[step],
            dst_ref=other_v.at[step],
            send_sem=term_sem.at[step],
            recv_sem=other_sem.at[step],
            device_id=where,
            device_id_type=MESH,
        )

    targets = [{"wide": flip} for flip in flips] + [
        {"narrow": spot} for spot in (relay.inner, relay.other, relay.outer)
    ]

    def gain_step(step):
        if step == 0:
            pass_on(0, targets[0]).start()
        if 1 <= step <= 3:
            pass_on(step - 1, targets[step - 1]).wait_recv()
            term_v[step] = term_v[step - 1] + other_v[step - 1]
        if step in (1, 2):
            pass_on(step, targets[step]).start()
        if step == 3:

            @pl.when(relay.is_end)
            def _():
                pass_on(3, targets[3]).start()

        if step in (4, 5):

            @pl.when(relay.is_mid)
            def _():
                pass_on(step - 1, targets[step - 1]).wait_recv()
                term_v[step] = term_v[step - 1] + other_v[step - 1]
                pass_on(step, targets[step]).start()

        if step == 6:

            @pl.when(relay.is_mid)
            def _():
                gains_out[...] = term_v[5]
                pass_on(4, targets[4]).wait_send()
                pass_on(5, targets[5]).wait_send()

            @pl.when(relay.is_end)
            def _():
                pass_on(5, targets[5]).wait_recv()
                gains_out[...] = other_v[5]
                pass_on(3, targets[3]).wait_send()

            for early in range(3):
                pass_on(early, targets[early]).wait_send()

    load(0).start()
    relay.greet(flips)
    term_v[0] = jnp.zeros(term_v.shape[1:], jnp.float32)
    weight_copy.wait()
    back_copy.wait()
    rows_copy.wait()

    @pl.loop(0, micro)
    def _(m):
        rows = rows_v[m].astype(jnp.float32)
        scale = lax.rsqrt(jnp.mean(rows * rows, axis=-1, keepdims=True) + EPSILON)
        for n in range(model // LANES):
            cols = pl.ds(n * LANES, LANES)
            part = dot_f32(back_v[m], weight_v[cols, :], NT)
            term_v[0, 0:1, cols] += jnp.sum(
                part * (rows_v[m, :, cols].astype(jnp.float32) * scale), axis=0, keepdims=True
            )
            part = part.astype(jnp.bfloat16)
            for r in range(per):
                own[m * per + r, :, cols] = part[r * SUB : (r + 1) * SUB]

        @pl.when(m == 0)
        def _():
            relay.send(0, AHEAD)

    term_v[0, 1:2, :] = gain_two_ref[...]
    term_v[0, 2:3, 0:HD] = gain_heads_ref[0:1, :]
    term_v[0, 2:3, HD : 2 * HD] = gain_heads_ref[1:2, :]
    for k in range(4):
        if k in GAIN_TICKS:
            gain_step(GAIN_TICKS.index(k))
        relay.send(AHEAD + k, 1)
        relay.tick(k)

    @pl.loop(0, micro)
    def _(m):
        slot = m % 2

        @pl.when(m < micro - 1)
        def _():
            load(m + 1).start()

        load(m).wait()

        @pl.when(m >= 2)
        def _():
            final_copy(m - 2).wait()

        for r in range(per):
            for turn in range(micro):
                if 4 + turn * per + r in GAIN_TICKS:

                    @pl.when(m == turn)
                    def _(step=GAIN_TICKS.index(4 + turn * per + r)):
                        gain_step(step)

            @pl.when(AHEAD + 4 + m * per + r < relay.count)
            def _():
                relay.send(AHEAD + 4 + m * per + r, 1)

            relay.tick(4 + m * per + r)
            span = pl.ds(r * SUB, SUB)
            rows = rows_v[m, span, :].astype(jnp.float32)
            scale = lax.rsqrt(jnp.mean(rows * rows, axis=-1, keepdims=True) + EPSILON)
            pulled = landed[m * per + r].astype(jnp.float32) * gain_ref[...]
            along = jnp.mean(pulled * rows, axis=-1, keepdims=True)
            output_v[slot, span, :] = middle_v[slot, span, :] + scale * (
                pulled - rows * (scale * scale * along)
            )
        final_copy(m).start()

    final_copy(micro - 2).wait()
    final_copy(micro - 1).wait()
    relay.drain(0)


def input_gradient(back, layer_input, grad_middle, gain_attn, weight, gain_two, gain_heads):
    micro, tok, model = layer_input.shape
    low = jnp.bfloat16
    count = micro * (tok // SUB)
    anywhere = pl.BlockSpec(memory_space=pl.ANY)
    inside = pl.BlockSpec(memory_space=pltpu.VMEM)
    return pl.pallas_call(
        input_kernel,
        out_shape=(
            jax.ShapeDtypeStruct((micro, tok, model), jnp.float32),
            jax.ShapeDtypeStruct((8, model), jnp.float32),
        ),
        in_specs=[anywhere] * 3 + [inside, anywhere, inside, inside],
        out_specs=[anywhere, inside],
        scratch_shapes=relay_scratch(count, model)
        + [
            pltpu.VMEM(weight.shape, low),
            pltpu.VMEM((micro, tok, weight.shape[1]), low),
            pltpu.VMEM((micro, tok, model), low),
            pltpu.VMEM((2, tok, model), jnp.float32),
            pltpu.VMEM((2, tok, model), jnp.float32),
            pltpu.VMEM((6, 8, model), jnp.float32),
            pltpu.VMEM((6, 8, model), jnp.float32),
            pltpu.SemaphoreType.DMA((3,)),
            pltpu.SemaphoreType.DMA((2,)),
            pltpu.SemaphoreType.DMA((2,)),
            pltpu.SemaphoreType.DMA((6,)),
            pltpu.SemaphoreType.DMA((6,)),
        ],
        compiler_params=pltpu.CompilerParams(
            collective_id=1, has_side_effects=True, vmem_limit_bytes=48 << 20
        ),
        cost_estimate=pl.CostEstimate(
            flops=1_000_000_000, bytes_accessed=1_000_000, transcendentals=0
        ),
        name="input_gradient",
    )(back, layer_input, grad_middle, gain_attn[None, :], weight, gain_two, gain_heads)


def widen_gate(rows_ref, gate_ref):
    gate_ref[...] = rows_ref[...].astype(jnp.float32)


def finish_kernel(
    input_rows,
    first_rows,
    last_rows,
    up_rows,
    down_rows,
    attn_rows,
    out_rows,
    grad_ref,
    output_ref,
    up_ref,
    down_ref,
    query_ref,
    key_ref,
    value_ref,
    out_ref,
):
    grad_ref[...] = input_rows[...]
    inside = pl.program_id(0) < pl.num_programs(0) * 3 // 4
    output_ref[...] = jnp.where(inside, first_rows[...], last_rows[...])
    up_ref[...] = up_rows[...].astype(jnp.float32)
    down_ref[...] = down_rows[...].astype(jnp.float32)
    first = 0
    for target in (query_ref, key_ref, value_ref):
        target[...] = attn_rows[:, first : first + target.shape[1]].astype(jnp.float32)
        first += target.shape[1]
    out_ref[...] = out_rows[...].astype(jnp.float32)


def finish(grad_input, first, last, feed, attn, columns):
    steps = 8
    rows, model = grad_input.shape
    piece, hid = feed.shape[0] // 2, feed.shape[1]
    part = rows // steps
    early = first.shape[0] // part - 1
    strip = piece // steps
    blocks = hid // piece
    heads = sum(columns) // piece
    rest = (attn.shape[1] - sum(columns)) // piece
    f32 = jnp.float32
    row = lambda i: (i, 0)
    return pl.pallas_call(
        finish_kernel,
        grid=(steps,),
        out_shape=(
            jax.ShapeDtypeStruct((rows, model), f32),
            jax.ShapeDtypeStruct((rows, model), jnp.bfloat16),
            jax.ShapeDtypeStruct((piece, hid), f32),
            jax.ShapeDtypeStruct((hid, piece), f32),
        )
        + tuple(jax.ShapeDtypeStruct((piece, column), f32) for column in columns)
        + (jax.ShapeDtypeStruct((rest * piece, piece), f32),),
        in_specs=[
            pl.BlockSpec((part, model), row),
            pl.BlockSpec((part, model), lambda i: (jnp.minimum(i, early), 0)),
            pl.BlockSpec((part, model), lambda i: (jnp.maximum(i - early - 1, 0), 0)),
            pl.BlockSpec((strip, hid), row),
            pl.BlockSpec((piece, piece), lambda i: (1, jnp.minimum(i, blocks - 1))),
            pl.BlockSpec((strip, attn.shape[1]), row),
            pl.BlockSpec((piece, piece), lambda i: (0, heads + jnp.minimum(i, rest - 1))),
        ],
        out_specs=[
            pl.BlockSpec((part, model), row),
            pl.BlockSpec((part, model), row),
            pl.BlockSpec((strip, hid), row),
            pl.BlockSpec((piece, piece), lambda i: (jnp.minimum(i, blocks - 1), 0)),
        ]
        + [pl.BlockSpec((strip, column), row) for column in columns]
        + [pl.BlockSpec((piece, piece), lambda i: (jnp.minimum(i, rest - 1), 0))],
        name="finish",
    )(grad_input, first, last, feed, feed, attn, attn)


def local_batched(
    layer_input,
    grad_out,
    lengths,
    w_query,
    w_key,
    w_value,
    w_out,
    w_gate,
    w_up,
    w_down,
    gain_attn,
    gain_ffn,
    gain_query,
    gain_key,
):
    micro, tok_rows, model = layer_input.shape
    width = lax.axis_size("wide")
    groups = w_key.shape[1] // HD
    total = tok_rows * width
    piece = w_out.shape[1]

    def stacked(weight):
        return jnp.moveaxis(weight.reshape(piece, -1, piece), 1, 0).reshape(-1, piece)

    pack = lax.all_gather(
        jnp.concatenate([w_out, stacked(w_gate)], axis=0), "wide", axis=0
    )

    head_gains = jnp.stack([gain_query, gain_key])
    hidden_one, raw, packed, w_qkv, cosine, sine = project(
        layer_input, gain_attn, (w_query, w_key, w_value), lengths, head_gains, width
    )
    packed = packed.reshape(total, 4 * HD)
    mixed, kept, log_total = attention_out(packed, lengths)
    (
        _,
        _,
        _,
        _,
        output,
        grad_middle,
        middle_low,
        grad_mixed,
        gain_two,
        feed_grads,
        mixed_low,
        gate_grads,
        late,
    ) = feed_forward(
        mixed.reshape(width, tok_rows, 2 * HD),
        layer_input,
        grad_out,
        gain_ffn,
        pack,
        w_up,
        w_down,
        w_out.shape[0],
    )
    cores = [list(range(core, width, 2)) for core in range(2)]

    def scatter(rows):
        return lax.psum_scatter(
            rows, "wide", scatter_dimension=0, axis_index_groups=cores, tiled=True
        )

    qkv_back, attn_grads, gain_heads, last_output = attention_gradients(
        lengths,
        packed,
        grad_mixed,
        kept,
        log_total,
        raw,
        hidden_one,
        mixed_low,
        middle_low,
        late,
        layer_input,
        cosine,
        sine,
        head_gains,
    )
    gate_grads = scatter(gate_grads.reshape(-1, w_gate.shape[1]))
    attn_grads, feed_grads = lax.optimization_barrier((attn_grads, feed_grads))
    attn_grads = scatter(attn_grads.reshape(model // 2, -1))
    feed_grads = scatter(feed_grads.reshape(-1, w_up.shape[1]))
    grad_input, gains = input_gradient(
        qkv_back, layer_input, grad_middle, gain_attn, w_qkv, gain_two, gain_heads
    )

    grad_gate = pl.pallas_call(
        widen_gate,
        out_shape=jax.ShapeDtypeStruct(w_gate.shape, jnp.float32),
        name="widen_gate",
    )(gate_grads)
    (
        grad_input,
        output,
        grad_up,
        grad_down,
        grad_query,
        grad_key,
        grad_value,
        grad_wout,
    ) = finish(
        grad_input.reshape(-1, model),
        output.reshape(-1, model),
        last_output,
        feed_grads,
        attn_grads,
        (w_query.shape[1], w_key.shape[1], w_value.shape[1]),
    )
    return (
        output.reshape(layer_input.shape),
        grad_input.reshape(layer_input.shape),
        grad_query,
        grad_key,
        grad_value,
        grad_wout,
        grad_gate,
        grad_up,
        grad_down,
        gains[0],
        gains[1],
        gains[2, :HD],
        gains[2, HD : 2 * HD],
    )


def local(mesh, layer_input, grad_out, lengths, w_query, w_key, *rest):
    width = mesh.shape["wide"]
    micro, tok_rows = layer_input.shape[:2]
    groups = w_key.shape[1] // HD
    fits = (
        groups == HEAD_GROUPS
        and micro * groups == width == 8
        and w_query.shape[1] == 2 * w_key.shape[1]
        and mesh.shape["narrow"] == 4
        and tok_rows == BLOCK
    )
    chosen = local_batched if fits else local_general
    return chosen(layer_input, grad_out, lengths, w_query, w_key, *rest)


def solution(mesh):
    in_specs = (
        P(None, "wide", None),
        P(None, "wide", None),
        P(),
        P("wide", "narrow"),
        P("wide", "narrow"),
        P("wide", "narrow"),
        P("narrow", "wide"),
        P("wide", "narrow"),
        P("wide", "narrow"),
        P("narrow", "wide"),
        P(),
        P(),
        P(),
        P(),
    )
    out_specs = (
        P(None, "wide", None),
        P(None, "wide", None),
        P("wide", "narrow"),
        P("wide", "narrow"),
        P("wide", "narrow"),
        P("narrow", "wide"),
        P("wide", "narrow"),
        P("wide", "narrow"),
        P("narrow", "wide"),
        P(),
        P(),
        P(),
        P(),
    )
    return jax.shard_map(
        functools.partial(local, mesh), mesh=mesh, in_specs=in_specs, out_specs=out_specs, check_vma=False)
```

```python
import functools
import math

import jax
import jax.numpy as jnp
from jax import lax
from jax.experimental import pallas as pl
from jax.experimental.pallas import tpu as pltpu
from jax.sharding import PartitionSpec as P

HD = 128
NDOC = 8


EPSILON = 1e-06
THETA = 1000000.0


def rms_norm(values, gain):
    return values * lax.rsqrt(jnp.mean(values * values, axis=-1, keepdims=True) + EPSILON) * gain


def unit_rows(values):
    return values * lax.rsqrt(jnp.mean(values * values, axis=-1, keepdims=True) + EPSILON)


def rotate(values, cosine, sine):
    midway = values.shape[-1] // 2
    turned = jnp.concatenate([-values[..., midway:], values[..., :midway]], axis=-1)
    return values * cosine + turned * sine


def layout(lengths_row, total):
    finish = jnp.cumsum(lengths_row)
    starts = finish - lengths_row
    places = jnp.arange(total, dtype=jnp.int32)
    segment = jnp.sum((places[:, None] >= finish[None, :]).astype(jnp.int32), axis=1)
    member = segment[:, None] == jnp.arange(finish.shape[0], dtype=jnp.int32)[None, :]
    opening = jnp.sum(jnp.where(member, starts[None, :], 0), axis=1)
    return (segment, places - opening)


def angles(place):
    frequency = jnp.exp(-math.log(THETA) * jnp.arange(0, HD, 2).astype(jnp.float32) / HD)
    turning = place.astype(jnp.float32)[:, None] * frequency[None, :]
    turning = jnp.concatenate([turning, turning], axis=-1)
    return (jnp.cos(turning), jnp.sin(turning))


def allowed(query_seg, query_idx, key_seg, key_idx):
    same_doc = query_seg[:, None] == key_seg[None, :]
    causal = key_idx[None, :] <= query_idx[:, None]
    usable = (key_seg[None, :] != NDOC - 1) | (key_idx[None, :] == query_idx[:, None])
    return same_doc & causal & usable


def attention_scores(query_low, key_all, mask_local, factor):
    scores = (
        jnp.einsum("tgrd,kgd->grtk", query_low, key_all, preferred_element_type=jnp.float32)
        * factor
    )
    return jnp.where(mask_local[None, None], scores, -1e30)


def one_batch(row_input, grad_row, lengths_row, gathered, gains):
    w_query, w_key, w_value, w_out, w_gate, w_up, w_down = gathered
    gain_attn, gain_ffn, gain_query, gain_key = gains
    tok_rows = row_input.shape[0]
    total = tok_rows * lax.axis_size("wide")
    groups = w_key.shape[1] // HD
    repeat = w_query.shape[1] // w_key.shape[1]
    factor = 1.0 / math.sqrt(HD)
    first_row = lax.axis_index("wide") * tok_rows
    segment, place = layout(lengths_row, total)
    positions = jnp.arange(total, dtype=jnp.int32)
    query_seg = lax.dynamic_slice_in_dim(segment, first_row, tok_rows)
    query_idx = lax.dynamic_slice_in_dim(positions, first_row, tok_rows)
    mask_local = allowed(query_seg, query_idx, segment, positions)
    cosine, sine = angles(lax.dynamic_slice_in_dim(place, first_row, tok_rows))

    def head_norm(rows, gain):
        return rotate(rms_norm(rows, gain), cosine[:, None, :], sine[:, None, :])

    input_float = row_input.astype(jnp.float32)
    grad_float = grad_row.astype(jnp.float32)
    normed_one, pull_one = jax.vjp(lambda rows: rms_norm(rows, gain_attn), input_float)
    hidden_one = normed_one.astype(jnp.bfloat16)
    query_raw = jnp.dot(hidden_one, w_query, preferred_element_type=jnp.float32).reshape(
        tok_rows, groups * repeat, HD
    )
    key_raw = jnp.dot(hidden_one, w_key, preferred_element_type=jnp.float32).reshape(
        tok_rows, groups, HD
    )
    value_low = jnp.dot(hidden_one, w_value, preferred_element_type=jnp.float32).astype(
        jnp.bfloat16
    )
    query_turned, pull_query = jax.vjp(head_norm, query_raw, gain_query)
    key_turned, pull_key = jax.vjp(head_norm, key_raw, gain_key)
    query_low = query_turned.astype(jnp.bfloat16).reshape(tok_rows, groups, repeat, HD)
    key_low = key_turned.astype(jnp.bfloat16).reshape(tok_rows, groups * HD)
    key_all, value_all = (
        lax.all_gather(key_low, "wide", axis=0, tiled=True),
        lax.all_gather(value_low, "wide", axis=0, tiled=True),
    )
    key_all = key_all.reshape(total, groups, HD)
    value_all = value_all.reshape(total, groups, HD)
    scores = attention_scores(query_low, key_all, mask_local, factor)
    highest = jnp.max(scores, axis=-1, keepdims=True)
    exponent = jnp.exp(scores - highest)
    denominator = jnp.sum(exponent, axis=-1, keepdims=True)
    log_total = highest + jnp.log(denominator)
    probs_low = (exponent / denominator).astype(jnp.bfloat16)
    mixed = jnp.einsum("grtk,kgd->tgrd", probs_low, value_all, preferred_element_type=jnp.float32)
    mixed_low = mixed.reshape(tok_rows, groups * repeat * HD).astype(jnp.bfloat16)
    attn_part = jnp.dot(mixed_low, w_out, preferred_element_type=jnp.float32)
    middle = input_float + lax.psum(attn_part.astype(jnp.bfloat16), "narrow").astype(jnp.float32)
    normed_two, pull_two = jax.vjp(lambda rows: rms_norm(rows, gain_ffn), middle)
    hidden_two = normed_two.astype(jnp.bfloat16)
    unit_two = unit_rows(middle)
    gate = jnp.dot(hidden_two, w_gate, preferred_element_type=jnp.float32)
    up_proj = jnp.dot(hidden_two, w_up, preferred_element_type=jnp.float32)
    active, pull_active = jax.vjp(
        lambda gate_in, up_in: jax.nn.silu(gate_in) * up_in, gate, up_proj
    )
    active_low = active.astype(jnp.bfloat16)
    ffn_part = jnp.dot(active_low, w_down, preferred_element_type=jnp.float32)
    output_low = (
        middle + lax.psum(ffn_part.astype(jnp.bfloat16), "narrow").astype(jnp.float32)
    ).astype(jnp.bfloat16)
    grad_wdown = jnp.einsum("tf,td->fd", active_low, grad_row, preferred_element_type=jnp.float32)
    grad_active = jnp.einsum("td,fd->tf", grad_row, w_down, preferred_element_type=jnp.float32)
    grad_gate, grad_upper = pull_active(grad_active)
    gate_back = grad_gate.astype(jnp.bfloat16)
    upper_back = grad_upper.astype(jnp.bfloat16)
    grad_wgate = jnp.einsum("td,tf->df", hidden_two, gate_back, preferred_element_type=jnp.float32)
    grad_wup = jnp.einsum("td,tf->df", hidden_two, upper_back, preferred_element_type=jnp.float32)
    partial_two = jnp.einsum(
        "tf,df->td", gate_back, w_gate, preferred_element_type=jnp.float32
    ) + jnp.einsum("tf,df->td", upper_back, w_up, preferred_element_type=jnp.float32)
    gain_two = jnp.sum(partial_two * unit_two, axis=0)
    grad_middle = (
        grad_float
        + pull_two(lax.psum(partial_two.astype(jnp.bfloat16), "narrow").astype(jnp.float32))[0]
    )
    middle_low = grad_middle.astype(jnp.bfloat16)
    grad_wout = jnp.einsum("th,td->hd", mixed_low, middle_low, preferred_element_type=jnp.float32)
    grad_mixed = jnp.einsum("td,hd->th", middle_low, w_out, preferred_element_type=jnp.float32)
    grad_mixed = grad_mixed.astype(jnp.bfloat16).reshape(tok_rows, groups, repeat, HD)
    scores = attention_scores(query_low, key_all, mask_local, factor)
    probs = jnp.exp(scores - log_total)
    grad_probs = jnp.einsum(
        "tgrd,kgd->grtk", grad_mixed, value_all, preferred_element_type=jnp.float32
    )
    weighted = jnp.sum(probs * grad_probs, axis=-1, keepdims=True)
    grad_scores = (probs * (grad_probs - weighted)).astype(jnp.bfloat16)
    grad_turned = (
        jnp.einsum("grtk,kgd->tgrd", grad_scores, key_all, preferred_element_type=jnp.float32)
        * factor
    )
    grad_keyall = (
        jnp.einsum("grtk,tgrd->kgd", grad_scores, query_low, preferred_element_type=jnp.float32)
        * factor
    )
    grad_valueall = jnp.einsum(
        "grtk,tgrd->kgd", probs.astype(jnp.bfloat16), grad_mixed, preferred_element_type=jnp.float32
    )
    grad_keys, grad_values = (
        lax.psum_scatter(
            grad_keyall.reshape(total, groups * HD).astype(jnp.bfloat16),
            "wide",
            scatter_dimension=0,
            tiled=True,
        ).astype(jnp.float32),
        lax.psum_scatter(
            grad_valueall.reshape(total, groups * HD).astype(jnp.bfloat16),
            "wide",
            scatter_dimension=0,
            tiled=True,
        ).astype(jnp.float32),
    )
    grad_qraw, gain_q = pull_query(grad_turned.reshape(tok_rows, groups * repeat, HD))
    grad_kraw, gain_k = pull_key(grad_keys.reshape(tok_rows, groups, HD))
    query_back = grad_qraw.reshape(tok_rows, groups * repeat * HD).astype(jnp.bfloat16)
    key_back = grad_kraw.reshape(tok_rows, groups * HD).astype(jnp.bfloat16)
    value_back = grad_values.astype(jnp.bfloat16)
    grad_wquery = jnp.einsum(
        "td,th->dh", hidden_one, query_back, preferred_element_type=jnp.float32
    )
    grad_wkey = jnp.einsum("td,th->dh", hidden_one, key_back, preferred_element_type=jnp.float32)
    grad_wvalue = jnp.einsum(
        "td,th->dh", hidden_one, value_back, preferred_element_type=jnp.float32
    )
    partial_one = (
        jnp.einsum("th,dh->td", query_back, w_query, preferred_element_type=jnp.float32)
        + jnp.einsum("th,dh->td", key_back, w_key, preferred_element_type=jnp.float32)
        + jnp.einsum("th,dh->td", value_back, w_value, preferred_element_type=jnp.float32)
    )
    gain_one = jnp.sum(partial_one * unit_rows(input_float), axis=0)
    grad_input = (
        grad_middle
        + pull_one(lax.psum(partial_one.astype(jnp.bfloat16), "narrow").astype(jnp.float32))[0]
    )
    weight_grads = (
        grad_wquery,
        grad_wkey,
        grad_wvalue,
        grad_wout,
        grad_wgate,
        grad_wup,
        grad_wdown,
    )
    return (output_low, grad_input, weight_grads, (gain_one, gain_two, gain_q, gain_k))


def local_general(
    layer_input,
    grad_out,
    lengths,
    w_query,
    w_key,
    w_value,
    w_out,
    w_gate,
    w_up,
    w_down,
    gain_attn,
    gain_ffn,
    gain_query,
    gain_key,
):
    width = lax.axis_size("wide")
    shards = (w_query, w_key, w_value, w_out, w_gate, w_up, w_down)
    along_rows = (True, True, True, False, True, True, False)
    gains = (gain_attn, gain_ffn, gain_query, gain_key)
    totals = tuple(
        (
            jnp.zeros(
                (
                    (piece.shape[0] * width, piece.shape[1])
                    if rows_first
                    else (piece.shape[0], piece.shape[1] * width)
                ),
                jnp.float32,
            )
            for piece, rows_first in zip(shards, along_rows)
        )
    )
    gain_terms = tuple((jnp.zeros(gain.shape, jnp.float32) for gain in gains))
    outputs = []
    grad_inputs = []
    for micro in range(layer_input.shape[0]):
        gathered = (
            lax.all_gather(w_query, "wide", axis=0, tiled=True),
            lax.all_gather(w_key, "wide", axis=0, tiled=True),
            lax.all_gather(w_value, "wide", axis=0, tiled=True),
            lax.all_gather(w_out, "wide", axis=1, tiled=True),
            lax.all_gather(w_gate, "wide", axis=0, tiled=True),
            lax.all_gather(w_up, "wide", axis=0, tiled=True),
            lax.all_gather(w_down, "wide", axis=1, tiled=True),
        )
        output, grad_input, weight_grads, gain_grads = one_batch(
            layer_input[micro], grad_out[micro], lengths[micro], gathered, gains
        )
        outputs.append(output)
        grad_inputs.append(grad_input)
        gain_terms = tuple((running + fresh for running, fresh in zip(gain_terms, gain_grads)))
        totals = tuple((running + fresh for running, fresh in zip(totals, weight_grads)))
    results = (
        lax.psum_scatter(
            totals[0].astype(jnp.bfloat16), "wide", scatter_dimension=0, tiled=True
        ).astype(jnp.float32),
        lax.psum_scatter(
            totals[1].astype(jnp.bfloat16), "wide", scatter_dimension=0, tiled=True
        ).astype(jnp.float32),
        lax.psum_scatter(
            totals[2].astype(jnp.bfloat16), "wide", scatter_dimension=0, tiled=True
        ).astype(jnp.float32),
        lax.psum_scatter(
            totals[3].astype(jnp.bfloat16), "wide", scatter_dimension=1, tiled=True
        ).astype(jnp.float32),
        lax.psum_scatter(
            totals[4].astype(jnp.bfloat16), "wide", scatter_dimension=0, tiled=True
        ).astype(jnp.float32),
        lax.psum_scatter(
            totals[5].astype(jnp.bfloat16), "wide", scatter_dimension=0, tiled=True
        ).astype(jnp.float32),
        lax.psum_scatter(
            totals[6].astype(jnp.bfloat16), "wide", scatter_dimension=1, tiled=True
        ).astype(jnp.float32),
    )
    gain_total = lax.psum(gain_terms, ("wide", "narrow"))
    return (
        jnp.stack(outputs),
        jnp.stack(grad_inputs),
        results[0],
        results[1],
        results[2],
        results[3],
        results[4],
        results[5],
        results[6],
        gain_total[0],
        gain_total[1],
        gain_total[2],
        gain_total[3],
    )


BLOCK = 256
HEAD_GROUPS = 2
NT = (((1,), (1,)), ((), ()))
TN = (((0,), (0,)), ((), ()))


def piece_starts(lengths_ref, micro, spot):
    start = jnp.zeros_like(spot)
    finish = jnp.int32(0)
    for piece in range(NDOC - 1):
        finish += lengths_ref[micro, piece]
        start = jnp.where(spot >= finish, finish if piece < NDOC - 2 else spot, start)
    return start


def query_lanes(lengths_ref, step_q):
    micro = lax.axis_index("wide") // HEAD_GROUPS
    lane = lax.broadcasted_iota(jnp.int32, (1, 2 * BLOCK), 1)
    spot = lane % BLOCK + step_q * BLOCK
    return spot, piece_starts(lengths_ref, micro, spot)


def key_fits(step_k, spot, start):
    key_spot = lax.broadcasted_iota(jnp.int32, (BLOCK, 1), 0) + step_k * BLOCK
    return (key_spot >= start) & (key_spot <= spot)


def attend_forward(lengths_ref, qkv_ref, mixed_ref, kept_ref, log_ref):
    step_q = pl.program_id(0)
    rows = pl.ds(step_q * BLOCK, BLOCK)
    factor = 1.0 / math.sqrt(HD)
    query = jnp.concatenate([qkv_ref[rows, 0:HD], qkv_ref[rows, HD : 2 * HD]], axis=0)
    spot, start = query_lanes(lengths_ref, step_q)
    micro = lax.axis_index("wide") // HEAD_GROUPS
    first = piece_starts(lengths_ref, micro, step_q * BLOCK) // BLOCK

    def one(step_k, carry):
        total, total_low, mixed = carry
        cols = pl.ds(step_k * BLOCK, BLOCK)
        scores = dot_f32(qkv_ref[cols, 2 * HD : 3 * HD], query, NT)
        exponent = jnp.where(key_fits(step_k, spot, start), jnp.exp(scores * factor), 0.0)
        low = exponent.astype(jnp.bfloat16)
        total += jnp.sum(exponent.reshape(-1, 8, 2 * BLOCK), axis=0)
        total_low += jnp.sum(low.astype(jnp.float32).reshape(-1, 8, 2 * BLOCK), axis=0)
        mixed += dot_f32(qkv_ref[cols, 3 * HD : 4 * HD], low, TN)
        return (total, total_low, mixed)

    zeros = jnp.zeros((8, 2 * BLOCK), jnp.float32)
    total, total_low, mixed = lax.fori_loop(
        first, step_q + 1, one, (zeros, zeros, jnp.zeros((HD, 2 * BLOCK), jnp.float32))
    )
    mixed = (mixed / jnp.sum(total_low, axis=0, keepdims=True)).T
    mixed = jnp.concatenate([mixed[:BLOCK], mixed[BLOCK:]], axis=1)
    mixed_ref[...] = mixed.astype(jnp.bfloat16)
    kept_ref[...] = mixed
    log_total = jnp.log(jnp.sum(total, axis=0, keepdims=True))
    log_ref[...] = jnp.broadcast_to(log_total, zeros.shape)[None]


def attention_out(qkv, lengths):
    total = qkv.shape[0]
    block = lambda i, *_: (i, 0)
    return pl.pallas_call(
        attend_forward,
        out_shape=(
            jax.ShapeDtypeStruct((total, 2 * HD), jnp.bfloat16),
            jax.ShapeDtypeStruct((total, 2 * HD), jnp.float32),
            jax.ShapeDtypeStruct((total // BLOCK, 8, 2 * BLOCK), jnp.float32),
        ),
        grid_spec=pltpu.PrefetchScalarGridSpec(
            num_scalar_prefetch=1,
            grid=(total // BLOCK,),
            in_specs=[pl.BlockSpec((total, 4 * HD), lambda i, *_: (0, 0))],
            out_specs=[
                pl.BlockSpec((BLOCK, 2 * HD), block),
                pl.BlockSpec((BLOCK, 2 * HD), block),
                pl.BlockSpec((1, 8, 2 * BLOCK), lambda i, *_: (i, 0, 0)),
            ],
        ),
        name="attend_forward",
    )(lengths, qkv)


def dot_f32(left, right, dims=(((1,), (0,)), ((), ()))):
    return lax.dot_general(left, right, dims, preferred_element_type=jnp.float32)


SUB = 64
RING = 8
STRIP = 16
FINE = 32
AHEAD = 6
GAIN_PLACES = (0, 2, 4, 6, 10, 13, 16)
LANES = 512
MESH = pl.DeviceIdType.MESH


class Relay:
    def __init__(self, count, own, landed, cross, sems):
        self.count, self.own, self.landed, self.cross = count, own, landed, cross
        self.out_sem, self.land_sem, self.back_sem, self.cross_sem = sems
        spot = lax.axis_index("narrow")
        self.is_end = (spot == 0) | (spot == 3)
        self.is_mid = (spot == 1) | (spot == 2)
        self.inner = 1 + spot // 3
        self.other = 3 - spot
        self.outer = jnp.where(spot == 2, 3, 0)

    def to_inner(self, k):
        return pltpu.make_async_remote_copy(
            src_ref=self.own.at[k],
            dst_ref=self.landed.at[k],
            send_sem=self.out_sem.at[k],
            recv_sem=self.land_sem.at[k],
            device_id={"narrow": self.inner},
            device_id_type=MESH,
        )

    def to_other(self, k):
        return pltpu.make_async_remote_copy(
            src_ref=self.own.at[k],
            dst_ref=self.cross.at[k % RING],
            send_sem=self.out_sem.at[k],
            recv_sem=self.cross_sem.at[k % RING],
            device_id={"narrow": self.other},
            device_id_type=MESH,
        )

    def to_outer(self, k):
        return pltpu.make_async_remote_copy(
            src_ref=self.landed.at[k],
            dst_ref=self.landed.at[k],
            send_sem=self.back_sem.at[k],
            recv_sem=self.land_sem.at[k],
            device_id={"narrow": self.outer},
            device_id_type=MESH,
        )

    def greet(self, peers):
        barrier = pltpu.get_barrier_semaphore()
        for peer in peers:
            pl.semaphore_signal(barrier, inc=1, device_id={"wide": peer}, device_id_type=MESH)

        @pl.when(self.is_end)
        def _():
            pl.semaphore_signal(
                barrier, inc=1, device_id={"narrow": self.inner}, device_id_type=MESH
            )
            pl.semaphore_wait(barrier, 1 + len(peers))

        @pl.when(self.is_mid)
        def _():
            pl.semaphore_signal(
                barrier, inc=1, device_id={"narrow": self.outer}, device_id_type=MESH
            )
            pl.semaphore_signal(
                barrier, inc=1, device_id={"narrow": self.other}, device_id_type=MESH
            )
            pl.semaphore_wait(barrier, 2 + len(peers))

    def send(self, first, number):
        @pl.when(self.is_end)
        def _():
            @pl.loop(0, number)
            def _(i):
                self.to_inner(first + i).start()

    def tick(self, k):
        @pl.when(self.is_mid & (k < self.count))
        def _():
            self.to_inner(k).wait_recv()

            @pl.loop(0, self.own.shape[1] // STRIP)
            def _(i):
                rows = pl.ds(pl.multiple_of(i * STRIP, STRIP), STRIP)
                self.own[k, rows] = (
                    self.own[k, rows].astype(jnp.float32) + self.landed[k, rows].astype(jnp.float32)
                ).astype(jnp.bfloat16)

            self.to_other(k).start()

        @pl.when(self.is_mid & (k >= 2) & (k < self.count + 2))
        def _():
            j = k - 2
            self.to_other(j).wait_recv()

            @pl.loop(0, self.own.shape[1] // STRIP)
            def _(i):
                rows = pl.ds(pl.multiple_of(i * STRIP, STRIP), STRIP)
                self.landed[j, rows] = (
                    self.own[j, rows].astype(jnp.float32)
                    + self.cross[j % RING, rows].astype(jnp.float32)
                ).astype(jnp.bfloat16)

            self.to_outer(j).start()

        @pl.when(self.is_end & (k >= 4) & (k < self.count + 4))
        def _():
            self.to_outer(k - 4).wait_recv()

    def place(self, p):
        self.tick(2 * p)
        self.tick(2 * p + 1)

    def drain(self, first):
        @pl.loop(first, self.count)
        def _(k):
            self.to_inner(k).wait_send()

        @pl.loop(0, self.count)
        def _(k):
            @pl.when(self.is_mid)
            def _():
                self.to_outer(k).wait_send()


def wide_peers(width):
    spot = lax.axis_index("wide")
    return [lax.rem(spot + step, width) for step in range(1, width)]


def greet_wide(width):
    barrier = pltpu.get_barrier_semaphore()
    for peer in wide_peers(width):
        pl.semaphore_signal(barrier, inc=1, device_id={"wide": peer}, device_id_type=MESH)
    pl.semaphore_wait(barrier, width - 1)


class Exchange:
    def __init__(self, block, slot, send_sem, land_sem):
        self.block, self.slot = block, slot
        self.send_sem, self.land_sem = send_sem, land_sem
        self.spot = lax.axis_index("wide")

    def remote(self, target, source):
        return pltpu.make_async_remote_copy(
            src_ref=self.block(target),
            dst_ref=self.slot(source),
            send_sem=self.send_sem.at[target],
            recv_sem=self.land_sem.at[source],
            device_id={"wide": target},
            device_id_type=MESH,
        )

    def here(self):
        return pltpu.make_async_copy(
            self.block(self.spot), self.slot(self.spot), self.land_sem.at[self.spot]
        )

    def send(self, target):
        @pl.when(target == self.spot)
        def _():
            self.here().start()

        @pl.when(target != self.spot)
        def _():
            self.remote(target, self.spot).start()

    def sent(self, target, home=False):
        @pl.when(target != self.spot)
        def _():
            self.remote(target, self.spot).wait_send()

        if home:

            @pl.when(target == self.spot)
            def _():
                self.here().wait()

    def wait(self, source, home=True):
        if home:

            @pl.when(source == self.spot)
            def _():
                self.here().wait()

        @pl.when(source != self.spot)
        def _():
            self.remote(self.spot, source).wait_recv()


class Gather:
    def __init__(self, parts, send_sem, land_sem):
        self.parts, self.send_sem, self.land_sem = parts, send_sem, land_sem
        me = lax.axis_index("wide")
        flip = lambda spot, bit: spot + bit - 2 * bit * (spot // bit % 2)
        self.me, self.near = me, flip(me, 1)
        self.across, self.along = flip(me, 2), flip(me, 4)
        self.far = flip(self.across, 4)
        self.flip = flip

    def move(self, part, kind, source, target, device):
        return pltpu.make_async_remote_copy(
            src_ref=source,
            dst_ref=target,
            send_sem=self.send_sem.at[part, kind],
            recv_sem=self.land_sem.at[part, kind],
            device_id={"wide": device},
            device_id_type=MESH,
        )

    def going(self, part, kind):
        own, slot, half = self.parts[part]
        across, along, near = self.across, self.along, self.near
        source, target, device = (
            lambda: (own, slot(self.me), across),
            lambda: (own, slot(self.me), along),
            lambda: (own, slot(self.me), near),
            lambda: (half(along, 0), half(along, 0), across),
            lambda: (half(across, 1), half(across, 1), along),
            lambda: (slot(across), slot(across), near),
            lambda: (slot(along), slot(along), near),
            lambda: (half(self.far, 0), half(self.far, 0), near),
            lambda: (half(self.far, 1), half(self.far, 1), near),
        )[kind]()
        return self.move(part, kind, source, target, device)

    def coming(self, part, kind):
        _, slot, half = self.parts[part]
        flip = self.flip
        place = (
            lambda: slot(self.across),
            lambda: slot(self.along),
            lambda: slot(self.near),
            lambda: half(self.far, 0),
            lambda: half(self.far, 1),
            lambda: slot(flip(self.across, 1)),
            lambda: slot(flip(self.along, 1)),
            lambda: half(flip(self.far, 1), 0),
            lambda: half(flip(self.far, 1), 1),
        )[kind]()
        return self.move(part, kind, place, place, self.near)

    def here(self, part):
        own, slot, _ = self.parts[part]
        return pltpu.make_async_copy(own, slot(self.me), self.land_sem.at[part, 9])

    def first(self, part):
        for kind in (0, 1, 2):
            self.going(part, kind).start()
        self.here(part).start()

    def second(self, part):
        self.coming(part, 1).wait_recv()
        self.going(part, 3).start()
        self.coming(part, 0).wait_recv()
        self.going(part, 4).start()
        self.going(part, 6).start()
        self.going(part, 5).start()

    def third(self, part):
        self.coming(part, 3).wait_recv()
        self.going(part, 7).start()
        self.coming(part, 4).wait_recv()
        self.going(part, 8).start()

    def fourth(self, part):
        self.here(part).wait()
        for kind in (2, 5, 6, 7, 8):
            self.coming(part, kind).wait_recv()

    def drain(self):
        for part in range(len(self.parts)):
            for kind in range(9):
                self.going(part, kind).wait_send()


def project_kernel(
    input_ref,
    gain_ref,
    query_w,
    key_w,
    value_w,
    lengths_ref,
    head_gain_ref,
    hidden_out,
    raw_out,
    packed_out,
    weight_out,
    cosine_ref,
    sine_ref,
    rows_v,
    weight_v,
    hidden_v,
    raw_v,
    pack_v,
    load_sem,
    keep_sem,
    hidden_sem,
    send_sem,
    land_sem,
    part_send,
    part_land,
):
    micro, tok, model = input_ref.shape
    width = packed_out.shape[0]
    groups = width // micro
    heads = 2 * groups
    spot = lax.axis_index("wide")
    swap = Exchange(
        lambda target: pack_v.at[target], lambda source: packed_out.at[source], send_sem, land_sem
    )
    load = pltpu.make_async_copy(input_ref, rows_v, load_sem.at[0])
    load.start()
    piece = query_w.shape[0]

    def part(own, first):
        cols = pl.ds(first, own.shape[1])
        return (
            own,
            lambda s: weight_v.at[pl.ds(pl.multiple_of(s * piece, piece), piece), cols],
            lambda s, h: weight_v.at[
                pl.ds(pl.multiple_of(s * piece + h * piece // 2, piece // 2), piece // 2), cols
            ],
        )

    q_cols, k_cols = query_w.shape[1], key_w.shape[1]
    gather = Gather(
        [part(query_w, 0), part(key_w, q_cols), part(value_w, q_cols + k_cols)],
        part_send,
        part_land,
    )
    greet_wide(width)
    for p in range(3):
        gather.first(p)
    load.wait()
    hidden_copy = pltpu.make_async_copy(hidden_v, hidden_out, hidden_sem)

    @pl.loop(0, micro)
    def _(m):
        rows = rows_v[m].astype(jnp.float32)
        scale = lax.rsqrt(jnp.mean(rows * rows, axis=-1, keepdims=True) + EPSILON)
        hidden_v[m] = (rows * scale * gain_ref[...]).astype(jnp.bfloat16)

    hidden_copy.start()
    lane = lax.broadcasted_iota(jnp.int32, (1, HD), 1)
    frequency = jnp.exp(
        -math.log(THETA) * (2 * (lane % (HD // 2))).astype(jnp.float32) / HD
    )
    sign = jnp.where(lane < HD // 2, -1.0, 1.0)
    token = lax.broadcasted_iota(jnp.int32, (tok, 1), 0) + spot * tok

    @pl.loop(0, micro)
    def _(m):
        start = jnp.zeros_like(token)
        finish = jnp.int32(0)
        for piece_index in range(NDOC - 1):
            finish += lengths_ref[m, piece_index]
            start = jnp.where(token >= finish, finish, start)
        turning = (token - start).astype(jnp.float32) * frequency
        span = pl.ds(pl.multiple_of(m * tok, tok), tok)
        cosine_ref[span, :] = jnp.cos(turning)
        sine_ref[span, :] = jnp.sin(turning) * sign

    for p in range(3):
        gather.second(p)
    for p in range(3):
        gather.third(p)
    for p in range(3):
        gather.fourth(p)
    weight_copy = pltpu.make_async_copy(weight_v, weight_out, load_sem.at[1])
    weight_copy.start()

    def turn(step):
        far = micro - 1 - step
        own = spot // groups
        return (own + far) % 2 + 2 * ((own // 2 + far // 2) % 2)

    def keep(step):
        return pltpu.make_async_copy(
            raw_v.at[step % 2], raw_out.at[turn(step)], keep_sem.at[step % 2]
        )

    @pl.loop(0, micro)
    def _(step):
        m = turn(step)

        @pl.when(step >= 2)
        def _():
            keep(step - 2).wait()

        heads_all = dot_f32(hidden_v[m], weight_v[...])
        span = pl.ds(pl.multiple_of(m * tok, tok), tok)
        cosine, sine = cosine_ref[span, :], sine_ref[span, :]
        raw_v[step % 2] = heads_all[:, : (heads + groups) * HD]
        for h in range(heads + groups):
            raw = heads_all[:, h * HD : (h + 1) * HD]
            gain = head_gain_ref[0:1, :] if h < heads else head_gain_ref[1:2, :]
            unit = raw * lax.rsqrt(jnp.mean(raw * raw, axis=-1, keepdims=True) + EPSILON) * gain
            turned = unit * cosine + pltpu.roll(unit, HD // 2, 1) * sine
            g, place = (h // 2, h % 2) if h < heads else (h - heads, 2)
            pack_v[m * groups + g, :, place * HD : (place + 1) * HD] = turned.astype(jnp.bfloat16)
        for g in range(groups):
            first = (heads + groups + g) * HD
            pack_v[m * groups + g, :, 3 * HD :] = heads_all[:, first : first + HD].astype(
                jnp.bfloat16
            )
            swap.send(m * groups + g)
        keep(step).start()

    keep(micro - 2).wait()
    keep(micro - 1).wait()

    @pl.loop(0, width)
    def _(d):
        swap.sent(d)
        swap.wait(d)

    gather.drain()
    hidden_copy.wait()
    weight_copy.wait()


def project(layer_input, gain_attn, weights, lengths, head_gains, width):
    micro, tok, model = layer_input.shape
    groups = width // micro
    low = jnp.bfloat16
    anywhere = pl.BlockSpec(memory_space=pl.ANY)
    inside = pl.BlockSpec(memory_space=pltpu.VMEM)
    raw = 3 * groups * HD
    columns = sum(weight.shape[1] for weight in weights)
    return pl.pallas_call(
        project_kernel,
        out_shape=(
            jax.ShapeDtypeStruct((micro, tok, model), low),
            jax.ShapeDtypeStruct((micro, tok, raw), jnp.float32),
            jax.ShapeDtypeStruct((width, tok, 4 * HD), low),
            jax.ShapeDtypeStruct((model, columns), low),
            jax.ShapeDtypeStruct((micro * tok, HD), jnp.float32),
            jax.ShapeDtypeStruct((micro * tok, HD), jnp.float32),
        ),
        in_specs=[anywhere, inside, anywhere, anywhere, anywhere]
        + [pl.BlockSpec(memory_space=pltpu.SMEM), inside],
        out_specs=[anywhere] * 4 + [inside] * 2,
        scratch_shapes=[
            pltpu.VMEM((micro, tok, model), low),
            pltpu.VMEM((model, columns), low),
            pltpu.VMEM((micro, tok, model), low),
            pltpu.VMEM((2, tok, raw), jnp.float32),
            pltpu.VMEM((width, tok, 4 * HD), low),
            pltpu.SemaphoreType.DMA((2,)),
            pltpu.SemaphoreType.DMA((2,)),
            pltpu.SemaphoreType.DMA,
            pltpu.SemaphoreType.DMA((width,)),
            pltpu.SemaphoreType.DMA((width,)),
            pltpu.SemaphoreType.DMA((3, 9)),
            pltpu.SemaphoreType.DMA((3, 10)),
        ],
        compiler_params=pltpu.CompilerParams(
            collective_id=2, has_side_effects=True, vmem_limit_bytes=40 << 20
        ),
        cost_estimate=pl.CostEstimate(
            flops=20_000_000_000, bytes_accessed=40_000_000, transcendentals=0
        ),
        name="project",
    )(layer_input, gain_attn[None, :], *weights, lengths, head_gains)


def weights_kernel(
    lengths_ref,
    qkv_ref,
    upper_ref,
    kept_ref,
    log_ref,
    raw_ref,
    hidden_ref,
    mixed_ref,
    low_ref,
    late_ref,
    input_ref,
    cosine_ref,
    sine_ref,
    head_gain_ref,
    _,
    back_out,
    grad_out,
    gain_out,
    output_out,
    own,
    landed,
    cross,
    out_sem,
    relay_sem,
    return_sem,
    cross_sem,
    land_v,
    raw_v,
    hidden_v,
    mixed_v,
    low_v,
    back_v,
    grad_v,
    pair_v,
    middle_v,
    rows_v,
    qkv_v,
    upper_v,
    kept_v,
    log_v,
    sent_v,
    query_sum,
    key_sum,
    value_sum,
    load_sem,
    back_sem,
    tile_sem,
    send_sems,
    land_sems,
    pair_sems,
    late_sem,
    attn_sem,
):
    micro, tok, heads_in = mixed_ref.shape
    width = upper_ref.shape[0]
    groups = width // micro
    heads = 2 * groups
    model = hidden_ref.shape[2]
    piece = model // width
    count = micro * tok
    factor = 1.0 / math.sqrt(HD)
    halves = (pl.ds(0, 2 * HD), pl.ds(2 * HD, 2 * HD))
    swaps = [
        Exchange(
            lambda target, cols=cols: sent_v.at[target, :, cols],
            lambda source, cols=cols: land_v.at[source, :, cols],
            send_sems.at[i],
            land_sems.at[i],
        )
        for i, cols in enumerate(halves)
    ]
    attn_loads = [
        pltpu.make_async_copy(source, target, attn_sem.at[i])
        for i, (source, target) in enumerate(
            ((qkv_ref, qkv_v), (upper_ref, upper_v), (kept_ref, kept_v), (log_ref, log_v))
        )
    ]
    loads = [
        pltpu.make_async_copy(mixed_ref, mixed_v, load_sem.at[0]),
        pltpu.make_async_copy(low_ref, low_v, load_sem.at[1]),
        pltpu.make_async_copy(raw_ref, raw_v, load_sem.at[2]),
        pltpu.make_async_copy(hidden_ref, hidden_v, load_sem.at[3]),
    ]
    per = tok // SUB
    relay = Relay(per, own, landed, cross, (out_sem, relay_sem, return_sem, cross_sem))
    late_loads = [
        pltpu.make_async_copy(late_ref.at[0], own, late_sem.at[0]),
        pltpu.make_async_copy(late_ref.at[1], middle_v, late_sem.at[1]),
        pltpu.make_async_copy(input_ref.at[micro - 1], rows_v, late_sem.at[2]),
    ]
    for copy in attn_loads + late_loads + loads:
        copy.start()
    key_sum[...] = jnp.zeros_like(key_sum)
    value_sum[...] = jnp.zeros_like(value_sum)
    relay.greet(wide_peers(width))
    spot = lax.axis_index("wide")
    for copy in late_loads:
        copy.wait()
    relay.send(0, per)
    for copy in attn_loads:
        copy.wait()
    band = width * tok // 2 // BLOCK

    @pl.loop(0, width)
    def _(step):
        far = micro - 1 - step // 2
        chip = spot // 2
        turn = (chip + far) % 2 + 2 * ((chip // 2 + far // 2) % 2)
        step_q = 2 * turn + step % 2
        rows = pl.ds(pl.multiple_of(step_q * BLOCK, BLOCK), BLOCK)
        query = jnp.concatenate([qkv_v[rows, 0:HD], qkv_v[rows, HD : 2 * HD]], axis=0)
        grad = jnp.concatenate([upper_v[step_q, :, 0:HD], upper_v[step_q, :, HD : 2 * HD]], axis=0)
        kept = jnp.concatenate([kept_v[rows, 0:HD], kept_v[rows, HD : 2 * HD]], axis=0)
        weighted = lax.dot_general(
            jnp.ones((8, HD), jnp.float32),
            grad.astype(jnp.float32) * kept,
            NT,
            precision=lax.Precision.HIGHEST,
            preferred_element_type=jnp.float32,
        )[0:1]
        log_total = log_v[step_q, 0:1, :]
        spots, start = query_lanes(lengths_ref, step_q)
        query_sum[...] = jnp.zeros_like(query_sum)

        @pl.loop(0, band + 1)
        def _(t):
            step_k = step_q - band + t

            @pl.when(step_k >= 0)
            def _():
                cols = pl.ds(pl.multiple_of(step_k * BLOCK, BLOCK), BLOCK)
                key = qkv_v[cols, 2 * HD : 3 * HD]
                scores = dot_f32(key, query, NT) * factor
                probs = jnp.where(
                    key_fits(step_k, spots, start), jnp.exp(scores - log_total), 0.0
                )
                grad_probs = dot_f32(qkv_v[cols, 3 * HD : 4 * HD], grad, NT)
                grad_scores = (probs * (grad_probs - weighted)).astype(jnp.bfloat16)
                value_sum[cols, :] += dot_f32(probs.astype(jnp.bfloat16), grad)
                key_sum[cols, :] += dot_f32(grad_scores, query)
                query_sum[...] += dot_f32(grad_scores, key, TN)

        part = (query_sum[...] * factor).astype(jnp.bfloat16)
        sent_v[step_q, :, 0:HD] = part[:BLOCK]
        sent_v[step_q, :, HD : 2 * HD] = part[BLOCK:]
        swaps[0].send(step_q)

        @pl.when(step % 2 == 1)
        def _():
            relay.tick(step // 2)

    @pl.loop(0, width)
    def _(i):
        rows = pl.ds(pl.multiple_of(i * BLOCK, BLOCK), BLOCK)
        sent_v[i, :, 2 * HD : 3 * HD] = (key_sum[rows, :] * factor).astype(jnp.bfloat16)
        sent_v[i, :, 3 * HD : 4 * HD] = value_sum[rows, :].astype(jnp.bfloat16)

    for step in range(width - 1, -1, -1):
        swaps[1].send(lax.rem(spot + step, width))
    loads[0].wait()
    loads[1].wait()
    mixed_all = mixed_v[...].reshape(count, heads_in)
    for n in range(model // LANES):
        low = low_v[:, :, n * LANES : (n + 1) * LANES].reshape(count, LANES)
        part = dot_f32(mixed_all, low, TN).astype(jnp.bfloat16)
        for i in range(LANES // piece):
            for b in range(heads_in // piece):
                grad_v[
                    n * (LANES // piece) + i, :, pl.ds(2 * heads_in + b * piece, piece)
                ] = part[b * piece : (b + 1) * piece, i * piece : (i + 1) * piece]
    loads[2].wait()
    gain_out[...] = jnp.zeros_like(gain_out)

    def back_copy(m):
        return pltpu.make_async_copy(back_v.at[m], back_out.at[m], back_sem.at[m])

    def turn_back(m, h):
        span = pl.ds(pl.multiple_of(m * tok, tok), tok)
        raw = raw_v[m, :, h * HD : (h + 1) * HD]
        kind = 0 if h < heads else 1
        gain = head_gain_ref[kind : kind + 1, :]
        g, place = (h // 2, h % 2) if h < heads else (h - heads, 2)
        grad = land_v[m * groups + g, :, place * HD : (place + 1) * HD].astype(jnp.float32)
        straight = grad * cosine_ref[span, :] + pltpu.roll(grad * sine_ref[span, :], HD // 2, 1)
        scale = lax.rsqrt(jnp.mean(raw * raw, axis=-1, keepdims=True) + EPSILON)
        gain_out[kind : kind + 1, :] += jnp.sum(straight * (raw * scale), axis=0, keepdims=True)
        pulled = straight * gain
        along = jnp.mean(pulled * raw, axis=-1, keepdims=True)
        back_v[m, :, h * HD : (h + 1) * HD] = (
            scale * (pulled - raw * (scale * scale * along))
        ).astype(jnp.bfloat16)

    @pl.loop(0, width)
    def _(d):
        swaps[0].wait(d)

    @pl.loop(0, micro)
    def _(m):
        for h in range(heads):
            turn_back(m, h)

        @pl.when(m == 1)
        def _():
            relay.tick(4)

    relay.tick(5)

    @pl.loop(0, width)
    def _(d):
        swaps[1].wait(d)

    @pl.loop(0, micro)
    def _(m):
        for h in range(heads, heads + groups):
            turn_back(m, h)
        for g in range(groups):
            first = (heads + groups + g) * HD
            back_v[m, :, first : first + HD] = land_v[m * groups + g, :, 3 * HD :]
        back_copy(m).start()

    loads[3].wait()

    core = lax.rem(spot, 2)
    near = spot + 1 - 2 * core

    def tile_copy(c):
        return pltpu.make_async_copy(grad_v.at[2 * c + core], grad_out.at[c, 2], tile_sem.at[c])

    def pair_copy(c):
        return pltpu.make_async_remote_copy(
            src_ref=grad_v.at[2 * c + 1 - core],
            dst_ref=pair_v.at[c],
            send_sem=pair_sems.at[0, c],
            recv_sem=pair_sems.at[1, c],
            device_id={"wide": near},
            device_id_type=MESH,
        )

    def tile(i):
        left = hidden_v[:, :, pl.ds(pl.multiple_of(i * piece, piece), piece)].reshape(count, piece)
        return dot_f32(left, back_v[...].reshape(count, 2 * heads_in), TN)

    @pl.loop(0, width // 2)
    def _(c):
        i = 2 * c + 1 - core
        grad_v[i, :, 0 : 2 * heads_in] = tile(i).astype(jnp.bfloat16)
        pair_copy(c).start()

        @pl.when(c % 2 == 1)
        def _():
            relay.tick(6 + c // 2)

    output_copy = pltpu.make_async_copy(rows_v, output_out, late_sem.at[3])
    for r in range(per):
        span = slice(r * SUB, (r + 1) * SUB)
        rows_v[span, :] = (
            rows_v[span, :].astype(jnp.float32)
            + middle_v[r].astype(jnp.float32)
            + landed[r].astype(jnp.float32)
        ).astype(jnp.bfloat16)
    output_copy.start()

    @pl.loop(0, width // 2)
    def _(c):
        i = 2 * c + core
        part = tile(i)
        pair_copy(c).wait_recv()
        grad_v[i, :, 0 : 2 * heads_in] = (
            part + pair_v[c, :, 0 : 2 * heads_in].astype(jnp.float32)
        ).astype(jnp.bfloat16)
        grad_v[i, :, 2 * heads_in :] = (
            grad_v[i, :, 2 * heads_in :].astype(jnp.float32)
            + pair_v[c, :, 2 * heads_in :].astype(jnp.float32)
        ).astype(jnp.bfloat16)
        tile_copy(c).start()

    @pl.loop(0, width // 2)
    def _(c):
        tile_copy(c).wait()
        pair_copy(c).wait_send()

    @pl.loop(0, width)
    def _(i):
        for swap in swaps:
            swap.sent(i)

    for m in range(micro):
        back_copy(m).wait()
    output_copy.wait()
    relay.drain(0)


def attention_gradients(
    lengths, qkv, upper, kept, log_total, raw, hidden, mixed, middle_low, late, layer_input, *rest
):
    micro, tok, heads_in = mixed.shape
    width = upper.shape[0]
    total = qkv.shape[0]
    model = hidden.shape[2]
    low = jnp.bfloat16
    anywhere = pl.BlockSpec(memory_space=pl.ANY)
    inside = pl.BlockSpec(memory_space=pltpu.VMEM)
    return pl.pallas_call(
        weights_kernel,
        out_shape=(
            jax.ShapeDtypeStruct((micro, tok, 2 * heads_in), low),
            jax.ShapeDtypeStruct((width // 2, 3, model // width, 3 * heads_in), low),
            jax.ShapeDtypeStruct((2, HD), jnp.float32),
            jax.ShapeDtypeStruct((tok, model), low),
        ),
        in_specs=[pl.BlockSpec(memory_space=pltpu.SMEM)]
        + [anywhere] * 10
        + [inside] * 3
        + [anywhere],
        input_output_aliases={14: 1},
        out_specs=[anywhere, anywhere, inside, anywhere],
        scratch_shapes=relay_scratch(tok // SUB, model)
        + [
            pltpu.VMEM((width, tok, 4 * HD), low),
            pltpu.VMEM(raw.shape, jnp.float32),
            pltpu.VMEM(hidden.shape, low),
            pltpu.VMEM(mixed.shape, low),
            pltpu.VMEM(middle_low.shape, low),
            pltpu.VMEM((micro, tok, 2 * heads_in), low),
            pltpu.VMEM((width, model // width, 3 * heads_in), low),
            pltpu.VMEM((width // 2, model // width, 3 * heads_in), low),
            pltpu.VMEM((tok // SUB, SUB, model), low),
            pltpu.VMEM((tok, model), low),
            pltpu.VMEM(qkv.shape, low),
            pltpu.VMEM(upper.shape, low),
            pltpu.VMEM(kept.shape, jnp.float32),
            pltpu.VMEM(log_total.shape, jnp.float32),
            pltpu.VMEM((width, tok, 4 * HD), low),
            pltpu.VMEM((2 * BLOCK, HD), jnp.float32),
            pltpu.VMEM((total, HD), jnp.float32),
            pltpu.VMEM((total, HD), jnp.float32),
            pltpu.SemaphoreType.DMA((4,)),
            pltpu.SemaphoreType.DMA((micro,)),
            pltpu.SemaphoreType.DMA((width // 2,)),
            pltpu.SemaphoreType.DMA((2, width)),
            pltpu.SemaphoreType.DMA((2, width)),
            pltpu.SemaphoreType.DMA((2, width // 2)),
            pltpu.SemaphoreType.DMA((4,)),
            pltpu.SemaphoreType.DMA((4,)),
        ],
        compiler_params=pltpu.CompilerParams(
            collective_id=3, has_side_effects=True, vmem_limit_bytes=56 << 20
        ),
        cost_estimate=pl.CostEstimate(
            flops=1_000_000_000, bytes_accessed=1_000_000, transcendentals=0
        ),
        name="attention_gradients",
    )(lengths, qkv, upper, kept, log_total, raw, hidden, mixed, middle_low, late, layer_input, *rest)


def relay_scratch(count, model, extra=0, rows=SUB):
    return [
        pltpu.VMEM((count + extra, rows, model), jnp.bfloat16),
        pltpu.VMEM((count, rows, model), jnp.bfloat16),
        pltpu.VMEM((RING, rows, model), jnp.bfloat16),
        pltpu.SemaphoreType.DMA((count,)),
        pltpu.SemaphoreType.DMA((count,)),
        pltpu.SemaphoreType.DMA((count,)),
        pltpu.SemaphoreType.DMA((RING,)),
    ]


def feed_kernel(
    mixed_ref,
    input_ref,
    grad_ref,
    gain_ref,
    pack_ref,
    up_w,
    down_w,
    hidden_out,
    active_out,
    gate_out,
    upper_out,
    output_out,
    middle_out,
    low_out,
    mixed_out,
    gain_out,
    weight_out,
    heads_out,
    early_out,
    late_out,
    own,
    landed,
    cross,
    out_sem,
    land_sem,
    back_sem,
    cross_sem,
    out_v,
    gate_v,
    up_v,
    down_v,
    mixed_v,
    rows_v,
    grads_v,
    hidden_v,
    stage_v,
    scale_v,
    middle_v,
    output_v,
    mixback_v,
    weight_sem,
    attn_sem,
    load_sem,
    hidden_sem,
    stage_sem,
    final_sem,
    reload_sem,
    tile_sem,
    ahead_sems,
    behind_sems,
    heads_sem,
    part_send,
    part_land,
    pair_sems,
    credit,
    late_sem,
):
    micro, tok, model = input_ref.shape
    width, _, piece = pack_ref.shape
    heads_in = out_v.shape[0]
    groups = width // micro
    per = tok // SUB
    hid = gate_v.shape[1]
    count = micro * tok
    blocks = hid // piece
    late = 3 * micro * per - per
    relay = Relay(late, own, landed, cross, (out_sem, land_sem, back_sem, cross_sem))
    n_up = hid // LANES
    n_down = model // LANES
    slots = n_up + n_down

    ahead = Exchange(
        lambda target: mixed_ref.at[target],
        lambda source: mixed_v.at[
            source // groups, :, pl.ds(pl.multiple_of((source % groups) * 2 * HD, 2 * HD), 2 * HD)
        ],
        ahead_sems.at[0],
        ahead_sems.at[1],
    )
    behind = Exchange(
        lambda target: mixback_v.at[
            target // groups % 2,
            :,
            pl.ds(pl.multiple_of((target % groups) * 2 * HD, 2 * HD), 2 * HD),
        ],
        lambda source: mixed_out.at[source],
        behind_sems.at[0],
        behind_sems.at[1],
    )
    attn_copies = [
        pltpu.make_async_copy(
            pack_ref.at[i, pl.ds(0, heads_in)],
            out_v.at[:, pl.ds(i * piece, piece)],
            attn_sem.at[i],
        )
        for i in range(width)
    ]
    weight_copies = [
        pltpu.make_async_copy(
            pack_ref.at[i, pl.ds(heads_in + j * piece, piece)],
            gate_v.at[pl.ds(i * piece, piece), pl.ds(j * piece, piece)],
            weight_sem.at[i, j],
        )
        for i in range(width)
        for j in range(blocks)
    ]

    def up_part(j):
        cols = pl.ds(j * LANES, LANES)
        return (
            up_w.at[:, cols],
            lambda s: up_v.at[pl.ds(pl.multiple_of(s * piece, piece), piece), cols],
            lambda s, h: up_v.at[
                pl.ds(pl.multiple_of(s * piece + h * piece // 2, piece // 2), piece // 2), cols
            ],
        )

    def down_part(j):
        return (
            down_w.at[pl.ds(j * LANES, LANES)],
            lambda s: down_v.at[
                pl.ds(j * LANES, LANES), pl.ds(pl.multiple_of(s * piece, piece), piece)
            ],
            lambda s, h: down_v.at[
                pl.ds(j * LANES + h * LANES // 2, LANES // 2),
                pl.ds(pl.multiple_of(s * piece, piece), piece),
            ],
        )

    gather = Gather(
        [make(j) for j in range(n_up) for make in (up_part, down_part)], part_send, part_land
    )

    def both(action, j):
        action(2 * j)
        action(2 * j + 1)

    for copy in attn_copies + weight_copies:
        copy.start()

    def loads(n):
        slot = n % 2
        return (
            pltpu.make_async_copy(input_ref.at[n % micro], rows_v.at[slot], load_sem.at[slot, 0]),
            pltpu.make_async_copy(grad_ref.at[n % micro], grads_v.at[slot], load_sem.at[slot, 1]),
        )

    def start_loads(n):
        for copy in loads(n):
            copy.start()

    def wait_loads(n):
        for copy in loads(n):
            copy.wait()

    start_loads(0)
    gain_out[...] = jnp.zeros_like(gain_out)
    relay.greet(wide_peers(width))
    spot = lax.axis_index("wide")
    for step in range(width):
        ahead.send(lax.rem(spot + step, width))
    both(gather.first, 0)
    both(gather.first, 1)
    for copy in attn_copies:
        copy.wait()

    def heads_copy(m):
        return pltpu.make_async_copy(mixed_v.at[m], heads_out.at[m], heads_sem.at[m])

    @pl.loop(0, micro)
    def _(m):
        for g in range(groups):
            ahead.wait(m * groups + g)
        heads_copy(m).start()
        for n in range(n_down):
            cols = pl.ds(n * LANES, LANES)
            part = dot_f32(mixed_v[m], out_v[:, cols]).astype(jnp.bfloat16)
            for r in range(per):
                own[m * per + r, :, cols] = part[r * SUB : (r + 1) * SUB]
        relay.send(m * per, per)

    first_ticks = per + 4

    for k in range(first_ticks):
        if k == 4:
            both(gather.second, 0)
        if k == 5:
            both(gather.first, 2)
        if k == 6:
            both(gather.second, 1)
        if k == 7:
            both(gather.third, 0)
        relay.tick(k)

    for copy in weight_copies:
        copy.wait()

    def hidden_copy(m):
        return pltpu.make_async_copy(hidden_v, hidden_out.at[m], hidden_sem)

    def stage_copies(m):
        return [
            pltpu.make_async_copy(stage_v.at[i], target.at[m], stage_sem.at[i])
            for i, target in enumerate((active_out, gate_out, upper_out))
        ]

    base = micro * per

    @pl.loop(0, micro)
    def _(m):
        slot = m % 2
        wait_loads(m)
        start_loads(m + 1)

        @pl.when(m > 0)
        def _():
            hidden_copy(m - 1).wait()
            for copy in stage_copies(m - 1):
                copy.wait()

        @pl.loop(0, per)
        def _(r):
            span = pl.ds(pl.multiple_of(r * SUB, SUB), SUB)
            middle = rows_v[slot, span, :].astype(jnp.float32) + landed[m * per + r].astype(
                jnp.float32
            )
            scale = lax.rsqrt(jnp.mean(middle * middle, axis=-1, keepdims=True) + EPSILON)
            scale_v[span, :] = scale
            hidden_v[span, :] = (middle * scale * gain_ref[...]).astype(jnp.bfloat16)

        hidden_copy(m).start()

        @pl.loop(0, n_up)
        def _(j):
            relay.tick(first_ticks + slots * m + j)
            for turn in range(n_up):

                @pl.when((m == 0) & (j == turn))
                def _():
                    if turn == 0:
                        both(gather.second, 2)
                    if turn + 1 < n_up:
                        both(gather.third, turn + 1)
                    both(gather.fourth, turn)

            cols = pl.ds(pl.multiple_of(j * LANES, LANES), LANES)
            gate = dot_f32(hidden_v[...], gate_v[:, cols])
            up_proj = dot_f32(hidden_v[...], up_v[:, cols])
            grad_active = dot_f32(grads_v[slot], down_v[cols, :], NT)
            squash = 1.0 / (1.0 + jnp.exp(-gate))
            silu = gate * squash
            stage_v[0, :, cols] = (silu * up_proj).astype(jnp.bfloat16)
            stage_v[1, :, cols] = (
                grad_active * up_proj * (squash * (1.0 + gate * (1.0 - squash)))
            ).astype(jnp.bfloat16)
            stage_v[2, :, cols] = (grad_active * silu).astype(jnp.bfloat16)
        for copy in stage_copies(m):
            copy.start()

        @pl.loop(0, n_down)
        def _(n):
            relay.tick(first_ticks + slots * m + n_up + n)
            cols = pl.ds(pl.multiple_of(n * LANES, LANES), LANES)
            back = dot_f32(stage_v[1], gate_v[cols, :], NT) + dot_f32(
                stage_v[2], up_v[cols, :], NT
            )
            ahead = dot_f32(stage_v[0], down_v[:, cols]).astype(jnp.bfloat16)
            gain_sum = jnp.zeros((1, LANES), jnp.float32)
            for r in range(per):
                part = slice(r * SUB, (r + 1) * SUB)
                own[base + 2 * per * m + r, :, cols] = back[part].astype(jnp.bfloat16)
                own[base + 2 * per * m + per + r, :, cols] = ahead[part]
                unit = (
                    rows_v[slot, pl.ds(r * SUB, SUB), cols].astype(jnp.float32)
                    + landed[m * per + r, :, cols].astype(jnp.float32)
                ) * scale_v[pl.ds(r * SUB, SUB), :]
                gain_sum += jnp.sum(back[part] * unit, axis=0, keepdims=True)
            gain_out[:, cols] += gain_sum

        relay.send(base + 2 * per * m, per)

        @pl.when(m < micro - 1)
        def _():
            relay.send(base + 2 * per * m + per, per)

    hidden_copy(micro - 1).wait()
    for copy in stage_copies(micro - 1):
        copy.wait()
    late_copies = [
        pltpu.make_async_copy(own.at[pl.ds(late, per)], late_out.at[0], late_sem.at[0]),
        pltpu.make_async_copy(
            landed.at[pl.ds((micro - 1) * per, per)], late_out.at[1], late_sem.at[1]
        ),
    ]
    for copy in late_copies:
        copy.start()

    gather.drain()
    core = lax.rem(spot, 2)
    near = gather.near

    def offer():
        pl.semaphore_signal(credit, inc=1, device_id={"wide": near}, device_id_type=MESH)

    offer()

    @pl.loop(0, base)
    def _(k):
        relay.to_inner(k).wait_send()

    def reloads(m):
        rows = pl.ds(m * tok, tok)
        return [
            pltpu.make_async_copy(hidden_out.at[m], down_v.at[rows], reload_sem.at[m, 0]),
            pltpu.make_async_copy(gate_out.at[m], gate_v.at[rows], reload_sem.at[m, 1]),
            pltpu.make_async_copy(
                upper_out.at[m], gate_v.at[pl.ds(count + m * tok, tok)], reload_sem.at[m, 2]
            ),
            pltpu.make_async_copy(active_out.at[m], up_v.at[rows], reload_sem.at[m, 3]),
        ] + [
            pltpu.make_async_copy(
                grad_ref.at[m, pl.ds(r * SUB, SUB)], own.at[m * per + r], reload_sem.at[m, 4 + r]
            )
            for r in range(per)
        ]

    for m in range(micro):
        for copy in reloads(m):
            copy.start()

    def pair_slot(q):
        return up_v.at[pl.ds(count + q * piece, piece)]

    def tile_copy(m, q):
        target = early_out.at[m] if q == 0 else weight_out.at[m, q - 1]
        return pltpu.make_async_copy(pair_slot(q), target, tile_sem.at[q])

    def pair_copy(q):
        return pltpu.make_async_remote_copy(
            src_ref=stage_v.at[q],
            dst_ref=pair_slot(q),
            send_sem=pair_sems.at[0, q],
            recv_sem=pair_sems.at[1, q],
            device_id={"wide": near},
            device_id_type=MESH,
        )

    def tile(i, q, store):
        cols = pl.ds(pl.multiple_of(i * piece, piece), piece)
        if q == 2:
            right = own[0:base, :, cols].reshape(count, piece)
            for j in range(blocks):
                span = slice(j * piece, (j + 1) * piece)
                store(span, dot_f32(up_v[0:count, span], right, TN))
        else:
            right = (gate_v[0:count], gate_v[count : 2 * count])[q]
            store(slice(0, hid), dot_f32(down_v[0:count, cols], right, TN))

    def give(m, q):
        @pl.when(m > 0)
        def _():
            pair_copy(q).wait_send()

        def store(span, part):
            stage_v[q, :, span] = part.astype(jnp.bfloat16)

        tile(2 * m + 1 - core, q, store)

    def keep(m, q):
        rows = pl.ds(count + q * piece, piece)
        pair_copy(q).wait_recv()

        def store(span, part):
            up_v[rows, span] = (part + up_v[rows, span].astype(jnp.float32)).astype(jnp.bfloat16)

        tile(2 * m + core, q, store)
        tile_copy(m, q).start()

    def final_copies(m):
        return [
            pltpu.make_async_copy(middle_v, middle_out.at[m], final_sem.at[0]),
            pltpu.make_async_copy(hidden_v, low_out.at[m], final_sem.at[1]),
        ]

    def output_copy(m):
        return pltpu.make_async_copy(output_v, output_out.at[m], final_sem.at[2])

    last_ticks = first_ticks + slots * micro
    rest = late + 4 - last_ticks
    turns = rest // micro

    @pl.loop(0, micro)
    def _(m):
        slot = m % 2
        wait_loads(m + micro)

        @pl.when(m < micro - 1)
        def _():
            start_loads(m + micro + 1)

        @pl.when(m > 0)
        def _():
            for copy in final_copies(m - 1):
                copy.wait()
            output_copy(m - 1).wait()

        @pl.when(m == 0)
        def _():
            for i in range(micro):
                for copy in reloads(i):
                    copy.wait()

        relay.tick(last_ticks + turns * m)
        give(m, 0)
        give(m, 1)
        give(m, 2)
        pl.semaphore_wait(credit, 1)
        for q in range(3):
            pair_copy(q).start()
        relay.tick(last_ticks + turns * m + 1)
        keep(m, 0)
        keep(m, 1)
        relay.tick(last_ticks + turns * m + 2)

        @pl.loop(0, per)
        def _(r):
            span = pl.ds(pl.multiple_of(r * SUB, SUB), SUB)
            middle = rows_v[slot, span, :].astype(jnp.float32) + landed[m * per + r].astype(
                jnp.float32
            )
            scale = lax.rsqrt(jnp.mean(middle * middle, axis=-1, keepdims=True) + EPSILON)
            pulled = landed[base + 2 * per * m + r].astype(jnp.float32) * gain_ref[...]
            along = jnp.mean(pulled * middle, axis=-1, keepdims=True)
            grad_middle = grads_v[slot, span, :].astype(jnp.float32) + scale * (
                pulled - middle * (scale * scale * along)
            )
            middle_v[span, :] = grad_middle
            hidden_v[span, :] = grad_middle.astype(jnp.bfloat16)

        @pl.when(m >= 2)
        def _():
            for g in range(groups):
                behind.sent((m - 2) * groups + g, home=True)

        mixback_v[m % 2] = dot_f32(hidden_v[...], out_v[...], NT).astype(jnp.bfloat16)
        for g in range(groups):
            behind.send(m * groups + g)

        @pl.when(m < micro - 1)
        def _():
            @pl.loop(0, per)
            def _(r):
                span = pl.ds(pl.multiple_of(r * SUB, SUB), SUB)
                output_v[span, :] = (
                    rows_v[slot, span, :].astype(jnp.float32)
                    + landed[m * per + r].astype(jnp.float32)
                    + landed[base + 2 * per * m + per + r].astype(jnp.float32)
                ).astype(jnp.bfloat16)

            output_copy(m).start()

        for copy in final_copies(m):
            copy.start()
        keep(m, 2)
        for q in range(3):
            tile_copy(m, q).wait()

        @pl.when(m < micro - 1)
        def _():
            offer()

    for copy in late_copies:
        copy.wait()
    for copy in final_copies(micro - 1):
        copy.wait()
    for q in range(3):
        pair_copy(q).wait_send()
    for m in range(micro):
        heads_copy(m).wait()

    @pl.loop(0, width)
    def _(d):
        ahead.sent(d)
        behind.wait(d, home=False)

    @pl.loop((micro - 2) * groups, width)
    def _(d):
        behind.sent(d, home=True)

    relay.drain(base)


def feed_forward(mixed, layer_input, grad_out, gain_ffn, pack, up_w, down_w, heads_in):
    micro, tok, model = layer_input.shape
    hid = up_w.shape[1]
    parts = 2 * (hid // LANES)
    width, _, piece = pack.shape
    groups = width // micro
    low = jnp.bfloat16
    count = 3 * micro * (tok // SUB)
    late = tok // SUB
    anywhere = pl.BlockSpec(memory_space=pl.ANY)
    inside = pl.BlockSpec(memory_space=pltpu.VMEM)
    return pl.pallas_call(
        feed_kernel,
        out_shape=(
            jax.ShapeDtypeStruct((micro, tok, model), low),
            jax.ShapeDtypeStruct((micro, tok, hid), low),
            jax.ShapeDtypeStruct((micro, tok, hid), low),
            jax.ShapeDtypeStruct((micro, tok, hid), low),
            jax.ShapeDtypeStruct((micro - 1, tok, model), low),
            jax.ShapeDtypeStruct((micro, tok, model), jnp.float32),
            jax.ShapeDtypeStruct((micro, tok, model), low),
            jax.ShapeDtypeStruct((width, tok, 2 * HD), low),
            jax.ShapeDtypeStruct((1, model), jnp.float32),
            jax.ShapeDtypeStruct((width // 2, 3, piece, hid), low),
            jax.ShapeDtypeStruct((micro, tok, heads_in), low),
            jax.ShapeDtypeStruct((width // 2, piece, hid), low),
            jax.ShapeDtypeStruct((2, late, SUB, model), low),
        ),
        in_specs=[anywhere] * 3 + [inside, anywhere, anywhere, anywhere],
        out_specs=[anywhere] * 8 + [inside] + [anywhere] * 4,
        scratch_shapes=relay_scratch(count - late, model, late)
        + [
            pltpu.VMEM((heads_in, model), low),
            pltpu.VMEM((model, hid), low),
            pltpu.VMEM((model, hid), low),
            pltpu.VMEM((hid, model), low),
            pltpu.VMEM((micro, tok, heads_in), low),
            pltpu.VMEM((2, tok, model), low),
            pltpu.VMEM((2, tok, model), low),
            pltpu.VMEM((tok, model), low),
            pltpu.VMEM((3, tok, hid), low),
            pltpu.VMEM((tok, 1), jnp.float32),
            pltpu.VMEM((tok, model), jnp.float32),
            pltpu.VMEM((tok, model), low),
            pltpu.VMEM((2, tok, heads_in), low),
            pltpu.SemaphoreType.DMA((width, hid // piece)),
            pltpu.SemaphoreType.DMA((width,)),
            pltpu.SemaphoreType.DMA((2, 2)),
            pltpu.SemaphoreType.DMA,
            pltpu.SemaphoreType.DMA((3,)),
            pltpu.SemaphoreType.DMA((3,)),
            pltpu.SemaphoreType.DMA((micro, 4 + tok // SUB)),
            pltpu.SemaphoreType.DMA((3,)),
            pltpu.SemaphoreType.DMA((2, width)),
            pltpu.SemaphoreType.DMA((2, width)),
            pltpu.SemaphoreType.DMA((micro,)),
            pltpu.SemaphoreType.DMA((parts, 9)),
            pltpu.SemaphoreType.DMA((parts, 10)),
            pltpu.SemaphoreType.DMA((2, 3)),
            pltpu.SemaphoreType.REGULAR,
            pltpu.SemaphoreType.DMA((2,)),
        ],
        compiler_params=pltpu.CompilerParams(
            collective_id=0, has_side_effects=True, vmem_limit_bytes=67043328
        ),
        cost_estimate=pl.CostEstimate(
            flops=240_000_000_000, bytes_accessed=900_000_000, transcendentals=0
        ),
        name="feed_forward",
    )(mixed, layer_input, grad_out, gain_ffn[None, :], pack, up_w, down_w)


def input_kernel(
    back_ref,
    input_ref,
    middle_ref,
    gain_ref,
    weight_ref,
    gain_two_ref,
    gain_heads_ref,
    output_out,
    gains_out,
    own,
    landed,
    cross,
    out_sem,
    land_sem,
    back_sem,
    cross_sem,
    weight_v,
    back_v,
    rows_v,
    middle_v,
    output_v,
    term_v,
    other_v,
    first_sem,
    load_sem,
    final_sem,
    term_sem,
    other_sem,
):
    micro, tok, model = input_ref.shape
    per = tok // FINE
    spot = lax.axis_index("wide")
    flips = [spot + bit - 2 * bit * (spot // bit % 2) for bit in (1, 2, 4)]
    relay = Relay(micro * per, own, landed, cross, (out_sem, land_sem, back_sem, cross_sem))
    weight_copy = pltpu.make_async_copy(weight_ref, weight_v, first_sem.at[0])
    back_copy = pltpu.make_async_copy(back_ref, back_v, first_sem.at[1])
    weight_copy.start()
    back_copy.start()

    rows_copy = pltpu.make_async_copy(input_ref, rows_v, first_sem.at[2])
    rows_copy.start()

    def load(m):
        return pltpu.make_async_copy(middle_ref.at[m], middle_v.at[m % 2], load_sem.at[m % 2])

    def final_copy(m):
        return pltpu.make_async_copy(output_v.at[m % 2], output_out.at[m], final_sem.at[m % 2])

    def pass_on(step, where):
        return pltpu.make_async_remote_copy(
            src_ref=term_v.at[step],
            dst_ref=other_v.at[step],
            send_sem=term_sem.at[step],
            recv_sem=other_sem.at[step],
            device_id=where,
            device_id_type=MESH,
        )

    targets = [{"wide": flip} for flip in flips] + [
        {"narrow": spot} for spot in (relay.inner, relay.other, relay.outer)
    ]

    def gain_step(step):
        if step == 0:
            pass_on(0, targets[0]).start()
        if 1 <= step <= 3:
            pass_on(step - 1, targets[step - 1]).wait_recv()
            term_v[step] = term_v[step - 1] + other_v[step - 1]
        if step in (1, 2):
            pass_on(step, targets[step]).start()
        if step == 3:

            @pl.when(relay.is_end)
            def _():
                pass_on(3, targets[3]).start()

        if step in (4, 5):

            @pl.when(relay.is_mid)
            def _():
                pass_on(step - 1, targets[step - 1]).wait_recv()
                term_v[step] = term_v[step - 1] + other_v[step - 1]
                pass_on(step, targets[step]).start()

        if step == 6:

            @pl.when(relay.is_mid)
            def _():
                gains_out[...] = term_v[5]
                pass_on(4, targets[4]).wait_send()
                pass_on(5, targets[5]).wait_send()

            @pl.when(relay.is_end)
            def _():
                pass_on(5, targets[5]).wait_recv()
                gains_out[...] = other_v[5]
                pass_on(3, targets[3]).wait_send()

            for early in range(3):
                pass_on(early, targets[early]).wait_send()

    load(0).start()
    relay.greet(flips)
    term_v[0] = jnp.zeros(term_v.shape[1:], jnp.float32)
    weight_copy.wait()
    back_copy.wait()
    rows_copy.wait()

    @pl.loop(0, micro)
    def _(m):
        rows = rows_v[m].astype(jnp.float32)
        scale = lax.rsqrt(jnp.mean(rows * rows, axis=-1, keepdims=True) + EPSILON)
        for n in range(model // LANES):
            cols = pl.ds(n * LANES, LANES)
            part = dot_f32(back_v[m], weight_v[cols, :], NT)
            term_v[0, 0:1, cols] += jnp.sum(
                part * (rows_v[m, :, cols].astype(jnp.float32) * scale), axis=0, keepdims=True
            )
            part = part.astype(jnp.bfloat16)
            for r in range(per):
                own[m * per + r, :, cols] = part[r * FINE : (r + 1) * FINE]

        @pl.when(m == 0)
        def _():
            relay.send(0, AHEAD)

    term_v[0, 1:2, :] = gain_two_ref[...]
    term_v[0, 2:3, 0:HD] = gain_heads_ref[0:1, :]
    term_v[0, 2:3, HD : 2 * HD] = gain_heads_ref[1:2, :]
    for k in range(2):
        if k in GAIN_PLACES:
            gain_step(GAIN_PLACES.index(k))
        relay.send(AHEAD + 2 * k, 2)
        relay.place(k)

    @pl.loop(0, micro)
    def _(m):
        slot = m % 2

        @pl.when(m < micro - 1)
        def _():
            load(m + 1).start()

        load(m).wait()

        @pl.when(m >= 2)
        def _():
            final_copy(m - 2).wait()

        for r in range(per // 2):
            for turn in range(micro):
                if 2 + turn * per // 2 + r in GAIN_PLACES:

                    @pl.when(m == turn)
                    def _(step=GAIN_PLACES.index(2 + turn * per // 2 + r)):
                        gain_step(step)

            @pl.when(AHEAD + 4 + m * per + 2 * r < relay.count)
            def _():
                relay.send(AHEAD + 4 + m * per + 2 * r, 2)

            relay.place(2 + m * per // 2 + r)
            for half in range(2):
                span = pl.ds((2 * r + half) * FINE, FINE)
                rows = rows_v[m, span, :].astype(jnp.float32)
                scale = lax.rsqrt(jnp.mean(rows * rows, axis=-1, keepdims=True) + EPSILON)
                pulled = landed[m * per + 2 * r + half].astype(jnp.float32) * gain_ref[...]
                along = jnp.mean(pulled * rows, axis=-1, keepdims=True)
                output_v[slot, span, :] = middle_v[slot, span, :] + scale * (
                    pulled - rows * (scale * scale * along)
                )
        final_copy(m).start()

    final_copy(micro - 2).wait()
    final_copy(micro - 1).wait()
    relay.drain(0)


def input_gradient(back, layer_input, grad_middle, gain_attn, weight, gain_two, gain_heads):
    micro, tok, model = layer_input.shape
    low = jnp.bfloat16
    count = micro * (tok // FINE)
    anywhere = pl.BlockSpec(memory_space=pl.ANY)
    inside = pl.BlockSpec(memory_space=pltpu.VMEM)
    return pl.pallas_call(
        input_kernel,
        out_shape=(
            jax.ShapeDtypeStruct((micro, tok, model), jnp.float32),
            jax.ShapeDtypeStruct((8, model), jnp.float32),
        ),
        in_specs=[anywhere] * 3 + [inside, anywhere, inside, inside],
        out_specs=[anywhere, inside],
        scratch_shapes=relay_scratch(count, model, rows=FINE)
        + [
            pltpu.VMEM(weight.shape, low),
            pltpu.VMEM((micro, tok, weight.shape[1]), low),
            pltpu.VMEM((micro, tok, model), low),
            pltpu.VMEM((2, tok, model), jnp.float32),
            pltpu.VMEM((2, tok, model), jnp.float32),
            pltpu.VMEM((6, 8, model), jnp.float32),
            pltpu.VMEM((6, 8, model), jnp.float32),
            pltpu.SemaphoreType.DMA((3,)),
            pltpu.SemaphoreType.DMA((2,)),
            pltpu.SemaphoreType.DMA((2,)),
            pltpu.SemaphoreType.DMA((6,)),
            pltpu.SemaphoreType.DMA((6,)),
        ],
        compiler_params=pltpu.CompilerParams(
            collective_id=1, has_side_effects=True, vmem_limit_bytes=48 << 20
        ),
        cost_estimate=pl.CostEstimate(
            flops=1_000_000_000, bytes_accessed=1_000_000, transcendentals=0
        ),
        name="input_gradient",
    )(back, layer_input, grad_middle, gain_attn[None, :], weight, gain_two, gain_heads)


def widen_gate(rows_ref, gate_ref):
    gate_ref[...] = rows_ref[...].astype(jnp.float32)


def finish_kernel(
    input_rows,
    first_rows,
    last_rows,
    up_rows,
    down_rows,
    attn_rows,
    out_rows,
    grad_ref,
    output_ref,
    up_ref,
    down_ref,
    query_ref,
    key_ref,
    value_ref,
    out_ref,
):
    grad_ref[...] = input_rows[...]
    inside = pl.program_id(0) < pl.num_programs(0) * 3 // 4
    output_ref[...] = jnp.where(inside, first_rows[...], last_rows[...])
    up_ref[...] = up_rows[...].astype(jnp.float32)
    down_ref[...] = down_rows[...].astype(jnp.float32)
    first = 0
    for target in (query_ref, key_ref, value_ref):
        target[...] = attn_rows[:, first : first + target.shape[1]].astype(jnp.float32)
        first += target.shape[1]
    out_ref[...] = out_rows[...].astype(jnp.float32)


def finish(grad_input, first, last, grads, columns):
    steps = 8
    rows, model = grad_input.shape
    piece, hid = grads.shape[0] // 3, grads.shape[1]
    part = rows // steps
    early = first.shape[0] // part - 1
    strip = piece // steps
    blocks = hid // piece
    heads = sum(columns) // piece
    rest = (hid - sum(columns)) // piece
    f32 = jnp.float32
    row = lambda i: (i, 0)
    return pl.pallas_call(
        finish_kernel,
        grid=(steps,),
        out_shape=(
            jax.ShapeDtypeStruct((rows, model), f32),
            jax.ShapeDtypeStruct((rows, model), jnp.bfloat16),
            jax.ShapeDtypeStruct((piece, hid), f32),
            jax.ShapeDtypeStruct((hid, piece), f32),
        )
        + tuple(jax.ShapeDtypeStruct((piece, column), f32) for column in columns)
        + (jax.ShapeDtypeStruct((rest * piece, piece), f32),),
        in_specs=[
            pl.BlockSpec((part, model), row),
            pl.BlockSpec((part, model), lambda i: (jnp.minimum(i, early), 0)),
            pl.BlockSpec((part, model), lambda i: (jnp.maximum(i - early - 1, 0), 0)),
            pl.BlockSpec((strip, hid), row),
            pl.BlockSpec((piece, piece), lambda i: (1, jnp.minimum(i, blocks - 1))),
            pl.BlockSpec((strip, hid), lambda i: (2 * steps + i, 0)),
            pl.BlockSpec((piece, piece), lambda i: (2, heads + jnp.minimum(i, rest - 1))),
        ],
        out_specs=[
            pl.BlockSpec((part, model), row),
            pl.BlockSpec((part, model), row),
            pl.BlockSpec((strip, hid), row),
            pl.BlockSpec((piece, piece), lambda i: (jnp.minimum(i, blocks - 1), 0)),
        ]
        + [pl.BlockSpec((strip, column), row) for column in columns]
        + [pl.BlockSpec((piece, piece), lambda i: (jnp.minimum(i, rest - 1), 0))],
        name="finish",
    )(grad_input, first, last, grads, grads, grads, grads)


def local_batched(
    layer_input,
    grad_out,
    lengths,
    w_query,
    w_key,
    w_value,
    w_out,
    w_gate,
    w_up,
    w_down,
    gain_attn,
    gain_ffn,
    gain_query,
    gain_key,
):
    micro, tok_rows, model = layer_input.shape
    width = lax.axis_size("wide")
    groups = w_key.shape[1] // HD
    total = tok_rows * width
    piece = w_out.shape[1]

    def stacked(weight):
        return jnp.moveaxis(weight.reshape(piece, -1, piece), 1, 0).reshape(-1, piece)

    pack = lax.all_gather(
        jnp.concatenate([w_out, stacked(w_gate)], axis=0), "wide", axis=0
    )

    head_gains = jnp.stack([gain_query, gain_key])
    hidden_one, raw, packed, w_qkv, cosine, sine = project(
        layer_input, gain_attn, (w_query, w_key, w_value), lengths, head_gains, width
    )
    packed = packed.reshape(total, 4 * HD)
    mixed, kept, log_total = attention_out(packed, lengths)
    (
        _,
        _,
        _,
        _,
        output,
        grad_middle,
        middle_low,
        grad_mixed,
        gain_two,
        feed_grads,
        mixed_low,
        gate_grads,
        late,
    ) = feed_forward(
        mixed.reshape(width, tok_rows, 2 * HD),
        layer_input,
        grad_out,
        gain_ffn,
        pack,
        w_up,
        w_down,
        w_out.shape[0],
    )
    cores = [list(range(core, width, 2)) for core in range(2)]

    def scatter(rows):
        return lax.psum_scatter(
            rows, "wide", scatter_dimension=0, axis_index_groups=cores, tiled=True
        )

    qkv_back, other_grads, gain_heads, last_output = attention_gradients(
        lengths,
        packed,
        grad_mixed,
        kept,
        log_total,
        raw,
        hidden_one,
        mixed_low,
        middle_low,
        late,
        layer_input,
        cosine,
        sine,
        head_gains,
        feed_grads,
    )
    gate_grads = scatter(gate_grads.reshape(-1, w_gate.shape[1]))
    other_grads = scatter(other_grads.reshape(-1, w_up.shape[1]))
    grad_input, gains = input_gradient(
        qkv_back, layer_input, grad_middle, gain_attn, w_qkv, gain_two, gain_heads
    )

    grad_gate = pl.pallas_call(
        widen_gate,
        out_shape=jax.ShapeDtypeStruct(w_gate.shape, jnp.float32),
        name="widen_gate",
    )(gate_grads)
    (
        grad_input,
        output,
        grad_up,
        grad_down,
        grad_query,
        grad_key,
        grad_value,
        grad_wout,
    ) = finish(
        grad_input.reshape(-1, model),
        output.reshape(-1, model),
        last_output,
        other_grads,
        (w_query.shape[1], w_key.shape[1], w_value.shape[1]),
    )
    return (
        output.reshape(layer_input.shape),
        grad_input.reshape(layer_input.shape),
        grad_query,
        grad_key,
        grad_value,
        grad_wout,
        grad_gate,
        grad_up,
        grad_down,
        gains[0],
        gains[1],
        gains[2, :HD],
        gains[2, HD : 2 * HD],
    )


def local(mesh, layer_input, grad_out, lengths, w_query, w_key, *rest):
    width = mesh.shape["wide"]
    micro, tok_rows = layer_input.shape[:2]
    groups = w_key.shape[1] // HD
    fits = (
        groups == HEAD_GROUPS
        and micro * groups == width == 8
        and w_query.shape[1] == 2 * w_key.shape[1]
        and mesh.shape["narrow"] == 4
        and tok_rows == BLOCK
    )
    chosen = local_batched if fits else local_general
    return chosen(layer_input, grad_out, lengths, w_query, w_key, *rest)


def solution(mesh):
    in_specs = (
        P(None, "wide", None),
        P(None, "wide", None),
        P(),
        P("wide", "narrow"),
        P("wide", "narrow"),
        P("wide", "narrow"),
        P("narrow", "wide"),
        P("wide", "narrow"),
        P("wide", "narrow"),
        P("narrow", "wide"),
        P(),
        P(),
        P(),
        P(),
    )
    out_specs = (
        P(None, "wide", None),
        P(None, "wide", None),
        P("wide", "narrow"),
        P("wide", "narrow"),
        P("wide", "narrow"),
        P("narrow", "wide"),
        P("wide", "narrow"),
        P("wide", "narrow"),
        P("narrow", "wide"),
        P(),
        P(),
        P(),
        P(),
    )
    return jax.shard_map(
        functools.partial(local, mesh), mesh=mesh, in_specs=in_specs, out_specs=out_specs, check_vma=False)
```

```python
import functools
import math

import jax
import jax.numpy as jnp
from jax import lax
from jax.experimental import pallas as pl
from jax.experimental.pallas import tpu as pltpu
from jax.sharding import PartitionSpec as P

HD = 128
NDOC = 8


EPSILON = 1e-06
THETA = 1000000.0


def rms_norm(values, gain):
    return values * lax.rsqrt(jnp.mean(values * values, axis=-1, keepdims=True) + EPSILON) * gain


def unit_rows(values):
    return values * lax.rsqrt(jnp.mean(values * values, axis=-1, keepdims=True) + EPSILON)


def rotate(values, cosine, sine):
    midway = values.shape[-1] // 2
    turned = jnp.concatenate([-values[..., midway:], values[..., :midway]], axis=-1)
    return values * cosine + turned * sine


def layout(lengths_row, total):
    finish = jnp.cumsum(lengths_row)
    starts = finish - lengths_row
    places = jnp.arange(total, dtype=jnp.int32)
    segment = jnp.sum((places[:, None] >= finish[None, :]).astype(jnp.int32), axis=1)
    member = segment[:, None] == jnp.arange(finish.shape[0], dtype=jnp.int32)[None, :]
    opening = jnp.sum(jnp.where(member, starts[None, :], 0), axis=1)
    return (segment, places - opening)


def angles(place):
    frequency = jnp.exp(-math.log(THETA) * jnp.arange(0, HD, 2).astype(jnp.float32) / HD)
    turning = place.astype(jnp.float32)[:, None] * frequency[None, :]
    turning = jnp.concatenate([turning, turning], axis=-1)
    return (jnp.cos(turning), jnp.sin(turning))


def allowed(query_seg, query_idx, key_seg, key_idx):
    same_doc = query_seg[:, None] == key_seg[None, :]
    causal = key_idx[None, :] <= query_idx[:, None]
    usable = (key_seg[None, :] != NDOC - 1) | (key_idx[None, :] == query_idx[:, None])
    return same_doc & causal & usable


def attention_scores(query_low, key_all, mask_local, factor):
    scores = (
        jnp.einsum("tgrd,kgd->grtk", query_low, key_all, preferred_element_type=jnp.float32)
        * factor
    )
    return jnp.where(mask_local[None, None], scores, -1e30)


def one_batch(row_input, grad_row, lengths_row, gathered, gains):
    w_query, w_key, w_value, w_out, w_gate, w_up, w_down = gathered
    gain_attn, gain_ffn, gain_query, gain_key = gains
    tok_rows = row_input.shape[0]
    total = tok_rows * lax.axis_size("wide")
    groups = w_key.shape[1] // HD
    repeat = w_query.shape[1] // w_key.shape[1]
    factor = 1.0 / math.sqrt(HD)
    first_row = lax.axis_index("wide") * tok_rows
    segment, place = layout(lengths_row, total)
    positions = jnp.arange(total, dtype=jnp.int32)
    query_seg = lax.dynamic_slice_in_dim(segment, first_row, tok_rows)
    query_idx = lax.dynamic_slice_in_dim(positions, first_row, tok_rows)
    mask_local = allowed(query_seg, query_idx, segment, positions)
    cosine, sine = angles(lax.dynamic_slice_in_dim(place, first_row, tok_rows))

    def head_norm(rows, gain):
        return rotate(rms_norm(rows, gain), cosine[:, None, :], sine[:, None, :])

    input_float = row_input.astype(jnp.float32)
    grad_float = grad_row.astype(jnp.float32)
    normed_one, pull_one = jax.vjp(lambda rows: rms_norm(rows, gain_attn), input_float)
    hidden_one = normed_one.astype(jnp.bfloat16)
    query_raw = jnp.dot(hidden_one, w_query, preferred_element_type=jnp.float32).reshape(
        tok_rows, groups * repeat, HD
    )
    key_raw = jnp.dot(hidden_one, w_key, preferred_element_type=jnp.float32).reshape(
        tok_rows, groups, HD
    )
    value_low = jnp.dot(hidden_one, w_value, preferred_element_type=jnp.float32).astype(
        jnp.bfloat16
    )
    query_turned, pull_query = jax.vjp(head_norm, query_raw, gain_query)
    key_turned, pull_key = jax.vjp(head_norm, key_raw, gain_key)
    query_low = query_turned.astype(jnp.bfloat16).reshape(tok_rows, groups, repeat, HD)
    key_low = key_turned.astype(jnp.bfloat16).reshape(tok_rows, groups * HD)
    key_all, value_all = (
        lax.all_gather(key_low, "wide", axis=0, tiled=True),
        lax.all_gather(value_low, "wide", axis=0, tiled=True),
    )
    key_all = key_all.reshape(total, groups, HD)
    value_all = value_all.reshape(total, groups, HD)
    scores = attention_scores(query_low, key_all, mask_local, factor)
    highest = jnp.max(scores, axis=-1, keepdims=True)
    exponent = jnp.exp(scores - highest)
    denominator = jnp.sum(exponent, axis=-1, keepdims=True)
    log_total = highest + jnp.log(denominator)
    probs_low = (exponent / denominator).astype(jnp.bfloat16)
    mixed = jnp.einsum("grtk,kgd->tgrd", probs_low, value_all, preferred_element_type=jnp.float32)
    mixed_low = mixed.reshape(tok_rows, groups * repeat * HD).astype(jnp.bfloat16)
    attn_part = jnp.dot(mixed_low, w_out, preferred_element_type=jnp.float32)
    middle = input_float + lax.psum(attn_part.astype(jnp.bfloat16), "narrow").astype(jnp.float32)
    normed_two, pull_two = jax.vjp(lambda rows: rms_norm(rows, gain_ffn), middle)
    hidden_two = normed_two.astype(jnp.bfloat16)
    unit_two = unit_rows(middle)
    gate = jnp.dot(hidden_two, w_gate, preferred_element_type=jnp.float32)
    up_proj = jnp.dot(hidden_two, w_up, preferred_element_type=jnp.float32)
    active, pull_active = jax.vjp(
        lambda gate_in, up_in: jax.nn.silu(gate_in) * up_in, gate, up_proj
    )
    active_low = active.astype(jnp.bfloat16)
    ffn_part = jnp.dot(active_low, w_down, preferred_element_type=jnp.float32)
    output_low = (
        middle + lax.psum(ffn_part.astype(jnp.bfloat16), "narrow").astype(jnp.float32)
    ).astype(jnp.bfloat16)
    grad_wdown = jnp.einsum("tf,td->fd", active_low, grad_row, preferred_element_type=jnp.float32)
    grad_active = jnp.einsum("td,fd->tf", grad_row, w_down, preferred_element_type=jnp.float32)
    grad_gate, grad_upper = pull_active(grad_active)
    gate_back = grad_gate.astype(jnp.bfloat16)
    upper_back = grad_upper.astype(jnp.bfloat16)
    grad_wgate = jnp.einsum("td,tf->df", hidden_two, gate_back, preferred_element_type=jnp.float32)
    grad_wup = jnp.einsum("td,tf->df", hidden_two, upper_back, preferred_element_type=jnp.float32)
    partial_two = jnp.einsum(
        "tf,df->td", gate_back, w_gate, preferred_element_type=jnp.float32
    ) + jnp.einsum("tf,df->td", upper_back, w_up, preferred_element_type=jnp.float32)
    gain_two = jnp.sum(partial_two * unit_two, axis=0)
    grad_middle = (
        grad_float
        + pull_two(lax.psum(partial_two.astype(jnp.bfloat16), "narrow").astype(jnp.float32))[0]
    )
    middle_low = grad_middle.astype(jnp.bfloat16)
    grad_wout = jnp.einsum("th,td->hd", mixed_low, middle_low, preferred_element_type=jnp.float32)
    grad_mixed = jnp.einsum("td,hd->th", middle_low, w_out, preferred_element_type=jnp.float32)
    grad_mixed = grad_mixed.astype(jnp.bfloat16).reshape(tok_rows, groups, repeat, HD)
    scores = attention_scores(query_low, key_all, mask_local, factor)
    probs = jnp.exp(scores - log_total)
    grad_probs = jnp.einsum(
        "tgrd,kgd->grtk", grad_mixed, value_all, preferred_element_type=jnp.float32
    )
    weighted = jnp.sum(probs * grad_probs, axis=-1, keepdims=True)
    grad_scores = (probs * (grad_probs - weighted)).astype(jnp.bfloat16)
    grad_turned = (
        jnp.einsum("grtk,kgd->tgrd", grad_scores, key_all, preferred_element_type=jnp.float32)
        * factor
    )
    grad_keyall = (
        jnp.einsum("grtk,tgrd->kgd", grad_scores, query_low, preferred_element_type=jnp.float32)
        * factor
    )
    grad_valueall = jnp.einsum(
        "grtk,tgrd->kgd", probs.astype(jnp.bfloat16), grad_mixed, preferred_element_type=jnp.float32
    )
    grad_keys, grad_values = (
        lax.psum_scatter(
            grad_keyall.reshape(total, groups * HD).astype(jnp.bfloat16),
            "wide",
            scatter_dimension=0,
            tiled=True,
        ).astype(jnp.float32),
        lax.psum_scatter(
            grad_valueall.reshape(total, groups * HD).astype(jnp.bfloat16),
            "wide",
            scatter_dimension=0,
            tiled=True,
        ).astype(jnp.float32),
    )
    grad_qraw, gain_q = pull_query(grad_turned.reshape(tok_rows, groups * repeat, HD))
    grad_kraw, gain_k = pull_key(grad_keys.reshape(tok_rows, groups, HD))
    query_back = grad_qraw.reshape(tok_rows, groups * repeat * HD).astype(jnp.bfloat16)
    key_back = grad_kraw.reshape(tok_rows, groups * HD).astype(jnp.bfloat16)
    value_back = grad_values.astype(jnp.bfloat16)
    grad_wquery = jnp.einsum(
        "td,th->dh", hidden_one, query_back, preferred_element_type=jnp.float32
    )
    grad_wkey = jnp.einsum("td,th->dh", hidden_one, key_back, preferred_element_type=jnp.float32)
    grad_wvalue = jnp.einsum(
        "td,th->dh", hidden_one, value_back, preferred_element_type=jnp.float32
    )
    partial_one = (
        jnp.einsum("th,dh->td", query_back, w_query, preferred_element_type=jnp.float32)
        + jnp.einsum("th,dh->td", key_back, w_key, preferred_element_type=jnp.float32)
        + jnp.einsum("th,dh->td", value_back, w_value, preferred_element_type=jnp.float32)
    )
    gain_one = jnp.sum(partial_one * unit_rows(input_float), axis=0)
    grad_input = (
        grad_middle
        + pull_one(lax.psum(partial_one.astype(jnp.bfloat16), "narrow").astype(jnp.float32))[0]
    )
    weight_grads = (
        grad_wquery,
        grad_wkey,
        grad_wvalue,
        grad_wout,
        grad_wgate,
        grad_wup,
        grad_wdown,
    )
    return (output_low, grad_input, weight_grads, (gain_one, gain_two, gain_q, gain_k))


def local_general(
    layer_input,
    grad_out,
    lengths,
    w_query,
    w_key,
    w_value,
    w_out,
    w_gate,
    w_up,
    w_down,
    gain_attn,
    gain_ffn,
    gain_query,
    gain_key,
):
    width = lax.axis_size("wide")
    shards = (w_query, w_key, w_value, w_out, w_gate, w_up, w_down)
    along_rows = (True, True, True, False, True, True, False)
    gains = (gain_attn, gain_ffn, gain_query, gain_key)
    totals = tuple(
        (
            jnp.zeros(
                (
                    (piece.shape[0] * width, piece.shape[1])
                    if rows_first
                    else (piece.shape[0], piece.shape[1] * width)
                ),
                jnp.float32,
            )
            for piece, rows_first in zip(shards, along_rows)
        )
    )
    gain_terms = tuple((jnp.zeros(gain.shape, jnp.float32) for gain in gains))
    outputs = []
    grad_inputs = []
    for micro in range(layer_input.shape[0]):
        gathered = (
            lax.all_gather(w_query, "wide", axis=0, tiled=True),
            lax.all_gather(w_key, "wide", axis=0, tiled=True),
            lax.all_gather(w_value, "wide", axis=0, tiled=True),
            lax.all_gather(w_out, "wide", axis=1, tiled=True),
            lax.all_gather(w_gate, "wide", axis=0, tiled=True),
            lax.all_gather(w_up, "wide", axis=0, tiled=True),
            lax.all_gather(w_down, "wide", axis=1, tiled=True),
        )
        output, grad_input, weight_grads, gain_grads = one_batch(
            layer_input[micro], grad_out[micro], lengths[micro], gathered, gains
        )
        outputs.append(output)
        grad_inputs.append(grad_input)
        gain_terms = tuple((running + fresh for running, fresh in zip(gain_terms, gain_grads)))
        totals = tuple((running + fresh for running, fresh in zip(totals, weight_grads)))
    results = (
        lax.psum_scatter(
            totals[0].astype(jnp.bfloat16), "wide", scatter_dimension=0, tiled=True
        ).astype(jnp.float32),
        lax.psum_scatter(
            totals[1].astype(jnp.bfloat16), "wide", scatter_dimension=0, tiled=True
        ).astype(jnp.float32),
        lax.psum_scatter(
            totals[2].astype(jnp.bfloat16), "wide", scatter_dimension=0, tiled=True
        ).astype(jnp.float32),
        lax.psum_scatter(
            totals[3].astype(jnp.bfloat16), "wide", scatter_dimension=1, tiled=True
        ).astype(jnp.float32),
        lax.psum_scatter(
            totals[4].astype(jnp.bfloat16), "wide", scatter_dimension=0, tiled=True
        ).astype(jnp.float32),
        lax.psum_scatter(
            totals[5].astype(jnp.bfloat16), "wide", scatter_dimension=0, tiled=True
        ).astype(jnp.float32),
        lax.psum_scatter(
            totals[6].astype(jnp.bfloat16), "wide", scatter_dimension=1, tiled=True
        ).astype(jnp.float32),
    )
    gain_total = lax.psum(gain_terms, ("wide", "narrow"))
    return (
        jnp.stack(outputs),
        jnp.stack(grad_inputs),
        results[0],
        results[1],
        results[2],
        results[3],
        results[4],
        results[5],
        results[6],
        gain_total[0],
        gain_total[1],
        gain_total[2],
        gain_total[3],
    )


BLOCK = 256
HEAD_GROUPS = 2
NT = (((1,), (1,)), ((), ()))
TN = (((0,), (0,)), ((), ()))


def piece_starts(lengths_ref, micro, spot):
    start = jnp.zeros_like(spot)
    finish = jnp.int32(0)
    for piece in range(NDOC - 1):
        finish += lengths_ref[micro, piece]
        start = jnp.where(spot >= finish, finish if piece < NDOC - 2 else spot, start)
    return start


def query_lanes(lengths_ref, step_q):
    micro = lax.axis_index("wide") // HEAD_GROUPS
    lane = lax.broadcasted_iota(jnp.int32, (1, 2 * BLOCK), 1)
    spot = lane % BLOCK + step_q * BLOCK
    return spot, piece_starts(lengths_ref, micro, spot)


def key_fits(step_k, spot, start):
    key_spot = lax.broadcasted_iota(jnp.int32, (BLOCK, 1), 0) + step_k * BLOCK
    return (key_spot >= start) & (key_spot <= spot)


def attend_forward(lengths_ref, qkv_ref, mixed_ref, kept_ref, log_ref):
    step_q = pl.program_id(0)
    rows = pl.ds(step_q * BLOCK, BLOCK)
    factor = 1.0 / math.sqrt(HD)
    query = jnp.concatenate([qkv_ref[rows, 0:HD], qkv_ref[rows, HD : 2 * HD]], axis=0)
    spot, start = query_lanes(lengths_ref, step_q)
    micro = lax.axis_index("wide") // HEAD_GROUPS
    first = piece_starts(lengths_ref, micro, step_q * BLOCK) // BLOCK

    def one(step_k, carry):
        total, total_low, mixed = carry
        cols = pl.ds(step_k * BLOCK, BLOCK)
        scores = dot_f32(qkv_ref[cols, 2 * HD : 3 * HD], query, NT)
        exponent = jnp.where(key_fits(step_k, spot, start), jnp.exp(scores * factor), 0.0)
        low = exponent.astype(jnp.bfloat16)
        total += jnp.sum(exponent.reshape(-1, 8, 2 * BLOCK), axis=0)
        total_low += jnp.sum(low.astype(jnp.float32).reshape(-1, 8, 2 * BLOCK), axis=0)
        mixed += dot_f32(qkv_ref[cols, 3 * HD : 4 * HD], low, TN)
        return (total, total_low, mixed)

    zeros = jnp.zeros((8, 2 * BLOCK), jnp.float32)
    total, total_low, mixed = lax.fori_loop(
        first, step_q + 1, one, (zeros, zeros, jnp.zeros((HD, 2 * BLOCK), jnp.float32))
    )
    mixed = (mixed / jnp.sum(total_low, axis=0, keepdims=True)).T
    mixed = jnp.concatenate([mixed[:BLOCK], mixed[BLOCK:]], axis=1)
    mixed_ref[...] = mixed.astype(jnp.bfloat16)
    kept_ref[...] = mixed
    log_total = jnp.log(jnp.sum(total, axis=0, keepdims=True))
    log_ref[...] = jnp.broadcast_to(log_total, zeros.shape)[None]


def attention_out(qkv, lengths):
    total = qkv.shape[0]
    block = lambda i, *_: (i, 0)
    return pl.pallas_call(
        attend_forward,
        out_shape=(
            jax.ShapeDtypeStruct((total, 2 * HD), jnp.bfloat16),
            jax.ShapeDtypeStruct((total, 2 * HD), jnp.float32),
            jax.ShapeDtypeStruct((total // BLOCK, 8, 2 * BLOCK), jnp.float32),
        ),
        grid_spec=pltpu.PrefetchScalarGridSpec(
            num_scalar_prefetch=1,
            grid=(total // BLOCK,),
            in_specs=[pl.BlockSpec((total, 4 * HD), lambda i, *_: (0, 0))],
            out_specs=[
                pl.BlockSpec((BLOCK, 2 * HD), block),
                pl.BlockSpec((BLOCK, 2 * HD), block),
                pl.BlockSpec((1, 8, 2 * BLOCK), lambda i, *_: (i, 0, 0)),
            ],
        ),
        name="attend_forward",
    )(lengths, qkv)


def dot_f32(left, right, dims=(((1,), (0,)), ((), ()))):
    return lax.dot_general(left, right, dims, preferred_element_type=jnp.float32)


SUB = 64
RING = 8
STRIP = 16
FINE = 32
AHEAD = 6
GAIN_PLACES = (0, 2, 4, 6, 10, 13, 16)
LANES = 512
MESH = pl.DeviceIdType.MESH


class Relay:
    def __init__(self, count, own, landed, cross, sems):
        self.count, self.own, self.landed, self.cross = count, own, landed, cross
        self.out_sem, self.land_sem, self.back_sem, self.cross_sem = sems
        spot = lax.axis_index("narrow")
        self.is_end = (spot == 0) | (spot == 3)
        self.is_mid = (spot == 1) | (spot == 2)
        self.inner = 1 + spot // 3
        self.other = 3 - spot
        self.outer = jnp.where(spot == 2, 3, 0)

    def to_inner(self, k):
        return pltpu.make_async_remote_copy(
            src_ref=self.own.at[k],
            dst_ref=self.landed.at[k],
            send_sem=self.out_sem.at[k],
            recv_sem=self.land_sem.at[k],
            device_id={"narrow": self.inner},
            device_id_type=MESH,
        )

    def to_other(self, k):
        return pltpu.make_async_remote_copy(
            src_ref=self.own.at[k],
            dst_ref=self.cross.at[k % RING],
            send_sem=self.out_sem.at[k],
            recv_sem=self.cross_sem.at[k % RING],
            device_id={"narrow": self.other},
            device_id_type=MESH,
        )

    def to_outer(self, k):
        return pltpu.make_async_remote_copy(
            src_ref=self.landed.at[k],
            dst_ref=self.landed.at[k],
            send_sem=self.back_sem.at[k],
            recv_sem=self.land_sem.at[k],
            device_id={"narrow": self.outer},
            device_id_type=MESH,
        )

    def greet(self, peers):
        barrier = pltpu.get_barrier_semaphore()
        for peer in peers:
            pl.semaphore_signal(barrier, inc=1, device_id={"wide": peer}, device_id_type=MESH)

        @pl.when(self.is_end)
        def _():
            pl.semaphore_signal(
                barrier, inc=1, device_id={"narrow": self.inner}, device_id_type=MESH
            )
            pl.semaphore_wait(barrier, 1 + len(peers))

        @pl.when(self.is_mid)
        def _():
            pl.semaphore_signal(
                barrier, inc=1, device_id={"narrow": self.outer}, device_id_type=MESH
            )
            pl.semaphore_signal(
                barrier, inc=1, device_id={"narrow": self.other}, device_id_type=MESH
            )
            pl.semaphore_wait(barrier, 2 + len(peers))

    def send(self, first, number):
        @pl.when(self.is_end)
        def _():
            @pl.loop(0, number)
            def _(i):
                self.to_inner(first + i).start()

    def tick(self, k):
        @pl.when(self.is_mid & (k < self.count))
        def _():
            self.to_inner(k).wait_recv()

            @pl.loop(0, self.own.shape[1] // STRIP)
            def _(i):
                rows = pl.ds(pl.multiple_of(i * STRIP, STRIP), STRIP)
                self.own[k, rows] = (
                    self.own[k, rows].astype(jnp.float32) + self.landed[k, rows].astype(jnp.float32)
                ).astype(jnp.bfloat16)

            self.to_other(k).start()

        @pl.when(self.is_mid & (k >= 2) & (k < self.count + 2))
        def _():
            j = k - 2
            self.to_other(j).wait_recv()

            @pl.loop(0, self.own.shape[1] // STRIP)
            def _(i):
                rows = pl.ds(pl.multiple_of(i * STRIP, STRIP), STRIP)
                self.landed[j, rows] = (
                    self.own[j, rows].astype(jnp.float32)
                    + self.cross[j % RING, rows].astype(jnp.float32)
                ).astype(jnp.bfloat16)

            self.to_outer(j).start()

        @pl.when(self.is_end & (k >= 4) & (k < self.count + 4))
        def _():
            self.to_outer(k - 4).wait_recv()

    def place(self, p):
        self.tick(2 * p)
        self.tick(2 * p + 1)

    def drain(self, first):
        @pl.loop(first, self.count)
        def _(k):
            self.to_inner(k).wait_send()

        @pl.loop(0, self.count)
        def _(k):
            @pl.when(self.is_mid)
            def _():
                self.to_outer(k).wait_send()


def wide_peers(width):
    spot = lax.axis_index("wide")
    return [lax.rem(spot + step, width) for step in range(1, width)]


def greet_wide(width):
    barrier = pltpu.get_barrier_semaphore()
    for peer in wide_peers(width):
        pl.semaphore_signal(barrier, inc=1, device_id={"wide": peer}, device_id_type=MESH)
    pl.semaphore_wait(barrier, width - 1)


class Exchange:
    def __init__(self, block, slot, send_sem, land_sem):
        self.block, self.slot = block, slot
        self.send_sem, self.land_sem = send_sem, land_sem
        self.spot = lax.axis_index("wide")

    def remote(self, target, source):
        return pltpu.make_async_remote_copy(
            src_ref=self.block(target),
            dst_ref=self.slot(source),
            send_sem=self.send_sem.at[target],
            recv_sem=self.land_sem.at[source],
            device_id={"wide": target},
            device_id_type=MESH,
        )

    def here(self):
        return pltpu.make_async_copy(
            self.block(self.spot), self.slot(self.spot), self.land_sem.at[self.spot]
        )

    def send(self, target):
        @pl.when(target == self.spot)
        def _():
            self.here().start()

        @pl.when(target != self.spot)
        def _():
            self.remote(target, self.spot).start()

    def sent(self, target, home=False):
        @pl.when(target != self.spot)
        def _():
            self.remote(target, self.spot).wait_send()

        if home:

            @pl.when(target == self.spot)
            def _():
                self.here().wait()

    def wait(self, source, home=True):
        if home:

            @pl.when(source == self.spot)
            def _():
                self.here().wait()

        @pl.when(source != self.spot)
        def _():
            self.remote(self.spot, source).wait_recv()


class Gather:
    def __init__(self, parts, send_sem, land_sem):
        self.parts, self.send_sem, self.land_sem = parts, send_sem, land_sem
        me = lax.axis_index("wide")
        flip = lambda spot, bit: spot + bit - 2 * bit * (spot // bit % 2)
        self.me, self.near = me, flip(me, 1)
        self.across, self.along = flip(me, 2), flip(me, 4)
        self.far = flip(self.across, 4)
        self.flip = flip

    def move(self, part, kind, source, target, device):
        return pltpu.make_async_remote_copy(
            src_ref=source,
            dst_ref=target,
            send_sem=self.send_sem.at[part, kind],
            recv_sem=self.land_sem.at[part, kind],
            device_id={"wide": device},
            device_id_type=MESH,
        )

    def going(self, part, kind):
        own, slot, half = self.parts[part]
        across, along, near = self.across, self.along, self.near
        source, target, device = (
            lambda: (own, slot(self.me), across),
            lambda: (own, slot(self.me), along),
            lambda: (own, slot(self.me), near),
            lambda: (half(along, 0), half(along, 0), across),
            lambda: (half(across, 1), half(across, 1), along),
            lambda: (slot(across), slot(across), near),
            lambda: (slot(along), slot(along), near),
            lambda: (half(self.far, 0), half(self.far, 0), near),
            lambda: (half(self.far, 1), half(self.far, 1), near),
        )[kind]()
        return self.move(part, kind, source, target, device)

    def coming(self, part, kind):
        _, slot, half = self.parts[part]
        flip = self.flip
        place = (
            lambda: slot(self.across),
            lambda: slot(self.along),
            lambda: slot(self.near),
            lambda: half(self.far, 0),
            lambda: half(self.far, 1),
            lambda: slot(flip(self.across, 1)),
            lambda: slot(flip(self.along, 1)),
            lambda: half(flip(self.far, 1), 0),
            lambda: half(flip(self.far, 1), 1),
        )[kind]()
        return self.move(part, kind, place, place, self.near)

    def here(self, part):
        own, slot, _ = self.parts[part]
        return pltpu.make_async_copy(own, slot(self.me), self.land_sem.at[part, 9])

    def first(self, part):
        for kind in (0, 1, 2):
            self.going(part, kind).start()
        self.here(part).start()

    def second(self, part):
        self.coming(part, 1).wait_recv()
        self.going(part, 3).start()
        self.coming(part, 0).wait_recv()
        self.going(part, 4).start()
        self.going(part, 6).start()
        self.going(part, 5).start()

    def third(self, part):
        self.coming(part, 3).wait_recv()
        self.going(part, 7).start()
        self.coming(part, 4).wait_recv()
        self.going(part, 8).start()

    def fourth(self, part):
        self.here(part).wait()
        for kind in (2, 5, 6, 7, 8):
            self.coming(part, kind).wait_recv()

    def drain(self):
        for part in range(len(self.parts)):
            for kind in range(9):
                self.going(part, kind).wait_send()


def project_kernel(
    input_ref,
    gain_ref,
    query_w,
    key_w,
    value_w,
    lengths_ref,
    head_gain_ref,
    hidden_out,
    raw_out,
    packed_out,
    weight_out,
    cosine_ref,
    sine_ref,
    rows_v,
    weight_v,
    hidden_v,
    raw_v,
    pack_v,
    load_sem,
    keep_sem,
    hidden_sem,
    send_sem,
    land_sem,
    part_send,
    part_land,
):
    micro, tok, model = input_ref.shape
    width = packed_out.shape[0]
    groups = width // micro
    heads = 2 * groups
    spot = lax.axis_index("wide")
    swap = Exchange(
        lambda target: pack_v.at[target], lambda source: packed_out.at[source], send_sem, land_sem
    )
    load = pltpu.make_async_copy(input_ref, rows_v, load_sem.at[0])
    load.start()
    piece = query_w.shape[0]

    def part(own, first):
        cols = pl.ds(first, own.shape[1])
        return (
            own,
            lambda s: weight_v.at[pl.ds(pl.multiple_of(s * piece, piece), piece), cols],
            lambda s, h: weight_v.at[
                pl.ds(pl.multiple_of(s * piece + h * piece // 2, piece // 2), piece // 2), cols
            ],
        )

    q_cols, k_cols = query_w.shape[1], key_w.shape[1]
    gather = Gather(
        [part(query_w, 0), part(key_w, q_cols), part(value_w, q_cols + k_cols)],
        part_send,
        part_land,
    )
    greet_wide(width)
    for p in range(3):
        gather.first(p)
    load.wait()
    hidden_copy = pltpu.make_async_copy(hidden_v, hidden_out, hidden_sem)

    @pl.loop(0, micro)
    def _(m):
        rows = rows_v[m].astype(jnp.float32)
        scale = lax.rsqrt(jnp.mean(rows * rows, axis=-1, keepdims=True) + EPSILON)
        hidden_v[m] = (rows * scale * gain_ref[...]).astype(jnp.bfloat16)

    hidden_copy.start()
    lane = lax.broadcasted_iota(jnp.int32, (1, HD), 1)
    frequency = jnp.exp(
        -math.log(THETA) * (2 * (lane % (HD // 2))).astype(jnp.float32) / HD
    )
    sign = jnp.where(lane < HD // 2, -1.0, 1.0)
    token = lax.broadcasted_iota(jnp.int32, (tok, 1), 0) + spot * tok

    @pl.loop(0, micro)
    def _(m):
        start = jnp.zeros_like(token)
        finish = jnp.int32(0)
        for piece_index in range(NDOC - 1):
            finish += lengths_ref[m, piece_index]
            start = jnp.where(token >= finish, finish, start)
        turning = (token - start).astype(jnp.float32) * frequency
        span = pl.ds(pl.multiple_of(m * tok, tok), tok)
        cosine_ref[span, :] = jnp.cos(turning)
        sine_ref[span, :] = jnp.sin(turning) * sign

    for p in range(3):
        gather.second(p)
    for p in range(3):
        gather.third(p)
    for p in range(3):
        gather.fourth(p)
    weight_copy = pltpu.make_async_copy(weight_v, weight_out, load_sem.at[1])
    weight_copy.start()

    def turn(step):
        far = micro - 1 - step
        own = spot // groups
        return (own + far) % 2 + 2 * ((own // 2 + far // 2) % 2)

    def keep(step):
        return pltpu.make_async_copy(
            raw_v.at[step % 2], raw_out.at[turn(step)], keep_sem.at[step % 2]
        )

    @pl.loop(0, micro)
    def _(step):
        m = turn(step)

        @pl.when(step >= 2)
        def _():
            keep(step - 2).wait()

        heads_all = dot_f32(hidden_v[m], weight_v[...])
        span = pl.ds(pl.multiple_of(m * tok, tok), tok)
        cosine, sine = cosine_ref[span, :], sine_ref[span, :]
        raw_v[step % 2] = heads_all[:, : (heads + groups) * HD]
        for h in range(heads + groups):
            raw = heads_all[:, h * HD : (h + 1) * HD]
            gain = head_gain_ref[0:1, :] if h < heads else head_gain_ref[1:2, :]
            unit = raw * lax.rsqrt(jnp.mean(raw * raw, axis=-1, keepdims=True) + EPSILON) * gain
            turned = unit * cosine + pltpu.roll(unit, HD // 2, 1) * sine
            g, place = (h // 2, h % 2) if h < heads else (h - heads, 2)
            pack_v[m * groups + g, :, place * HD : (place + 1) * HD] = turned.astype(jnp.bfloat16)
        for g in range(groups):
            first = (heads + groups + g) * HD
            pack_v[m * groups + g, :, 3 * HD :] = heads_all[:, first : first + HD].astype(
                jnp.bfloat16
            )
            swap.send(m * groups + g)
        keep(step).start()

    keep(micro - 2).wait()
    keep(micro - 1).wait()

    @pl.loop(0, width)
    def _(d):
        swap.sent(d)
        swap.wait(d)

    gather.drain()
    hidden_copy.wait()
    weight_copy.wait()


def project(layer_input, gain_attn, weights, lengths, head_gains, width):
    micro, tok, model = layer_input.shape
    groups = width // micro
    low = jnp.bfloat16
    anywhere = pl.BlockSpec(memory_space=pl.ANY)
    inside = pl.BlockSpec(memory_space=pltpu.VMEM)
    raw = 3 * groups * HD
    columns = sum(weight.shape[1] for weight in weights)
    return pl.pallas_call(
        project_kernel,
        out_shape=(
            jax.ShapeDtypeStruct((micro, tok, model), low),
            jax.ShapeDtypeStruct((micro, tok, raw), jnp.float32),
            jax.ShapeDtypeStruct((width, tok, 4 * HD), low),
            jax.ShapeDtypeStruct((model, columns), low),
            jax.ShapeDtypeStruct((micro * tok, HD), jnp.float32),
            jax.ShapeDtypeStruct((micro * tok, HD), jnp.float32),
        ),
        in_specs=[anywhere, inside, anywhere, anywhere, anywhere]
        + [pl.BlockSpec(memory_space=pltpu.SMEM), inside],
        out_specs=[anywhere] * 4 + [inside] * 2,
        scratch_shapes=[
            pltpu.VMEM((micro, tok, model), low),
            pltpu.VMEM((model, columns), low),
            pltpu.VMEM((micro, tok, model), low),
            pltpu.VMEM((2, tok, raw), jnp.float32),
            pltpu.VMEM((width, tok, 4 * HD), low),
            pltpu.SemaphoreType.DMA((2,)),
            pltpu.SemaphoreType.DMA((2,)),
            pltpu.SemaphoreType.DMA,
            pltpu.SemaphoreType.DMA((width,)),
            pltpu.SemaphoreType.DMA((width,)),
            pltpu.SemaphoreType.DMA((3, 9)),
            pltpu.SemaphoreType.DMA((3, 10)),
        ],
        compiler_params=pltpu.CompilerParams(
            collective_id=2, has_side_effects=True, vmem_limit_bytes=40 << 20
        ),
        cost_estimate=pl.CostEstimate(
            flops=20_000_000_000, bytes_accessed=40_000_000, transcendentals=0
        ),
        name="project",
    )(layer_input, gain_attn[None, :], *weights, lengths, head_gains)


def weights_kernel(
    lengths_ref,
    qkv_ref,
    upper_ref,
    kept_ref,
    log_ref,
    raw_ref,
    hidden_ref,
    mixed_ref,
    low_ref,
    late_ref,
    input_ref,
    cosine_ref,
    sine_ref,
    head_gain_ref,
    _,
    back_out,
    grad_out,
    gain_out,
    output_out,
    own,
    landed,
    cross,
    out_sem,
    relay_sem,
    return_sem,
    cross_sem,
    land_v,
    raw_v,
    hidden_v,
    mixed_v,
    low_v,
    back_v,
    grad_v,
    pair_v,
    middle_v,
    rows_v,
    qkv_v,
    upper_v,
    kept_v,
    log_v,
    sent_v,
    query_sum,
    key_sum,
    value_sum,
    load_sem,
    back_sem,
    tile_sem,
    send_sems,
    land_sems,
    pair_sems,
    late_sem,
    attn_sem,
):
    micro, tok, heads_in = mixed_ref.shape
    width = upper_ref.shape[0]
    groups = width // micro
    heads = 2 * groups
    model = hidden_ref.shape[2]
    piece = model // width
    count = micro * tok
    factor = 1.0 / math.sqrt(HD)
    halves = (pl.ds(0, 2 * HD), pl.ds(2 * HD, 2 * HD))
    swaps = [
        Exchange(
            lambda target, cols=cols: sent_v.at[target, :, cols],
            lambda source, cols=cols: land_v.at[source, :, cols],
            send_sems.at[i],
            land_sems.at[i],
        )
        for i, cols in enumerate(halves)
    ]
    attn_loads = [
        pltpu.make_async_copy(source, target, attn_sem.at[i])
        for i, (source, target) in enumerate(
            ((qkv_ref, qkv_v), (upper_ref, upper_v), (kept_ref, kept_v), (log_ref, log_v))
        )
    ]
    loads = [
        pltpu.make_async_copy(mixed_ref, mixed_v, load_sem.at[0]),
        pltpu.make_async_copy(low_ref, low_v, load_sem.at[1]),
        pltpu.make_async_copy(raw_ref, raw_v, load_sem.at[2]),
        pltpu.make_async_copy(hidden_ref, hidden_v, load_sem.at[3]),
    ]
    per = tok // SUB
    relay = Relay(per, own, landed, cross, (out_sem, relay_sem, return_sem, cross_sem))
    late_loads = [
        pltpu.make_async_copy(late_ref.at[0], own, late_sem.at[0]),
        pltpu.make_async_copy(late_ref.at[1], middle_v, late_sem.at[1]),
        pltpu.make_async_copy(input_ref.at[micro - 1], rows_v, late_sem.at[2]),
    ]
    for copy in attn_loads + late_loads + loads:
        copy.start()
    key_sum[...] = jnp.zeros_like(key_sum)
    value_sum[...] = jnp.zeros_like(value_sum)
    relay.greet(wide_peers(width))
    spot = lax.axis_index("wide")
    for copy in late_loads:
        copy.wait()
    relay.send(0, per)
    for copy in attn_loads:
        copy.wait()
    band = width * tok // 2 // BLOCK

    @pl.loop(0, width)
    def _(step):
        far = micro - 1 - step // 2
        chip = spot // 2
        turn = (chip + far) % 2 + 2 * ((chip // 2 + far // 2) % 2)
        step_q = 2 * turn + step % 2
        rows = pl.ds(pl.multiple_of(step_q * BLOCK, BLOCK), BLOCK)
        query = jnp.concatenate([qkv_v[rows, 0:HD], qkv_v[rows, HD : 2 * HD]], axis=0)
        grad = jnp.concatenate([upper_v[step_q, :, 0:HD], upper_v[step_q, :, HD : 2 * HD]], axis=0)
        kept = jnp.concatenate([kept_v[rows, 0:HD], kept_v[rows, HD : 2 * HD]], axis=0)
        weighted = lax.dot_general(
            jnp.ones((8, HD), jnp.float32),
            grad.astype(jnp.float32) * kept,
            NT,
            precision=lax.Precision.HIGHEST,
            preferred_element_type=jnp.float32,
        )[0:1]
        log_total = log_v[step_q, 0:1, :]
        spots, start = query_lanes(lengths_ref, step_q)
        query_sum[...] = jnp.zeros_like(query_sum)

        @pl.loop(0, band + 1)
        def _(t):
            step_k = step_q - band + t

            @pl.when(step_k >= 0)
            def _():
                cols = pl.ds(pl.multiple_of(step_k * BLOCK, BLOCK), BLOCK)
                key = qkv_v[cols, 2 * HD : 3 * HD]
                scores = dot_f32(key, query, NT) * factor
                probs = jnp.where(
                    key_fits(step_k, spots, start), jnp.exp(scores - log_total), 0.0
                )
                grad_probs = dot_f32(qkv_v[cols, 3 * HD : 4 * HD], grad, NT)
                grad_scores = (probs * (grad_probs - weighted)).astype(jnp.bfloat16)
                value_sum[cols, :] += dot_f32(probs.astype(jnp.bfloat16), grad)
                key_sum[cols, :] += dot_f32(grad_scores, query)
                query_sum[...] += dot_f32(grad_scores, key, TN)

        part = (query_sum[...] * factor).astype(jnp.bfloat16)
        sent_v[step_q, :, 0:HD] = part[:BLOCK]
        sent_v[step_q, :, HD : 2 * HD] = part[BLOCK:]
        swaps[0].send(step_q)

        @pl.when(step % 2 == 1)
        def _():
            relay.tick(step // 2)

    @pl.loop(0, width)
    def _(i):
        rows = pl.ds(pl.multiple_of(i * BLOCK, BLOCK), BLOCK)
        sent_v[i, :, 2 * HD : 3 * HD] = (key_sum[rows, :] * factor).astype(jnp.bfloat16)
        sent_v[i, :, 3 * HD : 4 * HD] = value_sum[rows, :].astype(jnp.bfloat16)

    for step in range(width - 1, -1, -1):
        swaps[1].send(lax.rem(spot + step, width))
    loads[0].wait()
    loads[1].wait()
    mixed_all = mixed_v[...].reshape(count, heads_in)
    for n in range(model // LANES):
        low = low_v[:, :, n * LANES : (n + 1) * LANES].reshape(count, LANES)
        part = dot_f32(mixed_all, low, TN).astype(jnp.bfloat16)
        for i in range(LANES // piece):
            for b in range(heads_in // piece):
                grad_v[
                    n * (LANES // piece) + i, :, pl.ds(2 * heads_in + b * piece, piece)
                ] = part[b * piece : (b + 1) * piece, i * piece : (i + 1) * piece]
    loads[2].wait()
    gain_out[...] = jnp.zeros_like(gain_out)

    def back_copy(m):
        return pltpu.make_async_copy(back_v.at[m], back_out.at[m], back_sem.at[m])

    def turn_back(m, h):
        span = pl.ds(pl.multiple_of(m * tok, tok), tok)
        raw = raw_v[m, :, h * HD : (h + 1) * HD]
        kind = 0 if h < heads else 1
        gain = head_gain_ref[kind : kind + 1, :]
        g, place = (h // 2, h % 2) if h < heads else (h - heads, 2)
        grad = land_v[m * groups + g, :, place * HD : (place + 1) * HD].astype(jnp.float32)
        straight = grad * cosine_ref[span, :] + pltpu.roll(grad * sine_ref[span, :], HD // 2, 1)
        scale = lax.rsqrt(jnp.mean(raw * raw, axis=-1, keepdims=True) + EPSILON)
        gain_out[kind : kind + 1, :] += jnp.sum(straight * (raw * scale), axis=0, keepdims=True)
        pulled = straight * gain
        along = jnp.mean(pulled * raw, axis=-1, keepdims=True)
        back_v[m, :, h * HD : (h + 1) * HD] = (
            scale * (pulled - raw * (scale * scale * along))
        ).astype(jnp.bfloat16)

    @pl.loop(0, width)
    def _(d):
        swaps[0].wait(d)

    @pl.loop(0, micro)
    def _(m):
        for h in range(heads):
            turn_back(m, h)

        @pl.when(m == 1)
        def _():
            relay.tick(4)

    relay.tick(5)

    @pl.loop(0, width)
    def _(d):
        swaps[1].wait(d)

    @pl.loop(0, micro)
    def _(m):
        for h in range(heads, heads + groups):
            turn_back(m, h)
        for g in range(groups):
            first = (heads + groups + g) * HD
            back_v[m, :, first : first + HD] = land_v[m * groups + g, :, 3 * HD :]
        back_copy(m).start()

    loads[3].wait()

    core = lax.rem(spot, 2)
    near = spot + 1 - 2 * core

    def tile_copy(c):
        return pltpu.make_async_copy(grad_v.at[2 * c + core], grad_out.at[c, 3], tile_sem.at[c])

    def pair_copy(c):
        return pltpu.make_async_remote_copy(
            src_ref=grad_v.at[2 * c + 1 - core],
            dst_ref=pair_v.at[c],
            send_sem=pair_sems.at[0, c],
            recv_sem=pair_sems.at[1, c],
            device_id={"wide": near},
            device_id_type=MESH,
        )

    def tile(i):
        left = hidden_v[:, :, pl.ds(pl.multiple_of(i * piece, piece), piece)].reshape(count, piece)
        return dot_f32(left, back_v[...].reshape(count, 2 * heads_in), TN)

    @pl.loop(0, width // 2)
    def _(c):
        i = 2 * c + 1 - core
        grad_v[i, :, 0 : 2 * heads_in] = tile(i).astype(jnp.bfloat16)
        pair_copy(c).start()

        @pl.when(c % 2 == 1)
        def _():
            relay.tick(6 + c // 2)

    output_copy = pltpu.make_async_copy(rows_v, output_out, late_sem.at[3])
    for r in range(per):
        span = slice(r * SUB, (r + 1) * SUB)
        rows_v[span, :] = (
            rows_v[span, :].astype(jnp.float32)
            + middle_v[r].astype(jnp.float32)
            + landed[r].astype(jnp.float32)
        ).astype(jnp.bfloat16)
    output_copy.start()

    @pl.loop(0, width // 2)
    def _(c):
        i = 2 * c + core
        part = tile(i)
        pair_copy(c).wait_recv()
        grad_v[i, :, 0 : 2 * heads_in] = (
            part + pair_v[c, :, 0 : 2 * heads_in].astype(jnp.float32)
        ).astype(jnp.bfloat16)
        grad_v[i, :, 2 * heads_in :] = (
            grad_v[i, :, 2 * heads_in :].astype(jnp.float32)
            + pair_v[c, :, 2 * heads_in :].astype(jnp.float32)
        ).astype(jnp.bfloat16)
        tile_copy(c).start()

    @pl.loop(0, width // 2)
    def _(c):
        tile_copy(c).wait()
        pair_copy(c).wait_send()

    @pl.loop(0, width)
    def _(i):
        for swap in swaps:
            swap.sent(i)

    for m in range(micro):
        back_copy(m).wait()
    output_copy.wait()
    relay.drain(0)


def attention_gradients(
    lengths, qkv, upper, kept, log_total, raw, hidden, mixed, middle_low, late, layer_input, *rest
):
    micro, tok, heads_in = mixed.shape
    width = upper.shape[0]
    total = qkv.shape[0]
    model = hidden.shape[2]
    low = jnp.bfloat16
    anywhere = pl.BlockSpec(memory_space=pl.ANY)
    inside = pl.BlockSpec(memory_space=pltpu.VMEM)
    return pl.pallas_call(
        weights_kernel,
        out_shape=(
            jax.ShapeDtypeStruct((micro, tok, 2 * heads_in), low),
            jax.ShapeDtypeStruct((width // 2, 4, model // width, 3 * heads_in), low),
            jax.ShapeDtypeStruct((2, HD), jnp.float32),
            jax.ShapeDtypeStruct((tok, model), low),
        ),
        in_specs=[pl.BlockSpec(memory_space=pltpu.SMEM)]
        + [anywhere] * 10
        + [inside] * 3
        + [anywhere],
        input_output_aliases={14: 1},
        out_specs=[anywhere, anywhere, inside, anywhere],
        scratch_shapes=relay_scratch(tok // SUB, model)
        + [
            pltpu.VMEM((width, tok, 4 * HD), low),
            pltpu.VMEM(raw.shape, jnp.float32),
            pltpu.VMEM(hidden.shape, low),
            pltpu.VMEM(mixed.shape, low),
            pltpu.VMEM(middle_low.shape, low),
            pltpu.VMEM((micro, tok, 2 * heads_in), low),
            pltpu.VMEM((width, model // width, 3 * heads_in), low),
            pltpu.VMEM((width // 2, model // width, 3 * heads_in), low),
            pltpu.VMEM((tok // SUB, SUB, model), low),
            pltpu.VMEM((tok, model), low),
            pltpu.VMEM(qkv.shape, low),
            pltpu.VMEM(upper.shape, low),
            pltpu.VMEM(kept.shape, jnp.float32),
            pltpu.VMEM(log_total.shape, jnp.float32),
            pltpu.VMEM((width, tok, 4 * HD), low),
            pltpu.VMEM((2 * BLOCK, HD), jnp.float32),
            pltpu.VMEM((total, HD), jnp.float32),
            pltpu.VMEM((total, HD), jnp.float32),
            pltpu.SemaphoreType.DMA((4,)),
            pltpu.SemaphoreType.DMA((micro,)),
            pltpu.SemaphoreType.DMA((width // 2,)),
            pltpu.SemaphoreType.DMA((2, width)),
            pltpu.SemaphoreType.DMA((2, width)),
            pltpu.SemaphoreType.DMA((2, width // 2)),
            pltpu.SemaphoreType.DMA((4,)),
            pltpu.SemaphoreType.DMA((4,)),
        ],
        compiler_params=pltpu.CompilerParams(
            collective_id=3, has_side_effects=True, vmem_limit_bytes=56 << 20
        ),
        cost_estimate=pl.CostEstimate(
            flops=1_000_000_000, bytes_accessed=1_000_000, transcendentals=0
        ),
        name="attention_gradients",
    )(lengths, qkv, upper, kept, log_total, raw, hidden, mixed, middle_low, late, layer_input, *rest)


def relay_scratch(count, model, extra=0, rows=SUB):
    return [
        pltpu.VMEM((count + extra, rows, model), jnp.bfloat16),
        pltpu.VMEM((count, rows, model), jnp.bfloat16),
        pltpu.VMEM((RING, rows, model), jnp.bfloat16),
        pltpu.SemaphoreType.DMA((count,)),
        pltpu.SemaphoreType.DMA((count,)),
        pltpu.SemaphoreType.DMA((count,)),
        pltpu.SemaphoreType.DMA((RING,)),
    ]


def feed_kernel(
    mixed_ref,
    input_ref,
    grad_ref,
    gain_ref,
    pack_ref,
    up_w,
    down_w,
    hidden_out,
    active_out,
    gate_out,
    upper_out,
    output_out,
    middle_out,
    low_out,
    mixed_out,
    gain_out,
    weight_out,
    heads_out,
    late_out,
    own,
    landed,
    cross,
    out_sem,
    land_sem,
    back_sem,
    cross_sem,
    out_v,
    gate_v,
    up_v,
    down_v,
    mixed_v,
    rows_v,
    grads_v,
    hidden_v,
    stage_v,
    scale_v,
    middle_v,
    output_v,
    mixback_v,
    weight_sem,
    attn_sem,
    load_sem,
    hidden_sem,
    stage_sem,
    final_sem,
    reload_sem,
    tile_sem,
    ahead_sems,
    behind_sems,
    heads_sem,
    part_send,
    part_land,
    pair_sems,
    credit,
    late_sem,
):
    micro, tok, model = input_ref.shape
    width, _, piece = pack_ref.shape
    heads_in = out_v.shape[0]
    groups = width // micro
    per = tok // SUB
    hid = gate_v.shape[1]
    count = micro * tok
    blocks = hid // piece
    late = 3 * micro * per - per
    relay = Relay(late, own, landed, cross, (out_sem, land_sem, back_sem, cross_sem))
    n_up = hid // LANES
    n_down = model // LANES
    slots = n_up + n_down

    ahead = Exchange(
        lambda target: mixed_ref.at[target],
        lambda source: mixed_v.at[
            source // groups, :, pl.ds(pl.multiple_of((source % groups) * 2 * HD, 2 * HD), 2 * HD)
        ],
        ahead_sems.at[0],
        ahead_sems.at[1],
    )
    behind = Exchange(
        lambda target: mixback_v.at[
            target // groups % 2,
            :,
            pl.ds(pl.multiple_of((target % groups) * 2 * HD, 2 * HD), 2 * HD),
        ],
        lambda source: mixed_out.at[source],
        behind_sems.at[0],
        behind_sems.at[1],
    )
    attn_copies = [
        pltpu.make_async_copy(
            pack_ref.at[i, pl.ds(0, heads_in)],
            out_v.at[:, pl.ds(i * piece, piece)],
            attn_sem.at[i],
        )
        for i in range(width)
    ]
    weight_copies = [
        pltpu.make_async_copy(
            pack_ref.at[i, pl.ds(heads_in + j * piece, piece)],
            gate_v.at[pl.ds(i * piece, piece), pl.ds(j * piece, piece)],
            weight_sem.at[i, j],
        )
        for i in range(width)
        for j in range(blocks)
    ]

    def up_part(j):
        cols = pl.ds(j * LANES, LANES)
        return (
            up_w.at[:, cols],
            lambda s: up_v.at[pl.ds(pl.multiple_of(s * piece, piece), piece), cols],
            lambda s, h: up_v.at[
                pl.ds(pl.multiple_of(s * piece + h * piece // 2, piece // 2), piece // 2), cols
            ],
        )

    def down_part(j):
        return (
            down_w.at[pl.ds(j * LANES, LANES)],
            lambda s: down_v.at[
                pl.ds(j * LANES, LANES), pl.ds(pl.multiple_of(s * piece, piece), piece)
            ],
            lambda s, h: down_v.at[
                pl.ds(j * LANES + h * LANES // 2, LANES // 2),
                pl.ds(pl.multiple_of(s * piece, piece), piece),
            ],
        )

    gather = Gather(
        [make(j) for j in range(n_up) for make in (up_part, down_part)], part_send, part_land
    )

    def both(action, j):
        action(2 * j)
        action(2 * j + 1)

    for copy in attn_copies + weight_copies:
        copy.start()

    def loads(n):
        slot = n % 2
        return (
            pltpu.make_async_copy(input_ref.at[n % micro], rows_v.at[slot], load_sem.at[slot, 0]),
            pltpu.make_async_copy(grad_ref.at[n % micro], grads_v.at[slot], load_sem.at[slot, 1]),
        )

    def start_loads(n):
        for copy in loads(n):
            copy.start()

    def wait_loads(n):
        for copy in loads(n):
            copy.wait()

    start_loads(0)
    gain_out[...] = jnp.zeros_like(gain_out)
    relay.greet(wide_peers(width))
    spot = lax.axis_index("wide")
    for step in range(width):
        ahead.send(lax.rem(spot + step, width))
    both(gather.first, 0)
    both(gather.first, 1)
    for copy in attn_copies:
        copy.wait()

    def heads_copy(m):
        return pltpu.make_async_copy(mixed_v.at[m], heads_out.at[m], heads_sem.at[m])

    @pl.loop(0, micro)
    def _(m):
        for g in range(groups):
            ahead.wait(m * groups + g)
        heads_copy(m).start()
        for n in range(n_down):
            cols = pl.ds(n * LANES, LANES)
            part = dot_f32(mixed_v[m], out_v[:, cols]).astype(jnp.bfloat16)
            for r in range(per):
                own[m * per + r, :, cols] = part[r * SUB : (r + 1) * SUB]
        relay.send(m * per, per)

    first_ticks = per + 4

    for k in range(first_ticks):
        if k == 4:
            both(gather.second, 0)
        if k == 5:
            both(gather.first, 2)
        if k == 6:
            both(gather.second, 1)
        if k == 7:
            both(gather.third, 0)
        relay.tick(k)

    for copy in weight_copies:
        copy.wait()

    def hidden_copy(m):
        return pltpu.make_async_copy(hidden_v, hidden_out.at[m], hidden_sem)

    def stage_copies(m):
        return [
            pltpu.make_async_copy(stage_v.at[i], target.at[m], stage_sem.at[i])
            for i, target in enumerate((active_out, gate_out, upper_out))
        ]

    base = micro * per

    @pl.loop(0, micro)
    def _(m):
        slot = m % 2
        wait_loads(m)
        start_loads(m + 1)

        @pl.when(m > 0)
        def _():
            hidden_copy(m - 1).wait()
            for copy in stage_copies(m - 1):
                copy.wait()

        @pl.loop(0, per)
        def _(r):
            span = pl.ds(pl.multiple_of(r * SUB, SUB), SUB)
            middle = rows_v[slot, span, :].astype(jnp.float32) + landed[m * per + r].astype(
                jnp.float32
            )
            scale = lax.rsqrt(jnp.mean(middle * middle, axis=-1, keepdims=True) + EPSILON)
            scale_v[span, :] = scale
            hidden_v[span, :] = (middle * scale * gain_ref[...]).astype(jnp.bfloat16)

        hidden_copy(m).start()

        @pl.loop(0, n_up)
        def _(j):
            relay.tick(first_ticks + slots * m + j)
            for turn in range(n_up):

                @pl.when((m == 0) & (j == turn))
                def _():
                    if turn == 0:
                        both(gather.second, 2)
                    if turn + 1 < n_up:
                        both(gather.third, turn + 1)
                    both(gather.fourth, turn)

            cols = pl.ds(pl.multiple_of(j * LANES, LANES), LANES)
            gate = dot_f32(hidden_v[...], gate_v[:, cols])
            up_proj = dot_f32(hidden_v[...], up_v[:, cols])
            grad_active = dot_f32(grads_v[slot], down_v[cols, :], NT)
            squash = 1.0 / (1.0 + jnp.exp(-gate))
            silu = gate * squash
            stage_v[0, :, cols] = (silu * up_proj).astype(jnp.bfloat16)
            stage_v[1, :, cols] = (
                grad_active * up_proj * (squash * (1.0 + gate * (1.0 - squash)))
            ).astype(jnp.bfloat16)
            stage_v[2, :, cols] = (grad_active * silu).astype(jnp.bfloat16)
        for copy in stage_copies(m):
            copy.start()

        @pl.loop(0, n_down)
        def _(n):
            relay.tick(first_ticks + slots * m + n_up + n)
            cols = pl.ds(pl.multiple_of(n * LANES, LANES), LANES)
            back = dot_f32(stage_v[1], gate_v[cols, :], NT) + dot_f32(
                stage_v[2], up_v[cols, :], NT
            )
            ahead = dot_f32(stage_v[0], down_v[:, cols]).astype(jnp.bfloat16)
            gain_sum = jnp.zeros((1, LANES), jnp.float32)
            for r in range(per):
                part = slice(r * SUB, (r + 1) * SUB)
                own[base + 2 * per * m + r, :, cols] = back[part].astype(jnp.bfloat16)
                own[base + 2 * per * m + per + r, :, cols] = ahead[part]
                unit = (
                    rows_v[slot, pl.ds(r * SUB, SUB), cols].astype(jnp.float32)
                    + landed[m * per + r, :, cols].astype(jnp.float32)
                ) * scale_v[pl.ds(r * SUB, SUB), :]
                gain_sum += jnp.sum(back[part] * unit, axis=0, keepdims=True)
            gain_out[:, cols] += gain_sum

        relay.send(base + 2 * per * m, per)

        @pl.when(m < micro - 1)
        def _():
            relay.send(base + 2 * per * m + per, per)

    hidden_copy(micro - 1).wait()
    for copy in stage_copies(micro - 1):
        copy.wait()
    late_copies = [
        pltpu.make_async_copy(own.at[pl.ds(late, per)], late_out.at[0], late_sem.at[0]),
        pltpu.make_async_copy(
            landed.at[pl.ds((micro - 1) * per, per)], late_out.at[1], late_sem.at[1]
        ),
    ]
    for copy in late_copies:
        copy.start()

    gather.drain()
    core = lax.rem(spot, 2)
    near = gather.near

    def offer():
        pl.semaphore_signal(credit, inc=1, device_id={"wide": near}, device_id_type=MESH)

    offer()

    @pl.loop(0, base)
    def _(k):
        relay.to_inner(k).wait_send()

    def reloads(m):
        rows = pl.ds(m * tok, tok)
        return [
            pltpu.make_async_copy(hidden_out.at[m], down_v.at[rows], reload_sem.at[m, 0]),
            pltpu.make_async_copy(gate_out.at[m], gate_v.at[rows], reload_sem.at[m, 1]),
            pltpu.make_async_copy(
                upper_out.at[m], gate_v.at[pl.ds(count + m * tok, tok)], reload_sem.at[m, 2]
            ),
            pltpu.make_async_copy(active_out.at[m], up_v.at[rows], reload_sem.at[m, 3]),
        ] + [
            pltpu.make_async_copy(
                grad_ref.at[m, pl.ds(r * SUB, SUB)], own.at[m * per + r], reload_sem.at[m, 4 + r]
            )
            for r in range(per)
        ]

    for m in range(micro):
        for copy in reloads(m):
            copy.start()

    def pair_slot(q):
        return up_v.at[pl.ds(count + q * piece, piece)]

    def tile_copy(m, q):
        return pltpu.make_async_copy(pair_slot(q), weight_out.at[m, q], tile_sem.at[q])

    def pair_copy(q):
        return pltpu.make_async_remote_copy(
            src_ref=stage_v.at[q],
            dst_ref=pair_slot(q),
            send_sem=pair_sems.at[0, q],
            recv_sem=pair_sems.at[1, q],
            device_id={"wide": near},
            device_id_type=MESH,
        )

    def tile(i, q, store):
        cols = pl.ds(pl.multiple_of(i * piece, piece), piece)
        if q == 2:
            right = own[0:base, :, cols].reshape(count, piece)
            for j in range(blocks):
                span = slice(j * piece, (j + 1) * piece)
                store(span, dot_f32(up_v[0:count, span], right, TN))
        else:
            right = (gate_v[0:count], gate_v[count : 2 * count])[q]
            store(slice(0, hid), dot_f32(down_v[0:count, cols], right, TN))

    def give(m, q):
        @pl.when(m > 0)
        def _():
            pair_copy(q).wait_send()

        def store(span, part):
            stage_v[q, :, span] = part.astype(jnp.bfloat16)

        tile(2 * m + 1 - core, q, store)

    def keep(m, q):
        rows = pl.ds(count + q * piece, piece)
        pair_copy(q).wait_recv()

        def store(span, part):
            up_v[rows, span] = (part + up_v[rows, span].astype(jnp.float32)).astype(jnp.bfloat16)

        tile(2 * m + core, q, store)
        tile_copy(m, q).start()

    def final_copies(m):
        return [
            pltpu.make_async_copy(middle_v, middle_out.at[m], final_sem.at[0]),
            pltpu.make_async_copy(hidden_v, low_out.at[m], final_sem.at[1]),
        ]

    def output_copy(m):
        return pltpu.make_async_copy(output_v, output_out.at[m], final_sem.at[2])

    last_ticks = first_ticks + slots * micro
    rest = late + 4 - last_ticks
    turns = rest // micro

    @pl.loop(0, micro)
    def _(m):
        slot = m % 2
        wait_loads(m + micro)

        @pl.when(m < micro - 1)
        def _():
            start_loads(m + micro + 1)

        @pl.when(m > 0)
        def _():
            for copy in final_copies(m - 1):
                copy.wait()
            output_copy(m - 1).wait()

        @pl.when(m == 0)
        def _():
            for i in range(micro):
                for copy in reloads(i):
                    copy.wait()

        relay.tick(last_ticks + turns * m)
        give(m, 0)
        give(m, 1)
        give(m, 2)
        pl.semaphore_wait(credit, 1)
        for q in range(3):
            pair_copy(q).start()
        relay.tick(last_ticks + turns * m + 1)
        keep(m, 0)
        keep(m, 1)
        relay.tick(last_ticks + turns * m + 2)

        @pl.loop(0, per)
        def _(r):
            span = pl.ds(pl.multiple_of(r * SUB, SUB), SUB)
            middle = rows_v[slot, span, :].astype(jnp.float32) + landed[m * per + r].astype(
                jnp.float32
            )
            scale = lax.rsqrt(jnp.mean(middle * middle, axis=-1, keepdims=True) + EPSILON)
            pulled = landed[base + 2 * per * m + r].astype(jnp.float32) * gain_ref[...]
            along = jnp.mean(pulled * middle, axis=-1, keepdims=True)
            grad_middle = grads_v[slot, span, :].astype(jnp.float32) + scale * (
                pulled - middle * (scale * scale * along)
            )
            middle_v[span, :] = grad_middle
            hidden_v[span, :] = grad_middle.astype(jnp.bfloat16)

        @pl.when(m >= 2)
        def _():
            for g in range(groups):
                behind.sent((m - 2) * groups + g, home=True)

        mixback_v[m % 2] = dot_f32(hidden_v[...], out_v[...], NT).astype(jnp.bfloat16)
        for g in range(groups):
            behind.send(m * groups + g)

        @pl.when(m < micro - 1)
        def _():
            @pl.loop(0, per)
            def _(r):
                span = pl.ds(pl.multiple_of(r * SUB, SUB), SUB)
                output_v[span, :] = (
                    rows_v[slot, span, :].astype(jnp.float32)
                    + landed[m * per + r].astype(jnp.float32)
                    + landed[base + 2 * per * m + per + r].astype(jnp.float32)
                ).astype(jnp.bfloat16)

            output_copy(m).start()

        for copy in final_copies(m):
            copy.start()
        keep(m, 2)
        for q in range(3):
            tile_copy(m, q).wait()

        @pl.when(m < micro - 1)
        def _():
            offer()

    for copy in late_copies:
        copy.wait()
    for copy in final_copies(micro - 1):
        copy.wait()
    for q in range(3):
        pair_copy(q).wait_send()
    for m in range(micro):
        heads_copy(m).wait()

    @pl.loop(0, width)
    def _(d):
        ahead.sent(d)
        behind.wait(d, home=False)

    @pl.loop((micro - 2) * groups, width)
    def _(d):
        behind.sent(d, home=True)

    relay.drain(base)


def feed_forward(mixed, layer_input, grad_out, gain_ffn, pack, up_w, down_w, heads_in):
    micro, tok, model = layer_input.shape
    hid = up_w.shape[1]
    parts = 2 * (hid // LANES)
    width, _, piece = pack.shape
    groups = width // micro
    low = jnp.bfloat16
    count = 3 * micro * (tok // SUB)
    late = tok // SUB
    anywhere = pl.BlockSpec(memory_space=pl.ANY)
    inside = pl.BlockSpec(memory_space=pltpu.VMEM)
    return pl.pallas_call(
        feed_kernel,
        out_shape=(
            jax.ShapeDtypeStruct((micro, tok, model), low),
            jax.ShapeDtypeStruct((micro, tok, hid), low),
            jax.ShapeDtypeStruct((micro, tok, hid), low),
            jax.ShapeDtypeStruct((micro, tok, hid), low),
            jax.ShapeDtypeStruct((micro - 1, tok, model), low),
            jax.ShapeDtypeStruct((micro, tok, model), jnp.float32),
            jax.ShapeDtypeStruct((micro, tok, model), low),
            jax.ShapeDtypeStruct((width, tok, 2 * HD), low),
            jax.ShapeDtypeStruct((1, model), jnp.float32),
            jax.ShapeDtypeStruct((width // 2, 4, piece, hid), low),
            jax.ShapeDtypeStruct((micro, tok, heads_in), low),
            jax.ShapeDtypeStruct((2, late, SUB, model), low),
        ),
        in_specs=[anywhere] * 3 + [inside, anywhere, anywhere, anywhere],
        out_specs=[anywhere] * 8 + [inside] + [anywhere] * 3,
        scratch_shapes=relay_scratch(count - late, model, late)
        + [
            pltpu.VMEM((heads_in, model), low),
            pltpu.VMEM((model, hid), low),
            pltpu.VMEM((model, hid), low),
            pltpu.VMEM((hid, model), low),
            pltpu.VMEM((micro, tok, heads_in), low),
            pltpu.VMEM((2, tok, model), low),
            pltpu.VMEM((2, tok, model), low),
            pltpu.VMEM((tok, model), low),
            pltpu.VMEM((3, tok, hid), low),
            pltpu.VMEM((tok, 1), jnp.float32),
            pltpu.VMEM((tok, model), jnp.float32),
            pltpu.VMEM((tok, model), low),
            pltpu.VMEM((2, tok, heads_in), low),
            pltpu.SemaphoreType.DMA((width, hid // piece)),
            pltpu.SemaphoreType.DMA((width,)),
            pltpu.SemaphoreType.DMA((2, 2)),
            pltpu.SemaphoreType.DMA,
            pltpu.SemaphoreType.DMA((3,)),
            pltpu.SemaphoreType.DMA((3,)),
            pltpu.SemaphoreType.DMA((micro, 4 + tok // SUB)),
            pltpu.SemaphoreType.DMA((3,)),
            pltpu.SemaphoreType.DMA((2, width)),
            pltpu.SemaphoreType.DMA((2, width)),
            pltpu.SemaphoreType.DMA((micro,)),
            pltpu.SemaphoreType.DMA((parts, 9)),
            pltpu.SemaphoreType.DMA((parts, 10)),
            pltpu.SemaphoreType.DMA((2, 3)),
            pltpu.SemaphoreType.REGULAR,
            pltpu.SemaphoreType.DMA((2,)),
        ],
        compiler_params=pltpu.CompilerParams(
            collective_id=0, has_side_effects=True, vmem_limit_bytes=67043328
        ),
        cost_estimate=pl.CostEstimate(
            flops=240_000_000_000, bytes_accessed=900_000_000, transcendentals=0
        ),
        name="feed_forward",
    )(mixed, layer_input, grad_out, gain_ffn[None, :], pack, up_w, down_w)


def input_kernel(
    back_ref,
    input_ref,
    middle_ref,
    gain_ref,
    weight_ref,
    gain_two_ref,
    gain_heads_ref,
    output_out,
    gains_out,
    own,
    landed,
    cross,
    out_sem,
    land_sem,
    back_sem,
    cross_sem,
    weight_v,
    back_v,
    rows_v,
    middle_v,
    output_v,
    term_v,
    other_v,
    first_sem,
    load_sem,
    final_sem,
    term_sem,
    other_sem,
):
    micro, tok, model = input_ref.shape
    per = tok // FINE
    spot = lax.axis_index("wide")
    flips = [spot + bit - 2 * bit * (spot // bit % 2) for bit in (1, 2, 4)]
    relay = Relay(micro * per, own, landed, cross, (out_sem, land_sem, back_sem, cross_sem))
    weight_copy = pltpu.make_async_copy(weight_ref, weight_v, first_sem.at[0])
    back_copy = pltpu.make_async_copy(back_ref, back_v, first_sem.at[1])
    weight_copy.start()
    back_copy.start()

    rows_copy = pltpu.make_async_copy(input_ref, rows_v, first_sem.at[2])
    rows_copy.start()

    def load(m):
        return pltpu.make_async_copy(middle_ref.at[m], middle_v.at[m % 2], load_sem.at[m % 2])

    def final_copy(m):
        return pltpu.make_async_copy(output_v.at[m % 2], output_out.at[m], final_sem.at[m % 2])

    def pass_on(step, where):
        return pltpu.make_async_remote_copy(
            src_ref=term_v.at[step],
            dst_ref=other_v.at[step],
            send_sem=term_sem.at[step],
            recv_sem=other_sem.at[step],
            device_id=where,
            device_id_type=MESH,
        )

    targets = [{"wide": flip} for flip in flips] + [
        {"narrow": spot} for spot in (relay.inner, relay.other, relay.outer)
    ]

    def gain_step(step):
        if step == 0:
            pass_on(0, targets[0]).start()
        if 1 <= step <= 3:
            pass_on(step - 1, targets[step - 1]).wait_recv()
            term_v[step] = term_v[step - 1] + other_v[step - 1]
        if step in (1, 2):
            pass_on(step, targets[step]).start()
        if step == 3:

            @pl.when(relay.is_end)
            def _():
                pass_on(3, targets[3]).start()

        if step in (4, 5):

            @pl.when(relay.is_mid)
            def _():
                pass_on(step - 1, targets[step - 1]).wait_recv()
                term_v[step] = term_v[step - 1] + other_v[step - 1]
                pass_on(step, targets[step]).start()

        if step == 6:

            @pl.when(relay.is_mid)
            def _():
                gains_out[...] = term_v[5]
                pass_on(4, targets[4]).wait_send()
                pass_on(5, targets[5]).wait_send()

            @pl.when(relay.is_end)
            def _():
                pass_on(5, targets[5]).wait_recv()
                gains_out[...] = other_v[5]
                pass_on(3, targets[3]).wait_send()

            for early in range(3):
                pass_on(early, targets[early]).wait_send()

    load(0).start()
    relay.greet(flips)
    term_v[0] = jnp.zeros(term_v.shape[1:], jnp.float32)
    weight_copy.wait()
    back_copy.wait()
    rows_copy.wait()

    @pl.loop(0, micro)
    def _(m):
        rows = rows_v[m].astype(jnp.float32)
        scale = lax.rsqrt(jnp.mean(rows * rows, axis=-1, keepdims=True) + EPSILON)
        for n in range(model // LANES):
            cols = pl.ds(n * LANES, LANES)
            part = dot_f32(back_v[m], weight_v[cols, :], NT)
            term_v[0, 0:1, cols] += jnp.sum(
                part * (rows_v[m, :, cols].astype(jnp.float32) * scale), axis=0, keepdims=True
            )
            part = part.astype(jnp.bfloat16)
            for r in range(per):
                own[m * per + r, :, cols] = part[r * FINE : (r + 1) * FINE]

        @pl.when(m == 0)
        def _():
            relay.send(0, AHEAD)

    term_v[0, 1:2, :] = gain_two_ref[...]
    term_v[0, 2:3, 0:HD] = gain_heads_ref[0:1, :]
    term_v[0, 2:3, HD : 2 * HD] = gain_heads_ref[1:2, :]
    for k in range(2):
        if k in GAIN_PLACES:
            gain_step(GAIN_PLACES.index(k))
        relay.send(AHEAD + 2 * k, 2)
        relay.place(k)

    @pl.loop(0, micro)
    def _(m):
        slot = m % 2

        @pl.when(m < micro - 1)
        def _():
            load(m + 1).start()

        load(m).wait()

        @pl.when(m >= 2)
        def _():
            final_copy(m - 2).wait()

        for r in range(per // 2):
            for turn in range(micro):
                if 2 + turn * per // 2 + r in GAIN_PLACES:

                    @pl.when(m == turn)
                    def _(step=GAIN_PLACES.index(2 + turn * per // 2 + r)):
                        gain_step(step)

            @pl.when(AHEAD + 4 + m * per + 2 * r < relay.count)
            def _():
                relay.send(AHEAD + 4 + m * per + 2 * r, 2)

            relay.place(2 + m * per // 2 + r)
            for half in range(2):
                span = pl.ds((2 * r + half) * FINE, FINE)
                rows = rows_v[m, span, :].astype(jnp.float32)
                scale = lax.rsqrt(jnp.mean(rows * rows, axis=-1, keepdims=True) + EPSILON)
                pulled = landed[m * per + 2 * r + half].astype(jnp.float32) * gain_ref[...]
                along = jnp.mean(pulled * rows, axis=-1, keepdims=True)
                output_v[slot, span, :] = middle_v[slot, span, :] + scale * (
                    pulled - rows * (scale * scale * along)
                )
        final_copy(m).start()

    final_copy(micro - 2).wait()
    final_copy(micro - 1).wait()
    relay.drain(0)


def input_gradient(back, layer_input, grad_middle, gain_attn, weight, gain_two, gain_heads):
    micro, tok, model = layer_input.shape
    low = jnp.bfloat16
    count = micro * (tok // FINE)
    anywhere = pl.BlockSpec(memory_space=pl.ANY)
    inside = pl.BlockSpec(memory_space=pltpu.VMEM)
    return pl.pallas_call(
        input_kernel,
        out_shape=(
            jax.ShapeDtypeStruct((micro, tok, model), jnp.float32),
            jax.ShapeDtypeStruct((8, model), jnp.float32),
        ),
        in_specs=[anywhere] * 3 + [inside, anywhere, inside, inside],
        out_specs=[anywhere, inside],
        scratch_shapes=relay_scratch(count, model, rows=FINE)
        + [
            pltpu.VMEM(weight.shape, low),
            pltpu.VMEM((micro, tok, weight.shape[1]), low),
            pltpu.VMEM((micro, tok, model), low),
            pltpu.VMEM((2, tok, model), jnp.float32),
            pltpu.VMEM((2, tok, model), jnp.float32),
            pltpu.VMEM((6, 8, model), jnp.float32),
            pltpu.VMEM((6, 8, model), jnp.float32),
            pltpu.SemaphoreType.DMA((3,)),
            pltpu.SemaphoreType.DMA((2,)),
            pltpu.SemaphoreType.DMA((2,)),
            pltpu.SemaphoreType.DMA((6,)),
            pltpu.SemaphoreType.DMA((6,)),
        ],
        compiler_params=pltpu.CompilerParams(
            collective_id=1, has_side_effects=True, vmem_limit_bytes=48 << 20
        ),
        cost_estimate=pl.CostEstimate(
            flops=1_000_000_000, bytes_accessed=1_000_000, transcendentals=0
        ),
        name="input_gradient",
    )(back, layer_input, grad_middle, gain_attn[None, :], weight, gain_two, gain_heads)


def finish_kernel(
    input_rows,
    first_rows,
    last_rows,
    gate_rows,
    up_rows,
    down_rows,
    attn_rows,
    out_rows,
    grad_ref,
    output_ref,
    gate_ref,
    up_ref,
    down_ref,
    query_ref,
    key_ref,
    value_ref,
    out_ref,
):
    grad_ref[...] = input_rows[...]
    inside = pl.program_id(0) < pl.num_programs(0) * 3 // 4
    output_ref[...] = jnp.where(inside, first_rows[...], last_rows[...])
    gate_ref[...] = gate_rows[...].astype(jnp.float32)
    up_ref[...] = up_rows[...].astype(jnp.float32)
    down_ref[...] = down_rows[...].astype(jnp.float32)
    first = 0
    for target in (query_ref, key_ref, value_ref):
        target[...] = attn_rows[:, first : first + target.shape[1]].astype(jnp.float32)
        first += target.shape[1]
    out_ref[...] = out_rows[...].astype(jnp.float32)


def finish(grad_input, first, last, grads, columns):
    steps = 8
    rows, model = grad_input.shape
    piece, hid = grads.shape[0] // 4, grads.shape[1]
    part = rows // steps
    early = first.shape[0] // part - 1
    strip = piece // steps
    blocks = hid // piece
    heads = sum(columns) // piece
    rest = (hid - sum(columns)) // piece
    f32 = jnp.float32
    row = lambda i: (i, 0)
    return pl.pallas_call(
        finish_kernel,
        grid=(steps,),
        out_shape=(
            jax.ShapeDtypeStruct((rows, model), f32),
            jax.ShapeDtypeStruct((rows, model), jnp.bfloat16),
            jax.ShapeDtypeStruct((piece, hid), f32),
            jax.ShapeDtypeStruct((piece, hid), f32),
            jax.ShapeDtypeStruct((hid, piece), f32),
        )
        + tuple(jax.ShapeDtypeStruct((piece, column), f32) for column in columns)
        + (jax.ShapeDtypeStruct((rest * piece, piece), f32),),
        in_specs=[
            pl.BlockSpec((part, model), row),
            pl.BlockSpec((part, model), lambda i: (jnp.minimum(i, early), 0)),
            pl.BlockSpec((part, model), lambda i: (jnp.maximum(i - early - 1, 0), 0)),
            pl.BlockSpec((strip, hid), row),
            pl.BlockSpec((strip, hid), lambda i: (steps + i, 0)),
            pl.BlockSpec((piece, piece), lambda i: (2, jnp.minimum(i, blocks - 1))),
            pl.BlockSpec((strip, hid), lambda i: (3 * steps + i, 0)),
            pl.BlockSpec((piece, piece), lambda i: (3, heads + jnp.minimum(i, rest - 1))),
        ],
        out_specs=[
            pl.BlockSpec((part, model), row),
            pl.BlockSpec((part, model), row),
            pl.BlockSpec((strip, hid), row),
            pl.BlockSpec((strip, hid), row),
            pl.BlockSpec((piece, piece), lambda i: (jnp.minimum(i, blocks - 1), 0)),
        ]
        + [pl.BlockSpec((strip, column), row) for column in columns]
        + [pl.BlockSpec((piece, piece), lambda i: (jnp.minimum(i, rest - 1), 0))],
        name="finish",
    )(grad_input, first, last, grads, grads, grads, grads, grads)


def local_batched(
    layer_input,
    grad_out,
    lengths,
    w_query,
    w_key,
    w_value,
    w_out,
    w_gate,
    w_up,
    w_down,
    gain_attn,
    gain_ffn,
    gain_query,
    gain_key,
):
    micro, tok_rows, model = layer_input.shape
    width = lax.axis_size("wide")
    groups = w_key.shape[1] // HD
    total = tok_rows * width
    piece = w_out.shape[1]

    def stacked(weight):
        return jnp.moveaxis(weight.reshape(piece, -1, piece), 1, 0).reshape(-1, piece)

    pack = lax.all_gather(
        jnp.concatenate([w_out, stacked(w_gate)], axis=0), "wide", axis=0
    )

    head_gains = jnp.stack([gain_query, gain_key])
    hidden_one, raw, packed, w_qkv, cosine, sine = project(
        layer_input, gain_attn, (w_query, w_key, w_value), lengths, head_gains, width
    )
    packed = packed.reshape(total, 4 * HD)
    mixed, kept, log_total = attention_out(packed, lengths)
    (
        _,
        _,
        _,
        _,
        output,
        grad_middle,
        middle_low,
        grad_mixed,
        gain_two,
        feed_grads,
        mixed_low,
        late,
    ) = feed_forward(
        mixed.reshape(width, tok_rows, 2 * HD),
        layer_input,
        grad_out,
        gain_ffn,
        pack,
        w_up,
        w_down,
        w_out.shape[0],
    )
    cores = [list(range(core, width, 2)) for core in range(2)]

    def scatter(rows):
        return lax.psum_scatter(
            rows, "wide", scatter_dimension=0, axis_index_groups=cores, tiled=True
        )

    qkv_back, other_grads, gain_heads, last_output = attention_gradients(
        lengths,
        packed,
        grad_mixed,
        kept,
        log_total,
        raw,
        hidden_one,
        mixed_low,
        middle_low,
        late,
        layer_input,
        cosine,
        sine,
        head_gains,
        feed_grads,
    )
    other_grads = scatter(other_grads.reshape(-1, w_up.shape[1]))
    grad_input, gains = input_gradient(
        qkv_back, layer_input, grad_middle, gain_attn, w_qkv, gain_two, gain_heads
    )

    (
        grad_input,
        output,
        grad_gate,
        grad_up,
        grad_down,
        grad_query,
        grad_key,
        grad_value,
        grad_wout,
    ) = finish(
        grad_input.reshape(-1, model),
        output.reshape(-1, model),
        last_output,
        other_grads,
        (w_query.shape[1], w_key.shape[1], w_value.shape[1]),
    )
    return (
        output.reshape(layer_input.shape),
        grad_input.reshape(layer_input.shape),
        grad_query,
        grad_key,
        grad_value,
        grad_wout,
        grad_gate,
        grad_up,
        grad_down,
        gains[0],
        gains[1],
        gains[2, :HD],
        gains[2, HD : 2 * HD],
    )


def local(mesh, layer_input, grad_out, lengths, w_query, w_key, *rest):
    width = mesh.shape["wide"]
    micro, tok_rows = layer_input.shape[:2]
    groups = w_key.shape[1] // HD
    fits = (
        groups == HEAD_GROUPS
        and micro * groups == width == 8
        and w_query.shape[1] == 2 * w_key.shape[1]
        and mesh.shape["narrow"] == 4
        and tok_rows == BLOCK
    )
    chosen = local_batched if fits else local_general
    return chosen(layer_input, grad_out, lengths, w_query, w_key, *rest)


def solution(mesh):
    in_specs = (
        P(None, "wide", None),
        P(None, "wide", None),
        P(),
        P("wide", "narrow"),
        P("wide", "narrow"),
        P("wide", "narrow"),
        P("narrow", "wide"),
        P("wide", "narrow"),
        P("wide", "narrow"),
        P("narrow", "wide"),
        P(),
        P(),
        P(),
        P(),
    )
    out_specs = (
        P(None, "wide", None),
        P(None, "wide", None),
        P("wide", "narrow"),
        P("wide", "narrow"),
        P("wide", "narrow"),
        P("narrow", "wide"),
        P("wide", "narrow"),
        P("wide", "narrow"),
        P("narrow", "wide"),
        P(),
        P(),
        P(),
        P(),
    )
    return jax.shard_map(
        functools.partial(local, mesh), mesh=mesh, in_specs=in_specs, out_specs=out_specs, check_vma=False)
```
